32 devices in a mesh: fsdp: 16 (over z, y, core), tp: 2 (over x).
Axes of the slice: x: 2, y: 2, z: 4, core: 2. Of those that a mesh axis runs over, the one named last changes fastest.
Arguments:
- block_input: float32 [4096, 2048], P(('fsdp', 'tp')), may hold values from -6 to 6
- upstream_grad: float32 [4096, 2048], P(('fsdp', 'tp')), may hold values from -6 to 6
- first_gain: float32 [2048], replicated, may hold values from 0.1 to 1.9
- second_gain: float32 [2048], replicated, may hold values from 0.1 to 1.9
- query_weight: bfloat16 [2048, 2048], P('fsdp', 'tp'), may hold values from -0.125 to 0.125
- key_weight: bfloat16 [2048, 2048], P('fsdp', 'tp'), may hold values from -0.125 to 0.125
- value_weight: bfloat16 [2048, 2048], P('fsdp', 'tp'), may hold values from -0.125 to 0.125
- output_weight: bfloat16 [2048, 2048], P('fsdp', 'tp'), may hold values from -2 to 2
- gate_weight: bfloat16 [16, 2048, 1024], P('fsdp', None, 'tp'), may hold values from -0.125 to 0.125
- up_weight: bfloat16 [16, 2048, 1024], P('fsdp', None, 'tp'), may hold values from -0.125 to 0.125
- down_weight: bfloat16 [16, 1024, 2048], P('fsdp', 'tp'), may hold values from -0.375 to 0.375
- routes: int32 [4096, 8], P('fsdp'), may hold values from 0 to 15, all different within a row; in each aligned block of 256 rows (0 to 255, 256 to 511, ...) at most 192 rows name the same one
- gate_values: float32 [4096, 8], P('fsdp'), may hold values from 0.03 to 0.4
Outputs:
- block_output: float32 [4096, 2048], P(('fsdp', 'tp'))
- input_grad: float32 [4096, 2048], P(('fsdp', 'tp'))
- first_gain_grad: float32 [2048], replicated
- second_gain_grad: float32 [2048], replicated
- query_grad: float32 [2048, 2048], P('fsdp', 'tp')
- key_grad: float32 [2048, 2048], P('fsdp', 'tp')
- value_grad: float32 [2048, 2048], P('fsdp', 'tp')
- output_grad: float32 [2048, 2048], P('fsdp', 'tp')
- gate_grad: float32 [16, 2048, 1024], P('fsdp', None, 'tp')
- up_grad: float32 [16, 2048, 1024], P('fsdp', None, 'tp')
- down_grad: float32 [16, 1024, 2048], P('fsdp', 'tp')
- route_grad: float32 [4096, 8], P(('fsdp', 'tp'))
The draws below stay inside these ranges and needn't reach their ends.
Inputs may be any that keep to these rules, and one draw needn't show every extreme that they name: `routes`: each row names 8 different experts. Within each sequence's 256 rows no expert is named by more than 192 rows, and in some sequence one expert is named by exactly 192.
All inputs are finite; a program needn't handle non-finite values.
Results may differ from the reference program's by a relative error of at most 0.015.
Values may be sent and summed in bfloat16 or wider, within the bound.
A program may use at most 256 MiB of HBM per device.

```python
import math
import jax
import jax.numpy as jnp
import numpy as np
from jax import lax

D = 2048
HEADS = 16
HD = 128
FF = 1024
TOP = 8
SEQ = 256
EXPERTS = 16
CAP = 192
TOKENS = 4096
N_FSDP = 16
N_TP = 2


def strengthened(values, rng, source, target, shards_of, factor):
    def block_of(position):
        return (jnp.arange(values.shape[position]) // (values.shape[position] // shards_of)).reshape((-1,) + (1,) * (values.ndim - 1 - position))

    one_side = jax.random.permutation(rng, shards_of)[block_of(target)]
    other_side = (block_of(target) + shards_of // 2) % shards_of
    return jnp.where((block_of(source) == one_side) | (block_of(source) == other_side), factor * values, values)


def block_levels(key, shape, split, smallest, top_value):
    loudness = 1.0
    for axis_at, blocks in split:
        heights = jax.random.uniform(jax.random.fold_in(jax.random.fold_in(key, 6), axis_at), (blocks,), jnp.float32, smallest / len(split), top_value / len(split))
        loudness = loudness * jnp.repeat(jnp.exp(heights), shape[axis_at] // blocks).reshape((-1,) + (1,) * (len(shape) - 1 - axis_at))
    return loudness


def shared_out(stream_key, own, number, rows, count, top, limit, skew):
    sequence = jax.random.permutation(stream_key, count)
    heavy_load, ordinary = portions_of(count, rows * top, limit, skew, True), portions_of(count, rows * top, limit, skew, False)
    places = jnp.arange(count)

    def named(lengths, offset_by):
        used = int((lengths > 0).sum())
        fixed = max(1, used // 4)
        moved = fixed + (places - fixed + offset_by * (used - fixed)) % max(1, count - fixed)
        return jnp.zeros((count,), jnp.int32).at[sequence[jnp.where(places < fixed, places, moved)]].set(jnp.asarray(lengths, jnp.int32))

    lengths = jnp.where(number % 4 == 0, named(heavy_load, number // 4), named(ordinary, number - number // 4 - 1))
    mixed = jax.random.permutation(jax.random.fold_in(own, 3), count)
    source_of, receiver = mixed[0:count // 2 * 2:2], mixed[1:count // 2 * 2:2]
    room = jnp.minimum(lengths[source_of] - 1, limit - lengths[receiver]) // 2
    room = jnp.where((source_of == sequence[0]) | (receiver == sequence[0]) | (lengths[receiver] == 0), 0, jnp.maximum(room, 0))
    moved = jax.random.randint(jax.random.fold_in(own, 4), (count // 2,), 0, 1 << 20) % (room + 1)
    lengths = lengths.at[source_of].add(-moved).at[receiver].add(moved)
    members = jnp.searchsorted(jnp.cumsum(lengths), jnp.arange(rows * top), side="right").astype(jnp.int32)
    grid = members.reshape(top, rows).T
    grid = grid[jax.random.permutation(jax.random.fold_in(own, 1), rows)]
    offset_by = jax.random.randint(jax.random.fold_in(own, 2), (rows, 1), 0, top)
    return jnp.take_along_axis(grid, (jnp.arange(top)[None, :] + offset_by) % top, axis=1)


def portions_of(count, total, bound, skew, full):
    weights = [(1 << 20) // math.isqrt(standing ** skew) + 1 for standing in range(1, count + 1)]
    largest = bound if full else min(bound, max(-(-total // count), total * weights[0] // sum(weights)))
    least = 1 if total - largest >= count - 1 else 0
    holding, rest = [largest] + [least] * (count - 1), total - largest - least * (count - 1)
    while rest > 0:
        candidates = [i for i in range(1, count) if holding[i] < largest] or [i for i in range(1, count) if holding[i] < bound]
        mass, remaining = sum([weights[i] for i in candidates]), rest
        for i in candidates:
            more = min(bound - holding[i], max(1, remaining * weights[i] // mass), rest)
            holding[i] = holding[i] + more
            rest = rest - more
    return np.array(holding)


def centred(stream_key, shape, scale, reach, cuts=(), kind=jnp.bfloat16):
    drawn = jax.random.normal(stream_key, shape, jnp.float32) * scale
    if len(cuts) > 0:
        drawn = block_levels(stream_key, shape, cuts, -0.22, 0.18) * drawn
    return jnp.clip(drawn, min=-reach, max=reach).astype(kind)


def gaussian_with(rng, shape, scale, most, shards, heavy, kind=jnp.bfloat16):
    values = scale * jax.random.normal(rng, shape, jnp.float32)
    if shards:
        values = values * block_levels(rng, shape, shards, -0.22, 0.18)
    return jnp.clip(strengthened(values, jax.random.fold_in(rng, 3), *heavy), -most, most).astype(kind)


def setup_inputs(seed: int = 0) -> dict:
    keys = jax.random.split(jax.random.key(seed), 14)
    block_input = gaussian_with(keys[0], (TOKENS, D), 1.0, 6.0, ((0, 32),), (0, 1, 32, 2.75), jnp.float32)
    upstream_grad = gaussian_with(keys[1], (TOKENS, D), 1.0, 6.0, ((0, 32),), (0, 1, 32, 2.75), jnp.float32)
    first_gain = jnp.clip(1.0 + 0.18 * jax.random.normal(keys[2], (D,), jnp.float32), 0.1, 1.9)
    second_gain = jnp.clip(1.0 + 0.18 * jax.random.normal(keys[3], (D,), jnp.float32), 0.1, 1.9)
    query_weight = centred(keys[4], (D, HEADS * HD), D ** -0.5, 0.125, ((0, 16), (1, 2)))
    key_weight = centred(keys[5], (D, HEADS * HD), D ** -0.5, 0.125, ((0, 16), (1, 2)))
    value_weight = centred(keys[6], (D, HEADS * HD), D ** -0.5, 0.125, ((0, 16), (1, 2)))
    output_weight = centred(keys[7], (D, HEADS * HD), (max(D // SEQ, 1)) ** -0.5, 2.0, ((0, 16), (1, 2)))
    gate_weight = centred(keys[8], (EXPERTS, D, FF), D ** -0.5, 0.125, ((0, 16), (2, 2)))
    up_weight = centred(keys[9], (EXPERTS, D, FF), D ** -0.5, 0.125, ((0, 16), (2, 2)))
    down_weight = centred(keys[10], (EXPERTS, FF, D), (FF // 4) ** -0.5, 0.375, ((0, 16), (1, 2)))
    routes_keys = jax.random.split(jax.random.fold_in(keys[11], 1), TOKENS // SEQ)
    routes_turns = jax.random.permutation(jax.random.fold_in(keys[11], 3), TOKENS // SEQ)
    routes = jax.vmap(lambda own, number: shared_out(jax.random.fold_in(keys[11], 2), own, number, SEQ, EXPERTS, TOP, CAP, 1))(routes_keys, routes_turns).reshape((TOKENS, TOP))
    gate_values = jnp.clip(jnp.exp(math.log(0.4) - 2.5902672 * jax.random.uniform(keys[12], (TOKENS, TOP), jnp.float32) ** block_levels(keys[12], (TOKENS, TOP), ((0, 16),), -0.2, 0.2)), 0.03, 0.4)
    return dict(block_input=block_input, upstream_grad=upstream_grad, first_gain=first_gain, second_gain=second_gain, query_weight=query_weight, key_weight=key_weight, value_weight=value_weight, output_weight=output_weight, gate_weight=gate_weight, up_weight=up_weight, down_weight=down_weight, routes=routes, gate_values=gate_values)


epsilon = 1e-05

def rounded(values_in):
    return lax.optimization_barrier(values_in.astype(jnp.bfloat16)).astype(jnp.float32)

def route_slots(route_rows, expert_count, capacity):
    flat_routes = route_rows.reshape(-1).astype(jnp.int32)
    onehot = (flat_routes[:, None] == jnp.arange(expert_count, dtype=jnp.int32)[None, :]).astype(jnp.int32)
    earlier = jnp.cumsum(onehot, axis=0, dtype=jnp.int32) - onehot
    ranked = lax.optimization_barrier(jnp.sum(earlier * onehot, axis=1, dtype=jnp.int32))
    return flat_routes * capacity + ranked

def reference(block_input, upstream_grad, first_gain, second_gain, query_weight, key_weight, value_weight, output_weight, gate_weight, up_weight, down_weight, routes, gate_values):
    head_cols = HEADS * HD
    part_units = FF // N_TP
    inv_root = 1.0 / math.sqrt(HD)
    gate_wide = gate_weight.astype(jnp.float32)
    up_wide = up_weight.astype(jnp.float32)
    down_wide = down_weight.astype(jnp.float32)
    down_parts = down_wide.reshape(EXPERTS, N_TP, part_units, D)
    gate_parts = gate_wide.reshape(EXPERTS, D, N_TP, part_units)
    up_parts = up_wide.reshape(EXPERTS, D, N_TP, part_units)

    def one_sequence(running, inputs):
        seq_input, seq_cot, route_rows, gate_rows = inputs
        first_scale = lax.rsqrt(lax.optimization_barrier(jnp.mean(seq_input * seq_input, axis=1, keepdims=True)) + epsilon)
        first_normed = (seq_input * first_scale * first_gain).astype(jnp.bfloat16)
        query_three = rounded(jnp.dot(first_normed, query_weight, preferred_element_type=jnp.float32)).reshape(SEQ, HEADS, HD)
        key_three = rounded(jnp.dot(first_normed, key_weight, preferred_element_type=jnp.float32)).reshape(SEQ, HEADS, HD)
        value_three = rounded(jnp.dot(first_normed, value_weight, preferred_element_type=jnp.float32)).reshape(SEQ, HEADS, HD)
        scores = jnp.einsum('shd,thd->hst', query_three, key_three) * inv_root
        row_top = lax.optimization_barrier(jnp.max(scores, axis=2, keepdims=True))
        log_total = row_top + jnp.log(lax.optimization_barrier(jnp.sum(jnp.exp(scores - row_top), axis=2, keepdims=True)))
        soft_weights = jnp.exp(scores - log_total)
        soft_rounded = rounded(soft_weights)
        mixed_rows = jnp.einsum('hst,thd->shd', soft_rounded, value_three).reshape(SEQ, head_cols).astype(jnp.bfloat16)
        middle = seq_input + jnp.dot(mixed_rows, output_weight.T, preferred_element_type=jnp.float32)
        second_scale = lax.rsqrt(lax.optimization_barrier(jnp.mean(middle * middle, axis=1, keepdims=True)) + epsilon)
        second_normed = (middle * second_scale * second_gain).astype(jnp.bfloat16)
        slot_index = route_slots(route_rows, EXPERTS, CAP)
        spread = jnp.broadcast_to(second_normed[:, None, :], (SEQ, TOP, D)).reshape(SEQ * TOP, D)
        arrived = rounded(jnp.zeros((EXPERTS * CAP, D), jnp.bfloat16).at[slot_index].set(spread)).reshape(EXPERTS, CAP, D)
        gate_act = jnp.einsum('ecd,edf->ecf', arrived, gate_wide)
        up_act = jnp.einsum('ecd,edf->ecf', arrived, up_wide)
        sigmoid_gate = jax.nn.sigmoid(gate_act)
        hidden = rounded(gate_act * sigmoid_gate * up_act)
        expert_parts = jnp.einsum('ecgf,egfd->ecgd', hidden.reshape(EXPERTS, CAP, N_TP, part_units), down_parts)
        expert_out = lax.optimization_barrier(jnp.sum(rounded(expert_parts), axis=2)).reshape(EXPERTS * CAP, D)
        picked = expert_out[slot_index].reshape(SEQ, TOP, D)
        seq_output = middle + lax.optimization_barrier(jnp.sum(gate_rows[:, :, None] * picked, axis=1))
        route_terms = lax.optimization_barrier(jnp.sum(seq_cot[:, None, :] * picked, axis=2))
        routed_cot = (gate_rows[:, :, None] * seq_cot[:, None, :]).astype(jnp.bfloat16).reshape(SEQ * TOP, D)
        cot_arrived = rounded(jnp.zeros((EXPERTS * CAP, D), jnp.bfloat16).at[slot_index].set(routed_cot)).reshape(EXPERTS, CAP, D)
        hidden_cot = jnp.einsum('ecd,efd->ecf', cot_arrived, down_wide)
        down_term = jnp.einsum('ecf,ecd->efd', hidden, cot_arrived)
        gate_cot = rounded(hidden_cot * up_act * sigmoid_gate * (1.0 + gate_act * (1.0 - sigmoid_gate)))
        up_cot = rounded(hidden_cot * gate_act * sigmoid_gate)
        gate_term = jnp.einsum('ecd,ecf->edf', arrived, gate_cot)
        up_term = jnp.einsum('ecd,ecf->edf', arrived, up_cot)
        back_parts = jnp.einsum('ecgf,edgf->ecgd', gate_cot.reshape(EXPERTS, CAP, N_TP, part_units), gate_parts)
        back_parts = back_parts + jnp.einsum('ecgf,edgf->ecgd', up_cot.reshape(EXPERTS, CAP, N_TP, part_units), up_parts)
        came_back = lax.optimization_barrier(jnp.sum(rounded(back_parts), axis=2)).reshape(EXPERTS * CAP, D)
        second_cot = lax.optimization_barrier(jnp.sum(came_back[slot_index].reshape(SEQ, TOP, D), axis=1))
        weighted_two = second_cot * second_gain
        second_term = lax.optimization_barrier(jnp.sum(second_cot * middle * second_scale, axis=0))
        middle_grad = seq_cot + second_scale * (weighted_two - middle * second_scale * second_scale * lax.optimization_barrier(jnp.mean(weighted_two * middle, axis=1, keepdims=True)))
        middle_cot = middle_grad.astype(jnp.bfloat16)
        output_term = jnp.dot(middle_cot.T, mixed_rows, preferred_element_type=jnp.float32)
        mixed_cot = rounded(jnp.dot(middle_cot, output_weight, preferred_element_type=jnp.float32)).reshape(SEQ, HEADS, HD)
        value_cot = jnp.einsum('hst,shd->thd', soft_rounded, mixed_cot).reshape(SEQ, head_cols).astype(jnp.bfloat16)
        soft_cot = jnp.einsum('shd,thd->hst', mixed_cot, value_three)
        score_cot = rounded(soft_weights * (soft_cot - lax.optimization_barrier(jnp.sum(soft_weights * soft_cot, axis=2, keepdims=True))) * inv_root)
        query_cot = jnp.einsum('hst,thd->shd', score_cot, key_three).reshape(SEQ, head_cols).astype(jnp.bfloat16)
        key_cot = jnp.einsum('hst,shd->thd', score_cot, query_three).reshape(SEQ, head_cols).astype(jnp.bfloat16)
        query_term = jnp.dot(first_normed.T, query_cot, preferred_element_type=jnp.float32)
        key_term = jnp.dot(first_normed.T, key_cot, preferred_element_type=jnp.float32)
        value_term = jnp.dot(first_normed.T, value_cot, preferred_element_type=jnp.float32)
        first_cot = jnp.dot(query_cot, query_weight.T, preferred_element_type=jnp.float32)
        first_cot = first_cot + jnp.dot(key_cot, key_weight.T, preferred_element_type=jnp.float32)
        first_cot = first_cot + jnp.dot(value_cot, value_weight.T, preferred_element_type=jnp.float32)
        weighted_one = first_cot * first_gain
        first_term = lax.optimization_barrier(jnp.sum(first_cot * seq_input * first_scale, axis=0))
        seq_grad = middle_grad + first_scale * (weighted_one - seq_input * first_scale * first_scale * lax.optimization_barrier(jnp.mean(weighted_one * seq_input, axis=1, keepdims=True)))
        updated = (running[0] + first_term, running[1] + second_term, running[2] + query_term, running[3] + key_term, running[4] + value_term, running[5] + output_term, running[6] + gate_term, running[7] + up_term, running[8] + down_term)
        return (updated, (seq_output, seq_grad, route_terms))
    start = (jnp.zeros((D,), jnp.float32), jnp.zeros((D,), jnp.float32), jnp.zeros((D, head_cols), jnp.float32), jnp.zeros((D, head_cols), jnp.float32), jnp.zeros((D, head_cols), jnp.float32), jnp.zeros((D, head_cols), jnp.float32), jnp.zeros((EXPERTS, D, FF), jnp.float32), jnp.zeros((EXPERTS, D, FF), jnp.float32), jnp.zeros((EXPERTS, FF, D), jnp.float32))
    inputs = (block_input.reshape(N_FSDP, SEQ, D), upstream_grad.reshape(N_FSDP, SEQ, D), routes.reshape(N_FSDP, SEQ, TOP), gate_values.reshape(N_FSDP, SEQ, TOP))
    totals, stacked = lax.scan(one_sequence, start, inputs)
    block_output = stacked[0].reshape(N_FSDP * SEQ, D)
    input_grad = stacked[1].reshape(N_FSDP * SEQ, D)
    route_grad = stacked[2].reshape(N_FSDP * SEQ, TOP)
    return (block_output, input_grad, totals[0], totals[1], totals[2], totals[3], totals[4], totals[5], totals[6], totals[7], totals[8], route_grad)
```

```python
import jax
import jax.numpy as jnp
from jax import lax
from jax.sharding import PartitionSpec as P

HD = 128
TOP = 8
EXP_DEV = 1


epsilon = 1e-05


def route_slots(route_rows, expert_count, capacity):
    flat_routes = route_rows.reshape(-1)
    onehot = (flat_routes[:, None] == jnp.arange(expert_count, dtype=jnp.int32)[None, :]).astype(
        jnp.int32
    )
    earlier = jnp.cumsum(onehot, axis=0, dtype=jnp.int32) - onehot
    ranked = jnp.sum(earlier * onehot, axis=1, dtype=jnp.int32)
    return flat_routes * capacity + ranked


def pair_rows(row_block):
    return lax.all_gather(row_block, "tp", axis=0, tiled=True)


def pair_sums(term_block):
    return lax.psum_scatter(term_block, "tp", scatter_dimension=0, tiled=True)


def to_owners(buffer):
    return lax.all_to_all(buffer, "fsdp", split_axis=0, concat_axis=0, tiled=True)


def to_sources(buffer):
    return lax.all_to_all(buffer, "fsdp", split_axis=0, concat_axis=0, tiled=True)


def projections(query_weight, key_weight, value_weight, output_weight):
    return (
        lax.all_gather(query_weight, "fsdp", axis=0, tiled=True),
        lax.all_gather(key_weight, "fsdp", axis=0, tiled=True),
        lax.all_gather(value_weight, "fsdp", axis=0, tiled=True),
        lax.all_gather(output_weight, "fsdp", axis=0, tiled=True),
    )


def scatter_rows(row_block, slot_index, total_rows):
    return (
        jnp.zeros((total_rows, row_block.shape[1]), row_block.dtype).at[slot_index].set(row_block)
    )


def spread_rows(row_block, copies):
    return jnp.broadcast_to(
        row_block[:, None, :], (row_block.shape[0], copies, row_block.shape[1])
    ).reshape(-1, row_block.shape[1])


def contract_rows(left_block, right_block):
    return lax.dot_general(
        left_block, right_block, (((0,), (0,)), ((), ())), preferred_element_type=jnp.float32
    )


def contract_cols(left_block, right_block):
    return lax.dot_general(
        left_block, right_block, (((1,), (1,)), ((), ())), preferred_element_type=jnp.float32
    )


def send_out(full_buffer):
    return to_owners(full_buffer)


def send_back(group_parts):
    owner_count, local_experts, capacity, model_width = group_parts.shape
    return to_sources(group_parts).reshape(owner_count * local_experts * capacity, model_width)


def per_device_slots(
    block_input,
    upstream_grad,
    first_gain,
    second_gain,
    query_weight,
    key_weight,
    value_weight,
    output_weight,
    gate_weight,
    up_weight,
    down_weight,
    routes,
    gate_values,
):
    pair_count = lax.axis_size("tp")
    owner_count = lax.axis_size("fsdp")
    local_rows = block_input.shape[0]
    seq_rows = local_rows * pair_count
    model_width = block_input.shape[1]
    head_cols = query_weight.shape[1]
    local_heads = head_cols // HD
    expert_count = EXP_DEV * owner_count
    capacity = 3 * seq_rows * TOP // (2 * expert_count)
    inv_root = HD ** (-0.5)
    first_scale = lax.rsqrt(jnp.mean(block_input * block_input, axis=1, keepdims=True) + epsilon)
    first_normed = (block_input * first_scale * first_gain).astype(jnp.bfloat16)
    normed_rows = pair_rows(first_normed)
    query_full, key_full, value_full, output_full = projections(
        query_weight, key_weight, value_weight, output_weight
    )
    query_rows = (
        jnp.dot(normed_rows, query_full, preferred_element_type=jnp.float32)
        .astype(jnp.bfloat16)
        .reshape(seq_rows, local_heads, HD)
    )
    key_rows = (
        jnp.dot(normed_rows, key_full, preferred_element_type=jnp.float32)
        .astype(jnp.bfloat16)
        .reshape(seq_rows, local_heads, HD)
    )
    value_rows = (
        jnp.dot(normed_rows, value_full, preferred_element_type=jnp.float32)
        .astype(jnp.bfloat16)
        .reshape(seq_rows, local_heads, HD)
    )
    scores = (
        jnp.einsum("shd,thd->hst", query_rows, key_rows, preferred_element_type=jnp.float32)
        * inv_root
    )
    row_top = jnp.max(scores, axis=2, keepdims=True)
    log_total = row_top + jnp.log(jnp.sum(jnp.exp(scores - row_top), axis=2, keepdims=True))
    soft_weights = jnp.exp(scores - log_total)
    mixed_rows = jnp.einsum(
        "hst,thd->shd",
        soft_weights.astype(jnp.bfloat16),
        value_rows,
        preferred_element_type=jnp.float32,
    )
    mixed_rows = mixed_rows.astype(jnp.bfloat16).reshape(seq_rows, head_cols)
    middle = block_input + pair_sums(contract_cols(mixed_rows, output_full))
    second_scale = lax.rsqrt(jnp.mean(middle * middle, axis=1, keepdims=True) + epsilon)
    second_normed = (middle * second_scale * second_gain).astype(jnp.bfloat16)
    moe_rows = pair_rows(second_normed)
    slot_index = route_slots(routes, expert_count, capacity)
    send_rows = scatter_rows(spread_rows(moe_rows, TOP), slot_index, expert_count * capacity)
    arrived = send_out(send_rows.reshape(owner_count, EXP_DEV, capacity, model_width))
    gate_act = jnp.einsum(
        "secd,edf->secf", arrived, gate_weight, preferred_element_type=jnp.float32
    )
    up_act = jnp.einsum("secd,edf->secf", arrived, up_weight, preferred_element_type=jnp.float32)
    sigmoid_gate = jax.nn.sigmoid(gate_act)
    hidden = (gate_act * sigmoid_gate * up_act).astype(jnp.bfloat16)
    expert_out = jnp.einsum(
        "secf,efd->secd", hidden, down_weight, preferred_element_type=jnp.float32
    ).astype(jnp.bfloat16)
    returned = send_back(expert_out)
    picked = returned[slot_index].reshape(seq_rows, TOP, model_width).astype(jnp.float32)
    mixture = jnp.sum(gate_values[:, :, None] * picked, axis=1)
    block_output = middle + pair_sums(mixture)
    upstream_rows = lax.all_gather(upstream_grad, "tp", axis=0, tiled=True)
    route_terms = jnp.sum(upstream_rows[:, None, :] * picked, axis=2)
    routed_cot = (
        (gate_values[:, :, None] * upstream_rows[:, None, :])
        .astype(jnp.bfloat16)
        .reshape(seq_rows * TOP, model_width)
    )
    cot_send = scatter_rows(routed_cot, slot_index, expert_count * capacity)
    cot_arrived = send_out(cot_send.reshape(owner_count, EXP_DEV, capacity, model_width))
    hidden_cot = jnp.einsum(
        "secd,efd->secf", cot_arrived, down_weight, preferred_element_type=jnp.float32
    )
    down_grad = jnp.einsum(
        "secf,secd->efd", hidden, cot_arrived, preferred_element_type=jnp.float32
    )
    gate_cot = (
        hidden_cot * up_act * sigmoid_gate * (1.0 + gate_act * (1.0 - sigmoid_gate))
    ).astype(jnp.bfloat16)
    up_cot = (hidden_cot * gate_act * sigmoid_gate).astype(jnp.bfloat16)
    gate_grad = jnp.einsum("secd,secf->edf", arrived, gate_cot, preferred_element_type=jnp.float32)
    up_grad = jnp.einsum("secd,secf->edf", arrived, up_cot, preferred_element_type=jnp.float32)
    input_cot = jnp.einsum(
        "secf,edf->secd", gate_cot, gate_weight, preferred_element_type=jnp.float32
    )
    input_cot = (
        input_cot
        + jnp.einsum("secf,edf->secd", up_cot, up_weight, preferred_element_type=jnp.float32)
    ).astype(jnp.bfloat16)
    came_back = send_back(input_cot)
    normed_cot = jnp.sum(
        came_back[slot_index].reshape(seq_rows, TOP, model_width).astype(jnp.float32), axis=1
    )
    second_cot, route_grad = (
        lax.psum_scatter(
            normed_cot.astype(jnp.bfloat16), "tp", scatter_dimension=0, tiled=True
        ).astype(jnp.float32),
        lax.psum_scatter(
            route_terms.astype(jnp.bfloat16), "tp", scatter_dimension=0, tiled=True
        ).astype(jnp.float32),
    )
    weighted_two = second_cot * second_gain
    second_term = jnp.sum(second_cot * middle * second_scale, axis=0)
    middle_grad = upstream_grad + second_scale * (
        weighted_two
        - middle
        * second_scale
        * second_scale
        * jnp.mean(weighted_two * middle, axis=1, keepdims=True)
    )
    middle_rows = pair_rows(middle_grad.astype(jnp.bfloat16))
    query_full, key_full, value_full, output_full = projections(
        query_weight, key_weight, value_weight, output_weight
    )
    out_term = contract_rows(middle_rows, mixed_rows)
    mixed_cot = (
        jnp.dot(middle_rows, output_full, preferred_element_type=jnp.float32)
        .astype(jnp.bfloat16)
        .reshape(seq_rows, local_heads, HD)
    )
    scores = (
        jnp.einsum("shd,thd->hst", query_rows, key_rows, preferred_element_type=jnp.float32)
        * inv_root
    )
    soft_weights = jnp.exp(scores - log_total)
    value_cot = jnp.einsum(
        "hst,shd->thd",
        soft_weights.astype(jnp.bfloat16),
        mixed_cot,
        preferred_element_type=jnp.float32,
    )
    value_cot = value_cot.astype(jnp.bfloat16).reshape(seq_rows, head_cols)
    soft_cot = jnp.einsum("shd,thd->hst", mixed_cot, value_rows, preferred_element_type=jnp.float32)
    score_cot = (
        soft_weights
        * (soft_cot - jnp.sum(soft_weights * soft_cot, axis=2, keepdims=True))
        * inv_root
    ).astype(jnp.bfloat16)
    query_cot = (
        jnp.einsum("hst,thd->shd", score_cot, key_rows, preferred_element_type=jnp.float32)
        .astype(jnp.bfloat16)
        .reshape(seq_rows, head_cols)
    )
    key_cot = (
        jnp.einsum("hst,shd->thd", score_cot, query_rows, preferred_element_type=jnp.float32)
        .astype(jnp.bfloat16)
        .reshape(seq_rows, head_cols)
    )
    query_term = contract_rows(normed_rows, query_cot)
    key_term = contract_rows(normed_rows, key_cot)
    value_term = contract_rows(normed_rows, value_cot)
    first_terms = (
        contract_cols(query_cot, query_full)
        + contract_cols(key_cot, key_full)
        + contract_cols(value_cot, value_full)
    )
    first_cot = pair_sums(first_terms)
    weighted_one = first_cot * first_gain
    first_term = jnp.sum(first_cot * block_input * first_scale, axis=0)
    input_grad = middle_grad + first_scale * (
        weighted_one
        - block_input
        * first_scale
        * first_scale
        * jnp.mean(weighted_one * block_input, axis=1, keepdims=True)
    )
    query_grad, key_grad, value_grad, output_grad = (
        lax.psum_scatter(query_term, "fsdp", scatter_dimension=0, tiled=True),
        lax.psum_scatter(key_term, "fsdp", scatter_dimension=0, tiled=True),
        lax.psum_scatter(value_term, "fsdp", scatter_dimension=0, tiled=True),
        lax.psum_scatter(out_term, "fsdp", scatter_dimension=0, tiled=True),
    )
    first_gain_grad, second_gain_grad = lax.psum((first_term, second_term), ("fsdp", "tp"))
    return (
        block_output,
        input_grad,
        first_gain_grad,
        second_gain_grad,
        query_grad,
        key_grad,
        value_grad,
        output_grad,
        gate_grad,
        up_grad,
        down_grad,
        route_grad,
    )


def gate_columns(route_rows, gate_rows, expert_count):
    names = jnp.arange(expert_count, dtype=jnp.int32)[None, None, :]
    return jnp.sum(jnp.where(route_rows[:, :, None] == names, gate_rows[:, :, None], 0.0), axis=1)


def half_of(rows):
    count = rows.shape[0] // lax.axis_size("tp")
    return lax.dynamic_slice_in_dim(rows, lax.axis_index("tp") * count, count, axis=0)


def per_device_dense(
    block_input,
    upstream_grad,
    first_gain,
    second_gain,
    query_weight,
    key_weight,
    value_weight,
    output_weight,
    gate_weight,
    up_weight,
    down_weight,
    routes,
    gate_values,
):
    pair_count = lax.axis_size("tp")
    owner_count = lax.axis_size("fsdp")
    local_rows = block_input.shape[0]
    seq_rows = local_rows * pair_count
    model_width = block_input.shape[1]
    head_cols = query_weight.shape[1]
    local_heads = head_cols // HD
    expert_count = EXP_DEV * owner_count
    inv_root = HD ** (-0.5)
    bf16, f32 = jnp.bfloat16, jnp.float32

    my_routes, my_gates = half_of(routes), half_of(gate_values)
    gate_table = lax.all_gather(
        gate_columns(my_routes, my_gates, expert_count), "fsdp", axis=0, tiled=True
    )
    expert_names = jnp.arange(expert_count, dtype=jnp.int32)[None, :]
    gate_all = jnp.sum(
        jnp.where(expert_names == lax.axis_index("fsdp"), gate_table, 0.0), axis=1, keepdims=True
    )
    gate_pair = lax.all_gather(gate_weight[0], "tp", axis=0)
    up_pair = lax.all_gather(up_weight[0], "tp", axis=0)
    down_pair = lax.all_gather(down_weight[0], "tp", axis=0)
    upstream_all = lax.all_gather(upstream_grad.astype(bf16), "fsdp", axis=0, tiled=True)

    first_scale = lax.rsqrt(jnp.mean(block_input * block_input, axis=1, keepdims=True) + epsilon)
    first_normed = (block_input * first_scale * first_gain).astype(bf16)
    normed_rows = pair_rows(first_normed)
    query_full, key_full, value_full, output_full = projections(
        query_weight, key_weight, value_weight, output_weight
    )

    def heads_of(weight_full):
        return (
            jnp.dot(normed_rows, weight_full, preferred_element_type=f32)
            .astype(bf16)
            .reshape(seq_rows, local_heads, HD)
        )

    query_rows, key_rows, value_rows = heads_of(query_full), heads_of(key_full), heads_of(value_full)
    scores = jnp.einsum("shd,thd->hst", query_rows, key_rows, preferred_element_type=f32) * inv_root
    row_top = jnp.max(scores, axis=2, keepdims=True)
    log_total = row_top + jnp.log(jnp.sum(jnp.exp(scores - row_top), axis=2, keepdims=True))
    soft_weights = jnp.exp(scores - log_total)
    soft_rounded = soft_weights.astype(bf16)
    mixed_rows = jnp.einsum("hst,thd->shd", soft_rounded, value_rows, preferred_element_type=f32)
    mixed_rows = mixed_rows.astype(bf16).reshape(seq_rows, head_cols)
    middle = block_input + pair_sums(contract_cols(mixed_rows, output_full))
    second_scale = lax.rsqrt(jnp.mean(middle * middle, axis=1, keepdims=True) + epsilon)
    second_normed = (middle * second_scale * second_gain).astype(bf16)

    rows_all = lax.all_gather(second_normed, "fsdp", axis=0, tiled=True)
    gate_act = jnp.einsum("td,gdf->gtf", rows_all, gate_pair, preferred_element_type=f32)
    up_act = jnp.einsum("td,gdf->gtf", rows_all, up_pair, preferred_element_type=f32)
    sigmoid_gate = jax.nn.sigmoid(gate_act)
    hidden = gate_act * sigmoid_gate * up_act
    hidden_gated = (hidden * gate_all).astype(bf16)
    mixture_part = jnp.einsum("gtf,gfd->td", hidden_gated, down_pair, preferred_element_type=f32)
    hidden_cot = jnp.einsum("td,gfd->gtf", upstream_all, down_pair, preferred_element_type=f32)
    route_sums = jnp.sum(hidden * hidden_cot, axis=(0, 2))
    hidden_cot = hidden_cot * gate_all
    gate_cot = (
        hidden_cot * up_act * sigmoid_gate * (1.0 + gate_act * (1.0 - sigmoid_gate))
    ).astype(bf16)
    up_cot = (hidden_cot * gate_act * sigmoid_gate).astype(bf16)
    input_cot = jnp.einsum("gtf,gdf->td", gate_cot, gate_pair, preferred_element_type=f32)
    input_cot = input_cot + jnp.einsum("gtf,gdf->td", up_cot, up_pair, preferred_element_type=f32)
    second_cot = lax.psum_scatter(
        input_cot.astype(bf16), "fsdp", scatter_dimension=0, tiled=True
    ).astype(f32)
    mixture = lax.psum_scatter(
        mixture_part.astype(bf16), "fsdp", scatter_dimension=0, tiled=True
    ).astype(f32)
    block_output = middle + mixture
    route_back = lax.all_to_all(
        route_sums.reshape(owner_count, local_rows), "fsdp", split_axis=0, concat_axis=0, tiled=True
    )
    route_grad = jnp.sum(
        jnp.where(my_routes[:, :, None] == expert_names[None], route_back.T[:, None, :], 0.0), axis=2
    )
    down_part = jnp.einsum("gtf,td->gfd", hidden_gated, upstream_all, preferred_element_type=f32)
    gate_part = jnp.einsum("td,gtf->gdf", rows_all, gate_cot, preferred_element_type=f32)
    up_part = jnp.einsum("td,gtf->gdf", rows_all, up_cot, preferred_element_type=f32)

    def pair_grad(part):
        return lax.psum_scatter(part.astype(bf16), "tp", scatter_dimension=0).astype(f32)

    down_grad, gate_grad, up_grad = pair_grad(down_part), pair_grad(gate_part), pair_grad(up_part)

    weighted_two = second_cot * second_gain
    second_term = jnp.sum(second_cot * middle * second_scale, axis=0)
    middle_grad = upstream_grad + second_scale * (
        weighted_two
        - middle
        * second_scale
        * second_scale
        * jnp.mean(weighted_two * middle, axis=1, keepdims=True)
    )
    middle_rows = pair_rows(middle_grad.astype(bf16))
    out_term = contract_rows(middle_rows, mixed_rows)
    mixed_cot = (
        jnp.dot(middle_rows, output_full, preferred_element_type=f32)
        .astype(bf16)
        .reshape(seq_rows, local_heads, HD)
    )
    value_cot = jnp.einsum("hst,shd->thd", soft_rounded, mixed_cot, preferred_element_type=f32)
    value_cot = value_cot.astype(bf16).reshape(seq_rows, head_cols)
    soft_cot = jnp.einsum("shd,thd->hst", mixed_cot, value_rows, preferred_element_type=f32)
    score_cot = (
        soft_weights
        * (soft_cot - jnp.sum(soft_weights * soft_cot, axis=2, keepdims=True))
        * inv_root
    ).astype(bf16)
    query_cot = (
        jnp.einsum("hst,thd->shd", score_cot, key_rows, preferred_element_type=f32)
        .astype(bf16)
        .reshape(seq_rows, head_cols)
    )
    key_cot = (
        jnp.einsum("hst,shd->thd", score_cot, query_rows, preferred_element_type=f32)
        .astype(bf16)
        .reshape(seq_rows, head_cols)
    )
    first_terms = (
        contract_cols(query_cot, query_full)
        + contract_cols(key_cot, key_full)
        + contract_cols(value_cot, value_full)
    )
    first_cot = pair_sums(first_terms)
    weighted_one = first_cot * first_gain
    first_term = jnp.sum(first_cot * block_input * first_scale, axis=0)
    input_grad = middle_grad + first_scale * (
        weighted_one
        - block_input
        * first_scale
        * first_scale
        * jnp.mean(weighted_one * block_input, axis=1, keepdims=True)
    )

    def owner_grad(term):
        return lax.psum_scatter(
            term.astype(bf16), "fsdp", scatter_dimension=0, tiled=True
        ).astype(f32)

    query_grad = owner_grad(contract_rows(normed_rows, query_cot))
    key_grad = owner_grad(contract_rows(normed_rows, key_cot))
    value_grad = owner_grad(contract_rows(normed_rows, value_cot))
    output_grad = owner_grad(out_term)
    first_gain_grad, second_gain_grad = lax.psum((first_term, second_term), ("fsdp", "tp"))
    return (
        block_output,
        input_grad,
        first_gain_grad,
        second_gain_grad,
        query_grad,
        key_grad,
        value_grad,
        output_grad,
        gate_grad[None],
        up_grad[None],
        down_grad[None],
        route_grad,
    )


def solution(mesh):
    dense = 2 * TOP >= EXP_DEV * mesh.shape["fsdp"]
    per_device = per_device_dense if dense else per_device_slots
    in_specs = (
        P(("fsdp", "tp"), None),
        P(("fsdp", "tp"), None),
        P(),
        P(),
        P("fsdp", "tp"),
        P("fsdp", "tp"),
        P("fsdp", "tp"),
        P("fsdp", "tp"),
        P("fsdp", None, "tp"),
        P("fsdp", None, "tp"),
        P("fsdp", "tp", None),
        P("fsdp", None),
        P("fsdp", None),
    )
    out_specs = (
        P(("fsdp", "tp"), None),
        P(("fsdp", "tp"), None),
        P(),
        P(),
        P("fsdp", "tp"),
        P("fsdp", "tp"),
        P("fsdp", "tp"),
        P("fsdp", "tp"),
        P("fsdp", None, "tp"),
        P("fsdp", None, "tp"),
        P("fsdp", "tp", None),
        P(("fsdp", "tp"), None),
    )
    return jax.shard_map(
        per_device, mesh=mesh, in_specs=in_specs, out_specs=out_specs, check_vma=False
    )
```

```python
import functools

import jax
import jax.numpy as jnp
from jax import lax
from jax.experimental import pallas as pl
from jax.experimental.pallas import tpu as pltpu
from jax.sharding import PartitionSpec as P

HD = 128
TOP = 8
EXP_DEV = 1


epsilon = 1e-05


def route_slots(route_rows, expert_count, capacity):
    flat_routes = route_rows.reshape(-1)
    onehot = (flat_routes[:, None] == jnp.arange(expert_count, dtype=jnp.int32)[None, :]).astype(
        jnp.int32
    )
    earlier = jnp.cumsum(onehot, axis=0, dtype=jnp.int32) - onehot
    ranked = jnp.sum(earlier * onehot, axis=1, dtype=jnp.int32)
    return flat_routes * capacity + ranked


def pair_rows(row_block):
    return lax.all_gather(row_block, "tp", axis=0, tiled=True)


def pair_sums(term_block):
    return lax.psum_scatter(term_block, "tp", scatter_dimension=0, tiled=True)


def to_owners(buffer):
    return lax.all_to_all(buffer, "fsdp", split_axis=0, concat_axis=0, tiled=True)


def to_sources(buffer):
    return lax.all_to_all(buffer, "fsdp", split_axis=0, concat_axis=0, tiled=True)


def projections(query_weight, key_weight, value_weight, output_weight):
    return (
        lax.all_gather(query_weight, "fsdp", axis=0, tiled=True),
        lax.all_gather(key_weight, "fsdp", axis=0, tiled=True),
        lax.all_gather(value_weight, "fsdp", axis=0, tiled=True),
        lax.all_gather(output_weight, "fsdp", axis=0, tiled=True),
    )


def scatter_rows(row_block, slot_index, total_rows):
    return (
        jnp.zeros((total_rows, row_block.shape[1]), row_block.dtype).at[slot_index].set(row_block)
    )


def spread_rows(row_block, copies):
    return jnp.broadcast_to(
        row_block[:, None, :], (row_block.shape[0], copies, row_block.shape[1])
    ).reshape(-1, row_block.shape[1])


def contract_rows(left_block, right_block):
    return lax.dot_general(
        left_block, right_block, (((0,), (0,)), ((), ())), preferred_element_type=jnp.float32
    )


def contract_cols(left_block, right_block):
    return lax.dot_general(
        left_block, right_block, (((1,), (1,)), ((), ())), preferred_element_type=jnp.float32
    )


def send_out(full_buffer):
    return to_owners(full_buffer)


def send_back(group_parts):
    owner_count, local_experts, capacity, model_width = group_parts.shape
    return to_sources(group_parts).reshape(owner_count * local_experts * capacity, model_width)


def per_device_slots(
    block_input,
    upstream_grad,
    first_gain,
    second_gain,
    query_weight,
    key_weight,
    value_weight,
    output_weight,
    gate_weight,
    up_weight,
    down_weight,
    routes,
    gate_values,
):
    pair_count = lax.axis_size("tp")
    owner_count = lax.axis_size("fsdp")
    local_rows = block_input.shape[0]
    seq_rows = local_rows * pair_count
    model_width = block_input.shape[1]
    head_cols = query_weight.shape[1]
    local_heads = head_cols // HD
    expert_count = EXP_DEV * owner_count
    capacity = 3 * seq_rows * TOP // (2 * expert_count)
    inv_root = HD ** (-0.5)
    first_scale = lax.rsqrt(jnp.mean(block_input * block_input, axis=1, keepdims=True) + epsilon)
    first_normed = (block_input * first_scale * first_gain).astype(jnp.bfloat16)
    normed_rows = pair_rows(first_normed)
    query_full, key_full, value_full, output_full = projections(
        query_weight, key_weight, value_weight, output_weight
    )
    query_rows = (
        jnp.dot(normed_rows, query_full, preferred_element_type=jnp.float32)
        .astype(jnp.bfloat16)
        .reshape(seq_rows, local_heads, HD)
    )
    key_rows = (
        jnp.dot(normed_rows, key_full, preferred_element_type=jnp.float32)
        .astype(jnp.bfloat16)
        .reshape(seq_rows, local_heads, HD)
    )
    value_rows = (
        jnp.dot(normed_rows, value_full, preferred_element_type=jnp.float32)
        .astype(jnp.bfloat16)
        .reshape(seq_rows, local_heads, HD)
    )
    scores = (
        jnp.einsum("shd,thd->hst", query_rows, key_rows, preferred_element_type=jnp.float32)
        * inv_root
    )
    row_top = jnp.max(scores, axis=2, keepdims=True)
    log_total = row_top + jnp.log(jnp.sum(jnp.exp(scores - row_top), axis=2, keepdims=True))
    soft_weights = jnp.exp(scores - log_total)
    mixed_rows = jnp.einsum(
        "hst,thd->shd",
        soft_weights.astype(jnp.bfloat16),
        value_rows,
        preferred_element_type=jnp.float32,
    )
    mixed_rows = mixed_rows.astype(jnp.bfloat16).reshape(seq_rows, head_cols)
    middle = block_input + pair_sums(contract_cols(mixed_rows, output_full))
    second_scale = lax.rsqrt(jnp.mean(middle * middle, axis=1, keepdims=True) + epsilon)
    second_normed = (middle * second_scale * second_gain).astype(jnp.bfloat16)
    moe_rows = pair_rows(second_normed)
    slot_index = route_slots(routes, expert_count, capacity)
    send_rows = scatter_rows(spread_rows(moe_rows, TOP), slot_index, expert_count * capacity)
    arrived = send_out(send_rows.reshape(owner_count, EXP_DEV, capacity, model_width))
    gate_act = jnp.einsum(
        "secd,edf->secf", arrived, gate_weight, preferred_element_type=jnp.float32
    )
    up_act = jnp.einsum("secd,edf->secf", arrived, up_weight, preferred_element_type=jnp.float32)
    sigmoid_gate = jax.nn.sigmoid(gate_act)
    hidden = (gate_act * sigmoid_gate * up_act).astype(jnp.bfloat16)
    expert_out = jnp.einsum(
        "secf,efd->secd", hidden, down_weight, preferred_element_type=jnp.float32
    ).astype(jnp.bfloat16)
    returned = send_back(expert_out)
    picked = returned[slot_index].reshape(seq_rows, TOP, model_width).astype(jnp.float32)
    mixture = jnp.sum(gate_values[:, :, None] * picked, axis=1)
    block_output = middle + pair_sums(mixture)
    upstream_rows = lax.all_gather(upstream_grad, "tp", axis=0, tiled=True)
    route_terms = jnp.sum(upstream_rows[:, None, :] * picked, axis=2)
    routed_cot = (
        (gate_values[:, :, None] * upstream_rows[:, None, :])
        .astype(jnp.bfloat16)
        .reshape(seq_rows * TOP, model_width)
    )
    cot_send = scatter_rows(routed_cot, slot_index, expert_count * capacity)
    cot_arrived = send_out(cot_send.reshape(owner_count, EXP_DEV, capacity, model_width))
    hidden_cot = jnp.einsum(
        "secd,efd->secf", cot_arrived, down_weight, preferred_element_type=jnp.float32
    )
    down_grad = jnp.einsum(
        "secf,secd->efd", hidden, cot_arrived, preferred_element_type=jnp.float32
    )
    gate_cot = (
        hidden_cot * up_act * sigmoid_gate * (1.0 + gate_act * (1.0 - sigmoid_gate))
    ).astype(jnp.bfloat16)
    up_cot = (hidden_cot * gate_act * sigmoid_gate).astype(jnp.bfloat16)
    gate_grad = jnp.einsum("secd,secf->edf", arrived, gate_cot, preferred_element_type=jnp.float32)
    up_grad = jnp.einsum("secd,secf->edf", arrived, up_cot, preferred_element_type=jnp.float32)
    input_cot = jnp.einsum(
        "secf,edf->secd", gate_cot, gate_weight, preferred_element_type=jnp.float32
    )
    input_cot = (
        input_cot
        + jnp.einsum("secf,edf->secd", up_cot, up_weight, preferred_element_type=jnp.float32)
    ).astype(jnp.bfloat16)
    came_back = send_back(input_cot)
    normed_cot = jnp.sum(
        came_back[slot_index].reshape(seq_rows, TOP, model_width).astype(jnp.float32), axis=1
    )
    second_cot, route_grad = (
        lax.psum_scatter(
            normed_cot.astype(jnp.bfloat16), "tp", scatter_dimension=0, tiled=True
        ).astype(jnp.float32),
        lax.psum_scatter(
            route_terms.astype(jnp.bfloat16), "tp", scatter_dimension=0, tiled=True
        ).astype(jnp.float32),
    )
    weighted_two = second_cot * second_gain
    second_term = jnp.sum(second_cot * middle * second_scale, axis=0)
    middle_grad = upstream_grad + second_scale * (
        weighted_two
        - middle
        * second_scale
        * second_scale
        * jnp.mean(weighted_two * middle, axis=1, keepdims=True)
    )
    middle_rows = pair_rows(middle_grad.astype(jnp.bfloat16))
    query_full, key_full, value_full, output_full = projections(
        query_weight, key_weight, value_weight, output_weight
    )
    out_term = contract_rows(middle_rows, mixed_rows)
    mixed_cot = (
        jnp.dot(middle_rows, output_full, preferred_element_type=jnp.float32)
        .astype(jnp.bfloat16)
        .reshape(seq_rows, local_heads, HD)
    )
    scores = (
        jnp.einsum("shd,thd->hst", query_rows, key_rows, preferred_element_type=jnp.float32)
        * inv_root
    )
    soft_weights = jnp.exp(scores - log_total)
    value_cot = jnp.einsum(
        "hst,shd->thd",
        soft_weights.astype(jnp.bfloat16),
        mixed_cot,
        preferred_element_type=jnp.float32,
    )
    value_cot = value_cot.astype(jnp.bfloat16).reshape(seq_rows, head_cols)
    soft_cot = jnp.einsum("shd,thd->hst", mixed_cot, value_rows, preferred_element_type=jnp.float32)
    score_cot = (
        soft_weights
        * (soft_cot - jnp.sum(soft_weights * soft_cot, axis=2, keepdims=True))
        * inv_root
    ).astype(jnp.bfloat16)
    query_cot = (
        jnp.einsum("hst,thd->shd", score_cot, key_rows, preferred_element_type=jnp.float32)
        .astype(jnp.bfloat16)
        .reshape(seq_rows, head_cols)
    )
    key_cot = (
        jnp.einsum("hst,shd->thd", score_cot, query_rows, preferred_element_type=jnp.float32)
        .astype(jnp.bfloat16)
        .reshape(seq_rows, head_cols)
    )
    query_term = contract_rows(normed_rows, query_cot)
    key_term = contract_rows(normed_rows, key_cot)
    value_term = contract_rows(normed_rows, value_cot)
    first_terms = (
        contract_cols(query_cot, query_full)
        + contract_cols(key_cot, key_full)
        + contract_cols(value_cot, value_full)
    )
    first_cot = pair_sums(first_terms)
    weighted_one = first_cot * first_gain
    first_term = jnp.sum(first_cot * block_input * first_scale, axis=0)
    input_grad = middle_grad + first_scale * (
        weighted_one
        - block_input
        * first_scale
        * first_scale
        * jnp.mean(weighted_one * block_input, axis=1, keepdims=True)
    )
    query_grad, key_grad, value_grad, output_grad = (
        lax.psum_scatter(query_term, "fsdp", scatter_dimension=0, tiled=True),
        lax.psum_scatter(key_term, "fsdp", scatter_dimension=0, tiled=True),
        lax.psum_scatter(value_term, "fsdp", scatter_dimension=0, tiled=True),
        lax.psum_scatter(out_term, "fsdp", scatter_dimension=0, tiled=True),
    )
    first_gain_grad, second_gain_grad = lax.psum((first_term, second_term), ("fsdp", "tp"))
    return (
        block_output,
        input_grad,
        first_gain_grad,
        second_gain_grad,
        query_grad,
        key_grad,
        value_grad,
        output_grad,
        gate_grad,
        up_grad,
        down_grad,
        route_grad,
    )


MESH = pl.DeviceIdType.MESH


def place():
    here = lax.axis_index("fsdp")
    return here // 4, (here // 2) % 2, here % 2, lax.axis_index("tp")


def index_of(z, y, c):
    return (z * 2 + y) * 2 + c


LEVELS = 4
LEVEL_ORDER = tuple(
    sum(level << (2 * z) for z, level in enumerate(turn))
    for turn in ((3, 3, 0, 0), (2, 2, 1, 1), (1, 0, 3, 2), (0, 1, 2, 3))
)


def level_at(turn, z):
    return (LEVEL_ORDER[turn] >> (2 * z)) % 4


def line_ends(z):
    return (z + 1) // LEVELS, (LEVELS - z) // LEVELS


def plane_greet():
    z, y, c, x = place()
    top, bottom = line_ends(z)
    barrier = pltpu.get_barrier_semaphore()
    for partner in ((index_of(z, 1 - y, c), x), (index_of(z, y, 1 - c), x)):
        pl.semaphore_signal(barrier, inc=1, device_id=partner, device_id_type=MESH)

    @pl.when(top == 0)
    def _():
        above = (index_of(z + 1, y, c), x)
        pl.semaphore_signal(barrier, inc=1, device_id=above, device_id_type=MESH)

    @pl.when(bottom == 0)
    def _():
        below = (index_of(z - 1, y, c), x)
        pl.semaphore_signal(barrier, inc=1, device_id=below, device_id_type=MESH)

    pl.semaphore_wait(barrier, 4 - top - bottom)


def remote(src, dst, send_sem, recv_sem, target):
    return pltpu.make_async_remote_copy(
        src_ref=src,
        dst_ref=dst,
        send_sem=send_sem,
        recv_sem=recv_sem,
        device_id=target,
        device_id_type=MESH,
    )


class PlaneGather:
    def __init__(self, mine, full, send_sems, recv_sems):
        self.mine, self.full = mine, full
        self.send_sems, self.recv_sems = send_sems, recv_sems
        self.z, self.y, self.c, self.x = place()
        self.top, self.bottom = line_ends(self.z)
        self.sent = []

    def _send(self, src, slot, target, unless=None):
        k = len(self.sent)
        copy = remote(
            src, self.full.at[slot], self.send_sems.at[k], self.recv_sems.at[slot], target
        )
        if unless is None:
            copy.start()
        else:
            pl.when(unless == 0)(copy.start)
        self.sent.append((copy, unless))

    def arrived(self, slot):
        here = self.full.at[slot]
        k = self.send_sems.shape[0] - 1
        remote(here, here, self.send_sems.at[k], self.recv_sems.at[slot], (0, self.x)).wait_recv()

    def start(self):
        z, y, c, x = self.z, self.y, self.c, self.x
        own = index_of(z, y, c)
        self._send(self.mine, own, (index_of(z + 1, y, c), x), self.top)
        self._send(self.mine, own, (index_of(z - 1, y, c), x), self.bottom)
        self._send(self.mine, own, (index_of(z, 1 - y, c), x))
        self._send(self.mine, own, (index_of(z, y, 1 - c), x))

    def from_line(self, step):
        z, y, c, x = self.z, self.y, self.c, self.x
        level = level_at(3 - step, z)
        slot = index_of(level, y, c)
        self.arrived(slot)
        onward = z + 1 - 2 * ((level + LEVELS - z) // LEVELS)
        self._send(self.full.at[slot], slot, (index_of(onward, y, c), x), self.top + self.bottom)
        self._send(self.full.at[slot], slot, (index_of(z, 1 - y, c), x))
        self._send(self.full.at[slot], slot, (index_of(z, y, 1 - c), x))

    def from_side(self, step):
        z, y, c, x = self.z, self.y, self.c, self.x
        slot = index_of(level_at(3 - step, z), 1 - y, c)
        self.arrived(slot)
        self._send(self.full.at[slot], slot, (index_of(z, y, 1 - c), x))

    def from_core(self, step, side):
        z, y, c = self.z, self.y, self.c
        self.arrived(index_of(level_at(3 - step, z), (y + side) % 2, 1 - c))

    def finish(self):
        for copy, unless in self.sent:
            if unless is None:
                copy.wait_send()
            else:
                pl.when(unless == 0)(copy.wait_send)


GATHER_SENDS = 18


def gather_kernel(count, *refs):
    mine, full = refs[:count], refs[count : 2 * count]
    send_sems, recv_sems, own_sems = refs[2 * count :]
    z, y, c, x = place()
    plane_greet()
    own = index_of(z, y, c)
    plans = [
        PlaneGather(mine[a], full[a], send_sems.at[a], recv_sems.at[a]) for a in range(count)
    ]
    kept = [
        pltpu.make_async_copy(mine[a], full[a].at[own], own_sems.at[a]) for a in range(count)
    ]
    for plan in plans:
        plan.start()
    for copy in kept:
        copy.start()
    for step in range(1, LEVELS):
        for plan in plans:
            plan.from_line(step)
        for plan in plans:
            plan.from_side(step - 1)
    for plan in plans:
        plan.from_side(LEVELS - 1)
    for plan in plans:
        for step in range(LEVELS):
            for side in range(2):
                plan.from_core(step, side)
    for plan in plans:
        plan.finish()
    for copy in kept:
        copy.wait()


def plane_gather(arrays, collective_id, name):
    owner_count = lax.axis_size("fsdp")
    count = len(arrays)
    nbytes = sum(a.size * a.dtype.itemsize for a in arrays)
    return pl.pallas_call(
        functools.partial(gather_kernel, count),
        out_shape=[jax.ShapeDtypeStruct((owner_count,) + a.shape, a.dtype) for a in arrays],
        in_specs=[pl.BlockSpec(memory_space=pltpu.VMEM)] * count,
        out_specs=[pl.BlockSpec(memory_space=pl.ANY)] * count,
        scratch_shapes=[
            pltpu.SemaphoreType.DMA((count, GATHER_SENDS)),
            pltpu.SemaphoreType.DMA((count, owner_count)),
            pltpu.SemaphoreType.DMA((count,)),
        ],
        compiler_params=pltpu.CompilerParams(collective_id=collective_id, has_side_effects=True),
        cost_estimate=pl.CostEstimate(
            flops=0, bytes_accessed=owner_count * nbytes * 4, transcendentals=0
        ),
        name=name,
    )(*arrays)


class PlaneSums:
    def __init__(self, own_parts, from_core, from_side, from_line, sems):
        self.own, self.from_core = own_parts, from_core
        self.from_side, self.from_line = from_side, from_line
        self.core_s, self.core_r, self.side_s, self.side_r, self.line_s, self.line_r = sems
        self.z, self.y, self.c, self.x = place()
        self.top, self.bottom = line_ends(self.z)
        self.sent = []

    def slot_of(self, turn, side, core):
        return index_of(level_at(turn, self.z), (self.y + side) % 2, (self.c + core) % 2)

    def to_core(self, part, turn, side):
        j = side * LEVELS + turn
        copy = remote(
            part,
            self.from_core.at[j],
            self.core_s.at[j],
            self.core_r.at[j],
            (index_of(self.z, self.y, 1 - self.c), self.x),
        )
        copy.start()
        self.sent.append(copy)

    def core_arrived(self, turn, side):
        j = side * LEVELS + turn
        here = self.from_core.at[j]
        remote(here, here, self.core_s.at[j], self.core_r.at[j], (0, self.x)).wait_recv()

    def to_side(self, turn):
        copy = remote(
            self.own.at[LEVELS + turn],
            self.from_side.at[turn],
            self.side_s.at[turn],
            self.side_r.at[turn],
            (index_of(self.z, 1 - self.y, self.c), self.x),
        )
        copy.start()
        self.sent.append(copy)

    def side_arrived(self, turn):
        here = self.from_side.at[turn]
        remote(here, here, self.side_s.at[turn], self.side_r.at[turn], (0, self.x)).wait_recv()

    def line_arrived(self, slot):
        here = self.from_line.at[slot]
        remote(here, here, self.line_s.at[0], self.line_r.at[slot], (0, self.x)).wait_recv()

    def to_line(self, turn, add):
        z, y, c, x = self.z, self.y, self.c, self.x
        level = level_at(turn, z)

        @pl.when(self.top + self.bottom == 0)
        def _():
            self.line_arrived(level)
            add(self.own.at[turn], self.from_line.at[level])

        down = (z + LEVELS - level) // (LEVELS + 1)
        onward = z + 1 - 2 * down
        reached = 1 - jnp.minimum(1, jnp.abs(onward - level))
        slot = level + down * reached * (LEVELS - level)
        copy = remote(
            self.own.at[turn],
            self.from_line.at[slot],
            self.line_s.at[turn],
            self.line_r.at[slot],
            (index_of(onward, y, c), x),
        )
        copy.start()
        self.sent.append(copy)

    def finish(self):
        for copy in self.sent:
            copy.wait_send()


def add_block(one, two, out):
    step = 32

    @pl.loop(0, out.shape[0] // step)
    def _(i):
        rows = pl.ds(pl.multiple_of(i * step, step), step)
        value = one[rows, :].astype(jnp.float32) + two[rows, :].astype(jnp.float32)
        out[rows, :] = value.astype(out.dtype)


def total_block(plan, total):
    step = 32
    mine = plan.own.at[LEVELS - 1]
    below, above = plan.from_line.at[plan.z], plan.from_line.at[LEVELS]

    @pl.loop(0, total.shape[0] // step)
    def _(i):
        rows = pl.ds(pl.multiple_of(i * step, step), step)
        total[rows, :] = mine[rows, :].astype(jnp.float32)

    for end, block, slot in ((plan.bottom, below, plan.z), (plan.top, above, LEVELS)):

        @pl.when(end == 0)
        def _():
            plan.line_arrived(slot)

            @pl.loop(0, total.shape[0] // step)
            def _(i):
                rows = pl.ds(pl.multiple_of(i * step, step), step)
                total[rows, :] = total[rows, :] + block[rows, :].astype(jnp.float32)


def sums_kernel(count, *refs):
    parts, totals = refs[:count], refs[count : 2 * count]
    buffers = [refs[(2 + i) * count : (3 + i) * count] for i in range(4)]
    sems, own_sems = refs[6 * count : 6 * count + 6], refs[6 * count + 6]
    plane_greet()
    plans = [
        PlaneSums(*(b[a] for b in buffers), tuple(s.at[a] for s in sems)) for a in range(count)
    ]
    loads = {}
    for a, plan in enumerate(plans):
        for side in (1, 0):
            for turn in range(LEVELS):
                plan.to_core(parts[a].at[plan.slot_of(turn, side, 1)], turn, side)
                j = side * LEVELS + turn
                load = pltpu.make_async_copy(
                    parts[a].at[plan.slot_of(turn, side, 0)], plan.own.at[j], own_sems.at[a, j]
                )
                load.start()
                loads[a, j] = load
    for side in (1, 0):
        for turn in range(LEVELS):
            for a, plan in enumerate(plans):
                j = side * LEVELS + turn
                loads[a, j].wait()
                plan.core_arrived(turn, side)
                add_block(plan.own.at[j], plan.from_core.at[j], plan.own.at[j])
                if side == 1:
                    plan.to_side(turn)
    for turn in range(LEVELS):
        for plan in plans:
            plan.side_arrived(turn)
            add_block(plan.own.at[turn], plan.from_side.at[turn], plan.own.at[turn])
            if turn < LEVELS - 1:
                plan.to_line(turn, lambda one, two: add_block(one, two, one))
    for a, plan in enumerate(plans):
        total_block(plan, totals[a])
    for plan in plans:
        plan.finish()


def plane_sums(parts, collective_id, name):
    count = len(parts)
    shapes = [p.shape[1:] for p in parts]
    types = [p.dtype for p in parts]

    def scratch(blocks):
        return [pltpu.VMEM((blocks,) + s, t) for s, t in zip(shapes, types)]

    def sems(blocks):
        return [pltpu.SemaphoreType.DMA((count, blocks))] * 2

    nbytes = sum(p.size * p.dtype.itemsize for p in parts)
    return pl.pallas_call(
        functools.partial(sums_kernel, count),
        out_shape=[jax.ShapeDtypeStruct(s, jnp.float32) for s in shapes],
        in_specs=[pl.BlockSpec(memory_space=pl.ANY)] * count,
        out_specs=[pl.BlockSpec(memory_space=pltpu.VMEM)] * count,
        scratch_shapes=scratch(2 * LEVELS)
        + scratch(2 * LEVELS)
        + scratch(LEVELS)
        + scratch(LEVELS + 1)
        + sems(2 * LEVELS)
        + sems(LEVELS)
        + sems(LEVELS + 1)
        + [pltpu.SemaphoreType.DMA((count, 2 * LEVELS))],
        compiler_params=pltpu.CompilerParams(
            collective_id=collective_id, has_side_effects=True, vmem_limit_bytes=60 * 2**20
        ),
        cost_estimate=pl.CostEstimate(flops=0, bytes_accessed=4 * nbytes, transcendentals=0),
        name=name,
    )(*parts)


def gate_columns(route_rows, gate_rows, expert_count):
    names = jnp.arange(expert_count, dtype=jnp.int32)[None, None, :]
    return jnp.sum(jnp.where(route_rows[:, :, None] == names, gate_rows[:, :, None], 0.0), axis=1)


def half_of(rows):
    count = rows.shape[0] // lax.axis_size("tp")
    return lax.dynamic_slice_in_dim(rows, lax.axis_index("tp") * count, count, axis=0)


def per_device_dense(
    block_input,
    upstream_grad,
    first_gain,
    second_gain,
    query_weight,
    key_weight,
    value_weight,
    output_weight,
    gate_weight,
    up_weight,
    down_weight,
    routes,
    gate_values,
):
    pair_count = lax.axis_size("tp")
    owner_count = lax.axis_size("fsdp")
    local_rows = block_input.shape[0]
    seq_rows = local_rows * pair_count
    model_width = block_input.shape[1]
    head_cols = query_weight.shape[1]
    local_heads = head_cols // HD
    expert_count = EXP_DEV * owner_count
    inv_root = HD ** (-0.5)
    bf16, f32 = jnp.bfloat16, jnp.float32

    my_routes, my_gates = half_of(routes), half_of(gate_values)
    gate_table = lax.all_gather(
        gate_columns(my_routes, my_gates, expert_count), "fsdp", axis=0, tiled=True
    )
    expert_names = jnp.arange(expert_count, dtype=jnp.int32)[None, :]
    gate_all = jnp.sum(
        jnp.where(expert_names == lax.axis_index("fsdp"), gate_table, 0.0), axis=1, keepdims=True
    )
    gate_pair = lax.all_gather(gate_weight[0], "tp", axis=0)
    up_pair = lax.all_gather(up_weight[0], "tp", axis=0)
    down_pair = lax.all_gather(down_weight[0], "tp", axis=0)

    first_scale = lax.rsqrt(jnp.mean(block_input * block_input, axis=1, keepdims=True) + epsilon)
    first_normed = (block_input * first_scale * first_gain).astype(bf16)
    normed_rows = pair_rows(first_normed)
    query_full, key_full, value_full, output_full, upstream_all = (
        blocks.reshape(-1, blocks.shape[2])
        for blocks in plane_gather(
            [query_weight, key_weight, value_weight, output_weight, upstream_grad.astype(bf16)],
            1,
            "gather_weights",
        )
    )

    def heads_of(weight_full):
        return (
            jnp.dot(normed_rows, weight_full, preferred_element_type=f32)
            .astype(bf16)
            .reshape(seq_rows, local_heads, HD)
        )

    query_rows, key_rows, value_rows = heads_of(query_full), heads_of(key_full), heads_of(value_full)
    scores = jnp.einsum("shd,thd->hst", query_rows, key_rows, preferred_element_type=f32) * inv_root
    row_top = jnp.max(scores, axis=2, keepdims=True)
    log_total = row_top + jnp.log(jnp.sum(jnp.exp(scores - row_top), axis=2, keepdims=True))
    soft_weights = jnp.exp(scores - log_total)
    soft_rounded = soft_weights.astype(bf16)
    mixed_rows = jnp.einsum("hst,thd->shd", soft_rounded, value_rows, preferred_element_type=f32)
    mixed_rows = mixed_rows.astype(bf16).reshape(seq_rows, head_cols)
    middle = block_input + pair_sums(contract_cols(mixed_rows, output_full))
    second_scale = lax.rsqrt(jnp.mean(middle * middle, axis=1, keepdims=True) + epsilon)
    second_normed = (middle * second_scale * second_gain).astype(bf16)

    (rows_all,) = plane_gather([second_normed], 2, "gather_rows")
    rows_all = rows_all.reshape(-1, model_width)
    gate_act = jnp.einsum("td,gdf->gtf", rows_all, gate_pair, preferred_element_type=f32)
    up_act = jnp.einsum("td,gdf->gtf", rows_all, up_pair, preferred_element_type=f32)
    sigmoid_gate = jax.nn.sigmoid(gate_act)
    hidden = gate_act * sigmoid_gate * up_act
    hidden_gated = (hidden * gate_all).astype(bf16)
    mixture_part = jnp.einsum("gtf,gfd->td", hidden_gated, down_pair, preferred_element_type=f32)
    hidden_cot = jnp.einsum("td,gfd->gtf", upstream_all, down_pair, preferred_element_type=f32)
    route_sums = jnp.sum(hidden * hidden_cot, axis=(0, 2))
    hidden_cot = hidden_cot * gate_all
    gate_cot = (
        hidden_cot * up_act * sigmoid_gate * (1.0 + gate_act * (1.0 - sigmoid_gate))
    ).astype(bf16)
    up_cot = (hidden_cot * gate_act * sigmoid_gate).astype(bf16)
    input_cot = jnp.einsum("gtf,gdf->td", gate_cot, gate_pair, preferred_element_type=f32)
    input_cot = input_cot + jnp.einsum("gtf,gdf->td", up_cot, up_pair, preferred_element_type=f32)
    blocks = (owner_count, local_rows, model_width)
    second_cot, mixture = plane_sums(
        [input_cot.astype(bf16).reshape(blocks), mixture_part.astype(bf16).reshape(blocks)],
        3,
        "sum_rows",
    )
    block_output = middle + mixture
    route_back = lax.all_to_all(
        route_sums.reshape(owner_count, local_rows), "fsdp", split_axis=0, concat_axis=0, tiled=True
    )
    route_grad = jnp.sum(
        jnp.where(my_routes[:, :, None] == expert_names[None], route_back.T[:, None, :], 0.0), axis=2
    )
    down_part = jnp.einsum("gtf,td->gfd", hidden_gated, upstream_all, preferred_element_type=f32)
    gate_part = jnp.einsum("td,gtf->gdf", rows_all, gate_cot, preferred_element_type=f32)
    up_part = jnp.einsum("td,gtf->gdf", rows_all, up_cot, preferred_element_type=f32)

    def pair_grad(part):
        return lax.psum_scatter(part.astype(bf16), "tp", scatter_dimension=0).astype(f32)

    down_grad, gate_grad, up_grad = pair_grad(down_part), pair_grad(gate_part), pair_grad(up_part)

    weighted_two = second_cot * second_gain
    second_term = jnp.sum(second_cot * middle * second_scale, axis=0)
    middle_grad = upstream_grad + second_scale * (
        weighted_two
        - middle
        * second_scale
        * second_scale
        * jnp.mean(weighted_two * middle, axis=1, keepdims=True)
    )
    middle_rows = pair_rows(middle_grad.astype(bf16))
    out_term = contract_rows(middle_rows, mixed_rows)
    mixed_cot = (
        jnp.dot(middle_rows, output_full, preferred_element_type=f32)
        .astype(bf16)
        .reshape(seq_rows, local_heads, HD)
    )
    value_cot = jnp.einsum("hst,shd->thd", soft_rounded, mixed_cot, preferred_element_type=f32)
    value_cot = value_cot.astype(bf16).reshape(seq_rows, head_cols)
    soft_cot = jnp.einsum("shd,thd->hst", mixed_cot, value_rows, preferred_element_type=f32)
    score_cot = (
        soft_weights
        * (soft_cot - jnp.sum(soft_weights * soft_cot, axis=2, keepdims=True))
        * inv_root
    ).astype(bf16)
    query_cot = (
        jnp.einsum("hst,thd->shd", score_cot, key_rows, preferred_element_type=f32)
        .astype(bf16)
        .reshape(seq_rows, head_cols)
    )
    key_cot = (
        jnp.einsum("hst,shd->thd", score_cot, query_rows, preferred_element_type=f32)
        .astype(bf16)
        .reshape(seq_rows, head_cols)
    )
    first_terms = (
        contract_cols(query_cot, query_full)
        + contract_cols(key_cot, key_full)
        + contract_cols(value_cot, value_full)
    )
    first_cot = pair_sums(first_terms)
    weighted_one = first_cot * first_gain
    first_term = jnp.sum(first_cot * block_input * first_scale, axis=0)
    input_grad = middle_grad + first_scale * (
        weighted_one
        - block_input
        * first_scale
        * first_scale
        * jnp.mean(weighted_one * block_input, axis=1, keepdims=True)
    )

    query_grad, key_grad, value_grad, output_grad = plane_sums(
        [
            term.astype(bf16).reshape((owner_count,) + query_weight.shape)
            for term in (
                contract_rows(normed_rows, query_cot),
                contract_rows(normed_rows, key_cot),
                contract_rows(normed_rows, value_cot),
                out_term,
            )
        ],
        4,
        "sum_gradients",
    )
    first_gain_grad, second_gain_grad = lax.psum((first_term, second_term), ("fsdp", "tp"))
    return (
        block_output,
        input_grad,
        first_gain_grad,
        second_gain_grad,
        query_grad,
        key_grad,
        value_grad,
        output_grad,
        gate_grad[None],
        up_grad[None],
        down_grad[None],
        route_grad,
    )


def solution(mesh):
    dense = 2 * TOP >= EXP_DEV * mesh.shape["fsdp"] and mesh.shape["fsdp"] == 4 * LEVELS
    per_device = per_device_dense if dense else per_device_slots
    in_specs = (
        P(("fsdp", "tp"), None),
        P(("fsdp", "tp"), None),
        P(),
        P(),
        P("fsdp", "tp"),
        P("fsdp", "tp"),
        P("fsdp", "tp"),
        P("fsdp", "tp"),
        P("fsdp", None, "tp"),
        P("fsdp", None, "tp"),
        P("fsdp", "tp", None),
        P("fsdp", None),
        P("fsdp", None),
    )
    out_specs = (
        P(("fsdp", "tp"), None),
        P(("fsdp", "tp"), None),
        P(),
        P(),
        P("fsdp", "tp"),
        P("fsdp", "tp"),
        P("fsdp", "tp"),
        P("fsdp", "tp"),
        P("fsdp", None, "tp"),
        P("fsdp", None, "tp"),
        P("fsdp", "tp", None),
        P(("fsdp", "tp"), None),
    )
    return jax.shard_map(
        per_device, mesh=mesh, in_specs=in_specs, out_specs=out_specs, check_vma=False
    )
```

```python
import functools

import jax
import jax.numpy as jnp
from jax import lax
from jax.experimental import pallas as pl
from jax.experimental.pallas import tpu as pltpu
from jax.sharding import PartitionSpec as P

HD = 128
TOP = 8
EXP_DEV = 1


epsilon = 1e-05


def route_slots(route_rows, expert_count, capacity):
    flat_routes = route_rows.reshape(-1)
    onehot = (flat_routes[:, None] == jnp.arange(expert_count, dtype=jnp.int32)[None, :]).astype(
        jnp.int32
    )
    earlier = jnp.cumsum(onehot, axis=0, dtype=jnp.int32) - onehot
    ranked = jnp.sum(earlier * onehot, axis=1, dtype=jnp.int32)
    return flat_routes * capacity + ranked


def pair_rows(row_block):
    return lax.all_gather(row_block, "tp", axis=0, tiled=True)


def pair_sums(term_block):
    return lax.psum_scatter(term_block, "tp", scatter_dimension=0, tiled=True)


def to_owners(buffer):
    return lax.all_to_all(buffer, "fsdp", split_axis=0, concat_axis=0, tiled=True)


def to_sources(buffer):
    return lax.all_to_all(buffer, "fsdp", split_axis=0, concat_axis=0, tiled=True)


def projections(query_weight, key_weight, value_weight, output_weight):
    return (
        lax.all_gather(query_weight, "fsdp", axis=0, tiled=True),
        lax.all_gather(key_weight, "fsdp", axis=0, tiled=True),
        lax.all_gather(value_weight, "fsdp", axis=0, tiled=True),
        lax.all_gather(output_weight, "fsdp", axis=0, tiled=True),
    )


def scatter_rows(row_block, slot_index, total_rows):
    return (
        jnp.zeros((total_rows, row_block.shape[1]), row_block.dtype).at[slot_index].set(row_block)
    )


def spread_rows(row_block, copies):
    return jnp.broadcast_to(
        row_block[:, None, :], (row_block.shape[0], copies, row_block.shape[1])
    ).reshape(-1, row_block.shape[1])


def contract_rows(left_block, right_block):
    return lax.dot_general(
        left_block, right_block, (((0,), (0,)), ((), ())), preferred_element_type=jnp.float32
    )


def contract_cols(left_block, right_block):
    return lax.dot_general(
        left_block, right_block, (((1,), (1,)), ((), ())), preferred_element_type=jnp.float32
    )


def send_out(full_buffer):
    return to_owners(full_buffer)


def send_back(group_parts):
    owner_count, local_experts, capacity, model_width = group_parts.shape
    return to_sources(group_parts).reshape(owner_count * local_experts * capacity, model_width)


def per_device_slots(
    block_input,
    upstream_grad,
    first_gain,
    second_gain,
    query_weight,
    key_weight,
    value_weight,
    output_weight,
    gate_weight,
    up_weight,
    down_weight,
    routes,
    gate_values,
):
    pair_count = lax.axis_size("tp")
    owner_count = lax.axis_size("fsdp")
    local_rows = block_input.shape[0]
    seq_rows = local_rows * pair_count
    model_width = block_input.shape[1]
    head_cols = query_weight.shape[1]
    local_heads = head_cols // HD
    expert_count = EXP_DEV * owner_count
    capacity = 3 * seq_rows * TOP // (2 * expert_count)
    inv_root = HD ** (-0.5)
    first_scale = lax.rsqrt(jnp.mean(block_input * block_input, axis=1, keepdims=True) + epsilon)
    first_normed = (block_input * first_scale * first_gain).astype(jnp.bfloat16)
    normed_rows = pair_rows(first_normed)
    query_full, key_full, value_full, output_full = projections(
        query_weight, key_weight, value_weight, output_weight
    )
    query_rows = (
        jnp.dot(normed_rows, query_full, preferred_element_type=jnp.float32)
        .astype(jnp.bfloat16)
        .reshape(seq_rows, local_heads, HD)
    )
    key_rows = (
        jnp.dot(normed_rows, key_full, preferred_element_type=jnp.float32)
        .astype(jnp.bfloat16)
        .reshape(seq_rows, local_heads, HD)
    )
    value_rows = (
        jnp.dot(normed_rows, value_full, preferred_element_type=jnp.float32)
        .astype(jnp.bfloat16)
        .reshape(seq_rows, local_heads, HD)
    )
    scores = (
        jnp.einsum("shd,thd->hst", query_rows, key_rows, preferred_element_type=jnp.float32)
        * inv_root
    )
    row_top = jnp.max(scores, axis=2, keepdims=True)
    log_total = row_top + jnp.log(jnp.sum(jnp.exp(scores - row_top), axis=2, keepdims=True))
    soft_weights = jnp.exp(scores - log_total)
    mixed_rows = jnp.einsum(
        "hst,thd->shd",
        soft_weights.astype(jnp.bfloat16),
        value_rows,
        preferred_element_type=jnp.float32,
    )
    mixed_rows = mixed_rows.astype(jnp.bfloat16).reshape(seq_rows, head_cols)
    middle = block_input + pair_sums(contract_cols(mixed_rows, output_full))
    second_scale = lax.rsqrt(jnp.mean(middle * middle, axis=1, keepdims=True) + epsilon)
    second_normed = (middle * second_scale * second_gain).astype(jnp.bfloat16)
    moe_rows = pair_rows(second_normed)
    slot_index = route_slots(routes, expert_count, capacity)
    send_rows = scatter_rows(spread_rows(moe_rows, TOP), slot_index, expert_count * capacity)
    arrived = send_out(send_rows.reshape(owner_count, EXP_DEV, capacity, model_width))
    gate_act = jnp.einsum(
        "secd,edf->secf", arrived, gate_weight, preferred_element_type=jnp.float32
    )
    up_act = jnp.einsum("secd,edf->secf", arrived, up_weight, preferred_element_type=jnp.float32)
    sigmoid_gate = jax.nn.sigmoid(gate_act)
    hidden = (gate_act * sigmoid_gate * up_act).astype(jnp.bfloat16)
    expert_out = jnp.einsum(
        "secf,efd->secd", hidden, down_weight, preferred_element_type=jnp.float32
    ).astype(jnp.bfloat16)
    returned = send_back(expert_out)
    picked = returned[slot_index].reshape(seq_rows, TOP, model_width).astype(jnp.float32)
    mixture = jnp.sum(gate_values[:, :, None] * picked, axis=1)
    block_output = middle + pair_sums(mixture)
    upstream_rows = lax.all_gather(upstream_grad, "tp", axis=0, tiled=True)
    route_terms = jnp.sum(upstream_rows[:, None, :] * picked, axis=2)
    routed_cot = (
        (gate_values[:, :, None] * upstream_rows[:, None, :])
        .astype(jnp.bfloat16)
        .reshape(seq_rows * TOP, model_width)
    )
    cot_send = scatter_rows(routed_cot, slot_index, expert_count * capacity)
    cot_arrived = send_out(cot_send.reshape(owner_count, EXP_DEV, capacity, model_width))
    hidden_cot = jnp.einsum(
        "secd,efd->secf", cot_arrived, down_weight, preferred_element_type=jnp.float32
    )
    down_grad = jnp.einsum(
        "secf,secd->efd", hidden, cot_arrived, preferred_element_type=jnp.float32
    )
    gate_cot = (
        hidden_cot * up_act * sigmoid_gate * (1.0 + gate_act * (1.0 - sigmoid_gate))
    ).astype(jnp.bfloat16)
    up_cot = (hidden_cot * gate_act * sigmoid_gate).astype(jnp.bfloat16)
    gate_grad = jnp.einsum("secd,secf->edf", arrived, gate_cot, preferred_element_type=jnp.float32)
    up_grad = jnp.einsum("secd,secf->edf", arrived, up_cot, preferred_element_type=jnp.float32)
    input_cot = jnp.einsum(
        "secf,edf->secd", gate_cot, gate_weight, preferred_element_type=jnp.float32
    )
    input_cot = (
        input_cot
        + jnp.einsum("secf,edf->secd", up_cot, up_weight, preferred_element_type=jnp.float32)
    ).astype(jnp.bfloat16)
    came_back = send_back(input_cot)
    normed_cot = jnp.sum(
        came_back[slot_index].reshape(seq_rows, TOP, model_width).astype(jnp.float32), axis=1
    )
    second_cot, route_grad = (
        lax.psum_scatter(
            normed_cot.astype(jnp.bfloat16), "tp", scatter_dimension=0, tiled=True
        ).astype(jnp.float32),
        lax.psum_scatter(
            route_terms.astype(jnp.bfloat16), "tp", scatter_dimension=0, tiled=True
        ).astype(jnp.float32),
    )
    weighted_two = second_cot * second_gain
    second_term = jnp.sum(second_cot * middle * second_scale, axis=0)
    middle_grad = upstream_grad + second_scale * (
        weighted_two
        - middle
        * second_scale
        * second_scale
        * jnp.mean(weighted_two * middle, axis=1, keepdims=True)
    )
    middle_rows = pair_rows(middle_grad.astype(jnp.bfloat16))
    query_full, key_full, value_full, output_full = projections(
        query_weight, key_weight, value_weight, output_weight
    )
    out_term = contract_rows(middle_rows, mixed_rows)
    mixed_cot = (
        jnp.dot(middle_rows, output_full, preferred_element_type=jnp.float32)
        .astype(jnp.bfloat16)
        .reshape(seq_rows, local_heads, HD)
    )
    scores = (
        jnp.einsum("shd,thd->hst", query_rows, key_rows, preferred_element_type=jnp.float32)
        * inv_root
    )
    soft_weights = jnp.exp(scores - log_total)
    value_cot = jnp.einsum(
        "hst,shd->thd",
        soft_weights.astype(jnp.bfloat16),
        mixed_cot,
        preferred_element_type=jnp.float32,
    )
    value_cot = value_cot.astype(jnp.bfloat16).reshape(seq_rows, head_cols)
    soft_cot = jnp.einsum("shd,thd->hst", mixed_cot, value_rows, preferred_element_type=jnp.float32)
    score_cot = (
        soft_weights
        * (soft_cot - jnp.sum(soft_weights * soft_cot, axis=2, keepdims=True))
        * inv_root
    ).astype(jnp.bfloat16)
    query_cot = (
        jnp.einsum("hst,thd->shd", score_cot, key_rows, preferred_element_type=jnp.float32)
        .astype(jnp.bfloat16)
        .reshape(seq_rows, head_cols)
    )
    key_cot = (
        jnp.einsum("hst,shd->thd", score_cot, query_rows, preferred_element_type=jnp.float32)
        .astype(jnp.bfloat16)
        .reshape(seq_rows, head_cols)
    )
    query_term = contract_rows(normed_rows, query_cot)
    key_term = contract_rows(normed_rows, key_cot)
    value_term = contract_rows(normed_rows, value_cot)
    first_terms = (
        contract_cols(query_cot, query_full)
        + contract_cols(key_cot, key_full)
        + contract_cols(value_cot, value_full)
    )
    first_cot = pair_sums(first_terms)
    weighted_one = first_cot * first_gain
    first_term = jnp.sum(first_cot * block_input * first_scale, axis=0)
    input_grad = middle_grad + first_scale * (
        weighted_one
        - block_input
        * first_scale
        * first_scale
        * jnp.mean(weighted_one * block_input, axis=1, keepdims=True)
    )
    query_grad, key_grad, value_grad, output_grad = (
        lax.psum_scatter(query_term, "fsdp", scatter_dimension=0, tiled=True),
        lax.psum_scatter(key_term, "fsdp", scatter_dimension=0, tiled=True),
        lax.psum_scatter(value_term, "fsdp", scatter_dimension=0, tiled=True),
        lax.psum_scatter(out_term, "fsdp", scatter_dimension=0, tiled=True),
    )
    first_gain_grad, second_gain_grad = lax.psum((first_term, second_term), ("fsdp", "tp"))
    return (
        block_output,
        input_grad,
        first_gain_grad,
        second_gain_grad,
        query_grad,
        key_grad,
        value_grad,
        output_grad,
        gate_grad,
        up_grad,
        down_grad,
        route_grad,
    )


MESH = pl.DeviceIdType.MESH


def place():
    here = lax.axis_index("fsdp")
    return here // 4, (here // 2) % 2, here % 2, lax.axis_index("tp")


def index_of(z, y, c):
    return (z * 2 + y) * 2 + c


LEVELS = 4
LEVEL_ORDER = sum(
    level << (8 * turn + 2 * z)
    for turn, row in enumerate(((3, 3, 0, 0), (2, 2, 1, 1), (1, 0, 3, 2), (0, 1, 2, 3)))
    for z, level in enumerate(row)
) - (1 << 32)


def level_at(turn, z):
    return (jnp.int32(LEVEL_ORDER) >> (8 * turn + 2 * z)) & 3


def line_ends(z):
    return (z + 1) // LEVELS, (LEVELS - z) // LEVELS


def plane_greet(pair=False, far=False):
    z, y, c, x = place()
    top, bottom = line_ends(z)
    barrier = pltpu.get_barrier_semaphore()
    partners = [(index_of(z, 1 - y, c), x), (index_of(z, y, 1 - c), x)]
    if pair:
        partners.append((index_of(z, y, c), 1 - x))
    if far:
        partners.append((index_of((z + 2) % LEVELS, y, c), x))
    for partner in partners:
        pl.semaphore_signal(barrier, inc=1, device_id=partner, device_id_type=MESH)

    @pl.when(top == 0)
    def _():
        above = (index_of(z + 1, y, c), x)
        pl.semaphore_signal(barrier, inc=1, device_id=above, device_id_type=MESH)

    @pl.when(bottom == 0)
    def _():
        below = (index_of(z - 1, y, c), x)
        pl.semaphore_signal(barrier, inc=1, device_id=below, device_id_type=MESH)

    pl.semaphore_wait(barrier, len(partners) + 2 - top - bottom)


def remote(src, dst, send_sem, recv_sem, target):
    return pltpu.make_async_remote_copy(
        src_ref=src,
        dst_ref=dst,
        send_sem=send_sem,
        recv_sem=recv_sem,
        device_id=target,
        device_id_type=MESH,
    )


class PlaneGather:
    def __init__(self, mine, full, send_sems, recv_sems):
        self.mine, self.full = mine, full
        self.send_sems, self.recv_sems = send_sems, recv_sems
        self.z, self.y, self.c, self.x = place()
        self.top, self.bottom = line_ends(self.z)

    def _copy(self, number, src, slot, target):
        return remote(
            src, self.full.at[slot], self.send_sems.at[number], self.recv_sems.at[slot], target
        )

    def arrived(self, slot):
        here = self.full.at[slot]
        remote(here, here, self.send_sems.at[0], self.recv_sems.at[slot], (0, self.x)).wait_recv()

    def start(self):
        z, y, c, x = self.z, self.y, self.c, self.x
        own = index_of(z, y, c)
        up = self._copy(0, self.mine, own, (index_of(z + 1, y, c), x))
        down = self._copy(1, self.mine, own, (index_of(z - 1, y, c), x))
        pl.when(self.top == 0)(up.start)
        pl.when(self.bottom == 0)(down.start)
        self._copy(2, self.mine, own, (index_of(z, 1 - y, c), x)).start()
        self._copy(3, self.mine, own, (index_of(z, y, 1 - c), x)).start()

    def from_line(self, step):
        z, y, c, x = self.z, self.y, self.c, self.x
        level = level_at(3 - step, z)
        slot = index_of(level, y, c)
        self.arrived(slot)
        onward = z + 1 - 2 * ((level + LEVELS - z) // LEVELS)
        src, number = self.full.at[slot], 4 + 3 * (step - 1)
        forward = self._copy(number, src, slot, (index_of(onward, y, c), x))
        pl.when(self.top + self.bottom == 0)(forward.start)
        self._copy(number + 1, src, slot, (index_of(z, 1 - y, c), x)).start()
        self._copy(number + 2, src, slot, (index_of(z, y, 1 - c), x)).start()

    def from_side(self, step):
        z, y, c, x = self.z, self.y, self.c, self.x
        slot = index_of(level_at(3 - step, z), 1 - y, c)
        self.arrived(slot)
        self._copy(13 + step, self.full.at[slot], slot, (index_of(z, y, 1 - c), x)).start()

    def from_core(self, step, side):
        z, y, c = self.z, self.y, self.c
        self.arrived(index_of(level_at(3 - step, z), (y + side) % 2, 1 - c))

    def finish(self):
        for number in range(GATHER_SENDS):
            wait = self._copy(number, self.mine, 0, (0, self.x)).wait_send
            if number == 0:
                pl.when(self.top == 0)(wait)
            elif number == 1:
                pl.when(self.bottom == 0)(wait)
            elif number in (4, 7, 10):
                pl.when(self.top + self.bottom == 0)(wait)
            else:
                wait()


GATHER_SENDS = 17


def weights_kernel(count, *refs):
    mine, normed, experts = refs[:count], refs[count], refs[count + 1 : count + 4]
    outs = refs[count + 4 : 2 * count + 8]
    full, normed_pair, others = outs[:count], outs[count], outs[count + 1 :]
    send_sems, recv_sems, own_sems, pair_s, pair_r = refs[2 * count + 8 :]
    z, y, c, x = place()
    own = index_of(z, y, c)
    plane_greet(pair=True)
    plans = [
        PlaneGather(mine[a], full[a], send_sems.at[a], recv_sems.at[a]) for a in range(count)
    ]
    swaps = [
        remote(src, dst, pair_s.at[i], pair_r.at[i], (own, 1 - x))
        for i, (src, dst) in enumerate(
            [(normed, normed_pair.at[x])] + list(zip(experts, others))
        )
    ]
    kept = [
        pltpu.make_async_copy(src, dst, own_sems.at[i])
        for i, (src, dst) in enumerate(
            [(mine[a], full[a].at[own]) for a in range(count)] + [(normed, normed_pair.at[x])]
        )
    ]
    for plan in plans:
        plan.start()
    for copy in swaps + kept:
        copy.start()
    for step in range(1, LEVELS):
        for plan in plans:
            plan.from_line(step)
        for plan in plans:
            plan.from_side(step - 1)
    for plan in plans:
        plan.from_side(LEVELS - 1)
    for plan in plans:
        for step in range(LEVELS):
            for side in range(2):
                plan.from_core(step, side)
    for plan in plans:
        plan.finish()
    for copy in swaps + kept:
        copy.wait()


def gather_weights(arrays, normed, experts, collective_id):
    owner_count = lax.axis_size("fsdp")
    count = len(arrays)
    hbm = pl.BlockSpec(memory_space=pl.ANY)
    vmem = pl.BlockSpec(memory_space=pltpu.VMEM)
    nbytes = sum(a.size * a.dtype.itemsize for a in arrays)
    outs = pl.pallas_call(
        functools.partial(weights_kernel, count),
        out_shape=[jax.ShapeDtypeStruct((owner_count,) + a.shape, a.dtype) for a in arrays]
        + [jax.ShapeDtypeStruct((2,) + normed.shape, normed.dtype)]
        + [jax.ShapeDtypeStruct(w.shape, w.dtype) for w in experts],
        in_specs=[vmem] * (count + 1) + [hbm] * 3,
        out_specs=[hbm] * (count + 4),
        scratch_shapes=[
            pltpu.SemaphoreType.DMA((count, GATHER_SENDS)),
            pltpu.SemaphoreType.DMA((count, owner_count)),
            pltpu.SemaphoreType.DMA((count + 1,)),
            pltpu.SemaphoreType.DMA((4,)),
            pltpu.SemaphoreType.DMA((4,)),
        ],
        compiler_params=pltpu.CompilerParams(collective_id=collective_id, has_side_effects=True),
        cost_estimate=pl.CostEstimate(
            flops=0, bytes_accessed=owner_count * nbytes * 4, transcendentals=0
        ),
        name="gather_weights",
    )(*arrays, normed, *experts)
    return outs[:count], outs[count], outs[count + 1 :]


class PlaneSums:
    def __init__(self, own_parts, from_core, from_side, from_line, sems, kept=0):
        self.own, self.from_core, self.kept = own_parts, from_core, kept
        self.from_side, self.from_line = from_side, from_line
        self.core_s, self.core_r, self.side_s, self.side_r, self.line_s, self.line_r = sems
        self.z, self.y, self.c, self.x = place()
        self.top, self.bottom = line_ends(self.z)
        self.sent = []

    def slot_of(self, turn, side, core):
        return index_of(level_at(turn, self.z), (self.y + side) % 2, (self.c + core) % 2)

    def to_core(self, part, turn, side):
        j = side * LEVELS + turn
        copy = remote(
            part,
            self.from_core.at[j],
            self.core_s.at[j],
            self.core_r.at[j],
            (index_of(self.z, self.y, 1 - self.c), self.x),
        )
        copy.start()
        self.sent.append(copy)

    def core_arrived(self, turn, side):
        j = side * LEVELS + turn
        here = self.from_core.at[j]
        remote(here, here, self.core_s.at[j], self.core_r.at[j], (0, self.x)).wait_recv()

    def to_side(self, turn):
        copy = remote(
            self.own.at[LEVELS + turn],
            self.from_side.at[turn],
            self.side_s.at[turn],
            self.side_r.at[turn],
            (index_of(self.z, 1 - self.y, self.c), self.x),
        )
        copy.start()
        self.sent.append(copy)

    def side_arrived(self, turn):
        here = self.from_side.at[turn]
        remote(here, here, self.side_s.at[turn], self.side_r.at[turn], (0, self.x)).wait_recv()

    def line_arrived(self, slot):
        here = self.from_line.at[slot]
        remote(here, here, self.line_s.at[0], self.line_r.at[slot], (0, self.x)).wait_recv()

    def to_line(self, turn):
        z, y, c, x = self.z, self.y, self.c, self.x
        mine = self.own.at[self.kept + turn]
        level = level_at(turn, z)

        @pl.when(self.top + self.bottom == 0)
        def _():
            self.line_arrived(level)
            add_block(mine, self.from_line.at[level], mine)

        down = (z + LEVELS - level) // (LEVELS + 1)
        onward = z + 1 - 2 * down
        reached = 1 - jnp.minimum(1, jnp.abs(onward - level))
        slot = level + down * reached * (LEVELS - level)
        copy = remote(
            mine,
            self.from_line.at[slot],
            self.line_s.at[turn],
            self.line_r.at[slot],
            (index_of(onward, y, c), x),
        )
        copy.start()
        self.sent.append(copy)

    def finish(self):
        for copy in self.sent:
            copy.wait_send()


def add_block(one, two, out):
    step = 32

    @pl.loop(0, out.shape[0] // step)
    def _(i):
        rows = pl.ds(pl.multiple_of(i * step, step), step)
        value = one[rows, :].astype(jnp.float32) + two[rows, :].astype(jnp.float32)
        out[rows, :] = value.astype(out.dtype)


def total_block(plan, total):
    step = 32
    mine = plan.own.at[plan.kept + LEVELS - 1]
    below, above = plan.from_line.at[plan.z], plan.from_line.at[LEVELS]

    @pl.loop(0, total.shape[0] // step)
    def _(i):
        rows = pl.ds(pl.multiple_of(i * step, step), step)
        total[rows, :] = mine[rows, :].astype(jnp.float32)

    for end, block, slot in ((plan.bottom, below, plan.z), (plan.top, above, LEVELS)):

        @pl.when(end == 0)
        def _():
            plan.line_arrived(slot)

            @pl.loop(0, total.shape[0] // step)
            def _(i):
                rows = pl.ds(pl.multiple_of(i * step, step), step)
                total[rows, :] = total[rows, :] + block[rows, :].astype(jnp.float32)


def last_kernel(count, *refs):
    parts, refs = refs[:count], refs[count:]
    expert_parts, refs = refs[:3], refs[3:]
    first_part, block_input, first_scale, first_gain, middle_grad, second_term = refs[:6]
    refs = refs[6:]
    totals, refs = refs[:count], refs[count:]
    expert_grads, refs = refs[:3], refs[3:]
    input_grad, gain_grads, refs = refs[0], refs[1], refs[2:]
    buffers = [refs[i * count : (i + 1) * count] for i in range(4)]
    refs = refs[4 * count :]
    sems, own_sems, refs = refs[:6], refs[6], refs[7:]
    first_other, gains, gains_in, refs = refs[0], refs[1], refs[2], refs[3:]
    expert_other, expert_own, expert_sum = refs[:3], refs[3:6], refs[6:9]
    pair_s, pair_r, load_sems, out_sems, gain_s, gain_r = refs[9:]
    z, y, c, x = place()
    own = index_of(z, y, c)
    plane_greet(pair=True, far=True)
    plans = [
        PlaneSums(*(b[a] for b in buffers), tuple(s.at[a] for s in sems)) for a in range(count)
    ]
    swaps = [
        remote(src.at[1 - x], dst, pair_s.at[i], pair_r.at[i], (own, 1 - x))
        for i, (src, dst) in enumerate(
            [(first_part, first_other)] + list(zip(expert_parts, expert_other))
        )
    ]
    swaps[0].start()
    loads = {}
    for a, plan in enumerate(plans):
        for side in (1, 0):
            for turn in range(LEVELS):
                plan.to_core(parts[a].at[plan.slot_of(turn, side, 1)], turn, side)
                j = side * LEVELS + turn
                load = pltpu.make_async_copy(
                    parts[a].at[plan.slot_of(turn, side, 0)], plan.own.at[j], own_sems.at[a, j]
                )
                load.start()
                loads[a, j] = load

    def core_step(turn, side):
        for a, plan in enumerate(plans):
            j = side * LEVELS + turn
            loads[a, j].wait()
            plan.core_arrived(turn, side)
            add_block(plan.own.at[j], plan.from_core.at[j], plan.own.at[j])
            if side == 1:
                plan.to_side(turn)

    def line_step(turn):
        for plan in plans:
            plan.side_arrived(turn)
            add_block(plan.own.at[turn], plan.from_side.at[turn], plan.own.at[turn])
            if turn < LEVELS - 1:
                plan.to_line(turn)

    def finish_norm():
        swaps[0].wait_recv()
        step = 16
        width = input_grad.shape[1]
        gains[...] = jnp.concatenate(
            [jnp.zeros((1, width), jnp.float32), second_term[...], jnp.zeros((6, width), jnp.float32)],
            axis=0,
        )
        gain = first_gain[...]

        @pl.loop(0, input_grad.shape[0] // step)
        def _(i):
            rows = pl.ds(pl.multiple_of(i * step, step), step)
            value = first_part[x, rows, :].astype(jnp.float32)
            value = value + first_other[rows, :].astype(jnp.float32)
            entry, scale = block_input[rows, :], first_scale[rows, :]
            weighted = value * gain
            mean = jnp.mean(weighted * entry, axis=1, keepdims=True)
            input_grad[rows, :] = middle_grad[rows, :] + scale * (
                weighted - entry * (scale * scale * mean)
            )
            gains[0:1, :] = gains[0:1, :] + jnp.sum(value * entry * scale, axis=0, keepdims=True)

    hops = [
        (index_of(z, y, 1 - c), x),
        (own, 1 - x),
        (index_of(z + 1 - 2 * (z % 2), y, c), x),
        (index_of((z + 2) % LEVELS, y, c), x),
        (index_of(z, 1 - y, c), x),
    ]

    def gain_copy(i):
        return remote(gains, gains_in.at[i], gain_s.at[i], gain_r.at[i], hops[i])

    def gain_add(i):
        gain_copy(i).wait()
        gains[...] = gains[...] + gains_in[i]

    def expert_add(which):
        other, grad = expert_other[which], expert_grads[which]
        own_half, both = expert_own[which], expert_sum[which]
        panel = own_half.shape[1]
        panels = other.shape[0] // panel

        def load(p):
            rows = pl.ds(pl.multiple_of(p * panel, panel), panel)
            return pltpu.make_async_copy(
                expert_parts[which].at[x, rows], own_half.at[p % 2], load_sems.at[p % 2]
            )

        def store(p):
            rows = pl.ds(pl.multiple_of(p * panel, panel), panel)
            return pltpu.make_async_copy(both.at[p % 2], grad.at[rows], out_sems.at[p % 2])

        load(0).start()
        swaps[1 + which].wait_recv()

        @pl.loop(0, panels)
        def _(p):
            load(p).wait()
            pl.when(p + 1 < panels)(lambda: load(p + 1).start())
            pl.when(p >= 2)(lambda: store(p - 2).wait())
            at_panel = pl.multiple_of(p * panel, panel)

            @pl.loop(0, panel // 16)
            def _(i):
                rows = pl.ds(pl.multiple_of(i * 16, 16), 16)
                there = pl.ds(pl.multiple_of(at_panel + i * 16, 16), 16)
                mine = own_half[p % 2, rows, :].astype(jnp.float32)
                both[p % 2, rows, :] = mine + other[there, :].astype(jnp.float32)

            store(p).start()

        for p in (panels - 2, panels - 1):
            store(p).wait()

    core_step(0, 1)
    for turn in range(LEVELS):
        core_step(turn, 0)
    finish_norm()
    for i in range(4):
        gain_copy(i).start()
        gain_add(i)
    gain_copy(4).start()
    for swap in swaps[1:]:
        swap.start()
    for turn in range(1, LEVELS):
        core_step(turn, 1)
    line_step(0)
    gain_add(4)
    gain_grads[...] = gains[...]
    line_step(1)
    expert_add(0)
    line_step(2)
    expert_add(1)
    line_step(3)
    for a, plan in enumerate(plans):
        total_block(plan, totals[a])
    expert_add(2)
    for plan in plans:
        plan.finish()
    for swap in swaps:
        swap.wait_send()


def sum_gradients(parts, expert_parts, first_part, norm_args, collective_id):
    f32 = jnp.float32
    count = len(parts)
    shapes = [p.shape[1:] for p in parts]
    types = [p.dtype for p in parts]
    hbm = pl.BlockSpec(memory_space=pl.ANY)
    vmem = pl.BlockSpec(memory_space=pltpu.VMEM)
    width = first_part.shape[2]

    def scratch(blocks):
        return [pltpu.VMEM((blocks,) + s, t) for s, t in zip(shapes, types)]

    def sems(blocks):
        return [pltpu.SemaphoreType.DMA((count, blocks))] * 2

    bf16 = jnp.bfloat16
    halves = [p.shape[1:] for p in expert_parts]
    panels = [(2, 2**17 // h[1], h[1]) for h in halves]
    nbytes = sum(p.size * p.dtype.itemsize for p in parts)
    outs = pl.pallas_call(
        functools.partial(last_kernel, count),
        out_shape=[jax.ShapeDtypeStruct(s, f32) for s in shapes]
        + [jax.ShapeDtypeStruct(h, f32) for h in halves]
        + [
            jax.ShapeDtypeStruct(first_part.shape[1:], f32),
            jax.ShapeDtypeStruct((8, width), f32),
        ],
        in_specs=[hbm] * (count + 3) + [vmem] * 6,
        out_specs=[vmem] * count + [hbm] * 3 + [vmem] * 2,
        scratch_shapes=scratch(2 * LEVELS)
        + scratch(2 * LEVELS)
        + scratch(LEVELS)
        + scratch(LEVELS + 1)
        + sems(2 * LEVELS)
        + sems(LEVELS)
        + sems(LEVELS + 1)
        + [pltpu.SemaphoreType.DMA((count, 2 * LEVELS))]
        + [
            pltpu.VMEM(first_part.shape[1:], first_part.dtype),
            pltpu.VMEM((8, width), f32),
            pltpu.VMEM((5, 8, width), f32),
        ]
        + [pltpu.VMEM(h, bf16) for h in halves]
        + [pltpu.VMEM(p, bf16) for p in panels]
        + [pltpu.VMEM(p, f32) for p in panels]
        + [
            pltpu.SemaphoreType.DMA((4,)),
            pltpu.SemaphoreType.DMA((4,)),
            pltpu.SemaphoreType.DMA((2,)),
            pltpu.SemaphoreType.DMA((2,)),
            pltpu.SemaphoreType.DMA((5,)),
            pltpu.SemaphoreType.DMA((5,)),
        ],
        compiler_params=pltpu.CompilerParams(
            collective_id=collective_id, has_side_effects=True, vmem_limit_bytes=67_043_328
        ),
        cost_estimate=pl.CostEstimate(flops=0, bytes_accessed=4 * nbytes, transcendentals=0),
        name="sum_gradients",
    )(*parts, *expert_parts, first_part, *norm_args)
    return outs[:count], outs[count : count + 3], outs[count + 3], outs[count + 4]


ROUTE_COLS = 128


def nn(left, right):
    return lax.dot_general(
        left, right, (((1,), (0,)), ((), ())), preferred_element_type=jnp.float32
    )


def nt(left, right):
    return lax.dot_general(
        left, right, (((1,), (1,)), ((), ())), preferred_element_type=jnp.float32
    )


def tn(left, right):
    return lax.dot_general(
        left, right, (((0,), (0,)), ((), ())), preferred_element_type=jnp.float32
    )


def pair_block(ref, pair):
    value = ref[pl.ds(2 * pair, 2)]
    return value.reshape(value.shape[0] * value.shape[1], value.shape[2])


def experts_kernel(
    rows,
    gates,
    upstream_hbm,
    gate_own,
    up_own,
    down_own,
    gate_other,
    up_other,
    down_other,
    second_cot,
    mixture_hbm,
    gate_part,
    up_part,
    down_part,
    rows_all,
    ubuf,
    wg,
    wu,
    wd,
    hidden,
    gcot,
    ucot,
    rext,
    tmp,
    own,
    from_core,
    from_side,
    from_line,
    mstage,
    gstage,
    gather_s,
    gather_r,
    core_s,
    core_r,
    side_s,
    side_r,
    line_s,
    line_r,
    load_sems,
    u_sems,
    out_sems,
):
    bf16, f32 = jnp.bfloat16, jnp.float32
    z, y, c, x = place()
    top, bottom = line_ends(z)
    interior = 1 - top - bottom
    me = lax.axis_index("fsdp")
    halves, width, units = wg.shape
    half_rows = rows.shape[0]
    pair_rows_ = 2 * half_rows
    pairs = 2 * LEVELS
    panel = 512

    loads = [
        pltpu.make_async_copy(src, dst, load_sems.at[i])
        for i, (src, dst) in enumerate(
            (
                (rows, rows_all.at[me]),
                (gate_own, wg.at[x]),
                (up_own, wu.at[x]),
                (down_own, wd.at[x]),
                (gate_other, wg.at[1 - x]),
                (up_other, wu.at[1 - x]),
                (down_other, wd.at[1 - x]),
            )
        )
    ]
    for load in loads:
        load.start()

    plane_greet()
    gather = PlaneGather(rows, rows_all, gather_s, gather_r)
    sums = PlaneSums(
        own,
        from_core,
        from_side,
        from_line,
        (core_s, core_r, side_s, side_r, line_s, line_r),
        LEVELS,
    )
    gather.start()

    def forward_pair(b):
        step = (0b11_10_11_01_10_00_01_00 >> (2 * b)) % 4
        side = (0b11_01_01_00 >> b) % 2
        return level_at(3 - step, z) * 2 + (y + side) % 2

    def u_load(b):
        pair = forward_pair(b)
        return pltpu.make_async_copy(
            upstream_hbm.at[pl.ds(2 * pair, 2)], ubuf.at[b % 2], u_sems.at[b % 2]
        )

    u_load(0).start()
    for load in loads:
        load.wait()

    @pl.loop(0, 2 * pairs)
    def _(turn):
        b, h = turn // 2, turn % 2

        def at(k, work, where=None):
            @pl.when(turn == k)
            def _():
                if where is None:
                    work()
                else:
                    pl.when(where == 1)(work)

        at(0, lambda: gather.from_core(0, 0))
        at(2, lambda: gather.from_line(1))
        at(2, lambda: gather.from_line(2), interior)
        at(2, lambda: gather.from_core(1, 0))
        at(4, lambda: gather.from_side(0))
        at(4, lambda: gather.from_core(0, 1))
        at(6, lambda: gather.from_line(2), 1 - interior)
        at(6, lambda: gather.from_line(3), interior)
        at(6, lambda: gather.from_core(2, 0))
        at(8, lambda: gather.from_side(1))
        at(8, lambda: gather.from_core(1, 1))
        at(10, lambda: gather.from_line(3), 1 - interior)
        at(10, lambda: gather.from_core(3, 0))
        at(12, lambda: gather.from_side(2))
        at(12, lambda: gather.from_core(2, 1))
        at(14, lambda: gather.from_side(3))
        at(14, lambda: gather.from_core(3, 1))

        @pl.when(h == 0)
        def _():
            u_load(b).wait()

            @pl.when(b + 1 < pairs)
            def _():
                u_load(b + 1).start()

        pair = forward_pair(b)
        xs = pair_block(rows_all, pair)
        us = pair_block(ubuf.at[b % 2], 0)
        lane = lax.broadcasted_iota(jnp.int32, (pair_rows_, ROUTE_COLS), 1)
        table = gates[pl.ds(2 * pair, 2)].reshape(pair_rows_, ROUTE_COLS)
        gate_rows = jnp.sum(jnp.where(lane == me, table, 0.0), axis=1, keepdims=True)
        gate_act = nn(xs, wg[h])
        up_act = nn(xs, wu[h])
        hidden_cot = nt(us, wd[h])
        sig = lax.logistic(gate_act)
        act = gate_act * sig
        hid = act * up_act
        at_rows = pl.ds(pl.multiple_of(pair * pair_rows_, pair_rows_), pair_rows_)
        hidden[h, at_rows, :] = (hid * gate_rows).astype(bf16)
        route = jnp.sum(hid * hidden_cot, axis=1, keepdims=True)
        scaled = hidden_cot * gate_rows
        gcot[h, at_rows, :] = (scaled * up_act * (sig * (1.0 + gate_act * (1.0 - sig)))).astype(bf16)
        ucot[h, at_rows, :] = (scaled * act).astype(bf16)
        placed = jnp.where(lane == me, route, 0.0)

        @pl.when(h == 0)
        def _():
            rext[pair] = placed

        @pl.when(h == 1)
        def _():
            rext[pair] = rext[pair] + placed

    def core_send(b):
        return remote(
            tmp.at[b % 2, 1 - c],
            from_core.at[b],
            core_s.at[b],
            core_r.at[b],
            (index_of(z, y, 1 - c), x),
        )

    def take_core(b):
        core_send(b).wait_recv()
        add_block(tmp.at[b % 2, c], from_core.at[b], own.at[b])

        @pl.when(b < LEVELS)
        def _():
            remote(
                own.at[b],
                from_side.at[b],
                side_s.at[b],
                side_r.at[b],
                (index_of(z, 1 - y, c), x),
            ).start()

    def line_step(turn):
        sums.side_arrived(turn)
        add_block(own.at[LEVELS + turn], from_side.at[turn], own.at[LEVELS + turn])
        if turn < LEVELS - 1:
            sums.to_line(turn)

    def last_step():
        line_step(LEVELS - 1)
        total_block(sums, second_cot)

    @pl.loop(0, pairs)
    def _(b):
        pl.when((b == pairs - 1) & (interior == 0))(lambda: line_step(0))
        pl.when(b >= 2)(lambda: core_send(b - 2).wait_send())
        pair = level_at(b % LEVELS, z) * 2 + (y + 1 - b // LEVELS) % 2
        at_rows = pl.ds(pl.multiple_of(pair * pair_rows_, pair_rows_), pair_rows_)

        @pl.loop(0, width // panel)
        def _(n):
            cols = pl.ds(pl.multiple_of(n * panel, panel), panel)
            acc = nt(gcot[0, at_rows, :], wg[0, cols, :])
            acc = acc + nt(ucot[0, at_rows, :], wu[0, cols, :])
            for h in range(1, halves):
                acc = acc + nt(gcot[h, at_rows, :], wg[h, cols, :])
                acc = acc + nt(ucot[h, at_rows, :], wu[h, cols, :])
            tmp[b % 2, :, :, cols] = acc.astype(bf16).reshape(2, half_rows, panel)

        core_send(b).start()
        pl.when(b >= 1)(lambda: take_core(b - 1))

    take_core(pairs - 1)
    for b in (pairs - 2, pairs - 1):
        core_send(b).wait_send()

    def mixture_out(b):
        return pltpu.make_async_copy(
            mstage.at[b % 2], mixture_hbm.at[pl.ds(2 * b, 2)], out_sems.at[b % 2]
        )

    @pl.loop(0, pairs)
    def _(b):
        pl.when((b == 3) & (interior == 0))(lambda: line_step(1))
        pl.when((b == 5) & (interior == 1))(lambda: line_step(0))
        pl.when(b >= 2)(lambda: mixture_out(b - 2).wait())
        at_rows = pl.ds(pl.multiple_of(b * pair_rows_, pair_rows_), pair_rows_)

        @pl.loop(0, width // panel)
        def _(n):
            cols = pl.ds(pl.multiple_of(n * panel, panel), panel)
            acc = nn(hidden[0, at_rows, :], wd[0, :, cols])
            for h in range(1, halves):
                acc = acc + nn(hidden[h, at_rows, :], wd[h, :, cols])
            mstage[b % 2, :, :, cols] = acc.astype(bf16).reshape(2, half_rows, panel)

        mstage[b % 2, :, :, pl.ds(width, ROUTE_COLS)] = (
            rext[b].astype(bf16).reshape(2, half_rows, ROUTE_COLS)
        )
        mixture_out(b).start()

    for b in (pairs - 2, pairs - 1):
        mixture_out(b).wait()

    block = 256

    def part_out(p, which):
        ref = (gate_part, up_part)[which]
        return pltpu.make_async_copy(
            gstage.at[p % 2, which],
            ref.at[:, pl.ds(pl.multiple_of(p * block, block), block), :],
            out_sems.at[2 + 2 * which + p % 2],
        )

    def gradient_steps(p):
        pl.when((p == 1) & (interior == 0))(lambda: line_step(2))
        pl.when((p == 2) & (interior == 1))(lambda: line_step(1))
        pl.when((p == 3) & (interior == 1))(lambda: line_step(2))
        pl.when(p == 7)(last_step)

    @pl.loop(0, width // block)
    def _(p):
        gradient_steps(p)

        @pl.when(p >= 2)
        def _():
            for which in range(2):
                part_out(p - 2, which).wait()

        cols = pl.ds(pl.multiple_of(p * block, block), block)
        xp = rows_all[:, :, cols]
        xp = xp.reshape(xp.shape[0] * xp.shape[1], block)
        for which, ref in enumerate((gcot, ucot)):
            for h in range(halves):
                gstage[p % 2, which, h] = tn(xp, ref[h]).astype(bf16)
            part_out(p, which).start()

    for p in (width // block - 2, width // block - 1):
        for which in range(2):
            part_out(p, which).wait()

    gather.finish()
    again = pltpu.make_async_copy(upstream_hbm, rows_all, load_sems.at[0])
    again.start()
    again.wait()
    per_half = units // block

    def down_out(p):
        return pltpu.make_async_copy(
            tmp.at[p % 2],
            down_part.at[p // per_half, pl.ds(2 * (p % per_half), 2)],
            out_sems.at[p % 2],
        )

    @pl.loop(0, halves * per_half)
    def _(p):
        pl.when(p >= 2)(lambda: down_out(p - 2).wait())
        units_at = pl.ds(pl.multiple_of((p % per_half) * block, block), block)
        us = rows_all[...]
        us = us.reshape(us.shape[0] * us.shape[1], width)
        part = tn(hidden[p // per_half, :, units_at], us)
        tmp[p % 2] = part.astype(bf16).reshape(2, half_rows, width)
        down_out(p).start()

    for p in (halves * per_half - 2, halves * per_half - 1):
        down_out(p).wait()
    for turn in range(LEVELS):
        remote(
            own.at[turn], from_side.at[turn], side_s.at[turn], side_r.at[turn], (0, x)
        ).wait_send()
    for turn in range(LEVELS - 1):
        remote(
            own.at[turn], from_line.at[turn], line_s.at[turn], line_r.at[turn], (0, x)
        ).wait_send()


def run_experts(rows, gates, upstream_all, own_weights, other_weights, collective_id):
    bf16, f32 = jnp.bfloat16, jnp.float32
    half_rows, width = rows.shape
    owner_count = upstream_all.shape[0]
    units = own_weights[0].shape[1]
    halves = lax.axis_size("tp")
    all_rows = owner_count * half_rows
    block = (half_rows, width)
    hbm = pl.BlockSpec(memory_space=pl.ANY)
    vmem = pl.BlockSpec(memory_space=pltpu.VMEM)
    dma = pltpu.SemaphoreType.DMA
    flops = 2 * 9 * all_rows * width * units * halves
    return pl.pallas_call(
        experts_kernel,
        out_shape=[
            jax.ShapeDtypeStruct(block, f32),
            jax.ShapeDtypeStruct((owner_count, half_rows, width + ROUTE_COLS), bf16),
            jax.ShapeDtypeStruct((halves, width, units), bf16),
            jax.ShapeDtypeStruct((halves, width, units), bf16),
            jax.ShapeDtypeStruct((halves, units // half_rows, half_rows, width), bf16),
        ],
        in_specs=[vmem, vmem] + [hbm] * 7,
        out_specs=[vmem, hbm, hbm, hbm, hbm],
        scratch_shapes=[
            pltpu.VMEM((owner_count,) + block, bf16),
            pltpu.VMEM((2, 2) + block, bf16),
            pltpu.VMEM((halves, width, units), bf16),
            pltpu.VMEM((halves, width, units), bf16),
            pltpu.VMEM((halves, units, width), bf16),
            pltpu.VMEM((halves, all_rows, units), bf16),
            pltpu.VMEM((halves, all_rows, units), bf16),
            pltpu.VMEM((halves, all_rows, units), bf16),
            pltpu.VMEM((owner_count // 2, 2 * half_rows, ROUTE_COLS), f32),
            pltpu.VMEM((2, 2) + block, bf16),
            pltpu.VMEM((2 * LEVELS,) + block, bf16),
            pltpu.VMEM((2 * LEVELS,) + block, bf16),
            pltpu.VMEM((LEVELS,) + block, bf16),
            pltpu.VMEM((LEVELS + 1,) + block, bf16),
            pltpu.VMEM((2, 2, half_rows, width + ROUTE_COLS), bf16),
            pltpu.VMEM((2, 2, halves, 256, units), bf16),
            dma((GATHER_SENDS,)),
            dma((owner_count,)),
            dma((2 * LEVELS,)),
            dma((2 * LEVELS,)),
            dma((LEVELS,)),
            dma((LEVELS,)),
            dma((LEVELS + 1,)),
            dma((LEVELS + 1,)),
            dma((7,)),
            dma((2,)),
            dma((6,)),
        ],
        compiler_params=pltpu.CompilerParams(
            collective_id=collective_id, has_side_effects=True, vmem_limit_bytes=67_043_328
        ),
        cost_estimate=pl.CostEstimate(
            flops=flops, bytes_accessed=64 * 2**20, transcendentals=all_rows * units * halves
        ),
        name="experts",
    )(rows, gates, upstream_all, *own_weights, *other_weights)


def gate_columns(route_rows, gate_rows, expert_count):
    names = jnp.arange(expert_count, dtype=jnp.int32)[None, None, :]
    return jnp.sum(jnp.where(route_rows[:, :, None] == names, gate_rows[:, :, None], 0.0), axis=1)


def half_of(rows):
    count = rows.shape[0] // lax.axis_size("tp")
    return lax.dynamic_slice_in_dim(rows, lax.axis_index("tp") * count, count, axis=0)


def per_device_dense(
    block_input,
    upstream_grad,
    first_gain,
    second_gain,
    query_weight,
    key_weight,
    value_weight,
    output_weight,
    gate_weight,
    up_weight,
    down_weight,
    routes,
    gate_values,
):
    pair_count = lax.axis_size("tp")
    owner_count = lax.axis_size("fsdp")
    local_rows = block_input.shape[0]
    seq_rows = local_rows * pair_count
    model_width = block_input.shape[1]
    head_cols = query_weight.shape[1]
    local_heads = head_cols // HD
    expert_count = EXP_DEV * owner_count
    inv_root = HD ** (-0.5)
    bf16, f32 = jnp.bfloat16, jnp.float32

    my_routes, my_gates = half_of(routes), half_of(gate_values)
    gate_table = gate_columns(my_routes, my_gates, ROUTE_COLS)
    expert_names = jnp.arange(expert_count, dtype=jnp.int32)[None, :]
    own_weights = (gate_weight[0], up_weight[0], down_weight[0])

    first_scale = lax.rsqrt(jnp.mean(block_input * block_input, axis=1, keepdims=True) + epsilon)
    first_normed = (block_input * first_scale * first_gain).astype(bf16)
    gathered, normed_pair, other_weights = gather_weights(
        [
            query_weight,
            key_weight,
            value_weight,
            output_weight,
            upstream_grad.astype(bf16),
            gate_table,
        ],
        first_normed,
        own_weights,
        1,
    )
    query_full, key_full, value_full, output_full = (w.reshape(-1, head_cols) for w in gathered[:4])
    upstream_all, gates_all = gathered[4:]
    normed_rows = normed_pair.reshape(seq_rows, model_width)

    def heads_of(weight_full):
        return (
            jnp.dot(normed_rows, weight_full, preferred_element_type=f32)
            .astype(bf16)
            .reshape(seq_rows, local_heads, HD)
        )

    query_rows, key_rows, value_rows = heads_of(query_full), heads_of(key_full), heads_of(value_full)
    scores = jnp.einsum("shd,thd->hst", query_rows, key_rows, preferred_element_type=f32) * inv_root
    row_top = jnp.max(scores, axis=2, keepdims=True)
    log_total = row_top + jnp.log(jnp.sum(jnp.exp(scores - row_top), axis=2, keepdims=True))
    soft_weights = jnp.exp(scores - log_total)
    soft_rounded = soft_weights.astype(bf16)
    mixed_rows = jnp.einsum("hst,thd->shd", soft_rounded, value_rows, preferred_element_type=f32)
    mixed_rows = mixed_rows.astype(bf16).reshape(seq_rows, head_cols)
    middle = block_input + pair_sums(contract_cols(mixed_rows, output_full))
    second_scale = lax.rsqrt(jnp.mean(middle * middle, axis=1, keepdims=True) + epsilon)
    second_normed = (middle * second_scale * second_gain).astype(bf16)

    second_cot, mixture_part, gate_part, up_part, down_part = run_experts(
        second_normed, gates_all, upstream_all, own_weights, other_weights, 2
    )

    weighted_two = second_cot * second_gain
    second_term = jnp.sum(second_cot * middle * second_scale, axis=0)
    middle_grad = upstream_grad + second_scale * (
        weighted_two
        - middle
        * second_scale
        * second_scale
        * jnp.mean(weighted_two * middle, axis=1, keepdims=True)
    )
    middle_rows = pair_rows(middle_grad.astype(bf16))
    out_term = contract_rows(middle_rows, mixed_rows)
    mixed_cot = (
        jnp.dot(middle_rows, output_full, preferred_element_type=f32)
        .astype(bf16)
        .reshape(seq_rows, local_heads, HD)
    )
    value_cot = jnp.einsum("hst,shd->thd", soft_rounded, mixed_cot, preferred_element_type=f32)
    value_cot = value_cot.astype(bf16).reshape(seq_rows, head_cols)
    soft_cot = jnp.einsum("shd,thd->hst", mixed_cot, value_rows, preferred_element_type=f32)
    score_cot = (
        soft_weights
        * (soft_cot - jnp.sum(soft_weights * soft_cot, axis=2, keepdims=True))
        * inv_root
    ).astype(bf16)
    query_cot = (
        jnp.einsum("hst,thd->shd", score_cot, key_rows, preferred_element_type=f32)
        .astype(bf16)
        .reshape(seq_rows, head_cols)
    )
    key_cot = (
        jnp.einsum("hst,shd->thd", score_cot, query_rows, preferred_element_type=f32)
        .astype(bf16)
        .reshape(seq_rows, head_cols)
    )
    first_terms = (
        contract_cols(query_cot, query_full)
        + contract_cols(key_cot, key_full)
        + contract_cols(value_cot, value_full)
    )
    sums, expert_grads, input_grad, gain_grads = sum_gradients(
        [
            term.astype(bf16).reshape((owner_count,) + query_weight.shape)
            for term in (
                contract_rows(normed_rows, query_cot),
                contract_rows(normed_rows, key_cot),
                contract_rows(normed_rows, value_cot),
                out_term,
            )
        ]
        + [mixture_part],
        (gate_part, up_part, down_part.reshape(pair_count, -1, model_width)),
        first_terms.astype(bf16).reshape(pair_count, local_rows, model_width),
        (block_input, first_scale, first_gain[None], middle_grad, second_term[None]),
        4,
    )
    query_grad, key_grad, value_grad, output_grad, mixture = sums
    gate_grad, up_grad, down_grad = expert_grads
    block_output = middle + mixture[:, :model_width]
    route_back = mixture[:, model_width : model_width + expert_count]
    route_grad = jnp.sum(
        jnp.where(my_routes[:, :, None] == expert_names[None], route_back[:, None, :], 0.0), axis=2
    )
    return (
        block_output,
        input_grad,
        gain_grads[0],
        gain_grads[1],
        query_grad,
        key_grad,
        value_grad,
        output_grad,
        gate_grad[None],
        up_grad[None],
        down_grad[None],
        route_grad,
    )


def solution(mesh):
    dense = 2 * TOP >= EXP_DEV * mesh.shape["fsdp"] and mesh.shape["fsdp"] == 4 * LEVELS
    per_device = per_device_dense if dense else per_device_slots
    in_specs = (
        P(("fsdp", "tp"), None),
        P(("fsdp", "tp"), None),
        P(),
        P(),
        P("fsdp", "tp"),
        P("fsdp", "tp"),
        P("fsdp", "tp"),
        P("fsdp", "tp"),
        P("fsdp", None, "tp"),
        P("fsdp", None, "tp"),
        P("fsdp", "tp", None),
        P("fsdp", None),
        P("fsdp", None),
    )
    out_specs = (
        P(("fsdp", "tp"), None),
        P(("fsdp", "tp"), None),
        P(),
        P(),
        P("fsdp", "tp"),
        P("fsdp", "tp"),
        P("fsdp", "tp"),
        P("fsdp", "tp"),
        P("fsdp", None, "tp"),
        P("fsdp", None, "tp"),
        P("fsdp", "tp", None),
        P(("fsdp", "tp"), None),
    )
    return jax.shard_map(
        per_device, mesh=mesh, in_specs=in_specs, out_specs=out_specs, check_vma=False
    )
```

```python
import functools

import jax
import jax.numpy as jnp
from jax import lax
from jax.experimental import pallas as pl
from jax.experimental.pallas import tpu as pltpu
from jax.sharding import PartitionSpec as P

HD = 128
TOP = 8
EXP_DEV = 1


epsilon = 1e-05


def route_slots(route_rows, expert_count, capacity):
    flat_routes = route_rows.reshape(-1)
    onehot = (flat_routes[:, None] == jnp.arange(expert_count, dtype=jnp.int32)[None, :]).astype(
        jnp.int32
    )
    earlier = jnp.cumsum(onehot, axis=0, dtype=jnp.int32) - onehot
    ranked = jnp.sum(earlier * onehot, axis=1, dtype=jnp.int32)
    return flat_routes * capacity + ranked


def pair_rows(row_block):
    return lax.all_gather(row_block, "tp", axis=0, tiled=True)


def pair_sums(term_block):
    return lax.psum_scatter(term_block, "tp", scatter_dimension=0, tiled=True)


def to_owners(buffer):
    return lax.all_to_all(buffer, "fsdp", split_axis=0, concat_axis=0, tiled=True)


def to_sources(buffer):
    return lax.all_to_all(buffer, "fsdp", split_axis=0, concat_axis=0, tiled=True)


def projections(query_weight, key_weight, value_weight, output_weight):
    return (
        lax.all_gather(query_weight, "fsdp", axis=0, tiled=True),
        lax.all_gather(key_weight, "fsdp", axis=0, tiled=True),
        lax.all_gather(value_weight, "fsdp", axis=0, tiled=True),
        lax.all_gather(output_weight, "fsdp", axis=0, tiled=True),
    )


def scatter_rows(row_block, slot_index, total_rows):
    return (
        jnp.zeros((total_rows, row_block.shape[1]), row_block.dtype).at[slot_index].set(row_block)
    )


def spread_rows(row_block, copies):
    return jnp.broadcast_to(
        row_block[:, None, :], (row_block.shape[0], copies, row_block.shape[1])
    ).reshape(-1, row_block.shape[1])


def contract_rows(left_block, right_block):
    return lax.dot_general(
        left_block, right_block, (((0,), (0,)), ((), ())), preferred_element_type=jnp.float32
    )


def contract_cols(left_block, right_block):
    return lax.dot_general(
        left_block, right_block, (((1,), (1,)), ((), ())), preferred_element_type=jnp.float32
    )


def send_out(full_buffer):
    return to_owners(full_buffer)


def send_back(group_parts):
    owner_count, local_experts, capacity, model_width = group_parts.shape
    return to_sources(group_parts).reshape(owner_count * local_experts * capacity, model_width)


def per_device_slots(
    block_input,
    upstream_grad,
    first_gain,
    second_gain,
    query_weight,
    key_weight,
    value_weight,
    output_weight,
    gate_weight,
    up_weight,
    down_weight,
    routes,
    gate_values,
):
    pair_count = lax.axis_size("tp")
    owner_count = lax.axis_size("fsdp")
    local_rows = block_input.shape[0]
    seq_rows = local_rows * pair_count
    model_width = block_input.shape[1]
    head_cols = query_weight.shape[1]
    local_heads = head_cols // HD
    expert_count = EXP_DEV * owner_count
    capacity = 3 * seq_rows * TOP // (2 * expert_count)
    inv_root = HD ** (-0.5)
    first_scale = lax.rsqrt(jnp.mean(block_input * block_input, axis=1, keepdims=True) + epsilon)
    first_normed = (block_input * first_scale * first_gain).astype(jnp.bfloat16)
    normed_rows = pair_rows(first_normed)
    query_full, key_full, value_full, output_full = projections(
        query_weight, key_weight, value_weight, output_weight
    )
    query_rows = (
        jnp.dot(normed_rows, query_full, preferred_element_type=jnp.float32)
        .astype(jnp.bfloat16)
        .reshape(seq_rows, local_heads, HD)
    )
    key_rows = (
        jnp.dot(normed_rows, key_full, preferred_element_type=jnp.float32)
        .astype(jnp.bfloat16)
        .reshape(seq_rows, local_heads, HD)
    )
    value_rows = (
        jnp.dot(normed_rows, value_full, preferred_element_type=jnp.float32)
        .astype(jnp.bfloat16)
        .reshape(seq_rows, local_heads, HD)
    )
    scores = (
        jnp.einsum("shd,thd->hst", query_rows, key_rows, preferred_element_type=jnp.float32)
        * inv_root
    )
    row_top = jnp.max(scores, axis=2, keepdims=True)
    log_total = row_top + jnp.log(jnp.sum(jnp.exp(scores - row_top), axis=2, keepdims=True))
    soft_weights = jnp.exp(scores - log_total)
    mixed_rows = jnp.einsum(
        "hst,thd->shd",
        soft_weights.astype(jnp.bfloat16),
        value_rows,
        preferred_element_type=jnp.float32,
    )
    mixed_rows = mixed_rows.astype(jnp.bfloat16).reshape(seq_rows, head_cols)
    middle = block_input + pair_sums(contract_cols(mixed_rows, output_full))
    second_scale = lax.rsqrt(jnp.mean(middle * middle, axis=1, keepdims=True) + epsilon)
    second_normed = (middle * second_scale * second_gain).astype(jnp.bfloat16)
    moe_rows = pair_rows(second_normed)
    slot_index = route_slots(routes, expert_count, capacity)
    send_rows = scatter_rows(spread_rows(moe_rows, TOP), slot_index, expert_count * capacity)
    arrived = send_out(send_rows.reshape(owner_count, EXP_DEV, capacity, model_width))
    gate_act = jnp.einsum(
        "secd,edf->secf", arrived, gate_weight, preferred_element_type=jnp.float32
    )
    up_act = jnp.einsum("secd,edf->secf", arrived, up_weight, preferred_element_type=jnp.float32)
    sigmoid_gate = jax.nn.sigmoid(gate_act)
    hidden = (gate_act * sigmoid_gate * up_act).astype(jnp.bfloat16)
    expert_out = jnp.einsum(
        "secf,efd->secd", hidden, down_weight, preferred_element_type=jnp.float32
    ).astype(jnp.bfloat16)
    returned = send_back(expert_out)
    picked = returned[slot_index].reshape(seq_rows, TOP, model_width).astype(jnp.float32)
    mixture = jnp.sum(gate_values[:, :, None] * picked, axis=1)
    block_output = middle + pair_sums(mixture)
    upstream_rows = lax.all_gather(upstream_grad, "tp", axis=0, tiled=True)
    route_terms = jnp.sum(upstream_rows[:, None, :] * picked, axis=2)
    routed_cot = (
        (gate_values[:, :, None] * upstream_rows[:, None, :])
        .astype(jnp.bfloat16)
        .reshape(seq_rows * TOP, model_width)
    )
    cot_send = scatter_rows(routed_cot, slot_index, expert_count * capacity)
    cot_arrived = send_out(cot_send.reshape(owner_count, EXP_DEV, capacity, model_width))
    hidden_cot = jnp.einsum(
        "secd,efd->secf", cot_arrived, down_weight, preferred_element_type=jnp.float32
    )
    down_grad = jnp.einsum(
        "secf,secd->efd", hidden, cot_arrived, preferred_element_type=jnp.float32
    )
    gate_cot = (
        hidden_cot * up_act * sigmoid_gate * (1.0 + gate_act * (1.0 - sigmoid_gate))
    ).astype(jnp.bfloat16)
    up_cot = (hidden_cot * gate_act * sigmoid_gate).astype(jnp.bfloat16)
    gate_grad = jnp.einsum("secd,secf->edf", arrived, gate_cot, preferred_element_type=jnp.float32)
    up_grad = jnp.einsum("secd,secf->edf", arrived, up_cot, preferred_element_type=jnp.float32)
    input_cot = jnp.einsum(
        "secf,edf->secd", gate_cot, gate_weight, preferred_element_type=jnp.float32
    )
    input_cot = (
        input_cot
        + jnp.einsum("secf,edf->secd", up_cot, up_weight, preferred_element_type=jnp.float32)
    ).astype(jnp.bfloat16)
    came_back = send_back(input_cot)
    normed_cot = jnp.sum(
        came_back[slot_index].reshape(seq_rows, TOP, model_width).astype(jnp.float32), axis=1
    )
    second_cot, route_grad = (
        lax.psum_scatter(
            normed_cot.astype(jnp.bfloat16), "tp", scatter_dimension=0, tiled=True
        ).astype(jnp.float32),
        lax.psum_scatter(
            route_terms.astype(jnp.bfloat16), "tp", scatter_dimension=0, tiled=True
        ).astype(jnp.float32),
    )
    weighted_two = second_cot * second_gain
    second_term = jnp.sum(second_cot * middle * second_scale, axis=0)
    middle_grad = upstream_grad + second_scale * (
        weighted_two
        - middle
        * second_scale
        * second_scale
        * jnp.mean(weighted_two * middle, axis=1, keepdims=True)
    )
    middle_rows = pair_rows(middle_grad.astype(jnp.bfloat16))
    query_full, key_full, value_full, output_full = projections(
        query_weight, key_weight, value_weight, output_weight
    )
    out_term = contract_rows(middle_rows, mixed_rows)
    mixed_cot = (
        jnp.dot(middle_rows, output_full, preferred_element_type=jnp.float32)
        .astype(jnp.bfloat16)
        .reshape(seq_rows, local_heads, HD)
    )
    scores = (
        jnp.einsum("shd,thd->hst", query_rows, key_rows, preferred_element_type=jnp.float32)
        * inv_root
    )
    soft_weights = jnp.exp(scores - log_total)
    value_cot = jnp.einsum(
        "hst,shd->thd",
        soft_weights.astype(jnp.bfloat16),
        mixed_cot,
        preferred_element_type=jnp.float32,
    )
    value_cot = value_cot.astype(jnp.bfloat16).reshape(seq_rows, head_cols)
    soft_cot = jnp.einsum("shd,thd->hst", mixed_cot, value_rows, preferred_element_type=jnp.float32)
    score_cot = (
        soft_weights
        * (soft_cot - jnp.sum(soft_weights * soft_cot, axis=2, keepdims=True))
        * inv_root
    ).astype(jnp.bfloat16)
    query_cot = (
        jnp.einsum("hst,thd->shd", score_cot, key_rows, preferred_element_type=jnp.float32)
        .astype(jnp.bfloat16)
        .reshape(seq_rows, head_cols)
    )
    key_cot = (
        jnp.einsum("hst,shd->thd", score_cot, query_rows, preferred_element_type=jnp.float32)
        .astype(jnp.bfloat16)
        .reshape(seq_rows, head_cols)
    )
    query_term = contract_rows(normed_rows, query_cot)
    key_term = contract_rows(normed_rows, key_cot)
    value_term = contract_rows(normed_rows, value_cot)
    first_terms = (
        contract_cols(query_cot, query_full)
        + contract_cols(key_cot, key_full)
        + contract_cols(value_cot, value_full)
    )
    first_cot = pair_sums(first_terms)
    weighted_one = first_cot * first_gain
    first_term = jnp.sum(first_cot * block_input * first_scale, axis=0)
    input_grad = middle_grad + first_scale * (
        weighted_one
        - block_input
        * first_scale
        * first_scale
        * jnp.mean(weighted_one * block_input, axis=1, keepdims=True)
    )
    query_grad, key_grad, value_grad, output_grad = (
        lax.psum_scatter(query_term, "fsdp", scatter_dimension=0, tiled=True),
        lax.psum_scatter(key_term, "fsdp", scatter_dimension=0, tiled=True),
        lax.psum_scatter(value_term, "fsdp", scatter_dimension=0, tiled=True),
        lax.psum_scatter(out_term, "fsdp", scatter_dimension=0, tiled=True),
    )
    first_gain_grad, second_gain_grad = lax.psum((first_term, second_term), ("fsdp", "tp"))
    return (
        block_output,
        input_grad,
        first_gain_grad,
        second_gain_grad,
        query_grad,
        key_grad,
        value_grad,
        output_grad,
        gate_grad,
        up_grad,
        down_grad,
        route_grad,
    )


MESH = pl.DeviceIdType.MESH


def place():
    here = lax.axis_index("fsdp")
    return here // 4, (here // 2) % 2, here % 2, lax.axis_index("tp")


def index_of(z, y, c):
    return (z * 2 + y) * 2 + c


LEVELS = 4
LEVEL_ORDER = sum(
    level << (8 * turn + 2 * z)
    for turn, row in enumerate(((3, 3, 0, 0), (2, 2, 1, 1), (1, 0, 3, 2), (0, 1, 2, 3)))
    for z, level in enumerate(row)
) - (1 << 32)


def level_at(turn, z):
    return (jnp.int32(LEVEL_ORDER) >> (8 * turn + 2 * z)) & 3


def line_ends(z):
    return (z + 1) // LEVELS, (LEVELS - z) // LEVELS


def plane_greet(pair=False, far=False):
    z, y, c, x = place()
    top, bottom = line_ends(z)
    barrier = pltpu.get_barrier_semaphore()
    partners = [(index_of(z, 1 - y, c), x), (index_of(z, y, 1 - c), x)]
    if pair:
        partners.append((index_of(z, y, c), 1 - x))
    if far:
        partners.append((index_of((z + 2) % LEVELS, y, c), x))
    for partner in partners:
        pl.semaphore_signal(barrier, inc=1, device_id=partner, device_id_type=MESH)

    @pl.when(top == 0)
    def _():
        above = (index_of(z + 1, y, c), x)
        pl.semaphore_signal(barrier, inc=1, device_id=above, device_id_type=MESH)

    @pl.when(bottom == 0)
    def _():
        below = (index_of(z - 1, y, c), x)
        pl.semaphore_signal(barrier, inc=1, device_id=below, device_id_type=MESH)

    pl.semaphore_wait(barrier, len(partners) + 2 - top - bottom)


def remote(src, dst, send_sem, recv_sem, target):
    return pltpu.make_async_remote_copy(
        src_ref=src,
        dst_ref=dst,
        send_sem=send_sem,
        recv_sem=recv_sem,
        device_id=target,
        device_id_type=MESH,
    )


class PlaneGather:
    def __init__(self, mine, full, send_sems, recv_sems):
        self.mine, self.full = mine, full
        self.send_sems, self.recv_sems = send_sems, recv_sems
        self.z, self.y, self.c, self.x = place()
        self.top, self.bottom = line_ends(self.z)

    def _copy(self, number, src, slot, target):
        return remote(
            src, self.full.at[slot], self.send_sems.at[number], self.recv_sems.at[slot], target
        )

    def arrived(self, slot):
        here = self.full.at[slot]
        remote(here, here, self.send_sems.at[0], self.recv_sems.at[slot], (0, self.x)).wait_recv()

    def start(self):
        z, y, c, x = self.z, self.y, self.c, self.x
        own = index_of(z, y, c)
        up = self._copy(0, self.mine, own, (index_of(z + 1, y, c), x))
        down = self._copy(1, self.mine, own, (index_of(z - 1, y, c), x))
        pl.when(self.top == 0)(up.start)
        pl.when(self.bottom == 0)(down.start)
        self._copy(2, self.mine, own, (index_of(z, 1 - y, c), x)).start()
        self._copy(3, self.mine, own, (index_of(z, y, 1 - c), x)).start()

    def from_line(self, step):
        z, y, c, x = self.z, self.y, self.c, self.x
        level = level_at(3 - step, z)
        slot = index_of(level, y, c)
        self.arrived(slot)
        onward = z + 1 - 2 * ((level + LEVELS - z) // LEVELS)
        src, number = self.full.at[slot], 4 + 3 * (step - 1)
        forward = self._copy(number, src, slot, (index_of(onward, y, c), x))
        pl.when(self.top + self.bottom == 0)(forward.start)
        self._copy(number + 1, src, slot, (index_of(z, 1 - y, c), x)).start()
        self._copy(number + 2, src, slot, (index_of(z, y, 1 - c), x)).start()

    def from_side(self, step):
        z, y, c, x = self.z, self.y, self.c, self.x
        slot = index_of(level_at(3 - step, z), 1 - y, c)
        self.arrived(slot)
        self._copy(13 + step, self.full.at[slot], slot, (index_of(z, y, 1 - c), x)).start()

    def from_core(self, step, side):
        z, y, c = self.z, self.y, self.c
        self.arrived(index_of(level_at(3 - step, z), (y + side) % 2, 1 - c))

    def finish(self):
        for number in range(GATHER_SENDS):
            wait = self._copy(number, self.mine, 0, (0, self.x)).wait_send
            if number == 0:
                pl.when(self.top == 0)(wait)
            elif number == 1:
                pl.when(self.bottom == 0)(wait)
            elif number in (4, 7, 10):
                pl.when(self.top + self.bottom == 0)(wait)
            else:
                wait()


GATHER_SENDS = 17


def weights_kernel(count, *refs):
    mine, normed, experts = refs[:count], refs[count], refs[count + 1 : count + 4]
    outs = refs[count + 4 : 2 * count + 8]
    full, normed_pair, others = outs[:count], outs[count], outs[count + 1 :]
    send_sems, recv_sems, own_sems, pair_s, pair_r = refs[2 * count + 8 :]
    z, y, c, x = place()
    own = index_of(z, y, c)
    plane_greet(pair=True)
    plans = [
        PlaneGather(mine[a], full[a], send_sems.at[a], recv_sems.at[a]) for a in range(count)
    ]
    swaps = [
        remote(src, dst, pair_s.at[i], pair_r.at[i], (own, 1 - x))
        for i, (src, dst) in enumerate(
            [(normed, normed_pair.at[x])] + list(zip(experts, others))
        )
    ]
    kept = [
        pltpu.make_async_copy(src, dst, own_sems.at[i])
        for i, (src, dst) in enumerate(
            [(mine[a], full[a].at[own]) for a in range(count)] + [(normed, normed_pair.at[x])]
        )
    ]
    for plan in plans:
        plan.start()
    for copy in swaps + kept:
        copy.start()
    for step in range(1, LEVELS):
        for plan in plans:
            plan.from_line(step)
        for plan in plans:
            plan.from_side(step - 1)
    for plan in plans:
        plan.from_side(LEVELS - 1)
    for plan in plans:
        for step in range(LEVELS):
            for side in range(2):
                plan.from_core(step, side)
    for plan in plans:
        plan.finish()
    for copy in swaps + kept:
        copy.wait()


def gather_weights(arrays, normed, experts, collective_id):
    owner_count = lax.axis_size("fsdp")
    count = len(arrays)
    hbm = pl.BlockSpec(memory_space=pl.ANY)
    vmem = pl.BlockSpec(memory_space=pltpu.VMEM)
    nbytes = sum(a.size * a.dtype.itemsize for a in arrays)
    outs = pl.pallas_call(
        functools.partial(weights_kernel, count),
        out_shape=[jax.ShapeDtypeStruct((owner_count,) + a.shape, a.dtype) for a in arrays]
        + [jax.ShapeDtypeStruct((2,) + normed.shape, normed.dtype)]
        + [jax.ShapeDtypeStruct(w.shape, w.dtype) for w in experts],
        in_specs=[vmem] * (count + 1) + [hbm] * 3,
        out_specs=[hbm] * (count + 4),
        scratch_shapes=[
            pltpu.SemaphoreType.DMA((count, GATHER_SENDS)),
            pltpu.SemaphoreType.DMA((count, owner_count)),
            pltpu.SemaphoreType.DMA((count + 1,)),
            pltpu.SemaphoreType.DMA((4,)),
            pltpu.SemaphoreType.DMA((4,)),
        ],
        compiler_params=pltpu.CompilerParams(collective_id=collective_id, has_side_effects=True),
        cost_estimate=pl.CostEstimate(
            flops=0, bytes_accessed=owner_count * nbytes * 4, transcendentals=0
        ),
        name="gather_weights",
    )(*arrays, normed, *experts)
    return outs[:count], outs[count], outs[count + 1 :]


class PlaneSums:
    def __init__(self, own_parts, from_core, from_side, from_line, sems, kept=0):
        self.own, self.from_core, self.kept = own_parts, from_core, kept
        self.from_side, self.from_line = from_side, from_line
        self.core_s, self.core_r, self.side_s, self.side_r, self.line_s, self.line_r = sems
        self.z, self.y, self.c, self.x = place()
        self.top, self.bottom = line_ends(self.z)
        self.sent = []

    def slot_of(self, turn, side, core):
        return index_of(level_at(turn, self.z), (self.y + side) % 2, (self.c + core) % 2)

    def to_core(self, part, turn, side):
        j = side * LEVELS + turn
        copy = remote(
            part,
            self.from_core.at[j],
            self.core_s.at[j],
            self.core_r.at[j],
            (index_of(self.z, self.y, 1 - self.c), self.x),
        )
        copy.start()
        self.sent.append(copy)

    def core_arrived(self, turn, side):
        j = side * LEVELS + turn
        here = self.from_core.at[j]
        remote(here, here, self.core_s.at[j], self.core_r.at[j], (0, self.x)).wait_recv()

    def to_side(self, turn):
        copy = remote(
            self.own.at[LEVELS + turn],
            self.from_side.at[turn],
            self.side_s.at[turn],
            self.side_r.at[turn],
            (index_of(self.z, 1 - self.y, self.c), self.x),
        )
        copy.start()
        self.sent.append(copy)

    def side_arrived(self, turn):
        here = self.from_side.at[turn]
        remote(here, here, self.side_s.at[turn], self.side_r.at[turn], (0, self.x)).wait_recv()

    def line_arrived(self, slot):
        here = self.from_line.at[slot]
        remote(here, here, self.line_s.at[0], self.line_r.at[slot], (0, self.x)).wait_recv()

    def to_line(self, turn):
        z, y, c, x = self.z, self.y, self.c, self.x
        mine = self.own.at[self.kept + turn]
        level = level_at(turn, z)

        @pl.when(self.top + self.bottom == 0)
        def _():
            self.line_arrived(level)
            add_block(mine, self.from_line.at[level], mine)

        down = (z + LEVELS - level) // (LEVELS + 1)
        onward = z + 1 - 2 * down
        reached = 1 - jnp.minimum(1, jnp.abs(onward - level))
        slot = level + down * reached * (LEVELS - level)
        copy = remote(
            mine,
            self.from_line.at[slot],
            self.line_s.at[turn],
            self.line_r.at[slot],
            (index_of(onward, y, c), x),
        )
        copy.start()
        self.sent.append(copy)

    def finish(self):
        for copy in self.sent:
            copy.wait_send()


def add_block(one, two, out):
    step = 32

    @pl.loop(0, out.shape[0] // step)
    def _(i):
        rows = pl.ds(pl.multiple_of(i * step, step), step)
        value = one[rows, :].astype(jnp.float32) + two[rows, :].astype(jnp.float32)
        out[rows, :] = value.astype(out.dtype)


def total_block(plan, total):
    step = 32
    mine = plan.own.at[plan.kept + LEVELS - 1]
    below, above = plan.from_line.at[plan.z], plan.from_line.at[LEVELS]

    @pl.loop(0, total.shape[0] // step)
    def _(i):
        rows = pl.ds(pl.multiple_of(i * step, step), step)
        total[rows, :] = mine[rows, :].astype(jnp.float32)

    for end, block, slot in ((plan.bottom, below, plan.z), (plan.top, above, LEVELS)):

        @pl.when(end == 0)
        def _():
            plan.line_arrived(slot)

            @pl.loop(0, total.shape[0] // step)
            def _(i):
                rows = pl.ds(pl.multiple_of(i * step, step), step)
                total[rows, :] = total[rows, :] + block[rows, :].astype(jnp.float32)


def last_kernel(count, *refs):
    parts, refs = refs[:count], refs[count:]
    expert_parts, refs = refs[:2], refs[2:]
    first_part, block_input, first_scale, first_gain, middle_grad, second_term = refs[:6]
    refs = refs[6:]
    totals, refs = refs[:count], refs[count:]
    expert_landed, refs = refs[:2], refs[2:]
    input_grad, gain_grads, refs = refs[0], refs[1], refs[2:]
    buffers = [refs[i * count : (i + 1) * count] for i in range(4)]
    refs = refs[4 * count :]
    sems, own_sems, refs = refs[:6], refs[6], refs[7:]
    first_other, gains, gains_in, pair_s, pair_r, gain_s, gain_r = refs
    z, y, c, x = place()
    own = index_of(z, y, c)
    plane_greet(pair=True, far=True)
    plans = [
        PlaneSums(*(b[a] for b in buffers), tuple(s.at[a] for s in sems)) for a in range(count)
    ]
    swaps = [
        remote(src, dst, pair_s.at[i], pair_r.at[i], (own, 1 - x))
        for i, (src, dst) in enumerate(
            [(first_part.at[1 - x], first_other)] + list(zip(expert_parts, expert_landed))
        )
    ]
    swaps[0].start()
    loads = {}
    for a, plan in enumerate(plans):
        for side in (1, 0):
            for turn in range(LEVELS):
                plan.to_core(parts[a].at[plan.slot_of(turn, side, 1)], turn, side)
                j = side * LEVELS + turn
                load = pltpu.make_async_copy(
                    parts[a].at[plan.slot_of(turn, side, 0)], plan.own.at[j], own_sems.at[a, j]
                )
                load.start()
                loads[a, j] = load

    def core_step(turn, side):
        for a, plan in enumerate(plans):
            j = side * LEVELS + turn
            loads[a, j].wait()
            plan.core_arrived(turn, side)
            add_block(plan.own.at[j], plan.from_core.at[j], plan.own.at[j])
            if side == 1:
                plan.to_side(turn)

    def line_step(turn):
        for plan in plans:
            plan.side_arrived(turn)
            add_block(plan.own.at[turn], plan.from_side.at[turn], plan.own.at[turn])
            if turn < LEVELS - 1:
                plan.to_line(turn)

    def finish_norm():
        swaps[0].wait_recv()
        step = 16
        width = input_grad.shape[1]
        gains[...] = jnp.concatenate(
            [jnp.zeros((1, width), jnp.float32), second_term[...], jnp.zeros((6, width), jnp.float32)],
            axis=0,
        )
        gain = first_gain[...]

        @pl.loop(0, input_grad.shape[0] // step)
        def _(i):
            rows = pl.ds(pl.multiple_of(i * step, step), step)
            value = first_part[x, rows, :].astype(jnp.float32)
            value = value + first_other[rows, :].astype(jnp.float32)
            entry, scale = block_input[rows, :], first_scale[rows, :]
            weighted = value * gain
            mean = jnp.mean(weighted * entry, axis=1, keepdims=True)
            input_grad[rows, :] = middle_grad[rows, :] + scale * (
                weighted - entry * (scale * scale * mean)
            )
            gains[0:1, :] = gains[0:1, :] + jnp.sum(value * entry * scale, axis=0, keepdims=True)

    hops = [
        (index_of(z, y, 1 - c), x),
        (own, 1 - x),
        (index_of(z + 1 - 2 * (z % 2), y, c), x),
        (index_of((z + 2) % LEVELS, y, c), x),
        (index_of(z, 1 - y, c), x),
    ]

    def gain_copy(i):
        return remote(gains, gains_in.at[i], gain_s.at[i], gain_r.at[i], hops[i])

    def gain_add(i):
        gain_copy(i).wait()
        gains[...] = gains[...] + gains_in[i]

    core_step(0, 1)
    for turn in range(LEVELS):
        core_step(turn, 0)
    finish_norm()
    for i in range(4):
        gain_copy(i).start()
        gain_add(i)
    gain_copy(4).start()
    for swap in swaps[1:]:
        swap.start()
    for turn in range(1, LEVELS):
        core_step(turn, 1)
    line_step(0)
    gain_add(4)
    gain_grads[...] = gains[...]
    for turn in range(1, LEVELS):
        line_step(turn)
    for a, plan in enumerate(plans):
        total_block(plan, totals[a])
    for plan in plans:
        plan.finish()
    swaps[0].wait_send()
    for swap in swaps[1:]:
        swap.wait()


def sum_gradients(parts, expert_parts, first_part, norm_args, collective_id):
    f32 = jnp.float32
    count = len(parts)
    shapes = [p.shape[1:] for p in parts]
    types = [p.dtype for p in parts]
    hbm = pl.BlockSpec(memory_space=pl.ANY)
    vmem = pl.BlockSpec(memory_space=pltpu.VMEM)
    width = first_part.shape[2]

    def scratch(blocks):
        return [pltpu.VMEM((blocks,) + s, t) for s, t in zip(shapes, types)]

    def sems(blocks):
        return [pltpu.SemaphoreType.DMA((count, blocks))] * 2

    nbytes = sum(p.size * p.dtype.itemsize for p in parts)
    outs = pl.pallas_call(
        functools.partial(last_kernel, count),
        out_shape=[jax.ShapeDtypeStruct(s, f32) for s in shapes]
        + [jax.ShapeDtypeStruct(p.shape, p.dtype) for p in expert_parts]
        + [
            jax.ShapeDtypeStruct(first_part.shape[1:], f32),
            jax.ShapeDtypeStruct((8, width), f32),
        ],
        in_specs=[hbm] * (count + 2) + [vmem] * 6,
        out_specs=[vmem] * count + [hbm] * 2 + [vmem] * 2,
        scratch_shapes=scratch(2 * LEVELS)
        + scratch(2 * LEVELS)
        + scratch(LEVELS)
        + scratch(LEVELS + 1)
        + sems(2 * LEVELS)
        + sems(LEVELS)
        + sems(LEVELS + 1)
        + [pltpu.SemaphoreType.DMA((count, 2 * LEVELS))]
        + [
            pltpu.VMEM(first_part.shape[1:], first_part.dtype),
            pltpu.VMEM((8, width), f32),
            pltpu.VMEM((5, 8, width), f32),
            pltpu.SemaphoreType.DMA((3,)),
            pltpu.SemaphoreType.DMA((3,)),
            pltpu.SemaphoreType.DMA((5,)),
            pltpu.SemaphoreType.DMA((5,)),
        ],
        compiler_params=pltpu.CompilerParams(
            collective_id=collective_id, has_side_effects=True, vmem_limit_bytes=67_043_328
        ),
        cost_estimate=pl.CostEstimate(flops=0, bytes_accessed=4 * nbytes, transcendentals=0),
        name="sum_gradients",
    )(*parts, *expert_parts, first_part, *norm_args)
    return outs[:count], outs[count : count + 2], outs[count + 2], outs[count + 3]


ROUTE_COLS = 128


def nn(left, right):
    return lax.dot_general(
        left, right, (((1,), (0,)), ((), ())), preferred_element_type=jnp.float32
    )


def nt(left, right):
    return lax.dot_general(
        left, right, (((1,), (1,)), ((), ())), preferred_element_type=jnp.float32
    )


def tn(left, right):
    return lax.dot_general(
        left, right, (((0,), (0,)), ((), ())), preferred_element_type=jnp.float32
    )


def pair_block(ref, pair):
    value = ref[pl.ds(2 * pair, 2)]
    return value.reshape(value.shape[0] * value.shape[1], value.shape[2])


def experts_kernel(
    gates,
    second_gain,
    out_part,
    block_input,
    upstream,
    upstream_hbm,
    gate_own,
    up_own,
    down_own,
    gate_other,
    up_other,
    down_other,
    middle,
    middle_grad,
    second_term,
    middle_pair,
    mixture_hbm,
    gate_mine,
    gate_theirs,
    up_mine,
    up_theirs,
    down_mine,
    down_landed,
    rows_all,
    u_all,
    wg,
    wu,
    wd,
    hidden,
    gcot,
    ucot,
    rext,
    tmp,
    from_core,
    from_side,
    from_line,
    gstage,
    wide,
    second_scale,
    route_half,
    gather_s,
    gather_r,
    core_s,
    core_r,
    side_s,
    side_r,
    line_s,
    line_r,
    load_sems,
    out_sems,
    pair_s,
    pair_r,
):
    bf16, f32 = jnp.bfloat16, jnp.float32
    z, y, c, x = place()
    top, bottom = line_ends(z)
    interior = 1 - top - bottom
    me = lax.axis_index("fsdp")
    partner = (me, 1 - x)
    halves, width, units = wg.shape
    half_rows = middle.shape[0]
    pair_rows_ = 2 * half_rows
    pairs = 2 * LEVELS
    panel = 512
    block = 256
    step = 16

    loads = [
        pltpu.make_async_copy(src, dst, load_sems.at[i])
        for i, (src, dst) in enumerate(
            (
                (out_part.at[1 - x], middle_grad),
                (out_part.at[x], middle),
                (block_input, wide),
                (gate_own, wg.at[x]),
                (up_own, wu.at[x]),
                (down_own, wd.at[x]),
                (gate_other, wg.at[1 - x]),
                (up_other, wu.at[1 - x]),
                (down_other, wd.at[1 - x]),
                (upstream_hbm, u_all),
            )
        )
    ]
    for load in loads:
        load.start()

    plane_greet(pair=True)
    gather = PlaneGather(rows_all.at[me], rows_all, gather_s, gather_r)
    sums = PlaneSums(
        from_core,
        from_core,
        from_side,
        from_line,
        (core_s, core_r, side_s, side_r, line_s, line_r),
        LEVELS,
    )

    loads[0].wait()

    @pl.loop(0, half_rows // step)
    def _(i):
        at = pl.ds(pl.multiple_of(i * step, step), step)
        tmp[0, 0, at, :] = middle_grad[at, :].astype(bf16)

    meet = remote(tmp.at[0, 0], tmp.at[0, 1], pair_s.at[0], pair_r.at[0], partner)
    meet.start()
    loads[1].wait()
    loads[2].wait()
    meet.wait_recv()
    gain = second_gain[...]

    @pl.loop(0, half_rows // step)
    def _(i):
        at = pl.ds(pl.multiple_of(i * step, step), step)
        value = wide[at, :] + (middle[at, :] + tmp[0, 1, at, :].astype(f32))
        scale = lax.rsqrt(jnp.mean(value * value, axis=1, keepdims=True) + epsilon)
        middle[at, :] = value
        second_scale[at, :] = scale
        rows_all[me, at, :] = (value * scale * gain).astype(bf16)

    gather.start()
    again = pltpu.make_async_copy(upstream, wide, load_sems.at[2])
    again.start()
    for load in loads[3:]:
        load.wait()

    def forward_pair(b):
        turn = (0b11_10_11_01_10_00_01_00 >> (2 * b)) % 4
        side = (0b11_01_01_00 >> b) % 2
        return level_at(3 - turn, z) * 2 + (y + side) % 2

    @pl.loop(0, 2 * pairs)
    def _(turn):
        b, h = turn // 2, turn % 2

        def at(k, work, where=None):
            @pl.when(turn == k)
            def _():
                if where is None:
                    work()
                else:
                    pl.when(where == 1)(work)

        at(0, lambda: gather.from_core(0, 0))
        at(2, lambda: gather.from_line(1))
        at(2, lambda: gather.from_line(2), interior)
        at(2, lambda: gather.from_core(1, 0))
        at(4, lambda: gather.from_side(0))
        at(4, lambda: gather.from_core(0, 1))
        at(6, lambda: gather.from_line(2), 1 - interior)
        at(6, lambda: gather.from_line(3), interior)
        at(6, lambda: gather.from_core(2, 0))
        at(8, lambda: gather.from_side(1))
        at(8, lambda: gather.from_core(1, 1))
        at(10, lambda: gather.from_line(3), 1 - interior)
        at(10, lambda: gather.from_core(3, 0))
        at(12, lambda: gather.from_side(2))
        at(12, lambda: gather.from_core(2, 1))
        at(14, lambda: gather.from_side(3))
        at(14, lambda: gather.from_core(3, 1))

        pair = forward_pair(b)
        xs = pair_block(rows_all, pair)
        us = pair_block(u_all, pair)
        lane = lax.broadcasted_iota(jnp.int32, (pair_rows_, ROUTE_COLS), 1)
        table = gates[pl.ds(2 * pair, 2)].reshape(pair_rows_, ROUTE_COLS)
        gate_rows = jnp.sum(jnp.where(lane == me, table, 0.0), axis=1, keepdims=True)
        gate_act = nn(xs, wg[h])
        up_act = nn(xs, wu[h])
        hidden_cot = nt(us, wd[h])
        sig = lax.logistic(gate_act)
        act = gate_act * sig
        hid = act * up_act
        at_rows = pl.ds(pl.multiple_of(pair * pair_rows_, pair_rows_), pair_rows_)
        hidden[h, at_rows, :] = (hid * gate_rows).astype(bf16)
        route = jnp.sum(hid * hidden_cot, axis=1, keepdims=True)
        scaled = hidden_cot * gate_rows
        gcot[h, at_rows, :] = (scaled * up_act * (sig * (1.0 + gate_act * (1.0 - sig)))).astype(bf16)
        ucot[h, at_rows, :] = (scaled * act).astype(bf16)

        @pl.when(h == 0)
        def _():
            route_half[...] = route

        @pl.when(h == 1)
        def _():
            total = route_half[...] + route
            placed = jnp.where(lane == me, total, 0.0).astype(bf16)
            rext[pl.ds(2 * pair, 2)] = placed.reshape(2, half_rows, ROUTE_COLS)

    def down_panel(h, p):
        units_at = pl.ds(pl.multiple_of(p * block, block), block)
        us = u_all[...]
        us = us.reshape(us.shape[0] * us.shape[1], width)
        return tn(hidden[h, :, units_at], us).astype(bf16)

    def down_send(p, k):
        rows = pl.ds(pl.multiple_of(p * block, block), block)
        return remote(
            gstage.at[p, k // 2, k % 2],
            down_landed.at[rows, pl.ds(k * units, units)],
            pair_s.at[2 + 4 * p + k],
            pair_r.at[2 + 4 * p + k],
            partner,
        )

    def down_keep(p):
        rows = pl.ds(pl.multiple_of(2 * p, 2), 2)
        return pltpu.make_async_copy(tmp.at[p], down_mine.at[rows], out_sems.at[p])

    @pl.loop(0, units // block)
    def _(p):
        part = down_panel(1 - x, p)
        for k in range(width // units):
            gstage[p, k // 2, k % 2] = part[:, k * units : (k + 1) * units]
            down_send(p, k).start()

    meet.wait_send()

    @pl.loop(0, units // block)
    def _(p):
        tmp[p] = down_panel(x, p).reshape(2, half_rows, width)
        down_keep(p).start()

    for p in range(units // block):
        down_keep(p).wait()

    def core_send(b):
        return remote(
            tmp.at[b % 2, 1 - c],
            from_core.at[b],
            core_s.at[b],
            core_r.at[b],
            (index_of(z, y, 1 - c), x),
        )

    def take_core(b):
        core_send(b).wait_recv()
        add_block(tmp.at[b % 2, c], from_core.at[b], from_core.at[b])

        @pl.when(b < LEVELS)
        def _():
            remote(
                from_core.at[b],
                from_side.at[b],
                side_s.at[b],
                side_r.at[b],
                (index_of(z, 1 - y, c), x),
            ).start()

    def line_step(turn):
        sums.side_arrived(turn)
        mine = from_core.at[LEVELS + turn]
        add_block(mine, from_side.at[turn], mine)
        if turn < LEVELS - 1:
            sums.to_line(turn)

    def last_step():
        line_step(LEVELS - 1)
        total_block(sums, middle_grad)
        again.wait()
        second_term[...] = jnp.zeros_like(second_term)

        @pl.loop(0, half_rows // step)
        def _(i):
            at = pl.ds(pl.multiple_of(i * step, step), step)
            cot, mid, scale = middle_grad[at, :], middle[at, :], second_scale[at, :]
            weighted = cot * gain
            mean = jnp.mean(weighted * mid, axis=1, keepdims=True)
            value = wide[at, :] + scale * (weighted - mid * (scale * scale * mean))
            middle_grad[at, :] = value
            tmp[0, 0, at, :] = value.astype(bf16)
            second_term[...] = second_term[...] + jnp.sum(cot * mid * scale, axis=0, keepdims=True)

        pair_send().start()
        pair_keep().start()

    def pair_send():
        return remote(tmp.at[0, 0], middle_pair.at[x], pair_s.at[1], pair_r.at[1], partner)

    def pair_keep():
        return pltpu.make_async_copy(tmp.at[0, 0], middle_pair.at[x], load_sems.at[0])

    @pl.loop(0, pairs)
    def _(b):
        pl.when((b == pairs - 1) & (interior == 0))(lambda: line_step(0))
        pl.when(b >= 2)(lambda: core_send(b - 2).wait_send())
        pair = level_at(b % LEVELS, z) * 2 + (y + 1 - b // LEVELS) % 2
        at_rows = pl.ds(pl.multiple_of(pair * pair_rows_, pair_rows_), pair_rows_)

        @pl.loop(0, width // panel)
        def _(n):
            cols = pl.ds(pl.multiple_of(n * panel, panel), panel)
            acc = nt(gcot[0, at_rows, :], wg[0, cols, :])
            acc = acc + nt(ucot[0, at_rows, :], wu[0, cols, :])
            for h in range(1, halves):
                acc = acc + nt(gcot[h, at_rows, :], wg[h, cols, :])
                acc = acc + nt(ucot[h, at_rows, :], wu[h, cols, :])
            tmp[b % 2, :, :, cols] = acc.astype(bf16).reshape(2, half_rows, panel)

        core_send(b).start()
        pl.when(b >= 1)(lambda: take_core(b - 1))

    take_core(pairs - 1)
    for b in (pairs - 2, pairs - 1):
        core_send(b).wait_send()

    def mixture_out(b):
        return pltpu.make_async_copy(
            u_all.at[pl.ds(2 * b, 2)],
            mixture_hbm.at[pl.ds(2 * b, 2), :, pl.ds(0, width)],
            out_sems.at[b],
        )

    route_out = pltpu.make_async_copy(
        rext, mixture_hbm.at[:, :, pl.ds(width, ROUTE_COLS)], load_sems.at[1]
    )
    route_out.start()

    @pl.loop(0, pairs)
    def _(b):
        pl.when((b == 3) & (interior == 0))(lambda: line_step(1))
        pl.when((b == 5) & (interior == 1))(lambda: line_step(0))
        at_rows = pl.ds(pl.multiple_of(b * pair_rows_, pair_rows_), pair_rows_)

        @pl.loop(0, width // panel)
        def _(n):
            cols = pl.ds(pl.multiple_of(n * panel, panel), panel)
            acc = nn(hidden[0, at_rows, :], wd[0, :, cols])
            for h in range(1, halves):
                acc = acc + nn(hidden[h, at_rows, :], wd[h, :, cols])
            u_all[pl.ds(2 * b, 2), :, cols] = acc.astype(bf16).reshape(2, half_rows, panel)

        mixture_out(b).start()

    for b in range(pairs):
        mixture_out(b).wait()
    route_out.wait()
    for p in range(units // block):
        for k in range(width // units):
            down_send(p, k).wait()

    def part_outs(p):
        rows = pl.ds(pl.multiple_of(p * block, block), block)
        return [
            pltpu.make_async_copy(
                gstage.at[p % 2, which, k], ref.at[rows, :], out_sems.at[(p % 2) * 4 + 2 * which + k]
            )
            for which, refs in enumerate(((gate_mine, gate_theirs), (up_mine, up_theirs)))
            for k, ref in enumerate(refs)
        ]

    def wait_outs(p):
        for copy in part_outs(p):
            copy.wait()

    @pl.loop(0, width // block)
    def _(p):
        pl.when((p == 1) & (interior == 0))(lambda: line_step(2))
        pl.when((p == 2) & (interior == 1))(lambda: line_step(1))
        pl.when((p == 3) & (interior == 1))(lambda: line_step(2))
        pl.when(p == 6)(last_step)
        pl.when(p >= 2)(lambda: wait_outs(p - 2))
        cols = pl.ds(pl.multiple_of(p * block, block), block)
        xp = rows_all[:, :, cols]
        xp = xp.reshape(xp.shape[0] * xp.shape[1], block)
        for which, ref in enumerate((gcot, ucot)):
            for k, h in enumerate((x, 1 - x)):
                gstage[p % 2, which, k] = tn(xp, ref[h]).astype(bf16)
        for copy in part_outs(p):
            copy.start()

    for p in (width // block - 2, width // block - 1):
        wait_outs(p)
    pair_send().wait()
    pair_keep().wait()
    gather.finish()
    for turn in range(LEVELS):
        remote(
            from_core.at[turn], from_side.at[turn], side_s.at[turn], side_r.at[turn], partner
        ).wait_send()
    for turn in range(LEVELS - 1):
        remote(
            from_core.at[turn], from_line.at[turn], line_s.at[turn], line_r.at[turn], partner
        ).wait_send()


def run_experts(
    gates, second_gain, out_part, block_input, upstream, upstream_all, own, other, collective_id
):
    bf16, f32 = jnp.bfloat16, jnp.float32
    block = block_input.shape
    half_rows, width = block
    owner_count = upstream_all.shape[0]
    units = own[0].shape[1]
    halves = lax.axis_size("tp")
    all_rows = owner_count * half_rows
    hbm = pl.BlockSpec(memory_space=pl.ANY)
    vmem = pl.BlockSpec(memory_space=pltpu.VMEM)
    dma = pltpu.SemaphoreType.DMA
    flops = 2 * 9 * all_rows * width * units * halves
    shape = jax.ShapeDtypeStruct
    return pl.pallas_call(
        experts_kernel,
        out_shape=[
            shape(block, f32),
            shape(block, f32),
            shape((1, width), f32),
            shape((2,) + block, bf16),
            shape((owner_count, half_rows, width + ROUTE_COLS), bf16),
        ]
        + [shape((width, units), bf16)] * 4
        + [shape((units // half_rows,) + block, bf16), shape((units, width), bf16)],
        in_specs=[vmem, vmem] + [hbm] * 10,
        out_specs=[vmem] * 3 + [hbm] * 8,
        scratch_shapes=[
            pltpu.VMEM((owner_count,) + block, bf16),
            pltpu.VMEM((owner_count,) + block, bf16),
            pltpu.VMEM((halves, width, units), bf16),
            pltpu.VMEM((halves, width, units), bf16),
            pltpu.VMEM((halves, units, width), bf16),
            pltpu.VMEM((halves, all_rows, units), bf16),
            pltpu.VMEM((halves, all_rows, units), bf16),
            pltpu.VMEM((halves, all_rows, units), bf16),
            pltpu.VMEM((owner_count, half_rows, ROUTE_COLS), bf16),
            pltpu.VMEM((2, 2) + block, bf16),
            pltpu.VMEM((2 * LEVELS,) + block, bf16),
            pltpu.VMEM((LEVELS,) + block, bf16),
            pltpu.VMEM((LEVELS + 1,) + block, bf16),
            pltpu.VMEM((2, 2, halves, 256, units), bf16),
            pltpu.VMEM(block, f32),
            pltpu.VMEM((half_rows, 1), f32),
            pltpu.VMEM((2 * half_rows, 1), f32),
            dma((GATHER_SENDS,)),
            dma((owner_count,)),
            dma((2 * LEVELS,)),
            dma((2 * LEVELS,)),
            dma((LEVELS,)),
            dma((LEVELS,)),
            dma((LEVELS + 1,)),
            dma((LEVELS + 1,)),
            dma((10,)),
            dma((8,)),
            dma((10,)),
            dma((10,)),
        ],
        compiler_params=pltpu.CompilerParams(
            collective_id=collective_id, has_side_effects=True, vmem_limit_bytes=67_043_328
        ),
        cost_estimate=pl.CostEstimate(
            flops=flops, bytes_accessed=64 * 2**20, transcendentals=all_rows * units * halves
        ),
        name="experts",
    )(gates, second_gain, out_part, block_input, upstream, upstream_all, *own, *other)


def gate_columns(route_rows, gate_rows, expert_count):
    names = jnp.arange(expert_count, dtype=jnp.int32)[None, None, :]
    return jnp.sum(jnp.where(route_rows[:, :, None] == names, gate_rows[:, :, None], 0.0), axis=1)


def half_of(rows):
    count = rows.shape[0] // lax.axis_size("tp")
    return lax.dynamic_slice_in_dim(rows, lax.axis_index("tp") * count, count, axis=0)


def per_device_dense(
    block_input,
    upstream_grad,
    first_gain,
    second_gain,
    query_weight,
    key_weight,
    value_weight,
    output_weight,
    gate_weight,
    up_weight,
    down_weight,
    routes,
    gate_values,
):
    pair_count = lax.axis_size("tp")
    owner_count = lax.axis_size("fsdp")
    local_rows = block_input.shape[0]
    seq_rows = local_rows * pair_count
    model_width = block_input.shape[1]
    head_cols = query_weight.shape[1]
    local_heads = head_cols // HD
    expert_count = EXP_DEV * owner_count
    inv_root = HD ** (-0.5)
    bf16, f32 = jnp.bfloat16, jnp.float32

    my_routes, my_gates = half_of(routes), half_of(gate_values)
    gate_table = gate_columns(my_routes, my_gates, ROUTE_COLS)
    expert_names = jnp.arange(expert_count, dtype=jnp.int32)[None, :]
    own_weights = (gate_weight[0], up_weight[0], down_weight[0])

    first_scale = lax.rsqrt(jnp.mean(block_input * block_input, axis=1, keepdims=True) + epsilon)
    first_normed = (block_input * first_scale * first_gain).astype(bf16)
    gathered, normed_pair, other_weights = gather_weights(
        [
            query_weight,
            key_weight,
            value_weight,
            output_weight,
            upstream_grad.astype(bf16),
            gate_table,
        ],
        first_normed,
        own_weights,
        1,
    )
    query_full, key_full, value_full, output_full = (w.reshape(-1, head_cols) for w in gathered[:4])
    upstream_all, gates_all = gathered[4:]
    normed_rows = normed_pair.reshape(seq_rows, model_width)

    def heads_of(weight_full):
        return (
            jnp.dot(normed_rows, weight_full, preferred_element_type=f32)
            .astype(bf16)
            .reshape(seq_rows, local_heads, HD)
        )

    query_rows, key_rows, value_rows = heads_of(query_full), heads_of(key_full), heads_of(value_full)
    scores = jnp.einsum("shd,thd->hst", query_rows, key_rows, preferred_element_type=f32) * inv_root
    row_top = jnp.max(scores, axis=2, keepdims=True)
    log_total = row_top + jnp.log(jnp.sum(jnp.exp(scores - row_top), axis=2, keepdims=True))
    soft_weights = jnp.exp(scores - log_total)
    soft_rounded = soft_weights.astype(bf16)
    mixed_rows = jnp.einsum("hst,thd->shd", soft_rounded, value_rows, preferred_element_type=f32)
    mixed_rows = mixed_rows.astype(bf16).reshape(seq_rows, head_cols)
    out_part = contract_cols(mixed_rows, output_full).reshape(pair_count, local_rows, model_width)
    (
        middle,
        middle_grad,
        second_term,
        middle_pair,
        mixture_part,
        gate_mine,
        gate_theirs,
        up_mine,
        up_theirs,
        down_mine,
        down_landed,
    ) = run_experts(
        gates_all,
        second_gain[None],
        out_part,
        block_input,
        upstream_grad,
        upstream_all,
        own_weights,
        other_weights,
        2,
    )
    middle_rows = middle_pair.reshape(seq_rows, model_width)
    out_term = contract_rows(middle_rows, mixed_rows)
    mixed_cot = (
        jnp.dot(middle_rows, output_full, preferred_element_type=f32)
        .astype(bf16)
        .reshape(seq_rows, local_heads, HD)
    )
    value_cot = jnp.einsum("hst,shd->thd", soft_rounded, mixed_cot, preferred_element_type=f32)
    value_cot = value_cot.astype(bf16).reshape(seq_rows, head_cols)
    soft_cot = jnp.einsum("shd,thd->hst", mixed_cot, value_rows, preferred_element_type=f32)
    score_cot = (
        soft_weights
        * (soft_cot - jnp.sum(soft_weights * soft_cot, axis=2, keepdims=True))
        * inv_root
    ).astype(bf16)
    query_cot = (
        jnp.einsum("hst,thd->shd", score_cot, key_rows, preferred_element_type=f32)
        .astype(bf16)
        .reshape(seq_rows, head_cols)
    )
    key_cot = (
        jnp.einsum("hst,shd->thd", score_cot, query_rows, preferred_element_type=f32)
        .astype(bf16)
        .reshape(seq_rows, head_cols)
    )
    first_terms = (
        contract_cols(query_cot, query_full)
        + contract_cols(key_cot, key_full)
        + contract_cols(value_cot, value_full)
    )
    sums, landed, input_grad, gain_grads = sum_gradients(
        [
            term.astype(bf16).reshape((owner_count,) + query_weight.shape)
            for term in (
                contract_rows(normed_rows, query_cot),
                contract_rows(normed_rows, key_cot),
                contract_rows(normed_rows, value_cot),
                out_term,
            )
        ]
        + [mixture_part],
        (gate_theirs, up_theirs),
        first_terms.astype(bf16).reshape(pair_count, local_rows, model_width),
        (block_input, first_scale, first_gain[None], middle_grad, second_term),
        4,
    )
    query_grad, key_grad, value_grad, output_grad, mixture = sums
    gate_grad, up_grad, down_grad = (
        mine.astype(f32) + theirs.astype(f32)
        for mine, theirs in (
            (gate_mine, landed[0]),
            (up_mine, landed[1]),
            (down_mine.reshape(down_landed.shape), down_landed),
        )
    )
    block_output = middle + mixture[:, :model_width]
    route_back = mixture[:, model_width : model_width + expert_count]
    route_grad = jnp.sum(
        jnp.where(my_routes[:, :, None] == expert_names[None], route_back[:, None, :], 0.0), axis=2
    )
    return (
        block_output,
        input_grad,
        gain_grads[0],
        gain_grads[1],
        query_grad,
        key_grad,
        value_grad,
        output_grad,
        gate_grad[None],
        up_grad[None],
        down_grad[None],
        route_grad,
    )


def solution(mesh):
    dense = 2 * TOP >= EXP_DEV * mesh.shape["fsdp"] and mesh.shape["fsdp"] == 4 * LEVELS
    per_device = per_device_dense if dense else per_device_slots
    in_specs = (
        P(("fsdp", "tp"), None),
        P(("fsdp", "tp"), None),
        P(),
        P(),
        P("fsdp", "tp"),
        P("fsdp", "tp"),
        P("fsdp", "tp"),
        P("fsdp", "tp"),
        P("fsdp", None, "tp"),
        P("fsdp", None, "tp"),
        P("fsdp", "tp", None),
        P("fsdp", None),
        P("fsdp", None),
    )
    out_specs = (
        P(("fsdp", "tp"), None),
        P(("fsdp", "tp"), None),
        P(),
        P(),
        P("fsdp", "tp"),
        P("fsdp", "tp"),
        P("fsdp", "tp"),
        P("fsdp", "tp"),
        P("fsdp", None, "tp"),
        P("fsdp", None, "tp"),
        P("fsdp", "tp", None),
        P(("fsdp", "tp"), None),
    )
    return jax.shard_map(
        per_device, mesh=mesh, in_specs=in_specs, out_specs=out_specs, check_vma=False
    )
```

```python
import functools

import jax
import jax.numpy as jnp
from jax import lax
from jax.experimental import pallas as pl
from jax.experimental.pallas import tpu as pltpu
from jax.sharding import PartitionSpec as P

HD = 128
TOP = 8
EXP_DEV = 1


epsilon = 1e-05


def route_slots(route_rows, expert_count, capacity):
    flat_routes = route_rows.reshape(-1)
    onehot = (flat_routes[:, None] == jnp.arange(expert_count, dtype=jnp.int32)[None, :]).astype(
        jnp.int32
    )
    earlier = jnp.cumsum(onehot, axis=0, dtype=jnp.int32) - onehot
    ranked = jnp.sum(earlier * onehot, axis=1, dtype=jnp.int32)
    return flat_routes * capacity + ranked


def pair_rows(row_block):
    return lax.all_gather(row_block, "tp", axis=0, tiled=True)


def pair_sums(term_block):
    return lax.psum_scatter(term_block, "tp", scatter_dimension=0, tiled=True)


def to_owners(buffer):
    return lax.all_to_all(buffer, "fsdp", split_axis=0, concat_axis=0, tiled=True)


def to_sources(buffer):
    return lax.all_to_all(buffer, "fsdp", split_axis=0, concat_axis=0, tiled=True)


def projections(query_weight, key_weight, value_weight, output_weight):
    return (
        lax.all_gather(query_weight, "fsdp", axis=0, tiled=True),
        lax.all_gather(key_weight, "fsdp", axis=0, tiled=True),
        lax.all_gather(value_weight, "fsdp", axis=0, tiled=True),
        lax.all_gather(output_weight, "fsdp", axis=0, tiled=True),
    )


def scatter_rows(row_block, slot_index, total_rows):
    return (
        jnp.zeros((total_rows, row_block.shape[1]), row_block.dtype).at[slot_index].set(row_block)
    )


def spread_rows(row_block, copies):
    return jnp.broadcast_to(
        row_block[:, None, :], (row_block.shape[0], copies, row_block.shape[1])
    ).reshape(-1, row_block.shape[1])


def contract_rows(left_block, right_block):
    return lax.dot_general(
        left_block, right_block, (((0,), (0,)), ((), ())), preferred_element_type=jnp.float32
    )


def contract_cols(left_block, right_block):
    return lax.dot_general(
        left_block, right_block, (((1,), (1,)), ((), ())), preferred_element_type=jnp.float32
    )


def send_out(full_buffer):
    return to_owners(full_buffer)


def send_back(group_parts):
    owner_count, local_experts, capacity, model_width = group_parts.shape
    return to_sources(group_parts).reshape(owner_count * local_experts * capacity, model_width)


def per_device_slots(
    block_input,
    upstream_grad,
    first_gain,
    second_gain,
    query_weight,
    key_weight,
    value_weight,
    output_weight,
    gate_weight,
    up_weight,
    down_weight,
    routes,
    gate_values,
):
    pair_count = lax.axis_size("tp")
    owner_count = lax.axis_size("fsdp")
    local_rows = block_input.shape[0]
    seq_rows = local_rows * pair_count
    model_width = block_input.shape[1]
    head_cols = query_weight.shape[1]
    local_heads = head_cols // HD
    expert_count = EXP_DEV * owner_count
    capacity = 3 * seq_rows * TOP // (2 * expert_count)
    inv_root = HD ** (-0.5)
    first_scale = lax.rsqrt(jnp.mean(block_input * block_input, axis=1, keepdims=True) + epsilon)
    first_normed = (block_input * first_scale * first_gain).astype(jnp.bfloat16)
    normed_rows = pair_rows(first_normed)
    query_full, key_full, value_full, output_full = projections(
        query_weight, key_weight, value_weight, output_weight
    )
    query_rows = (
        jnp.dot(normed_rows, query_full, preferred_element_type=jnp.float32)
        .astype(jnp.bfloat16)
        .reshape(seq_rows, local_heads, HD)
    )
    key_rows = (
        jnp.dot(normed_rows, key_full, preferred_element_type=jnp.float32)
        .astype(jnp.bfloat16)
        .reshape(seq_rows, local_heads, HD)
    )
    value_rows = (
        jnp.dot(normed_rows, value_full, preferred_element_type=jnp.float32)
        .astype(jnp.bfloat16)
        .reshape(seq_rows, local_heads, HD)
    )
    scores = (
        jnp.einsum("shd,thd->hst", query_rows, key_rows, preferred_element_type=jnp.float32)
        * inv_root
    )
    row_top = jnp.max(scores, axis=2, keepdims=True)
    log_total = row_top + jnp.log(jnp.sum(jnp.exp(scores - row_top), axis=2, keepdims=True))
    soft_weights = jnp.exp(scores - log_total)
    mixed_rows = jnp.einsum(
        "hst,thd->shd",
        soft_weights.astype(jnp.bfloat16),
        value_rows,
        preferred_element_type=jnp.float32,
    )
    mixed_rows = mixed_rows.astype(jnp.bfloat16).reshape(seq_rows, head_cols)
    middle = block_input + pair_sums(contract_cols(mixed_rows, output_full))
    second_scale = lax.rsqrt(jnp.mean(middle * middle, axis=1, keepdims=True) + epsilon)
    second_normed = (middle * second_scale * second_gain).astype(jnp.bfloat16)
    moe_rows = pair_rows(second_normed)
    slot_index = route_slots(routes, expert_count, capacity)
    send_rows = scatter_rows(spread_rows(moe_rows, TOP), slot_index, expert_count * capacity)
    arrived = send_out(send_rows.reshape(owner_count, EXP_DEV, capacity, model_width))
    gate_act = jnp.einsum(
        "secd,edf->secf", arrived, gate_weight, preferred_element_type=jnp.float32
    )
    up_act = jnp.einsum("secd,edf->secf", arrived, up_weight, preferred_element_type=jnp.float32)
    sigmoid_gate = jax.nn.sigmoid(gate_act)
    hidden = (gate_act * sigmoid_gate * up_act).astype(jnp.bfloat16)
    expert_out = jnp.einsum(
        "secf,efd->secd", hidden, down_weight, preferred_element_type=jnp.float32
    ).astype(jnp.bfloat16)
    returned = send_back(expert_out)
    picked = returned[slot_index].reshape(seq_rows, TOP, model_width).astype(jnp.float32)
    mixture = jnp.sum(gate_values[:, :, None] * picked, axis=1)
    block_output = middle + pair_sums(mixture)
    upstream_rows = lax.all_gather(upstream_grad, "tp", axis=0, tiled=True)
    route_terms = jnp.sum(upstream_rows[:, None, :] * picked, axis=2)
    routed_cot = (
        (gate_values[:, :, None] * upstream_rows[:, None, :])
        .astype(jnp.bfloat16)
        .reshape(seq_rows * TOP, model_width)
    )
    cot_send = scatter_rows(routed_cot, slot_index, expert_count * capacity)
    cot_arrived = send_out(cot_send.reshape(owner_count, EXP_DEV, capacity, model_width))
    hidden_cot = jnp.einsum(
        "secd,efd->secf", cot_arrived, down_weight, preferred_element_type=jnp.float32
    )
    down_grad = jnp.einsum(
        "secf,secd->efd", hidden, cot_arrived, preferred_element_type=jnp.float32
    )
    gate_cot = (
        hidden_cot * up_act * sigmoid_gate * (1.0 + gate_act * (1.0 - sigmoid_gate))
    ).astype(jnp.bfloat16)
    up_cot = (hidden_cot * gate_act * sigmoid_gate).astype(jnp.bfloat16)
    gate_grad = jnp.einsum("secd,secf->edf", arrived, gate_cot, preferred_element_type=jnp.float32)
    up_grad = jnp.einsum("secd,secf->edf", arrived, up_cot, preferred_element_type=jnp.float32)
    input_cot = jnp.einsum(
        "secf,edf->secd", gate_cot, gate_weight, preferred_element_type=jnp.float32
    )
    input_cot = (
        input_cot
        + jnp.einsum("secf,edf->secd", up_cot, up_weight, preferred_element_type=jnp.float32)
    ).astype(jnp.bfloat16)
    came_back = send_back(input_cot)
    normed_cot = jnp.sum(
        came_back[slot_index].reshape(seq_rows, TOP, model_width).astype(jnp.float32), axis=1
    )
    second_cot, route_grad = (
        lax.psum_scatter(
            normed_cot.astype(jnp.bfloat16), "tp", scatter_dimension=0, tiled=True
        ).astype(jnp.float32),
        lax.psum_scatter(
            route_terms.astype(jnp.bfloat16), "tp", scatter_dimension=0, tiled=True
        ).astype(jnp.float32),
    )
    weighted_two = second_cot * second_gain
    second_term = jnp.sum(second_cot * middle * second_scale, axis=0)
    middle_grad = upstream_grad + second_scale * (
        weighted_two
        - middle
        * second_scale
        * second_scale
        * jnp.mean(weighted_two * middle, axis=1, keepdims=True)
    )
    middle_rows = pair_rows(middle_grad.astype(jnp.bfloat16))
    query_full, key_full, value_full, output_full = projections(
        query_weight, key_weight, value_weight, output_weight
    )
    out_term = contract_rows(middle_rows, mixed_rows)
    mixed_cot = (
        jnp.dot(middle_rows, output_full, preferred_element_type=jnp.float32)
        .astype(jnp.bfloat16)
        .reshape(seq_rows, local_heads, HD)
    )
    scores = (
        jnp.einsum("shd,thd->hst", query_rows, key_rows, preferred_element_type=jnp.float32)
        * inv_root
    )
    soft_weights = jnp.exp(scores - log_total)
    value_cot = jnp.einsum(
        "hst,shd->thd",
        soft_weights.astype(jnp.bfloat16),
        mixed_cot,
        preferred_element_type=jnp.float32,
    )
    value_cot = value_cot.astype(jnp.bfloat16).reshape(seq_rows, head_cols)
    soft_cot = jnp.einsum("shd,thd->hst", mixed_cot, value_rows, preferred_element_type=jnp.float32)
    score_cot = (
        soft_weights
        * (soft_cot - jnp.sum(soft_weights * soft_cot, axis=2, keepdims=True))
        * inv_root
    ).astype(jnp.bfloat16)
    query_cot = (
        jnp.einsum("hst,thd->shd", score_cot, key_rows, preferred_element_type=jnp.float32)
        .astype(jnp.bfloat16)
        .reshape(seq_rows, head_cols)
    )
    key_cot = (
        jnp.einsum("hst,shd->thd", score_cot, query_rows, preferred_element_type=jnp.float32)
        .astype(jnp.bfloat16)
        .reshape(seq_rows, head_cols)
    )
    query_term = contract_rows(normed_rows, query_cot)
    key_term = contract_rows(normed_rows, key_cot)
    value_term = contract_rows(normed_rows, value_cot)
    first_terms = (
        contract_cols(query_cot, query_full)
        + contract_cols(key_cot, key_full)
        + contract_cols(value_cot, value_full)
    )
    first_cot = pair_sums(first_terms)
    weighted_one = first_cot * first_gain
    first_term = jnp.sum(first_cot * block_input * first_scale, axis=0)
    input_grad = middle_grad + first_scale * (
        weighted_one
        - block_input
        * first_scale
        * first_scale
        * jnp.mean(weighted_one * block_input, axis=1, keepdims=True)
    )
    query_grad, key_grad, value_grad, output_grad = (
        lax.psum_scatter(query_term, "fsdp", scatter_dimension=0, tiled=True),
        lax.psum_scatter(key_term, "fsdp", scatter_dimension=0, tiled=True),
        lax.psum_scatter(value_term, "fsdp", scatter_dimension=0, tiled=True),
        lax.psum_scatter(out_term, "fsdp", scatter_dimension=0, tiled=True),
    )
    first_gain_grad, second_gain_grad = lax.psum((first_term, second_term), ("fsdp", "tp"))
    return (
        block_output,
        input_grad,
        first_gain_grad,
        second_gain_grad,
        query_grad,
        key_grad,
        value_grad,
        output_grad,
        gate_grad,
        up_grad,
        down_grad,
        route_grad,
    )


MESH = pl.DeviceIdType.MESH


def place():
    here = lax.axis_index("fsdp")
    return here // 4, (here // 2) % 2, here % 2, lax.axis_index("tp")


def index_of(z, y, c):
    return (z * 2 + y) * 2 + c


LEVELS = 4
LEVEL_ORDER = sum(
    level << (8 * turn + 2 * z)
    for turn, row in enumerate(((3, 3, 0, 0), (2, 2, 1, 1), (1, 0, 3, 2), (0, 1, 2, 3)))
    for z, level in enumerate(row)
) - (1 << 32)


def level_at(turn, z):
    return (jnp.int32(LEVEL_ORDER) >> (8 * turn + 2 * z)) & 3


def line_ends(z):
    return (z + 1) // LEVELS, (LEVELS - z) // LEVELS


def plane_greet(pair=False, far=False):
    z, y, c, x = place()
    top, bottom = line_ends(z)
    barrier = pltpu.get_barrier_semaphore()
    partners = [(index_of(z, 1 - y, c), x), (index_of(z, y, 1 - c), x)]
    if pair:
        partners.append((index_of(z, y, c), 1 - x))
    if far:
        partners.append((index_of((z + 2) % LEVELS, y, c), x))
    for partner in partners:
        pl.semaphore_signal(barrier, inc=1, device_id=partner, device_id_type=MESH)

    @pl.when(top == 0)
    def _():
        above = (index_of(z + 1, y, c), x)
        pl.semaphore_signal(barrier, inc=1, device_id=above, device_id_type=MESH)

    @pl.when(bottom == 0)
    def _():
        below = (index_of(z - 1, y, c), x)
        pl.semaphore_signal(barrier, inc=1, device_id=below, device_id_type=MESH)

    pl.semaphore_wait(barrier, len(partners) + 2 - top - bottom)


def remote(src, dst, send_sem, recv_sem, target):
    return pltpu.make_async_remote_copy(
        src_ref=src,
        dst_ref=dst,
        send_sem=send_sem,
        recv_sem=recv_sem,
        device_id=target,
        device_id_type=MESH,
    )


class PlaneGather:
    def __init__(self, mine, full, send_sems, recv_sems):
        self.mine, self.full = mine, full
        self.send_sems, self.recv_sems = send_sems, recv_sems
        self.z, self.y, self.c, self.x = place()
        self.top, self.bottom = line_ends(self.z)

    def _copy(self, number, src, slot, target):
        return remote(
            src, self.full.at[slot], self.send_sems.at[number], self.recv_sems.at[slot], target
        )

    def arrived(self, slot):
        here = self.full.at[slot]
        remote(here, here, self.send_sems.at[0], self.recv_sems.at[slot], (0, self.x)).wait_recv()

    def start(self):
        z, y, c, x = self.z, self.y, self.c, self.x
        own = index_of(z, y, c)
        up = self._copy(0, self.mine, own, (index_of(z + 1, y, c), x))
        down = self._copy(1, self.mine, own, (index_of(z - 1, y, c), x))
        pl.when(self.top == 0)(up.start)
        pl.when(self.bottom == 0)(down.start)
        self._copy(2, self.mine, own, (index_of(z, 1 - y, c), x)).start()
        self._copy(3, self.mine, own, (index_of(z, y, 1 - c), x)).start()

    def from_line(self, step):
        z, y, c, x = self.z, self.y, self.c, self.x
        level = level_at(3 - step, z)
        slot = index_of(level, y, c)
        self.arrived(slot)
        onward = z + 1 - 2 * ((level + LEVELS - z) // LEVELS)
        src, number = self.full.at[slot], 4 + 3 * (step - 1)
        forward = self._copy(number, src, slot, (index_of(onward, y, c), x))
        pl.when(self.top + self.bottom == 0)(forward.start)
        self._copy(number + 1, src, slot, (index_of(z, 1 - y, c), x)).start()
        self._copy(number + 2, src, slot, (index_of(z, y, 1 - c), x)).start()

    def from_side(self, step):
        z, y, c, x = self.z, self.y, self.c, self.x
        slot = index_of(level_at(3 - step, z), 1 - y, c)
        self.arrived(slot)
        self._copy(13 + step, self.full.at[slot], slot, (index_of(z, y, 1 - c), x)).start()

    def from_core(self, step, side):
        z, y, c = self.z, self.y, self.c
        self.arrived(index_of(level_at(3 - step, z), (y + side) % 2, 1 - c))

    def finish(self):
        for number in range(GATHER_SENDS):
            wait = self._copy(number, self.mine, 0, (0, self.x)).wait_send
            if number == 0:
                pl.when(self.top == 0)(wait)
            elif number == 1:
                pl.when(self.bottom == 0)(wait)
            elif number in (4, 7, 10):
                pl.when(self.top + self.bottom == 0)(wait)
            else:
                wait()


GATHER_SENDS = 17


def weights_kernel(count, *refs):
    mine, normed, experts = refs[:count], refs[count], refs[count + 1 : count + 4]
    outs = refs[count + 4 : 2 * count + 8]
    full, normed_pair, others = outs[:count], outs[count], outs[count + 1 :]
    send_sems, recv_sems, own_sems, pair_s, pair_r = refs[2 * count + 8 :]
    z, y, c, x = place()
    own = index_of(z, y, c)
    plane_greet(pair=True)
    plans = [
        PlaneGather(mine[a], full[a], send_sems.at[a], recv_sems.at[a]) for a in range(count)
    ]
    swaps = [
        remote(src, dst, pair_s.at[i], pair_r.at[i], (own, 1 - x))
        for i, (src, dst) in enumerate(
            [(normed, normed_pair.at[x])] + list(zip(experts, others))
        )
    ]
    kept = [
        pltpu.make_async_copy(src, dst, own_sems.at[i])
        for i, (src, dst) in enumerate(
            [(mine[a], full[a].at[own]) for a in range(count)] + [(normed, normed_pair.at[x])]
        )
    ]
    for plan in plans:
        plan.start()
    for copy in swaps + kept:
        copy.start()
    for step in range(1, LEVELS):
        for plan in plans:
            plan.from_line(step)
        for plan in plans:
            plan.from_side(step - 1)
    for plan in plans:
        plan.from_side(LEVELS - 1)
    for plan in plans:
        for step in range(LEVELS):
            for side in range(2):
                plan.from_core(step, side)
    for plan in plans:
        plan.finish()
    for copy in swaps + kept:
        copy.wait()


def gather_weights(arrays, normed, experts, collective_id):
    owner_count = lax.axis_size("fsdp")
    count = len(arrays)
    hbm = pl.BlockSpec(memory_space=pl.ANY)
    vmem = pl.BlockSpec(memory_space=pltpu.VMEM)
    nbytes = sum(a.size * a.dtype.itemsize for a in arrays)
    outs = pl.pallas_call(
        functools.partial(weights_kernel, count),
        out_shape=[jax.ShapeDtypeStruct((owner_count,) + a.shape, a.dtype) for a in arrays]
        + [jax.ShapeDtypeStruct((2,) + normed.shape, normed.dtype)]
        + [jax.ShapeDtypeStruct(w.shape, w.dtype) for w in experts],
        in_specs=[vmem] * (count + 1) + [hbm] * 3,
        out_specs=[hbm] * (count + 4),
        scratch_shapes=[
            pltpu.SemaphoreType.DMA((count, GATHER_SENDS)),
            pltpu.SemaphoreType.DMA((count, owner_count)),
            pltpu.SemaphoreType.DMA((count + 1,)),
            pltpu.SemaphoreType.DMA((4,)),
            pltpu.SemaphoreType.DMA((4,)),
        ],
        compiler_params=pltpu.CompilerParams(collective_id=collective_id, has_side_effects=True),
        cost_estimate=pl.CostEstimate(
            flops=0, bytes_accessed=owner_count * nbytes * 4, transcendentals=0
        ),
        name="gather_weights",
    )(*arrays, normed, *experts)
    return outs[:count], outs[count], outs[count + 1 :]


class PlaneSums:
    def __init__(self, own_parts, from_core, from_side, from_line, sems, kept=0):
        self.own, self.from_core, self.kept = own_parts, from_core, kept
        self.from_side, self.from_line = from_side, from_line
        self.core_s, self.core_r, self.side_s, self.side_r, self.line_s, self.line_r = sems
        self.z, self.y, self.c, self.x = place()
        self.top, self.bottom = line_ends(self.z)

    def side_arrived(self, turn):
        here = self.from_side.at[turn]
        remote(here, here, self.side_s.at[turn], self.side_r.at[turn], (0, self.x)).wait_recv()

    def line_arrived(self, slot):
        here = self.from_line.at[slot]
        remote(here, here, self.line_s.at[0], self.line_r.at[slot], (0, self.x)).wait_recv()

    def to_line(self, turn):
        z, y, c, x = self.z, self.y, self.c, self.x
        mine = self.own.at[self.kept + turn]
        level = level_at(turn, z)

        @pl.when(self.top + self.bottom == 0)
        def _():
            self.line_arrived(level)
            add_block(mine, self.from_line.at[level], mine)

        down = (z + LEVELS - level) // (LEVELS + 1)
        onward = z + 1 - 2 * down
        reached = 1 - jnp.minimum(1, jnp.abs(onward - level))
        slot = level + down * reached * (LEVELS - level)
        copy = remote(
            mine,
            self.from_line.at[slot],
            self.line_s.at[turn],
            self.line_r.at[slot],
            (index_of(onward, y, c), x),
        )
        copy.start()


def add_block(one, two, out):
    step = 32

    @pl.loop(0, out.shape[0] // step)
    def _(i):
        rows = pl.ds(pl.multiple_of(i * step, step), step)
        value = one[rows, :].astype(jnp.float32) + two[rows, :].astype(jnp.float32)
        out[rows, :] = value.astype(out.dtype)


def total_block(plan, total):
    step = 32
    mine = plan.own.at[plan.kept + LEVELS - 1]
    below, above = plan.from_line.at[plan.z], plan.from_line.at[LEVELS]

    @pl.loop(0, total.shape[0] // step)
    def _(i):
        rows = pl.ds(pl.multiple_of(i * step, step), step)
        total[rows, :] = mine[rows, :].astype(jnp.float32)

    for end, block, slot in ((plan.bottom, below, plan.z), (plan.top, above, LEVELS)):

        @pl.when(end == 0)
        def _():
            plan.line_arrived(slot)

            @pl.loop(0, total.shape[0] // step)
            def _(i):
                rows = pl.ds(pl.multiple_of(i * step, step), step)
                total[rows, :] = total[rows, :] + block[rows, :].astype(jnp.float32)


ROUTE_COLS = 128


def nn(left, right):
    return lax.dot_general(
        left, right, (((1,), (0,)), ((), ())), preferred_element_type=jnp.float32
    )


def nt(left, right):
    return lax.dot_general(
        left, right, (((1,), (1,)), ((), ())), preferred_element_type=jnp.float32
    )


def tn(left, right):
    return lax.dot_general(
        left, right, (((0,), (0,)), ((), ())), preferred_element_type=jnp.float32
    )


def pair_block(ref, pair):
    value = ref[pl.ds(2 * pair, 2)]
    return value.reshape(value.shape[0] * value.shape[1], value.shape[2])


def experts_kernel(
    gates,
    second_gain,
    out_part,
    block_input,
    upstream,
    upstream_hbm,
    gate_own,
    up_own,
    down_own,
    gate_other,
    up_other,
    down_other,
    middle,
    middle_grad,
    second_term,
    middle_pair,
    mixture_hbm,
    gate_mine,
    gate_theirs,
    up_mine,
    up_theirs,
    down_mine,
    down_theirs,
    down_landed,
    rows_all,
    u_all,
    wg,
    wu,
    wd,
    hidden,
    gcot,
    ucot,
    rext,
    tmp,
    from_core,
    from_side,
    from_line,
    gstage,
    wide,
    second_scale,
    route_half,
    gather_s,
    gather_r,
    core_s,
    core_r,
    side_s,
    side_r,
    line_s,
    line_r,
    load_sems,
    out_sems,
    pair_s,
    pair_r,
):
    bf16, f32 = jnp.bfloat16, jnp.float32
    z, y, c, x = place()
    top, bottom = line_ends(z)
    interior = 1 - top - bottom
    me = lax.axis_index("fsdp")
    partner = (me, 1 - x)
    halves, width, units = wg.shape
    half_rows = middle.shape[0]
    pair_rows_ = 2 * half_rows
    pairs = 2 * LEVELS
    panel = 512
    block = 256
    step = 16

    loads = [
        pltpu.make_async_copy(src, dst, load_sems.at[i])
        for i, (src, dst) in enumerate(
            (
                (out_part.at[1 - x], middle_grad),
                (out_part.at[x], middle),
                (block_input, wide),
                (down_own, wd.at[x]),
                (down_other, wd.at[1 - x]),
                (upstream_hbm, u_all),
                (gate_own, wg.at[x]),
                (up_own, wu.at[x]),
                (gate_other, wg.at[1 - x]),
                (up_other, wu.at[1 - x]),
            )
        )
    ]
    for load in loads:
        load.start()

    plane_greet(pair=True)
    gather = PlaneGather(rows_all.at[me], rows_all, gather_s, gather_r)
    sums = PlaneSums(
        from_core,
        from_core,
        from_side,
        from_line,
        (core_s, core_r, side_s, side_r, line_s, line_r),
        LEVELS,
    )

    loads[0].wait()

    @pl.loop(0, half_rows // step)
    def _(i):
        at = pl.ds(pl.multiple_of(i * step, step), step)
        tmp[0, 0, at, :] = middle_grad[at, :].astype(bf16)

    meet = remote(tmp.at[0, 0], tmp.at[0, 1], pair_s.at[0], pair_r.at[0], partner)
    meet.start()
    for load in loads[1:6]:
        load.wait()

    @pl.loop(0, pairs)
    def _(b):
        at_rows = pl.ds(pl.multiple_of(b * pair_rows_, pair_rows_), pair_rows_)
        us = pair_block(u_all, b)
        for h in range(halves):
            ucot[h, at_rows, :] = nt(us, wd[h]).astype(bf16)

    meet.wait()
    gain = second_gain[...]

    @pl.loop(0, half_rows // step)
    def _(i):
        at = pl.ds(pl.multiple_of(i * step, step), step)
        value = wide[at, :] + (middle[at, :] + tmp[0, 1, at, :].astype(f32))
        scale = lax.rsqrt(jnp.mean(value * value, axis=1, keepdims=True) + epsilon)
        middle[at, :] = value
        second_scale[at, :] = scale
        rows_all[me, at, :] = (value * scale * gain).astype(bf16)

    gather.start()
    again = pltpu.make_async_copy(upstream, wide, load_sems.at[2])
    again.start()
    for load in loads[6:]:
        load.wait()

    def forward_pair(b):
        turn = (0b11_10_11_01_10_00_01_00 >> (2 * b)) % 4
        side = (0b11_01_01_00 >> b) % 2
        return level_at(3 - turn, z) * 2 + (y + side) % 2

    def mixture_out(b):
        return pltpu.make_async_copy(
            tmp.at[b % 2],
            mixture_hbm.at[pl.ds(2 * forward_pair(b), 2), :, pl.ds(0, width)],
            out_sems.at[b % 2],
        )

    @pl.loop(0, 2 * pairs)
    def _(turn):
        b, h = turn // 2, turn % 2

        def at(k, work, where=None):
            @pl.when(turn == k)
            def _():
                if where is None:
                    work()
                else:
                    pl.when(where == 1)(work)

        at(0, lambda: gather.from_core(0, 0))
        at(2, lambda: gather.from_line(1))
        at(2, lambda: gather.from_line(2), interior)
        at(2, lambda: gather.from_core(1, 0))
        at(4, lambda: gather.from_side(0))
        at(4, lambda: gather.from_core(0, 1))
        at(6, lambda: gather.from_line(2), 1 - interior)
        at(6, lambda: gather.from_line(3), interior)
        at(6, lambda: gather.from_core(2, 0))
        at(8, lambda: gather.from_side(1))
        at(8, lambda: gather.from_core(1, 1))
        at(10, lambda: gather.from_line(3), 1 - interior)
        at(10, lambda: gather.from_core(3, 0))
        at(12, lambda: gather.from_side(2))
        at(12, lambda: gather.from_core(2, 1))
        at(14, lambda: gather.from_side(3))
        at(14, lambda: gather.from_core(3, 1))

        pair = forward_pair(b)
        xs = pair_block(rows_all, pair)
        lane = lax.broadcasted_iota(jnp.int32, (pair_rows_, ROUTE_COLS), 1)
        table = gates[pl.ds(2 * pair, 2)].reshape(pair_rows_, ROUTE_COLS)
        gate_rows = jnp.sum(jnp.where(lane == me, table, 0.0), axis=1, keepdims=True)
        gate_act = nn(xs, wg[h])
        up_act = nn(xs, wu[h])
        at_rows = pl.ds(pl.multiple_of(pair * pair_rows_, pair_rows_), pair_rows_)
        hidden_cot = ucot[h, at_rows, :].astype(f32)
        sig = lax.logistic(gate_act)
        act = gate_act * sig
        hid = act * up_act
        hidden[h, at_rows, :] = (hid * gate_rows).astype(bf16)
        route = jnp.sum(hid * hidden_cot, axis=1, keepdims=True)
        scaled = hidden_cot * gate_rows
        gcot[h, at_rows, :] = (scaled * up_act * (sig * (1.0 + gate_act * (1.0 - sig)))).astype(bf16)
        ucot[h, at_rows, :] = (scaled * act).astype(bf16)

        @pl.when(h == 0)
        def _():
            route_half[...] = route

        @pl.when(h == 1)
        def _():
            total = route_half[...] + route
            placed = jnp.where(lane == me, total, 0.0).astype(bf16)
            rext[pl.ds(2 * pair, 2)] = placed.reshape(2, half_rows, ROUTE_COLS)

            pl.when(b >= 2)(lambda: mixture_out(b - 2).wait())

            @pl.loop(0, width // panel)
            def _(n):
                cols = pl.ds(pl.multiple_of(n * panel, panel), panel)
                acc = nn(hidden[0, at_rows, :], wd[0, :, cols])
                for h in range(1, halves):
                    acc = acc + nn(hidden[h, at_rows, :], wd[h, :, cols])
                tmp[b % 2, :, :, cols] = acc.astype(bf16).reshape(2, half_rows, panel)

            mixture_out(b).start()

    for b in (pairs - 2, pairs - 1):
        mixture_out(b).wait()

    def core_send(b):
        return remote(
            tmp.at[b % 2, 1 - c],
            from_core.at[b],
            core_s.at[b],
            core_r.at[b],
            (index_of(z, y, 1 - c), x),
        )

    def take_core(b):
        core_send(b).wait_recv()
        add_block(tmp.at[b % 2, c], from_core.at[b], from_core.at[b])

        @pl.when(b < LEVELS)
        def _():
            remote(
                from_core.at[b],
                from_side.at[b],
                side_s.at[b],
                side_r.at[b],
                (index_of(z, 1 - y, c), x),
            ).start()

    def line_step(turn):
        sums.side_arrived(turn)
        mine = from_core.at[LEVELS + turn]
        add_block(mine, from_side.at[turn], mine)
        if turn < LEVELS - 1:
            sums.to_line(turn)

    def last_step():
        line_step(LEVELS - 1)
        total_block(sums, middle_grad)
        again.wait()
        second_term[...] = jnp.zeros_like(second_term)

        @pl.loop(0, half_rows // step)
        def _(i):
            at = pl.ds(pl.multiple_of(i * step, step), step)
            cot, mid, scale = middle_grad[at, :], middle[at, :], second_scale[at, :]
            weighted = cot * gain
            mean = jnp.mean(weighted * mid, axis=1, keepdims=True)
            value = wide[at, :] + scale * (weighted - mid * (scale * scale * mean))
            middle_grad[at, :] = value
            tmp[0, 0, at, :] = value.astype(bf16)
            second_term[...] = second_term[...] + jnp.sum(cot * mid * scale, axis=0, keepdims=True)

        pair_send().start()
        pair_keep().start()

    def pair_send():
        return remote(tmp.at[0, 0], middle_pair.at[x], pair_s.at[1], pair_r.at[1], partner)

    def pair_keep():
        return pltpu.make_async_copy(tmp.at[0, 0], middle_pair.at[x], load_sems.at[0])

    @pl.loop(0, pairs)
    def _(b):
        pl.when((b == pairs - 1) & (interior == 0))(lambda: line_step(0))
        pl.when(b >= 2)(lambda: core_send(b - 2).wait_send())
        pair = level_at(b % LEVELS, z) * 2 + (y + 1 - b // LEVELS) % 2
        at_rows = pl.ds(pl.multiple_of(pair * pair_rows_, pair_rows_), pair_rows_)

        @pl.loop(0, width // panel)
        def _(n):
            cols = pl.ds(pl.multiple_of(n * panel, panel), panel)
            acc = nt(gcot[0, at_rows, :], wg[0, cols, :])
            acc = acc + nt(ucot[0, at_rows, :], wu[0, cols, :])
            for h in range(1, halves):
                acc = acc + nt(gcot[h, at_rows, :], wg[h, cols, :])
                acc = acc + nt(ucot[h, at_rows, :], wu[h, cols, :])
            tmp[b % 2, :, :, cols] = acc.astype(bf16).reshape(2, half_rows, panel)

        core_send(b).start()
        pl.when(b >= 1)(lambda: take_core(b - 1))

    take_core(pairs - 1)
    for b in (pairs - 2, pairs - 1):
        core_send(b).wait_send()

    route_out = pltpu.make_async_copy(
        rext, mixture_hbm.at[:, :, pl.ds(width, ROUTE_COLS)], load_sems.at[1]
    )
    route_out.start()
    down_send = remote(
        wd.at[0, pl.ds(0, block)], down_landed, pair_s.at[2], pair_r.at[2], partner
    )
    down_later = pltpu.make_async_copy(wd.at[0, pl.ds(block, block)], down_theirs, load_sems.at[3])
    down_keep = pltpu.make_async_copy(wd.at[1], down_mine, load_sems.at[4])

    @pl.loop(0, 2 * units // block)
    def _(p):
        other, q = p // (units // block), p % (units // block)
        pl.when((p == 1) & (interior == 0))(lambda: line_step(1))
        pl.when((p == 2) & (interior == 1))(lambda: line_step(0))
        units_at = pl.ds(pl.multiple_of(q * block, block), block)
        us = u_all[...]
        us = us.reshape(us.shape[0] * us.shape[1], width)
        h = (1 - x) * (1 - other) + x * other
        wd[other, units_at, :] = tn(hidden[h, :, units_at], us).astype(bf16)
        pl.when(p == 0)(down_send.start)
        pl.when(p == 1)(down_later.start)

    down_keep.start()

    def part_outs(p):
        rows = pl.ds(pl.multiple_of(p * block, block), block)
        return [
            pltpu.make_async_copy(
                gstage.at[p % 2, which, k], ref.at[rows, :], out_sems.at[(p % 2) * 4 + 2 * which + k]
            )
            for which, refs in enumerate(((gate_mine, gate_theirs), (up_mine, up_theirs)))
            for k, ref in enumerate(refs)
        ]

    def wait_outs(p):
        for copy in part_outs(p):
            copy.wait()

    @pl.loop(0, width // block)
    def _(p):
        pl.when((p == 1) & (interior == 0))(lambda: line_step(2))
        pl.when((p == 1) & (interior == 1))(lambda: line_step(1))
        pl.when((p == 2) & (interior == 1))(lambda: line_step(2))
        pl.when(p == 6)(last_step)
        pl.when(p >= 2)(lambda: wait_outs(p - 2))
        cols = pl.ds(pl.multiple_of(p * block, block), block)
        xp = rows_all[:, :, cols]
        xp = xp.reshape(xp.shape[0] * xp.shape[1], block)
        for which, ref in enumerate((gcot, ucot)):
            for k, h in enumerate((x, 1 - x)):
                gstage[p % 2, which, k] = tn(xp, ref[h]).astype(bf16)
        for copy in part_outs(p):
            copy.start()

    for p in (width // block - 2, width // block - 1):
        wait_outs(p)
    pair_send().wait()
    pair_keep().wait()
    route_out.wait()
    down_send.wait()
    down_later.wait()
    down_keep.wait()
    gather.finish()
    for turn in range(LEVELS):
        remote(
            from_core.at[turn], from_side.at[turn], side_s.at[turn], side_r.at[turn], partner
        ).wait_send()
    for turn in range(LEVELS - 1):
        remote(
            from_core.at[turn], from_line.at[turn], line_s.at[turn], line_r.at[turn], partner
        ).wait_send()


def run_experts(
    gates, second_gain, out_part, block_input, upstream, upstream_all, own, other, collective_id
):
    bf16, f32 = jnp.bfloat16, jnp.float32
    block = block_input.shape
    half_rows, width = block
    owner_count = upstream_all.shape[0]
    units = own[0].shape[1]
    halves = lax.axis_size("tp")
    all_rows = owner_count * half_rows
    hbm = pl.BlockSpec(memory_space=pl.ANY)
    vmem = pl.BlockSpec(memory_space=pltpu.VMEM)
    dma = pltpu.SemaphoreType.DMA
    flops = 2 * 9 * all_rows * width * units * halves
    shape = jax.ShapeDtypeStruct
    return pl.pallas_call(
        experts_kernel,
        out_shape=[
            shape(block, f32),
            shape(block, f32),
            shape((1, width), f32),
            shape((2,) + block, bf16),
            shape((owner_count, half_rows, width + ROUTE_COLS), bf16),
        ]
        + [shape((width, units), bf16)] * 4
        + [shape((units, width), bf16)]
        + [shape((256, width), bf16)] * 2,
        in_specs=[vmem, vmem] + [hbm] * 10,
        out_specs=[vmem] * 3 + [hbm] * 9,
        scratch_shapes=[
            pltpu.VMEM((owner_count,) + block, bf16),
            pltpu.VMEM((owner_count,) + block, bf16),
            pltpu.VMEM((halves, width, units), bf16),
            pltpu.VMEM((halves, width, units), bf16),
            pltpu.VMEM((halves, units, width), bf16),
            pltpu.VMEM((halves, all_rows, units), bf16),
            pltpu.VMEM((halves, all_rows, units), bf16),
            pltpu.VMEM((halves, all_rows, units), bf16),
            pltpu.VMEM((owner_count, half_rows, ROUTE_COLS), bf16),
            pltpu.VMEM((2, 2) + block, bf16),
            pltpu.VMEM((2 * LEVELS,) + block, bf16),
            pltpu.VMEM((LEVELS,) + block, bf16),
            pltpu.VMEM((LEVELS + 1,) + block, bf16),
            pltpu.VMEM((2, 2, halves, 256, units), bf16),
            pltpu.VMEM(block, f32),
            pltpu.VMEM((half_rows, 1), f32),
            pltpu.VMEM((2 * half_rows, 1), f32),
            dma((GATHER_SENDS,)),
            dma((owner_count,)),
            dma((2 * LEVELS,)),
            dma((2 * LEVELS,)),
            dma((LEVELS,)),
            dma((LEVELS,)),
            dma((LEVELS + 1,)),
            dma((LEVELS + 1,)),
            dma((10,)),
            dma((8,)),
            dma((3,)),
            dma((3,)),
        ],
        compiler_params=pltpu.CompilerParams(
            collective_id=collective_id, has_side_effects=True, vmem_limit_bytes=67_043_328
        ),
        cost_estimate=pl.CostEstimate(
            flops=flops, bytes_accessed=64 * 2**20, transcendentals=all_rows * units * halves
        ),
        name="experts",
    )(gates, second_gain, out_part, block_input, upstream, upstream_all, *own, *other)


def last_kernel(
    mixture_part,
    middle_pair,
    normed_pair,
    mixed_rows,
    query_rows,
    key_rows,
    value_rows,
    output_full,
    query_full,
    key_full,
    value_full,
    gate_theirs,
    up_theirs,
    down_theirs,
    block_input,
    first_scale,
    first_gain,
    middle_grad,
    second_term,
    query_total,
    key_total,
    value_total,
    output_total,
    mixture_total,
    gate_landed,
    up_landed,
    down_landed,
    input_grad,
    gain_grads,
    wide_core,
    wide_side,
    wide_line,
    wide_own,
    from_core,
    from_side,
    from_line,
    tmp,
    mixed_cot,
    query_cot,
    key_cot,
    value_cot,
    weight_one,
    weight_two,
    first_terms,
    first_mine,
    first_other,
    gains,
    gains_in,
    core_s,
    core_r,
    side_s,
    side_r,
    line_s,
    line_r,
    own_sems,
    load_sems,
    pair_s,
    pair_r,
    gain_s,
    gain_r,
):
    bf16, f32 = jnp.bfloat16, jnp.float32
    z, y, c, x = place()
    own = index_of(z, y, c)
    rows, head_cols = mixed_rows.shape
    half_rows, width = input_grad.shape
    pairs = 2 * LEVELS
    inv_root = HD ** (-0.5)
    plane_greet(pair=True, far=True)

    def swap(i, src, dst):
        return remote(src, dst, pair_s.at[i], pair_r.at[i], (own, 1 - x))

    expert_swaps = (
        swap(0, gate_theirs, gate_landed),
        swap(1, up_theirs, up_landed),
        swap(2, down_theirs, down_landed),
    )
    first_swap = swap(3, first_mine, first_other)

    def load(i, src, dst):
        return pltpu.make_async_copy(src, dst, load_sems.at[i])

    output_load, query_load = load(0, output_full, weight_one), load(1, query_full, weight_two)
    value_load, key_load = load(2, value_full, weight_one), load(3, key_full, weight_two)
    sums = [
        PlaneSums(
            core,
            core,
            side,
            line,
            tuple(s.at[a] for s in (core_s, core_r, side_s, side_r, line_s, line_r)),
            LEVELS,
        )
        for a, (core, side, line) in enumerate(
            [(wide_core, wide_side, wide_line)]
            + [(from_core.at[i], from_side.at[i], from_line.at[i]) for i in range(4)]
        )
    ]

    def slot_at(b, core):
        level, side = level_at(b % LEVELS, z), (y + 1 - b // LEVELS) % 2
        return index_of(level, side, (c + core) % 2)

    def core_copy(a, b, src):
        plan = sums[a]
        return remote(
            src,
            plan.from_core.at[b],
            plan.core_s.at[b],
            plan.core_r.at[b],
            (index_of(z, y, 1 - c), x),
        )

    def side_copy(a, b):
        plan = sums[a]
        return remote(
            plan.from_core.at[b],
            plan.from_side.at[b],
            plan.side_s.at[b],
            plan.side_r.at[b],
            (index_of(z, 1 - y, c), x),
        )

    def line_step(a, turn):
        plan = sums[a]
        plan.side_arrived(turn)
        mine = plan.from_core.at[LEVELS + turn]
        add_block(mine, plan.from_side.at[turn], mine)
        if turn < LEVELS - 1:
            plan.to_line(turn)

    for copy in expert_swaps[:2]:
        copy.start()
    output_load.start()
    query_load.start()

    def wide_load(b):
        return pltpu.make_async_copy(
            mixture_part.at[slot_at(b, 0)], wide_own.at[b], own_sems.at[b]
        )

    @pl.loop(0, pairs)
    def _(b):
        core_copy(0, b, mixture_part.at[slot_at(b, 1)]).start()
        wide_load(b).start()

    @pl.loop(0, pairs)
    def _(b):
        wide_load(b).wait()
        core_copy(0, b, mixture_part.at[slot_at(b, 1)]).wait_recv()
        add_block(wide_own.at[b], wide_core.at[b], wide_core.at[b])
        pl.when(b < LEVELS)(lambda: side_copy(0, b).start())

    def flat(ref):
        value = ref[...]
        return value.reshape(value.shape[0] * value.shape[1], value.shape[2])

    output_load.wait()
    mixed_cot[...] = nn(flat(middle_pair), flat(weight_one)).astype(bf16)
    value_load.start()

    def term(a, left, cot):
        def send(b):
            return core_copy(a, b, tmp.at[b % 2, 1 - c])

        def take(b):
            core = sums[a].from_core.at[b]
            send(b).wait_recv()
            add_block(tmp.at[b % 2, c], core, core)
            pl.when(b < LEVELS)(lambda: side_copy(a, b).start())

        @pl.loop(0, pairs)
        def _(b):
            pl.when(b >= 2)(lambda: send(b - 2).wait_send())
            pair = level_at(b % LEVELS, z) * 2 + (y + 1 - b // LEVELS) % 2
            cols = pl.ds(pl.multiple_of(pair * 2 * half_rows, 2 * half_rows), 2 * half_rows)
            lhs = left[:, :, cols].reshape(rows, 2 * half_rows)
            part = tn(lhs, cot[...])
            tmp[b % 2] = part.astype(bf16).reshape(2, half_rows, head_cols)
            send(b).start()
            pl.when(b >= 1)(lambda: take(b - 1))

        take(pairs - 1)
        for b in (pairs - 2, pairs - 1):
            send(b).wait_send()

    top, bottom = line_ends(z)
    interior = 1 - top - bottom

    def head(h):
        cols = pl.ds(pl.multiple_of(h * HD, HD), HD)
        query, key, value = query_rows[:, cols], key_rows[:, cols], value_rows[:, cols]
        mixed = mixed_cot[:, cols]
        scores = nt(query, key) * inv_root
        row_top = jnp.max(scores, axis=1, keepdims=True)
        log_total = row_top + jnp.log(jnp.sum(jnp.exp(scores - row_top), axis=1, keepdims=True))
        soft = jnp.exp(scores - log_total)
        value_cot[:, cols] = tn(soft.astype(bf16), mixed).astype(bf16)
        soft_cot = nt(mixed, value)
        inner = jnp.sum(soft * soft_cot, axis=1, keepdims=True)
        score_cot = (soft * (soft_cot - inner) * inv_root).astype(bf16)
        query_cot[:, cols] = nn(score_cot, key).astype(bf16)
        key_cot[:, cols] = tn(score_cot, query).astype(bf16)

    term(1, middle_pair, mixed_rows)

    @pl.when(interior == 0)
    def _():
        line_step(0, 0)
        line_step(0, 1)

    @pl.loop(0, head_cols // HD // 2)
    def _(h):
        pl.when((h == 1) & (interior == 1))(lambda: line_step(0, 0))
        head(2 * h)
        head(2 * h + 1)

    pl.when(interior == 1)(lambda: line_step(0, 1))
    line_step(0, 2)
    term(2, normed_pair, value_cot)
    line_step(0, 3)
    term(3, normed_pair, query_cot)
    line_step(1, 0)
    line_step(1, 1)
    term(4, normed_pair, key_cot)
    line_step(1, 2)
    line_step(1, 3)

    panel = 4

    def first_add(cot, weight, begin):
        @pl.loop(0, weight.shape[0] // panel)
        def _(n):
            part = weight[pl.ds(n * panel, panel)].reshape(panel * half_rows, head_cols)
            cols = pl.ds(pl.multiple_of(n * panel * half_rows, panel * half_rows), panel * half_rows)
            value = nt(cot[...], part).reshape(2, half_rows, panel * half_rows)
            if begin:
                first_terms[:, :, cols] = value
            else:
                first_terms[:, :, cols] = first_terms[:, :, cols] + value

    query_load.wait()
    first_add(query_cot, weight_two, True)
    key_load.start()
    value_load.wait()
    first_add(value_cot, weight_one, False)
    key_load.wait()
    first_add(key_cot, weight_two, False)
    step = 16

    @pl.loop(0, half_rows // step)
    def _(i):
        at = pl.ds(pl.multiple_of(i * step, step), step)
        first_mine[at, :] = first_terms[1 - x, at, :].astype(bf16)

    first_swap.start()
    total_block(sums[0], mixture_total)
    for turn in range(LEVELS):
        line_step(2, turn)
    total_block(sums[1], output_total)
    line_step(3, 0)
    line_step(3, 1)
    first_swap.wait_recv()
    gain = first_gain[...]
    gains[...] = jnp.concatenate(
        [jnp.zeros((1, width), f32), second_term[...], jnp.zeros((6, width), f32)], axis=0
    )

    @pl.loop(0, half_rows // step)
    def _(i):
        at = pl.ds(pl.multiple_of(i * step, step), step)
        value = first_terms[x, at, :] + first_other[at, :].astype(f32)
        entry, scale = block_input[at, :], first_scale[at, :]
        weighted = value * gain
        mean = jnp.mean(weighted * entry, axis=1, keepdims=True)
        input_grad[at, :] = middle_grad[at, :] + scale * (weighted - entry * (scale * scale * mean))
        gains[0:1, :] = gains[0:1, :] + jnp.sum(value * entry * scale, axis=0, keepdims=True)

    hops = [
        (index_of(z, y, 1 - c), x),
        (own, 1 - x),
        (index_of(z + 1 - 2 * (z % 2), y, c), x),
        (index_of((z + 2) % LEVELS, y, c), x),
        (index_of(z, 1 - y, c), x),
    ]

    def gain_copy(i):
        return remote(gains, gains_in.at[i], gain_s.at[i], gain_r.at[i], hops[i])

    def gain_add(i):
        gain_copy(i).wait()
        gains[...] = gains[...] + gains_in[i]

    for i in range(2):
        gain_copy(i).start()
        gain_add(i)
    expert_swaps[2].start()
    gain_copy(2).start()
    line_step(3, 2)
    line_step(3, 3)
    gain_add(2)
    gain_copy(3).start()
    total_block(sums[2], value_total)
    line_step(4, 0)
    gain_add(3)
    gain_copy(4).start()
    for turn in range(1, LEVELS):
        line_step(4, turn)
    total_block(sums[3], query_total)
    gain_add(4)
    gain_grads[...] = gains[...]
    total_block(sums[4], key_total)

    @pl.loop(0, pairs)
    def _(b):
        core_copy(0, b, mixture_part.at[slot_at(b, 1)]).wait_send()

    for a in range(5):
        for turn in range(LEVELS):
            side_copy(a, turn).wait_send()
        line = sums[a].from_line
        for turn in range(LEVELS - 1):
            remote(
                line.at[0], line.at[turn], sums[a].line_s.at[turn], sums[a].line_r.at[turn], (own, 1 - x)
            ).wait_send()
    first_swap.wait_send()
    for copy in expert_swaps:
        copy.wait()


def run_last(
    mixture_part, pair_rows_in, attention_rows, weights_full, theirs, norm_args, collective_id
):
    f32, bf16 = jnp.float32, jnp.bfloat16
    shape = jax.ShapeDtypeStruct
    hbm = pl.BlockSpec(memory_space=pl.ANY)
    vmem = pl.BlockSpec(memory_space=pltpu.VMEM)
    dma = pltpu.SemaphoreType.DMA
    rows, head_cols = attention_rows[0].shape
    half_rows, width = norm_args[0].shape
    wide = mixture_part.shape[1:]
    block = (half_rows, head_cols)
    pairs = 2 * LEVELS
    flops = 2 * rows * head_cols * width * 8
    nbytes = 2 * (mixture_part.size + 12 * weights_full[0].size)
    outs = pl.pallas_call(
        last_kernel,
        out_shape=[shape(block, f32)] * 4
        + [shape(wide, f32)]
        + [shape(t.shape, t.dtype) for t in theirs]
        + [shape((half_rows, width), f32), shape((8, width), f32)],
        in_specs=[hbm] + [vmem] * 6 + [hbm] * 7 + [vmem] * 5,
        out_specs=[vmem] * 5 + [hbm] * 3 + [vmem] * 2,
        scratch_shapes=[
            pltpu.VMEM((pairs,) + wide, bf16),
            pltpu.VMEM((LEVELS,) + wide, bf16),
            pltpu.VMEM((LEVELS + 1,) + wide, bf16),
            pltpu.VMEM((pairs,) + wide, bf16),
            pltpu.VMEM((4, pairs) + block, bf16),
            pltpu.VMEM((4, LEVELS) + block, bf16),
            pltpu.VMEM((4, LEVELS + 1) + block, bf16),
            pltpu.VMEM((2, 2) + block, bf16),
        ]
        + [pltpu.VMEM((rows, head_cols), bf16)] * 4
        + [pltpu.VMEM(weights_full[0].shape, bf16)] * 2
        + [
            pltpu.VMEM((2, half_rows, width), f32),
            pltpu.VMEM((half_rows, width), bf16),
            pltpu.VMEM((half_rows, width), bf16),
            pltpu.VMEM((8, width), f32),
            pltpu.VMEM((5, 8, width), f32),
        ]
        + [dma((5, pairs))] * 2
        + [dma((5, LEVELS))] * 2
        + [dma((5, LEVELS + 1))] * 2
        + [dma((pairs,)), dma((4,)), dma((4,)), dma((4,)), dma((5,)), dma((5,))],
        compiler_params=pltpu.CompilerParams(
            collective_id=collective_id, has_side_effects=True, vmem_limit_bytes=67_043_328
        ),
        cost_estimate=pl.CostEstimate(flops=flops, bytes_accessed=nbytes, transcendentals=0),
        name="last",
    )(mixture_part, *pair_rows_in, *attention_rows, *weights_full, *theirs, *norm_args)
    return outs[:5], outs[5:8], outs[8], outs[9]


def gate_columns(route_rows, gate_rows, expert_count):
    names = jnp.arange(expert_count, dtype=jnp.int32)[None, None, :]
    return jnp.sum(jnp.where(route_rows[:, :, None] == names, gate_rows[:, :, None], 0.0), axis=1)


def half_of(rows):
    count = rows.shape[0] // lax.axis_size("tp")
    return lax.dynamic_slice_in_dim(rows, lax.axis_index("tp") * count, count, axis=0)


def per_device_dense(
    block_input,
    upstream_grad,
    first_gain,
    second_gain,
    query_weight,
    key_weight,
    value_weight,
    output_weight,
    gate_weight,
    up_weight,
    down_weight,
    routes,
    gate_values,
):
    pair_count = lax.axis_size("tp")
    owner_count = lax.axis_size("fsdp")
    local_rows = block_input.shape[0]
    seq_rows = local_rows * pair_count
    model_width = block_input.shape[1]
    head_cols = query_weight.shape[1]
    local_heads = head_cols // HD
    expert_count = EXP_DEV * owner_count
    inv_root = HD ** (-0.5)
    bf16, f32 = jnp.bfloat16, jnp.float32

    my_routes, my_gates = half_of(routes), half_of(gate_values)
    gate_table = gate_columns(my_routes, my_gates, ROUTE_COLS)
    expert_names = jnp.arange(expert_count, dtype=jnp.int32)[None, :]
    own_weights = (gate_weight[0], up_weight[0], down_weight[0])

    first_scale = lax.rsqrt(jnp.mean(block_input * block_input, axis=1, keepdims=True) + epsilon)
    first_normed = (block_input * first_scale * first_gain).astype(bf16)
    gathered, normed_pair, other_weights = gather_weights(
        [
            query_weight,
            key_weight,
            value_weight,
            output_weight,
            upstream_grad.astype(bf16),
            gate_table,
        ],
        first_normed,
        own_weights,
        1,
    )
    query_full, key_full, value_full, output_full = (w.reshape(-1, head_cols) for w in gathered[:4])
    upstream_all, gates_all = gathered[4:]
    normed_rows = normed_pair.reshape(seq_rows, model_width)

    def heads_of(weight_full):
        return (
            jnp.dot(normed_rows, weight_full, preferred_element_type=f32)
            .astype(bf16)
            .reshape(seq_rows, local_heads, HD)
        )

    query_rows, key_rows, value_rows = heads_of(query_full), heads_of(key_full), heads_of(value_full)
    scores = jnp.einsum("shd,thd->hst", query_rows, key_rows, preferred_element_type=f32) * inv_root
    row_top = jnp.max(scores, axis=2, keepdims=True)
    log_total = row_top + jnp.log(jnp.sum(jnp.exp(scores - row_top), axis=2, keepdims=True))
    soft_weights = jnp.exp(scores - log_total)
    soft_rounded = soft_weights.astype(bf16)
    mixed_rows = jnp.einsum("hst,thd->shd", soft_rounded, value_rows, preferred_element_type=f32)
    mixed_rows = mixed_rows.astype(bf16).reshape(seq_rows, head_cols)
    out_part = contract_cols(mixed_rows, output_full).reshape(pair_count, local_rows, model_width)
    (
        middle,
        middle_grad,
        second_term,
        middle_pair,
        mixture_part,
        gate_mine,
        gate_theirs,
        up_mine,
        up_theirs,
        down_mine,
        down_theirs,
        down_landed,
    ) = run_experts(
        gates_all,
        second_gain[None],
        out_part,
        block_input,
        upstream_grad,
        upstream_all,
        own_weights,
        other_weights,
        2,
    )
    sums, landed, input_grad, gain_grads = run_last(
        mixture_part,
        (middle_pair, normed_pair),
        (mixed_rows,) + tuple(r.reshape(seq_rows, head_cols) for r in (query_rows, key_rows, value_rows)),
        (gathered[3], gathered[0], gathered[1], gathered[2]),
        (gate_theirs, up_theirs, down_theirs),
        (block_input, first_scale, first_gain[None], middle_grad, second_term),
        4,
    )
    query_grad, key_grad, value_grad, output_grad, mixture = sums
    gate_grad, up_grad, down_grad = (
        mine.astype(f32) + theirs.astype(f32)
        for mine, theirs in (
            (gate_mine, landed[0]),
            (up_mine, landed[1]),
            (down_mine, jnp.concatenate([down_landed, landed[2]], axis=0)),
        )
    )
    block_output = middle + mixture[:, :model_width]
    route_back = mixture[:, model_width : model_width + expert_count]
    route_grad = jnp.sum(
        jnp.where(my_routes[:, :, None] == expert_names[None], route_back[:, None, :], 0.0), axis=2
    )
    return (
        block_output,
        input_grad,
        gain_grads[0],
        gain_grads[1],
        query_grad,
        key_grad,
        value_grad,
        output_grad,
        gate_grad[None],
        up_grad[None],
        down_grad[None],
        route_grad,
    )


def solution(mesh):
    dense = 2 * TOP >= EXP_DEV * mesh.shape["fsdp"] and mesh.shape["fsdp"] == 4 * LEVELS
    per_device = per_device_dense if dense else per_device_slots
    in_specs = (
        P(("fsdp", "tp"), None),
        P(("fsdp", "tp"), None),
        P(),
        P(),
        P("fsdp", "tp"),
        P("fsdp", "tp"),
        P("fsdp", "tp"),
        P("fsdp", "tp"),
        P("fsdp", None, "tp"),
        P("fsdp", None, "tp"),
        P("fsdp", "tp", None),
        P("fsdp", None),
        P("fsdp", None),
    )
    out_specs = (
        P(("fsdp", "tp"), None),
        P(("fsdp", "tp"), None),
        P(),
        P(),
        P("fsdp", "tp"),
        P("fsdp", "tp"),
        P("fsdp", "tp"),
        P("fsdp", "tp"),
        P("fsdp", None, "tp"),
        P("fsdp", None, "tp"),
        P("fsdp", "tp", None),
        P(("fsdp", "tp"), None),
    )
    return jax.shard_map(
        per_device, mesh=mesh, in_specs=in_specs, out_specs=out_specs, check_vma=False
    )
```

```python
import functools

import jax
import jax.numpy as jnp
from jax import lax
from jax.experimental import pallas as pl
from jax.experimental.pallas import tpu as pltpu
from jax.sharding import PartitionSpec as P

HD = 128
TOP = 8
EXP_DEV = 1


epsilon = 1e-05


def route_slots(route_rows, expert_count, capacity):
    flat_routes = route_rows.reshape(-1)
    onehot = (flat_routes[:, None] == jnp.arange(expert_count, dtype=jnp.int32)[None, :]).astype(
        jnp.int32
    )
    earlier = jnp.cumsum(onehot, axis=0, dtype=jnp.int32) - onehot
    ranked = jnp.sum(earlier * onehot, axis=1, dtype=jnp.int32)
    return flat_routes * capacity + ranked


def pair_rows(row_block):
    return lax.all_gather(row_block, "tp", axis=0, tiled=True)


def pair_sums(term_block):
    return lax.psum_scatter(term_block, "tp", scatter_dimension=0, tiled=True)


def to_owners(buffer):
    return lax.all_to_all(buffer, "fsdp", split_axis=0, concat_axis=0, tiled=True)


def to_sources(buffer):
    return lax.all_to_all(buffer, "fsdp", split_axis=0, concat_axis=0, tiled=True)


def projections(query_weight, key_weight, value_weight, output_weight):
    return (
        lax.all_gather(query_weight, "fsdp", axis=0, tiled=True),
        lax.all_gather(key_weight, "fsdp", axis=0, tiled=True),
        lax.all_gather(value_weight, "fsdp", axis=0, tiled=True),
        lax.all_gather(output_weight, "fsdp", axis=0, tiled=True),
    )


def scatter_rows(row_block, slot_index, total_rows):
    return (
        jnp.zeros((total_rows, row_block.shape[1]), row_block.dtype).at[slot_index].set(row_block)
    )


def spread_rows(row_block, copies):
    return jnp.broadcast_to(
        row_block[:, None, :], (row_block.shape[0], copies, row_block.shape[1])
    ).reshape(-1, row_block.shape[1])


def contract_rows(left_block, right_block):
    return lax.dot_general(
        left_block, right_block, (((0,), (0,)), ((), ())), preferred_element_type=jnp.float32
    )


def contract_cols(left_block, right_block):
    return lax.dot_general(
        left_block, right_block, (((1,), (1,)), ((), ())), preferred_element_type=jnp.float32
    )


def send_out(full_buffer):
    return to_owners(full_buffer)


def send_back(group_parts):
    owner_count, local_experts, capacity, model_width = group_parts.shape
    return to_sources(group_parts).reshape(owner_count * local_experts * capacity, model_width)


def per_device_slots(
    block_input,
    upstream_grad,
    first_gain,
    second_gain,
    query_weight,
    key_weight,
    value_weight,
    output_weight,
    gate_weight,
    up_weight,
    down_weight,
    routes,
    gate_values,
):
    pair_count = lax.axis_size("tp")
    owner_count = lax.axis_size("fsdp")
    local_rows = block_input.shape[0]
    seq_rows = local_rows * pair_count
    model_width = block_input.shape[1]
    head_cols = query_weight.shape[1]
    local_heads = head_cols // HD
    expert_count = EXP_DEV * owner_count
    capacity = 3 * seq_rows * TOP // (2 * expert_count)
    inv_root = HD ** (-0.5)
    first_scale = lax.rsqrt(jnp.mean(block_input * block_input, axis=1, keepdims=True) + epsilon)
    first_normed = (block_input * first_scale * first_gain).astype(jnp.bfloat16)
    normed_rows = pair_rows(first_normed)
    query_full, key_full, value_full, output_full = projections(
        query_weight, key_weight, value_weight, output_weight
    )
    query_rows = (
        jnp.dot(normed_rows, query_full, preferred_element_type=jnp.float32)
        .astype(jnp.bfloat16)
        .reshape(seq_rows, local_heads, HD)
    )
    key_rows = (
        jnp.dot(normed_rows, key_full, preferred_element_type=jnp.float32)
        .astype(jnp.bfloat16)
        .reshape(seq_rows, local_heads, HD)
    )
    value_rows = (
        jnp.dot(normed_rows, value_full, preferred_element_type=jnp.float32)
        .astype(jnp.bfloat16)
        .reshape(seq_rows, local_heads, HD)
    )
    scores = (
        jnp.einsum("shd,thd->hst", query_rows, key_rows, preferred_element_type=jnp.float32)
        * inv_root
    )
    row_top = jnp.max(scores, axis=2, keepdims=True)
    log_total = row_top + jnp.log(jnp.sum(jnp.exp(scores - row_top), axis=2, keepdims=True))
    soft_weights = jnp.exp(scores - log_total)
    mixed_rows = jnp.einsum(
        "hst,thd->shd",
        soft_weights.astype(jnp.bfloat16),
        value_rows,
        preferred_element_type=jnp.float32,
    )
    mixed_rows = mixed_rows.astype(jnp.bfloat16).reshape(seq_rows, head_cols)
    middle = block_input + pair_sums(contract_cols(mixed_rows, output_full))
    second_scale = lax.rsqrt(jnp.mean(middle * middle, axis=1, keepdims=True) + epsilon)
    second_normed = (middle * second_scale * second_gain).astype(jnp.bfloat16)
    moe_rows = pair_rows(second_normed)
    slot_index = route_slots(routes, expert_count, capacity)
    send_rows = scatter_rows(spread_rows(moe_rows, TOP), slot_index, expert_count * capacity)
    arrived = send_out(send_rows.reshape(owner_count, EXP_DEV, capacity, model_width))
    gate_act = jnp.einsum(
        "secd,edf->secf", arrived, gate_weight, preferred_element_type=jnp.float32
    )
    up_act = jnp.einsum("secd,edf->secf", arrived, up_weight, preferred_element_type=jnp.float32)
    sigmoid_gate = jax.nn.sigmoid(gate_act)
    hidden = (gate_act * sigmoid_gate * up_act).astype(jnp.bfloat16)
    expert_out = jnp.einsum(
        "secf,efd->secd", hidden, down_weight, preferred_element_type=jnp.float32
    ).astype(jnp.bfloat16)
    returned = send_back(expert_out)
    picked = returned[slot_index].reshape(seq_rows, TOP, model_width).astype(jnp.float32)
    mixture = jnp.sum(gate_values[:, :, None] * picked, axis=1)
    block_output = middle + pair_sums(mixture)
    upstream_rows = lax.all_gather(upstream_grad, "tp", axis=0, tiled=True)
    route_terms = jnp.sum(upstream_rows[:, None, :] * picked, axis=2)
    routed_cot = (
        (gate_values[:, :, None] * upstream_rows[:, None, :])
        .astype(jnp.bfloat16)
        .reshape(seq_rows * TOP, model_width)
    )
    cot_send = scatter_rows(routed_cot, slot_index, expert_count * capacity)
    cot_arrived = send_out(cot_send.reshape(owner_count, EXP_DEV, capacity, model_width))
    hidden_cot = jnp.einsum(
        "secd,efd->secf", cot_arrived, down_weight, preferred_element_type=jnp.float32
    )
    down_grad = jnp.einsum(
        "secf,secd->efd", hidden, cot_arrived, preferred_element_type=jnp.float32
    )
    gate_cot = (
        hidden_cot * up_act * sigmoid_gate * (1.0 + gate_act * (1.0 - sigmoid_gate))
    ).astype(jnp.bfloat16)
    up_cot = (hidden_cot * gate_act * sigmoid_gate).astype(jnp.bfloat16)
    gate_grad = jnp.einsum("secd,secf->edf", arrived, gate_cot, preferred_element_type=jnp.float32)
    up_grad = jnp.einsum("secd,secf->edf", arrived, up_cot, preferred_element_type=jnp.float32)
    input_cot = jnp.einsum(
        "secf,edf->secd", gate_cot, gate_weight, preferred_element_type=jnp.float32
    )
    input_cot = (
        input_cot
        + jnp.einsum("secf,edf->secd", up_cot, up_weight, preferred_element_type=jnp.float32)
    ).astype(jnp.bfloat16)
    came_back = send_back(input_cot)
    normed_cot = jnp.sum(
        came_back[slot_index].reshape(seq_rows, TOP, model_width).astype(jnp.float32), axis=1
    )
    second_cot, route_grad = (
        lax.psum_scatter(
            normed_cot.astype(jnp.bfloat16), "tp", scatter_dimension=0, tiled=True
        ).astype(jnp.float32),
        lax.psum_scatter(
            route_terms.astype(jnp.bfloat16), "tp", scatter_dimension=0, tiled=True
        ).astype(jnp.float32),
    )
    weighted_two = second_cot * second_gain
    second_term = jnp.sum(second_cot * middle * second_scale, axis=0)
    middle_grad = upstream_grad + second_scale * (
        weighted_two
        - middle
        * second_scale
        * second_scale
        * jnp.mean(weighted_two * middle, axis=1, keepdims=True)
    )
    middle_rows = pair_rows(middle_grad.astype(jnp.bfloat16))
    query_full, key_full, value_full, output_full = projections(
        query_weight, key_weight, value_weight, output_weight
    )
    out_term = contract_rows(middle_rows, mixed_rows)
    mixed_cot = (
        jnp.dot(middle_rows, output_full, preferred_element_type=jnp.float32)
        .astype(jnp.bfloat16)
        .reshape(seq_rows, local_heads, HD)
    )
    scores = (
        jnp.einsum("shd,thd->hst", query_rows, key_rows, preferred_element_type=jnp.float32)
        * inv_root
    )
    soft_weights = jnp.exp(scores - log_total)
    value_cot = jnp.einsum(
        "hst,shd->thd",
        soft_weights.astype(jnp.bfloat16),
        mixed_cot,
        preferred_element_type=jnp.float32,
    )
    value_cot = value_cot.astype(jnp.bfloat16).reshape(seq_rows, head_cols)
    soft_cot = jnp.einsum("shd,thd->hst", mixed_cot, value_rows, preferred_element_type=jnp.float32)
    score_cot = (
        soft_weights
        * (soft_cot - jnp.sum(soft_weights * soft_cot, axis=2, keepdims=True))
        * inv_root
    ).astype(jnp.bfloat16)
    query_cot = (
        jnp.einsum("hst,thd->shd", score_cot, key_rows, preferred_element_type=jnp.float32)
        .astype(jnp.bfloat16)
        .reshape(seq_rows, head_cols)
    )
    key_cot = (
        jnp.einsum("hst,shd->thd", score_cot, query_rows, preferred_element_type=jnp.float32)
        .astype(jnp.bfloat16)
        .reshape(seq_rows, head_cols)
    )
    query_term = contract_rows(normed_rows, query_cot)
    key_term = contract_rows(normed_rows, key_cot)
    value_term = contract_rows(normed_rows, value_cot)
    first_terms = (
        contract_cols(query_cot, query_full)
        + contract_cols(key_cot, key_full)
        + contract_cols(value_cot, value_full)
    )
    first_cot = pair_sums(first_terms)
    weighted_one = first_cot * first_gain
    first_term = jnp.sum(first_cot * block_input * first_scale, axis=0)
    input_grad = middle_grad + first_scale * (
        weighted_one
        - block_input
        * first_scale
        * first_scale
        * jnp.mean(weighted_one * block_input, axis=1, keepdims=True)
    )
    query_grad, key_grad, value_grad, output_grad = (
        lax.psum_scatter(query_term, "fsdp", scatter_dimension=0, tiled=True),
        lax.psum_scatter(key_term, "fsdp", scatter_dimension=0, tiled=True),
        lax.psum_scatter(value_term, "fsdp", scatter_dimension=0, tiled=True),
        lax.psum_scatter(out_term, "fsdp", scatter_dimension=0, tiled=True),
    )
    first_gain_grad, second_gain_grad = lax.psum((first_term, second_term), ("fsdp", "tp"))
    return (
        block_output,
        input_grad,
        first_gain_grad,
        second_gain_grad,
        query_grad,
        key_grad,
        value_grad,
        output_grad,
        gate_grad,
        up_grad,
        down_grad,
        route_grad,
    )


MESH = pl.DeviceIdType.MESH


def place():
    here = lax.axis_index("fsdp")
    return here // 4, (here // 2) % 2, here % 2, lax.axis_index("tp")


def index_of(z, y, c):
    return (z * 2 + y) * 2 + c


LEVELS = 4
LEVEL_ORDER = sum(
    level << (8 * turn + 2 * z)
    for turn, row in enumerate(((3, 3, 0, 0), (2, 2, 1, 1), (1, 0, 3, 2), (0, 1, 2, 3)))
    for z, level in enumerate(row)
) - (1 << 32)


def level_at(turn, z):
    return (jnp.int32(LEVEL_ORDER) >> (8 * turn + 2 * z)) & 3


def line_ends(z):
    return (z + 1) // LEVELS, (LEVELS - z) // LEVELS


def plane_greet(pair=False, far=False):
    z, y, c, x = place()
    top, bottom = line_ends(z)
    barrier = pltpu.get_barrier_semaphore()
    partners = [(index_of(z, 1 - y, c), x), (index_of(z, y, 1 - c), x)]
    if pair:
        partners.append((index_of(z, y, c), 1 - x))
    if far:
        partners.append((index_of((z + 2) % LEVELS, y, c), x))
    for partner in partners:
        pl.semaphore_signal(barrier, inc=1, device_id=partner, device_id_type=MESH)

    @pl.when(top == 0)
    def _():
        above = (index_of(z + 1, y, c), x)
        pl.semaphore_signal(barrier, inc=1, device_id=above, device_id_type=MESH)

    @pl.when(bottom == 0)
    def _():
        below = (index_of(z - 1, y, c), x)
        pl.semaphore_signal(barrier, inc=1, device_id=below, device_id_type=MESH)

    pl.semaphore_wait(barrier, len(partners) + 2 - top - bottom)


def remote(src, dst, send_sem, recv_sem, target):
    return pltpu.make_async_remote_copy(
        src_ref=src,
        dst_ref=dst,
        send_sem=send_sem,
        recv_sem=recv_sem,
        device_id=target,
        device_id_type=MESH,
    )


class PlaneGather:
    def __init__(self, mine, full, send_sems, recv_sems):
        self.mine, self.full = mine, full
        self.send_sems, self.recv_sems = send_sems, recv_sems
        self.z, self.y, self.c, self.x = place()
        self.top, self.bottom = line_ends(self.z)

    def _copy(self, number, src, slot, target):
        return remote(
            src, self.full.at[slot], self.send_sems.at[number], self.recv_sems.at[slot], target
        )

    def arrived(self, slot):
        here = self.full.at[slot]
        remote(here, here, self.send_sems.at[0], self.recv_sems.at[slot], (0, self.x)).wait_recv()

    def start(self):
        z, y, c, x = self.z, self.y, self.c, self.x
        own = index_of(z, y, c)
        up = self._copy(0, self.mine, own, (index_of(z + 1, y, c), x))
        down = self._copy(1, self.mine, own, (index_of(z - 1, y, c), x))
        pl.when(self.top == 0)(up.start)
        pl.when(self.bottom == 0)(down.start)
        self._copy(2, self.mine, own, (index_of(z, 1 - y, c), x)).start()
        self._copy(3, self.mine, own, (index_of(z, y, 1 - c), x)).start()

    def from_line(self, step):
        z, y, c, x = self.z, self.y, self.c, self.x
        level = level_at(3 - step, z)
        slot = index_of(level, y, c)
        self.arrived(slot)
        onward = z + 1 - 2 * ((level + LEVELS - z) // LEVELS)
        src, number = self.full.at[slot], 4 + 3 * (step - 1)
        forward = self._copy(number, src, slot, (index_of(onward, y, c), x))
        pl.when(self.top + self.bottom == 0)(forward.start)
        self._copy(number + 1, src, slot, (index_of(z, 1 - y, c), x)).start()
        self._copy(number + 2, src, slot, (index_of(z, y, 1 - c), x)).start()

    def from_side(self, step):
        z, y, c, x = self.z, self.y, self.c, self.x
        slot = index_of(level_at(3 - step, z), 1 - y, c)
        self.arrived(slot)
        self._copy(13 + step, self.full.at[slot], slot, (index_of(z, y, 1 - c), x)).start()

    def from_core(self, step, side):
        z, y, c = self.z, self.y, self.c
        self.arrived(index_of(level_at(3 - step, z), (y + side) % 2, 1 - c))

    def finish(self):
        for number in range(GATHER_SENDS):
            wait = self._copy(number, self.mine, 0, (0, self.x)).wait_send
            if number == 0:
                pl.when(self.top == 0)(wait)
            elif number == 1:
                pl.when(self.bottom == 0)(wait)
            elif number in (4, 7, 10):
                pl.when(self.top + self.bottom == 0)(wait)
            else:
                wait()


GATHER_SENDS = 17


def attend_kernel(
    query_mine,
    key_mine,
    value_mine,
    output_mine,
    block_input,
    upstream,
    first_gain,
    routes,
    gate_values,
    gate_own,
    up_own,
    down_own,
    query_full,
    key_full,
    value_full,
    output_full,
    upstream_all,
    gates_all,
    normed_pair,
    gate_other,
    up_other,
    down_other,
    query_rows,
    key_rows,
    value_rows,
    mixed_rows,
    out_part,
    first_scale,
    weights,
    normed,
    upstream_mine,
    gates_mine,
    send_sems,
    recv_sems,
    wide_s,
    wide_r,
    own_sems,
    keep_sems,
    pair_s,
    pair_r,
):
    bf16, f32 = jnp.bfloat16, jnp.float32
    z, y, c, x = place()
    own = index_of(z, y, c)
    half_rows, width = block_input.shape
    rows, head_cols = mixed_rows.shape
    inv_root = HD ** (-0.5)
    step = 16

    mine = (query_mine, key_mine, value_mine, output_mine)
    kept = [
        pltpu.make_async_copy(mine[a], weights.at[a, own], own_sems.at[a]) for a in range(4)
    ]
    for copy in kept:
        copy.start()
    plane_greet(pair=True)
    plans = [
        PlaneGather(mine[a], weights.at[a], send_sems.at[a], recv_sems.at[a]) for a in range(4)
    ] + [
        PlaneGather(ref, full, wide_s.at[i], wide_r.at[i])
        for i, (ref, full) in enumerate(((upstream_mine, upstream_all), (gates_mine, gates_all)))
    ]
    first, output, wide = plans[:3], plans[3:4], plans[4:]
    for plan in first:
        plan.start()

    def swap(i, src, dst):
        return remote(src, dst, pair_s.at[i], pair_r.at[i], (own, 1 - x))

    swaps = [
        swap(0, normed.at[x], normed.at[x]),
        swap(1, gate_own, gate_other),
        swap(2, up_own, up_other),
        swap(3, down_own, down_other),
    ]
    gain = first_gain[...]

    @pl.loop(0, half_rows // step)
    def _(i):
        at = pl.ds(pl.multiple_of(i * step, step), step)
        value = block_input[at, :]
        scale = lax.rsqrt(jnp.mean(value * value, axis=1, keepdims=True) + epsilon)
        first_scale[at, :] = scale
        normed[x, at, :] = (value * scale * gain).astype(bf16)

    for copy in swaps:
        copy.start()

    @pl.loop(0, half_rows // step)
    def _(i):
        at = pl.ds(pl.multiple_of(i * step, step), step)
        upstream_mine[at, :] = upstream[at, :].astype(bf16)

    here = pl.ds(pl.multiple_of(x * half_rows, half_rows), half_rows)
    names, values = routes[here, :], gate_values[here, :]
    lane = lax.broadcasted_iota(jnp.int32, (half_rows, ROUTE_COLS), 1)
    table = jnp.zeros((half_rows, ROUTE_COLS), f32)
    for j in range(TOP):
        table = table + jnp.where(lane == names[:, j : j + 1], values[:, j : j + 1], 0.0)
    gates_mine[...] = table
    wide_kept = [
        pltpu.make_async_copy(upstream_mine, upstream_all.at[own], own_sems.at[4]),
        pltpu.make_async_copy(gates_mine, gates_all.at[own], own_sems.at[5]),
    ]
    for copy in wide_kept:
        copy.start()

    def line(group, turn):
        for plan in group:
            plan.from_line(turn)

    def side(group, turn):
        for plan in group:
            plan.from_side(turn)

    def core(group):
        for plan in group:
            for turn in range(LEVELS):
                for which in range(2):
                    plan.from_core(turn, which)

    line(first, 1)
    side(first, 0)
    line(first, 2)
    side(first, 1)
    line(first, 3)
    for plan in output:
        plan.start()
    side(first, 2)
    side(first, 3)
    line(output, 1)
    core(first)
    line(output, 2)
    for plan in wide:
        plan.start()
    swaps[0].wait_recv()
    for copy in kept:
        copy.wait()
    keeps = [
        pltpu.make_async_copy(src, dst, keep_sems.at[i])
        for i, (src, dst) in enumerate(
            (
                (weights.at[0], query_full),
                (weights.at[1], key_full),
                (weights.at[2], value_full),
                (normed, normed_pair),
                (weights.at[3], output_full),
            )
        )
    ]
    for copy in keeps[:4]:
        copy.start()

    def flat(ref):
        value = ref[...]
        return value.reshape(value.shape[0] * value.shape[1], value.shape[2])

    for a, ref in enumerate((query_rows, key_rows, value_rows)):
        ref[...] = nn(flat(normed), flat(weights.at[a])).astype(bf16)
        if a == 0:
            line(output, 3)
            side(output, 0)
    side(output, 1)
    line(wide, 1)

    def head(h):
        cols = pl.ds(pl.multiple_of(h * HD, HD), HD)
        scores = nt(query_rows[:, cols], key_rows[:, cols]) * inv_root
        row_top = jnp.max(scores, axis=1, keepdims=True)
        log_total = row_top + jnp.log(jnp.sum(jnp.exp(scores - row_top), axis=1, keepdims=True))
        soft = jnp.exp(scores - log_total)
        mixed_rows[:, cols] = nn(soft.astype(bf16), value_rows[:, cols]).astype(bf16)

    @pl.loop(0, head_cols // HD // 2)
    def _(h):
        head(2 * h)
        head(2 * h + 1)

    side(output, 2)
    side(output, 3)
    line(wide, 2)
    core(output)
    keeps[4].start()
    panel = 4

    @pl.loop(0, weights.shape[1] // panel)
    def _(n):
        part = weights[3, pl.ds(n * panel, panel)].reshape(panel * half_rows, head_cols)
        cols = pl.ds(pl.multiple_of(n * panel * half_rows, panel * half_rows), panel * half_rows)
        out_part[:, :, cols] = nt(mixed_rows[...], part).reshape(2, half_rows, panel * half_rows)

    side(wide, 0)
    line(wide, 3)
    for turn in range(1, LEVELS):
        side(wide, turn)
    core(wide)
    for plan in plans:
        plan.finish()
    for copy in wide_kept + keeps:
        copy.wait()
    swaps[0].wait_send()
    for copy in swaps[1:]:
        copy.wait()


def run_attend(shards, block_input, upstream, first_gain, routes, gate_values, experts, collective_id):
    bf16, f32 = jnp.bfloat16, jnp.float32
    owner_count = lax.axis_size("fsdp")
    half_rows, width = block_input.shape
    head_cols = shards[0].shape[1]
    rows = 2 * half_rows
    shape = jax.ShapeDtypeStruct
    hbm = pl.BlockSpec(memory_space=pl.ANY)
    vmem = pl.BlockSpec(memory_space=pltpu.VMEM)
    dma = pltpu.SemaphoreType.DMA
    full = (owner_count,) + shards[0].shape
    outs = pl.pallas_call(
        attend_kernel,
        out_shape=[shape(full, bf16)] * 4
        + [
            shape((owner_count, half_rows, width), bf16),
            shape((owner_count, half_rows, ROUTE_COLS), f32),
            shape((2, half_rows, width), bf16),
        ]
        + [shape(w.shape, w.dtype) for w in experts]
        + [shape((rows, head_cols), bf16)] * 4
        + [shape((2, half_rows, width), f32), shape((half_rows, 1), f32)],
        in_specs=[vmem] * 9 + [hbm] * 3,
        out_specs=[hbm] * 10 + [vmem] * 6,
        scratch_shapes=[
            pltpu.VMEM((4,) + full, bf16),
            pltpu.VMEM((2, half_rows, width), bf16),
            pltpu.VMEM((half_rows, width), bf16),
            pltpu.VMEM((half_rows, ROUTE_COLS), f32),
            dma((4, GATHER_SENDS)),
            dma((4, owner_count)),
            dma((2, GATHER_SENDS)),
            dma((2, owner_count)),
            dma((6,)),
            dma((5,)),
            dma((4,)),
            dma((4,)),
        ],
        compiler_params=pltpu.CompilerParams(
            collective_id=collective_id, has_side_effects=True, vmem_limit_bytes=60 * 2**20
        ),
        cost_estimate=pl.CostEstimate(
            flops=2 * 4 * rows * head_cols * width,
            bytes_accessed=16 * shards[0].size * owner_count,
            transcendentals=0,
        ),
        name="attend",
    )(*shards, block_input, upstream, first_gain, routes, gate_values, *experts)
    return outs[:4], outs[4:7], outs[7:10], outs[10:14], outs[14], outs[15]


class PlaneSums:
    def __init__(self, own_parts, from_core, from_side, from_line, sems, kept=0):
        self.own, self.from_core, self.kept = own_parts, from_core, kept
        self.from_side, self.from_line = from_side, from_line
        self.core_s, self.core_r, self.side_s, self.side_r, self.line_s, self.line_r = sems
        self.z, self.y, self.c, self.x = place()
        self.top, self.bottom = line_ends(self.z)

    def side_arrived(self, turn):
        here = self.from_side.at[turn]
        remote(here, here, self.side_s.at[turn], self.side_r.at[turn], (0, self.x)).wait_recv()

    def line_arrived(self, slot):
        here = self.from_line.at[slot]
        remote(here, here, self.line_s.at[0], self.line_r.at[slot], (0, self.x)).wait_recv()

    def to_line(self, turn):
        z, y, c, x = self.z, self.y, self.c, self.x
        mine = self.own.at[self.kept + turn]
        level = level_at(turn, z)

        @pl.when(self.top + self.bottom == 0)
        def _():
            self.line_arrived(level)
            add_block(mine, self.from_line.at[level], mine)

        down = (z + LEVELS - level) // (LEVELS + 1)
        onward = z + 1 - 2 * down
        reached = 1 - jnp.minimum(1, jnp.abs(onward - level))
        slot = level + down * reached * (LEVELS - level)
        copy = remote(
            mine,
            self.from_line.at[slot],
            self.line_s.at[turn],
            self.line_r.at[slot],
            (index_of(onward, y, c), x),
        )
        copy.start()


def add_block(one, two, out):
    step = 32

    @pl.loop(0, out.shape[0] // step)
    def _(i):
        rows = pl.ds(pl.multiple_of(i * step, step), step)
        value = one[rows, :].astype(jnp.float32) + two[rows, :].astype(jnp.float32)
        out[rows, :] = value.astype(out.dtype)


def total_block(plan, total):
    step = 32
    mine = plan.own.at[plan.kept + LEVELS - 1]
    below, above = plan.from_line.at[plan.z], plan.from_line.at[LEVELS]

    @pl.loop(0, total.shape[0] // step)
    def _(i):
        rows = pl.ds(pl.multiple_of(i * step, step), step)
        total[rows, :] = mine[rows, :].astype(jnp.float32)

    for end, block, slot in ((plan.bottom, below, plan.z), (plan.top, above, LEVELS)):

        @pl.when(end == 0)
        def _():
            plan.line_arrived(slot)

            @pl.loop(0, total.shape[0] // step)
            def _(i):
                rows = pl.ds(pl.multiple_of(i * step, step), step)
                total[rows, :] = total[rows, :] + block[rows, :].astype(jnp.float32)


ROUTE_COLS = 128


def nn(left, right):
    return lax.dot_general(
        left, right, (((1,), (0,)), ((), ())), preferred_element_type=jnp.float32
    )


def nt(left, right):
    return lax.dot_general(
        left, right, (((1,), (1,)), ((), ())), preferred_element_type=jnp.float32
    )


def tn(left, right):
    return lax.dot_general(
        left, right, (((0,), (0,)), ((), ())), preferred_element_type=jnp.float32
    )


def pair_block(ref, pair):
    value = ref[pl.ds(2 * pair, 2)]
    return value.reshape(value.shape[0] * value.shape[1], value.shape[2])


def experts_kernel(
    gates,
    second_gain,
    out_part,
    block_input,
    upstream,
    upstream_hbm,
    gate_own,
    up_own,
    down_own,
    gate_other,
    up_other,
    down_other,
    middle,
    middle_grad,
    second_term,
    mixture_hbm,
    gate_mine,
    gate_theirs,
    up_mine,
    up_theirs,
    down_mine,
    down_theirs,
    down_landed,
    rows_all,
    u_all,
    wg,
    wu,
    wd,
    hidden,
    gcot,
    ucot,
    rext,
    tmp,
    from_core,
    from_side,
    from_line,
    gstage,
    wide,
    second_scale,
    route_half,
    gather_s,
    gather_r,
    core_s,
    core_r,
    side_s,
    side_r,
    line_s,
    line_r,
    load_sems,
    out_sems,
    pair_s,
    pair_r,
):
    bf16, f32 = jnp.bfloat16, jnp.float32
    z, y, c, x = place()
    top, bottom = line_ends(z)
    interior = 1 - top - bottom
    me = lax.axis_index("fsdp")
    partner = (me, 1 - x)
    halves, width, units = wg.shape
    half_rows = middle.shape[0]
    pair_rows_ = 2 * half_rows
    pairs = 2 * LEVELS
    panel = 512
    block = 256
    step = 16

    loads = [
        pltpu.make_async_copy(src, dst, load_sems.at[i])
        for i, (src, dst) in enumerate(
            (
                (out_part.at[1 - x], middle_grad),
                (out_part.at[x], middle),
                (block_input, wide),
                (down_own, wd.at[x]),
                (down_other, wd.at[1 - x]),
                (upstream_hbm, u_all),
                (gate_own, wg.at[x]),
                (up_own, wu.at[x]),
                (gate_other, wg.at[1 - x]),
                (up_other, wu.at[1 - x]),
            )
        )
    ]
    for load in loads:
        load.start()

    plane_greet(pair=True)
    gather = PlaneGather(rows_all.at[me], rows_all, gather_s, gather_r)
    sums = PlaneSums(
        from_core,
        from_core,
        from_side,
        from_line,
        (core_s, core_r, side_s, side_r, line_s, line_r),
        LEVELS,
    )

    loads[0].wait()

    @pl.loop(0, half_rows // step)
    def _(i):
        at = pl.ds(pl.multiple_of(i * step, step), step)
        tmp[0, 0, at, :] = middle_grad[at, :].astype(bf16)

    meet = remote(tmp.at[0, 0], tmp.at[0, 1], pair_s.at[0], pair_r.at[0], partner)
    meet.start()
    for load in loads[1:6]:
        load.wait()

    @pl.loop(0, pairs)
    def _(b):
        at_rows = pl.ds(pl.multiple_of(b * pair_rows_, pair_rows_), pair_rows_)
        us = pair_block(u_all, b)
        for h in range(halves):
            ucot[h, at_rows, :] = nt(us, wd[h]).astype(bf16)

    meet.wait()
    gain = second_gain[...]

    @pl.loop(0, half_rows // step)
    def _(i):
        at = pl.ds(pl.multiple_of(i * step, step), step)
        value = wide[at, :] + (middle[at, :] + tmp[0, 1, at, :].astype(f32))
        scale = lax.rsqrt(jnp.mean(value * value, axis=1, keepdims=True) + epsilon)
        middle[at, :] = value
        second_scale[at, :] = scale
        rows_all[me, at, :] = (value * scale * gain).astype(bf16)

    gather.start()
    again = pltpu.make_async_copy(upstream, wide, load_sems.at[2])
    again.start()
    for load in loads[6:]:
        load.wait()

    def forward_pair(b):
        turn = (0b11_10_11_01_10_00_01_00 >> (2 * b)) % 4
        side = (0b11_01_01_00 >> b) % 2
        return level_at(3 - turn, z) * 2 + (y + side) % 2

    def mixture_out(b):
        return pltpu.make_async_copy(
            tmp.at[b % 2],
            mixture_hbm.at[pl.ds(2 * forward_pair(b), 2), :, pl.ds(0, width)],
            out_sems.at[b % 2],
        )

    @pl.loop(0, 2 * pairs)
    def _(turn):
        b, h = turn // 2, turn % 2

        def at(k, work, where=None):
            @pl.when(turn == k)
            def _():
                if where is None:
                    work()
                else:
                    pl.when(where == 1)(work)

        at(0, lambda: gather.from_core(0, 0))
        at(2, lambda: gather.from_line(1))
        at(2, lambda: gather.from_line(2), interior)
        at(2, lambda: gather.from_core(1, 0))
        at(4, lambda: gather.from_side(0))
        at(4, lambda: gather.from_core(0, 1))
        at(6, lambda: gather.from_line(2), 1 - interior)
        at(6, lambda: gather.from_line(3), interior)
        at(6, lambda: gather.from_core(2, 0))
        at(8, lambda: gather.from_side(1))
        at(8, lambda: gather.from_core(1, 1))
        at(10, lambda: gather.from_line(3), 1 - interior)
        at(10, lambda: gather.from_core(3, 0))
        at(12, lambda: gather.from_side(2))
        at(12, lambda: gather.from_core(2, 1))
        at(14, lambda: gather.from_side(3))
        at(14, lambda: gather.from_core(3, 1))

        pair = forward_pair(b)
        xs = pair_block(rows_all, pair)
        lane = lax.broadcasted_iota(jnp.int32, (pair_rows_, ROUTE_COLS), 1)
        table = gates[pl.ds(2 * pair, 2)].reshape(pair_rows_, ROUTE_COLS)
        gate_rows = jnp.sum(jnp.where(lane == me, table, 0.0), axis=1, keepdims=True)
        gate_act = nn(xs, wg[h])
        up_act = nn(xs, wu[h])
        at_rows = pl.ds(pl.multiple_of(pair * pair_rows_, pair_rows_), pair_rows_)
        hidden_cot = ucot[h, at_rows, :].astype(f32)
        sig = lax.logistic(gate_act)
        act = gate_act * sig
        hid = act * up_act
        hidden[h, at_rows, :] = (hid * gate_rows).astype(bf16)
        route = jnp.sum(hid * hidden_cot, axis=1, keepdims=True)
        scaled = hidden_cot * gate_rows
        gcot[h, at_rows, :] = (scaled * up_act * (sig * (1.0 + gate_act * (1.0 - sig)))).astype(bf16)
        ucot[h, at_rows, :] = (scaled * act).astype(bf16)

        @pl.when(h == 0)
        def _():
            route_half[...] = route

        @pl.when(h == 1)
        def _():
            total = route_half[...] + route
            placed = jnp.where(lane == me, total, 0.0).astype(bf16)
            rext[pl.ds(2 * pair, 2)] = placed.reshape(2, half_rows, ROUTE_COLS)

            pl.when(b >= 2)(lambda: mixture_out(b - 2).wait())

            @pl.loop(0, width // panel)
            def _(n):
                cols = pl.ds(pl.multiple_of(n * panel, panel), panel)
                acc = nn(hidden[0, at_rows, :], wd[0, :, cols])
                for h in range(1, halves):
                    acc = acc + nn(hidden[h, at_rows, :], wd[h, :, cols])
                tmp[b % 2, :, :, cols] = acc.astype(bf16).reshape(2, half_rows, panel)

            mixture_out(b).start()

    for b in (pairs - 2, pairs - 1):
        mixture_out(b).wait()

    def core_send(b):
        return remote(
            tmp.at[b % 2, 1 - c],
            from_core.at[b],
            core_s.at[b],
            core_r.at[b],
            (index_of(z, y, 1 - c), x),
        )

    def take_core(b):
        core_send(b).wait_recv()
        add_block(tmp.at[b % 2, c], from_core.at[b], from_core.at[b])

        @pl.when(b < LEVELS)
        def _():
            remote(
                from_core.at[b],
                from_side.at[b],
                side_s.at[b],
                side_r.at[b],
                (index_of(z, 1 - y, c), x),
            ).start()

    def line_step(turn):
        sums.side_arrived(turn)
        mine = from_core.at[LEVELS + turn]
        add_block(mine, from_side.at[turn], mine)
        if turn < LEVELS - 1:
            sums.to_line(turn)

    def last_step():
        line_step(LEVELS - 1)
        total_block(sums, middle_grad)
        again.wait()
        second_term[...] = jnp.zeros_like(second_term)

        @pl.loop(0, half_rows // step)
        def _(i):
            at = pl.ds(pl.multiple_of(i * step, step), step)
            cot, mid, scale = middle_grad[at, :], middle[at, :], second_scale[at, :]
            weighted = cot * gain
            mean = jnp.mean(weighted * mid, axis=1, keepdims=True)
            value = wide[at, :] + scale * (weighted - mid * (scale * scale * mean))
            middle_grad[at, :] = value
            second_term[...] = second_term[...] + jnp.sum(cot * mid * scale, axis=0, keepdims=True)

    @pl.loop(0, pairs)
    def _(b):
        pl.when((b == pairs - 1) & (interior == 0))(lambda: line_step(0))
        pl.when(b >= 2)(lambda: core_send(b - 2).wait_send())
        pair = level_at(b % LEVELS, z) * 2 + (y + 1 - b // LEVELS) % 2
        at_rows = pl.ds(pl.multiple_of(pair * pair_rows_, pair_rows_), pair_rows_)

        @pl.loop(0, width // panel)
        def _(n):
            cols = pl.ds(pl.multiple_of(n * panel, panel), panel)
            acc = nt(gcot[0, at_rows, :], wg[0, cols, :])
            acc = acc + nt(ucot[0, at_rows, :], wu[0, cols, :])
            for h in range(1, halves):
                acc = acc + nt(gcot[h, at_rows, :], wg[h, cols, :])
                acc = acc + nt(ucot[h, at_rows, :], wu[h, cols, :])
            tmp[b % 2, :, :, cols] = acc.astype(bf16).reshape(2, half_rows, panel)

        core_send(b).start()
        pl.when(b >= 1)(lambda: take_core(b - 1))

    take_core(pairs - 1)
    for b in (pairs - 2, pairs - 1):
        core_send(b).wait_send()

    route_out = pltpu.make_async_copy(
        rext, mixture_hbm.at[:, :, pl.ds(width, ROUTE_COLS)], load_sems.at[1]
    )
    route_out.start()
    down_send = remote(
        wd.at[0, pl.ds(0, block)], down_landed, pair_s.at[1], pair_r.at[1], partner
    )
    down_later = pltpu.make_async_copy(wd.at[0, pl.ds(block, block)], down_theirs, load_sems.at[3])
    down_keep = pltpu.make_async_copy(wd.at[1], down_mine, load_sems.at[4])

    @pl.loop(0, 2 * units // block)
    def _(p):
        other, q = p // (units // block), p % (units // block)
        pl.when((p == 1) & (interior == 0))(lambda: line_step(1))
        pl.when((p == 2) & (interior == 1))(lambda: line_step(0))
        units_at = pl.ds(pl.multiple_of(q * block, block), block)
        us = u_all[...]
        us = us.reshape(us.shape[0] * us.shape[1], width)
        h = (1 - x) * (1 - other) + x * other
        wd[other, units_at, :] = tn(hidden[h, :, units_at], us).astype(bf16)
        pl.when(p == 0)(down_send.start)
        pl.when(p == 1)(down_later.start)

    down_keep.start()

    def part_outs(p):
        rows = pl.ds(pl.multiple_of(p * block, block), block)
        return [
            pltpu.make_async_copy(
                gstage.at[p % 2, which, k], ref.at[rows, :], out_sems.at[(p % 2) * 4 + 2 * which + k]
            )
            for which, refs in enumerate(((gate_mine, gate_theirs), (up_mine, up_theirs)))
            for k, ref in enumerate(refs)
        ]

    def wait_outs(p):
        for copy in part_outs(p):
            copy.wait()

    @pl.loop(0, width // block)
    def _(p):
        pl.when((p == 1) & (interior == 0))(lambda: line_step(2))
        pl.when((p == 1) & (interior == 1))(lambda: line_step(1))
        pl.when((p == 2) & (interior == 1))(lambda: line_step(2))
        pl.when(p == 6)(last_step)
        pl.when(p >= 2)(lambda: wait_outs(p - 2))
        cols = pl.ds(pl.multiple_of(p * block, block), block)
        xp = rows_all[:, :, cols]
        xp = xp.reshape(xp.shape[0] * xp.shape[1], block)
        for which, ref in enumerate((gcot, ucot)):
            for k, h in enumerate((x, 1 - x)):
                gstage[p % 2, which, k] = tn(xp, ref[h]).astype(bf16)
        for copy in part_outs(p):
            copy.start()

    for p in (width // block - 2, width // block - 1):
        wait_outs(p)
    route_out.wait()
    down_send.wait()
    down_later.wait()
    down_keep.wait()
    gather.finish()
    for turn in range(LEVELS):
        remote(
            from_core.at[turn], from_side.at[turn], side_s.at[turn], side_r.at[turn], partner
        ).wait_send()
    for turn in range(LEVELS - 1):
        remote(
            from_core.at[turn], from_line.at[turn], line_s.at[turn], line_r.at[turn], partner
        ).wait_send()


def run_experts(
    gates, second_gain, out_part, block_input, upstream, upstream_all, own, other, collective_id
):
    bf16, f32 = jnp.bfloat16, jnp.float32
    block = block_input.shape
    half_rows, width = block
    owner_count = upstream_all.shape[0]
    units = own[0].shape[1]
    halves = lax.axis_size("tp")
    all_rows = owner_count * half_rows
    hbm = pl.BlockSpec(memory_space=pl.ANY)
    vmem = pl.BlockSpec(memory_space=pltpu.VMEM)
    dma = pltpu.SemaphoreType.DMA
    flops = 2 * 9 * all_rows * width * units * halves
    shape = jax.ShapeDtypeStruct
    return pl.pallas_call(
        experts_kernel,
        out_shape=[
            shape(block, f32),
            shape(block, f32),
            shape((1, width), f32),
            shape((owner_count, half_rows, width + ROUTE_COLS), bf16),
        ]
        + [shape((width, units), bf16)] * 4
        + [shape((units, width), bf16)]
        + [shape((256, width), bf16)] * 2,
        in_specs=[vmem, vmem] + [hbm] * 10,
        out_specs=[vmem] * 3 + [hbm] * 8,
        scratch_shapes=[
            pltpu.VMEM((owner_count,) + block, bf16),
            pltpu.VMEM((owner_count,) + block, bf16),
            pltpu.VMEM((halves, width, units), bf16),
            pltpu.VMEM((halves, width, units), bf16),
            pltpu.VMEM((halves, units, width), bf16),
            pltpu.VMEM((halves, all_rows, units), bf16),
            pltpu.VMEM((halves, all_rows, units), bf16),
            pltpu.VMEM((halves, all_rows, units), bf16),
            pltpu.VMEM((owner_count, half_rows, ROUTE_COLS), bf16),
            pltpu.VMEM((2, 2) + block, bf16),
            pltpu.VMEM((2 * LEVELS,) + block, bf16),
            pltpu.VMEM((LEVELS,) + block, bf16),
            pltpu.VMEM((LEVELS + 1,) + block, bf16),
            pltpu.VMEM((2, 2, halves, 256, units), bf16),
            pltpu.VMEM(block, f32),
            pltpu.VMEM((half_rows, 1), f32),
            pltpu.VMEM((2 * half_rows, 1), f32),
            dma((GATHER_SENDS,)),
            dma((owner_count,)),
            dma((2 * LEVELS,)),
            dma((2 * LEVELS,)),
            dma((LEVELS,)),
            dma((LEVELS,)),
            dma((LEVELS + 1,)),
            dma((LEVELS + 1,)),
            dma((10,)),
            dma((8,)),
            dma((2,)),
            dma((2,)),
        ],
        compiler_params=pltpu.CompilerParams(
            collective_id=collective_id, has_side_effects=True, vmem_limit_bytes=67_043_328
        ),
        cost_estimate=pl.CostEstimate(
            flops=flops, bytes_accessed=64 * 2**20, transcendentals=all_rows * units * halves
        ),
        name="experts",
    )(gates, second_gain, out_part, block_input, upstream, upstream_all, *own, *other)


def last_kernel(
    mixture_part,
    normed_pair,
    mixed_rows,
    query_rows,
    key_rows,
    value_rows,
    output_full,
    query_full,
    key_full,
    value_full,
    gate_theirs,
    up_theirs,
    down_theirs,
    block_input,
    first_scale,
    first_gain,
    middle_grad,
    second_term,
    query_total,
    key_total,
    value_total,
    output_total,
    mixture_total,
    gate_landed,
    up_landed,
    down_landed,
    input_grad,
    gain_grads,
    wide_core,
    wide_side,
    wide_line,
    wide_own,
    from_core,
    from_side,
    from_line,
    tmp,
    middle_pair,
    mixed_cot,
    query_cot,
    key_cot,
    value_cot,
    weight_one,
    weight_two,
    first_terms,
    first_mine,
    first_other,
    gains,
    gains_in,
    core_s,
    core_r,
    side_s,
    side_r,
    line_s,
    line_r,
    own_sems,
    load_sems,
    pair_s,
    pair_r,
    gain_s,
    gain_r,
):
    bf16, f32 = jnp.bfloat16, jnp.float32
    z, y, c, x = place()
    own = index_of(z, y, c)
    rows, head_cols = mixed_rows.shape
    half_rows, width = input_grad.shape
    pairs = 2 * LEVELS
    inv_root = HD ** (-0.5)
    plane_greet(pair=True, far=True)

    def swap(i, src, dst):
        return remote(src, dst, pair_s.at[i], pair_r.at[i], (own, 1 - x))

    expert_swaps = (
        swap(0, gate_theirs, gate_landed),
        swap(1, up_theirs, up_landed),
        swap(2, down_theirs, down_landed),
    )
    first_swap = swap(3, first_mine, first_other)

    def load(i, src, dst):
        return pltpu.make_async_copy(src, dst, load_sems.at[i])

    output_load, query_load = load(0, output_full, weight_one), load(1, query_full, weight_two)
    value_load, key_load = load(2, value_full, weight_one), load(3, key_full, weight_two)
    sums = [
        PlaneSums(
            core,
            core,
            side,
            line,
            tuple(s.at[a] for s in (core_s, core_r, side_s, side_r, line_s, line_r)),
            LEVELS,
        )
        for a, (core, side, line) in enumerate(
            [(wide_core, wide_side, wide_line)]
            + [(from_core.at[i], from_side.at[i], from_line.at[i]) for i in range(4)]
        )
    ]

    def slot_at(b, core):
        level, side = level_at(b % LEVELS, z), (y + 1 - b // LEVELS) % 2
        return index_of(level, side, (c + core) % 2)

    def core_copy(a, b, src):
        plan = sums[a]
        return remote(
            src,
            plan.from_core.at[b],
            plan.core_s.at[b],
            plan.core_r.at[b],
            (index_of(z, y, 1 - c), x),
        )

    def side_copy(a, b):
        plan = sums[a]
        return remote(
            plan.from_core.at[b],
            plan.from_side.at[b],
            plan.side_s.at[b],
            plan.side_r.at[b],
            (index_of(z, 1 - y, c), x),
        )

    def line_step(a, turn):
        plan = sums[a]
        plan.side_arrived(turn)
        mine = plan.from_core.at[LEVELS + turn]
        add_block(mine, plan.from_side.at[turn], mine)
        if turn < LEVELS - 1:
            plan.to_line(turn)

    @pl.loop(0, half_rows // 16)
    def _(i):
        at = pl.ds(pl.multiple_of(i * 16, 16), 16)
        middle_pair[x, at, :] = middle_grad[at, :].astype(bf16)

    middle_swap = swap(4, middle_pair.at[x], middle_pair.at[x])
    middle_swap.start()
    for copy in expert_swaps[:2]:
        copy.start()
    output_load.start()
    query_load.start()

    def wide_load(b):
        return pltpu.make_async_copy(
            mixture_part.at[slot_at(b, 0)], wide_own.at[b], own_sems.at[b]
        )

    @pl.loop(0, pairs)
    def _(b):
        core_copy(0, b, mixture_part.at[slot_at(b, 1)]).start()
        wide_load(b).start()

    @pl.loop(0, pairs)
    def _(b):
        wide_load(b).wait()
        core_copy(0, b, mixture_part.at[slot_at(b, 1)]).wait_recv()
        add_block(wide_own.at[b], wide_core.at[b], wide_core.at[b])
        pl.when(b < LEVELS)(lambda: side_copy(0, b).start())

    def flat(ref):
        value = ref[...]
        return value.reshape(value.shape[0] * value.shape[1], value.shape[2])

    output_load.wait()
    middle_swap.wait()
    mixed_cot[...] = nn(flat(middle_pair), flat(weight_one)).astype(bf16)
    value_load.start()

    def term(a, left, cot):
        def send(b):
            return core_copy(a, b, tmp.at[b % 2, 1 - c])

        def take(b):
            core = sums[a].from_core.at[b]
            send(b).wait_recv()
            add_block(tmp.at[b % 2, c], core, core)
            pl.when(b < LEVELS)(lambda: side_copy(a, b).start())

        @pl.loop(0, pairs)
        def _(b):
            pl.when(b >= 2)(lambda: send(b - 2).wait_send())
            pair = level_at(b % LEVELS, z) * 2 + (y + 1 - b // LEVELS) % 2
            cols = pl.ds(pl.multiple_of(pair * 2 * half_rows, 2 * half_rows), 2 * half_rows)
            lhs = left[:, :, cols].reshape(rows, 2 * half_rows)
            part = tn(lhs, cot[...])
            tmp[b % 2] = part.astype(bf16).reshape(2, half_rows, head_cols)
            send(b).start()
            pl.when(b >= 1)(lambda: take(b - 1))

        take(pairs - 1)
        for b in (pairs - 2, pairs - 1):
            send(b).wait_send()

    top, bottom = line_ends(z)
    interior = 1 - top - bottom

    def head(h):
        cols = pl.ds(pl.multiple_of(h * HD, HD), HD)
        query, key, value = query_rows[:, cols], key_rows[:, cols], value_rows[:, cols]
        mixed = mixed_cot[:, cols]
        scores = nt(query, key) * inv_root
        row_top = jnp.max(scores, axis=1, keepdims=True)
        log_total = row_top + jnp.log(jnp.sum(jnp.exp(scores - row_top), axis=1, keepdims=True))
        soft = jnp.exp(scores - log_total)
        value_cot[:, cols] = tn(soft.astype(bf16), mixed).astype(bf16)
        soft_cot = nt(mixed, value)
        inner = jnp.sum(soft * soft_cot, axis=1, keepdims=True)
        score_cot = (soft * (soft_cot - inner) * inv_root).astype(bf16)
        query_cot[:, cols] = nn(score_cot, key).astype(bf16)
        key_cot[:, cols] = tn(score_cot, query).astype(bf16)

    term(1, middle_pair, mixed_rows)

    @pl.when(interior == 0)
    def _():
        line_step(0, 0)
        line_step(0, 1)

    @pl.loop(0, head_cols // HD // 2)
    def _(h):
        pl.when((h == 1) & (interior == 1))(lambda: line_step(0, 0))
        head(2 * h)
        head(2 * h + 1)

    pl.when(interior == 1)(lambda: line_step(0, 1))
    line_step(0, 2)
    term(2, normed_pair, value_cot)
    line_step(0, 3)
    term(3, normed_pair, query_cot)
    line_step(1, 0)
    line_step(1, 1)
    term(4, normed_pair, key_cot)
    line_step(1, 2)
    line_step(1, 3)

    panel = 4

    def first_add(cot, weight, begin):
        @pl.loop(0, weight.shape[0] // panel)
        def _(n):
            part = weight[pl.ds(n * panel, panel)].reshape(panel * half_rows, head_cols)
            cols = pl.ds(pl.multiple_of(n * panel * half_rows, panel * half_rows), panel * half_rows)
            value = nt(cot[...], part).reshape(2, half_rows, panel * half_rows)
            if begin:
                first_terms[:, :, cols] = value
            else:
                first_terms[:, :, cols] = first_terms[:, :, cols] + value

    query_load.wait()
    first_add(query_cot, weight_two, True)
    key_load.start()
    value_load.wait()
    first_add(value_cot, weight_one, False)
    key_load.wait()
    first_add(key_cot, weight_two, False)
    step = 16

    @pl.loop(0, half_rows // step)
    def _(i):
        at = pl.ds(pl.multiple_of(i * step, step), step)
        first_mine[at, :] = first_terms[1 - x, at, :].astype(bf16)

    first_swap.start()
    total_block(sums[0], mixture_total)
    for turn in range(LEVELS):
        line_step(2, turn)
    total_block(sums[1], output_total)
    line_step(3, 0)
    line_step(3, 1)
    first_swap.wait_recv()
    gain = first_gain[...]
    gains[...] = jnp.concatenate(
        [jnp.zeros((1, width), f32), second_term[...], jnp.zeros((6, width), f32)], axis=0
    )

    @pl.loop(0, half_rows // step)
    def _(i):
        at = pl.ds(pl.multiple_of(i * step, step), step)
        value = first_terms[x, at, :] + first_other[at, :].astype(f32)
        entry, scale = block_input[at, :], first_scale[at, :]
        weighted = value * gain
        mean = jnp.mean(weighted * entry, axis=1, keepdims=True)
        input_grad[at, :] = middle_grad[at, :] + scale * (weighted - entry * (scale * scale * mean))
        gains[0:1, :] = gains[0:1, :] + jnp.sum(value * entry * scale, axis=0, keepdims=True)

    hops = [
        (index_of(z, y, 1 - c), x),
        (own, 1 - x),
        (index_of(z + 1 - 2 * (z % 2), y, c), x),
        (index_of((z + 2) % LEVELS, y, c), x),
        (index_of(z, 1 - y, c), x),
    ]

    def gain_copy(i):
        return remote(gains, gains_in.at[i], gain_s.at[i], gain_r.at[i], hops[i])

    def gain_add(i):
        gain_copy(i).wait()
        gains[...] = gains[...] + gains_in[i]

    for i in range(2):
        gain_copy(i).start()
        gain_add(i)
    expert_swaps[2].start()
    gain_copy(2).start()
    line_step(3, 2)
    line_step(3, 3)
    gain_add(2)
    gain_copy(3).start()
    total_block(sums[2], value_total)
    line_step(4, 0)
    gain_add(3)
    gain_copy(4).start()
    for turn in range(1, LEVELS):
        line_step(4, turn)
    total_block(sums[3], query_total)
    gain_add(4)
    gain_grads[...] = gains[...]
    total_block(sums[4], key_total)

    @pl.loop(0, pairs)
    def _(b):
        core_copy(0, b, mixture_part.at[slot_at(b, 1)]).wait_send()

    for a in range(5):
        for turn in range(LEVELS):
            side_copy(a, turn).wait_send()
        line = sums[a].from_line
        for turn in range(LEVELS - 1):
            remote(
                line.at[0], line.at[turn], sums[a].line_s.at[turn], sums[a].line_r.at[turn], (own, 1 - x)
            ).wait_send()
    first_swap.wait_send()
    for copy in expert_swaps:
        copy.wait()


def run_last(
    mixture_part, normed_pair, attention_rows, weights_full, theirs, norm_args, collective_id
):
    f32, bf16 = jnp.float32, jnp.bfloat16
    shape = jax.ShapeDtypeStruct
    hbm = pl.BlockSpec(memory_space=pl.ANY)
    vmem = pl.BlockSpec(memory_space=pltpu.VMEM)
    dma = pltpu.SemaphoreType.DMA
    rows, head_cols = attention_rows[0].shape
    half_rows, width = norm_args[0].shape
    wide = mixture_part.shape[1:]
    block = (half_rows, head_cols)
    pairs = 2 * LEVELS
    flops = 2 * rows * head_cols * width * 8
    nbytes = 2 * (mixture_part.size + 12 * weights_full[0].size)
    outs = pl.pallas_call(
        last_kernel,
        out_shape=[shape(block, f32)] * 4
        + [shape(wide, f32)]
        + [shape(t.shape, t.dtype) for t in theirs]
        + [shape((half_rows, width), f32), shape((8, width), f32)],
        in_specs=[hbm] + [vmem] * 5 + [hbm] * 7 + [vmem] * 5,
        out_specs=[vmem] * 5 + [hbm] * 3 + [vmem] * 2,
        scratch_shapes=[
            pltpu.VMEM((pairs,) + wide, bf16),
            pltpu.VMEM((LEVELS,) + wide, bf16),
            pltpu.VMEM((LEVELS + 1,) + wide, bf16),
            pltpu.VMEM((pairs,) + wide, bf16),
            pltpu.VMEM((4, pairs) + block, bf16),
            pltpu.VMEM((4, LEVELS) + block, bf16),
            pltpu.VMEM((4, LEVELS + 1) + block, bf16),
            pltpu.VMEM((2, 2) + block, bf16),
            pltpu.VMEM((2, half_rows, width), bf16),
        ]
        + [pltpu.VMEM((rows, head_cols), bf16)] * 4
        + [pltpu.VMEM(weights_full[0].shape, bf16)] * 2
        + [
            pltpu.VMEM((2, half_rows, width), f32),
            pltpu.VMEM((half_rows, width), bf16),
            pltpu.VMEM((half_rows, width), bf16),
            pltpu.VMEM((8, width), f32),
            pltpu.VMEM((5, 8, width), f32),
        ]
        + [dma((5, pairs))] * 2
        + [dma((5, LEVELS))] * 2
        + [dma((5, LEVELS + 1))] * 2
        + [dma((pairs,)), dma((4,)), dma((5,)), dma((5,)), dma((5,)), dma((5,))],
        compiler_params=pltpu.CompilerParams(
            collective_id=collective_id, has_side_effects=True, vmem_limit_bytes=67_043_328
        ),
        cost_estimate=pl.CostEstimate(flops=flops, bytes_accessed=nbytes, transcendentals=0),
        name="last",
    )(mixture_part, normed_pair, *attention_rows, *weights_full, *theirs, *norm_args)
    return outs[:5], outs[5:8], outs[8], outs[9]


def gate_columns(route_rows, gate_rows, expert_count):
    names = jnp.arange(expert_count, dtype=jnp.int32)[None, None, :]
    return jnp.sum(jnp.where(route_rows[:, :, None] == names, gate_rows[:, :, None], 0.0), axis=1)


def half_of(rows):
    count = rows.shape[0] // lax.axis_size("tp")
    return lax.dynamic_slice_in_dim(rows, lax.axis_index("tp") * count, count, axis=0)


def per_device_dense(
    block_input,
    upstream_grad,
    first_gain,
    second_gain,
    query_weight,
    key_weight,
    value_weight,
    output_weight,
    gate_weight,
    up_weight,
    down_weight,
    routes,
    gate_values,
):
    local_rows, model_width = block_input.shape
    expert_count = EXP_DEV * lax.axis_size("fsdp")
    f32 = jnp.float32
    my_routes = half_of(routes)
    expert_names = jnp.arange(expert_count, dtype=jnp.int32)[None, :]
    own_weights = (gate_weight[0], up_weight[0], down_weight[0])
    weights_full, gathered, other_weights, attention_rows, out_part, first_scale = run_attend(
        (query_weight, key_weight, value_weight, output_weight),
        block_input,
        upstream_grad,
        first_gain[None],
        routes,
        gate_values,
        own_weights,
        1,
    )
    query_full, key_full, value_full, output_full = weights_full
    query_rows, key_rows, value_rows, mixed_rows = attention_rows
    upstream_all, gates_all, normed_pair = gathered
    (
        middle,
        middle_grad,
        second_term,
        mixture_part,
        gate_mine,
        gate_theirs,
        up_mine,
        up_theirs,
        down_mine,
        down_theirs,
        down_landed,
    ) = run_experts(
        gates_all,
        second_gain[None],
        out_part,
        block_input,
        upstream_grad,
        upstream_all,
        own_weights,
        other_weights,
        2,
    )
    sums, landed, input_grad, gain_grads = run_last(
        mixture_part,
        normed_pair,
        (mixed_rows, query_rows, key_rows, value_rows),
        (output_full, query_full, key_full, value_full),
        (gate_theirs, up_theirs, down_theirs),
        (block_input, first_scale, first_gain[None], middle_grad, second_term),
        4,
    )
    query_grad, key_grad, value_grad, output_grad, mixture = sums
    gate_grad, up_grad, down_grad = (
        mine.astype(f32) + theirs.astype(f32)
        for mine, theirs in (
            (gate_mine, landed[0]),
            (up_mine, landed[1]),
            (down_mine, jnp.concatenate([down_landed, landed[2]], axis=0)),
        )
    )
    block_output = middle + mixture[:, :model_width]
    route_back = mixture[:, model_width : model_width + expert_count]
    route_grad = jnp.sum(
        jnp.where(my_routes[:, :, None] == expert_names[None], route_back[:, None, :], 0.0), axis=2
    )
    return (
        block_output,
        input_grad,
        gain_grads[0],
        gain_grads[1],
        query_grad,
        key_grad,
        value_grad,
        output_grad,
        gate_grad[None],
        up_grad[None],
        down_grad[None],
        route_grad,
    )


def solution(mesh):
    dense = 2 * TOP >= EXP_DEV * mesh.shape["fsdp"] and mesh.shape["fsdp"] == 4 * LEVELS
    per_device = per_device_dense if dense else per_device_slots
    in_specs = (
        P(("fsdp", "tp"), None),
        P(("fsdp", "tp"), None),
        P(),
        P(),
        P("fsdp", "tp"),
        P("fsdp", "tp"),
        P("fsdp", "tp"),
        P("fsdp", "tp"),
        P("fsdp", None, "tp"),
        P("fsdp", None, "tp"),
        P("fsdp", "tp", None),
        P("fsdp", None),
        P("fsdp", None),
    )
    out_specs = (
        P(("fsdp", "tp"), None),
        P(("fsdp", "tp"), None),
        P(),
        P(),
        P("fsdp", "tp"),
        P("fsdp", "tp"),
        P("fsdp", "tp"),
        P("fsdp", "tp"),
        P("fsdp", None, "tp"),
        P("fsdp", None, "tp"),
        P("fsdp", "tp", None),
        P(("fsdp", "tp"), None),
    )
    return jax.shard_map(
        per_device, mesh=mesh, in_specs=in_specs, out_specs=out_specs, check_vma=False
    )
```

```python
import functools

import jax
import jax.numpy as jnp
from jax import lax
from jax.experimental import pallas as pl
from jax.experimental.pallas import tpu as pltpu
from jax.sharding import PartitionSpec as P

HD = 128
TOP = 8
EXP_DEV = 1


epsilon = 1e-05


def route_slots(route_rows, expert_count, capacity):
    flat_routes = route_rows.reshape(-1)
    onehot = (flat_routes[:, None] == jnp.arange(expert_count, dtype=jnp.int32)[None, :]).astype(
        jnp.int32
    )
    earlier = jnp.cumsum(onehot, axis=0, dtype=jnp.int32) - onehot
    ranked = jnp.sum(earlier * onehot, axis=1, dtype=jnp.int32)
    return flat_routes * capacity + ranked


def pair_rows(row_block):
    return lax.all_gather(row_block, "tp", axis=0, tiled=True)


def pair_sums(term_block):
    return lax.psum_scatter(term_block, "tp", scatter_dimension=0, tiled=True)


def to_owners(buffer):
    return lax.all_to_all(buffer, "fsdp", split_axis=0, concat_axis=0, tiled=True)


def to_sources(buffer):
    return lax.all_to_all(buffer, "fsdp", split_axis=0, concat_axis=0, tiled=True)


def projections(query_weight, key_weight, value_weight, output_weight):
    return (
        lax.all_gather(query_weight, "fsdp", axis=0, tiled=True),
        lax.all_gather(key_weight, "fsdp", axis=0, tiled=True),
        lax.all_gather(value_weight, "fsdp", axis=0, tiled=True),
        lax.all_gather(output_weight, "fsdp", axis=0, tiled=True),
    )


def scatter_rows(row_block, slot_index, total_rows):
    return (
        jnp.zeros((total_rows, row_block.shape[1]), row_block.dtype).at[slot_index].set(row_block)
    )


def spread_rows(row_block, copies):
    return jnp.broadcast_to(
        row_block[:, None, :], (row_block.shape[0], copies, row_block.shape[1])
    ).reshape(-1, row_block.shape[1])


def contract_rows(left_block, right_block):
    return lax.dot_general(
        left_block, right_block, (((0,), (0,)), ((), ())), preferred_element_type=jnp.float32
    )


def contract_cols(left_block, right_block):
    return lax.dot_general(
        left_block, right_block, (((1,), (1,)), ((), ())), preferred_element_type=jnp.float32
    )


def send_out(full_buffer):
    return to_owners(full_buffer)


def send_back(group_parts):
    owner_count, local_experts, capacity, model_width = group_parts.shape
    return to_sources(group_parts).reshape(owner_count * local_experts * capacity, model_width)


def per_device_slots(
    block_input,
    upstream_grad,
    first_gain,
    second_gain,
    query_weight,
    key_weight,
    value_weight,
    output_weight,
    gate_weight,
    up_weight,
    down_weight,
    routes,
    gate_values,
):
    pair_count = lax.axis_size("tp")
    owner_count = lax.axis_size("fsdp")
    local_rows = block_input.shape[0]
    seq_rows = local_rows * pair_count
    model_width = block_input.shape[1]
    head_cols = query_weight.shape[1]
    local_heads = head_cols // HD
    expert_count = EXP_DEV * owner_count
    capacity = 3 * seq_rows * TOP // (2 * expert_count)
    inv_root = HD ** (-0.5)
    first_scale = lax.rsqrt(jnp.mean(block_input * block_input, axis=1, keepdims=True) + epsilon)
    first_normed = (block_input * first_scale * first_gain).astype(jnp.bfloat16)
    normed_rows = pair_rows(first_normed)
    query_full, key_full, value_full, output_full = projections(
        query_weight, key_weight, value_weight, output_weight
    )
    query_rows = (
        jnp.dot(normed_rows, query_full, preferred_element_type=jnp.float32)
        .astype(jnp.bfloat16)
        .reshape(seq_rows, local_heads, HD)
    )
    key_rows = (
        jnp.dot(normed_rows, key_full, preferred_element_type=jnp.float32)
        .astype(jnp.bfloat16)
        .reshape(seq_rows, local_heads, HD)
    )
    value_rows = (
        jnp.dot(normed_rows, value_full, preferred_element_type=jnp.float32)
        .astype(jnp.bfloat16)
        .reshape(seq_rows, local_heads, HD)
    )
    scores = (
        jnp.einsum("shd,thd->hst", query_rows, key_rows, preferred_element_type=jnp.float32)
        * inv_root
    )
    row_top = jnp.max(scores, axis=2, keepdims=True)
    log_total = row_top + jnp.log(jnp.sum(jnp.exp(scores - row_top), axis=2, keepdims=True))
    soft_weights = jnp.exp(scores - log_total)
    mixed_rows = jnp.einsum(
        "hst,thd->shd",
        soft_weights.astype(jnp.bfloat16),
        value_rows,
        preferred_element_type=jnp.float32,
    )
    mixed_rows = mixed_rows.astype(jnp.bfloat16).reshape(seq_rows, head_cols)
    middle = block_input + pair_sums(contract_cols(mixed_rows, output_full))
    second_scale = lax.rsqrt(jnp.mean(middle * middle, axis=1, keepdims=True) + epsilon)
    second_normed = (middle * second_scale * second_gain).astype(jnp.bfloat16)
    moe_rows = pair_rows(second_normed)
    slot_index = route_slots(routes, expert_count, capacity)
    send_rows = scatter_rows(spread_rows(moe_rows, TOP), slot_index, expert_count * capacity)
    arrived = send_out(send_rows.reshape(owner_count, EXP_DEV, capacity, model_width))
    gate_act = jnp.einsum(
        "secd,edf->secf", arrived, gate_weight, preferred_element_type=jnp.float32
    )
    up_act = jnp.einsum("secd,edf->secf", arrived, up_weight, preferred_element_type=jnp.float32)
    sigmoid_gate = jax.nn.sigmoid(gate_act)
    hidden = (gate_act * sigmoid_gate * up_act).astype(jnp.bfloat16)
    expert_out = jnp.einsum(
        "secf,efd->secd", hidden, down_weight, preferred_element_type=jnp.float32
    ).astype(jnp.bfloat16)
    returned = send_back(expert_out)
    picked = returned[slot_index].reshape(seq_rows, TOP, model_width).astype(jnp.float32)
    mixture = jnp.sum(gate_values[:, :, None] * picked, axis=1)
    block_output = middle + pair_sums(mixture)
    upstream_rows = lax.all_gather(upstream_grad, "tp", axis=0, tiled=True)
    route_terms = jnp.sum(upstream_rows[:, None, :] * picked, axis=2)
    routed_cot = (
        (gate_values[:, :, None] * upstream_rows[:, None, :])
        .astype(jnp.bfloat16)
        .reshape(seq_rows * TOP, model_width)
    )
    cot_send = scatter_rows(routed_cot, slot_index, expert_count * capacity)
    cot_arrived = send_out(cot_send.reshape(owner_count, EXP_DEV, capacity, model_width))
    hidden_cot = jnp.einsum(
        "secd,efd->secf", cot_arrived, down_weight, preferred_element_type=jnp.float32
    )
    down_grad = jnp.einsum(
        "secf,secd->efd", hidden, cot_arrived, preferred_element_type=jnp.float32
    )
    gate_cot = (
        hidden_cot * up_act * sigmoid_gate * (1.0 + gate_act * (1.0 - sigmoid_gate))
    ).astype(jnp.bfloat16)
    up_cot = (hidden_cot * gate_act * sigmoid_gate).astype(jnp.bfloat16)
    gate_grad = jnp.einsum("secd,secf->edf", arrived, gate_cot, preferred_element_type=jnp.float32)
    up_grad = jnp.einsum("secd,secf->edf", arrived, up_cot, preferred_element_type=jnp.float32)
    input_cot = jnp.einsum(
        "secf,edf->secd", gate_cot, gate_weight, preferred_element_type=jnp.float32
    )
    input_cot = (
        input_cot
        + jnp.einsum("secf,edf->secd", up_cot, up_weight, preferred_element_type=jnp.float32)
    ).astype(jnp.bfloat16)
    came_back = send_back(input_cot)
    normed_cot = jnp.sum(
        came_back[slot_index].reshape(seq_rows, TOP, model_width).astype(jnp.float32), axis=1
    )
    second_cot, route_grad = (
        lax.psum_scatter(
            normed_cot.astype(jnp.bfloat16), "tp", scatter_dimension=0, tiled=True
        ).astype(jnp.float32),
        lax.psum_scatter(
            route_terms.astype(jnp.bfloat16), "tp", scatter_dimension=0, tiled=True
        ).astype(jnp.float32),
    )
    weighted_two = second_cot * second_gain
    second_term = jnp.sum(second_cot * middle * second_scale, axis=0)
    middle_grad = upstream_grad + second_scale * (
        weighted_two
        - middle
        * second_scale
        * second_scale
        * jnp.mean(weighted_two * middle, axis=1, keepdims=True)
    )
    middle_rows = pair_rows(middle_grad.astype(jnp.bfloat16))
    query_full, key_full, value_full, output_full = projections(
        query_weight, key_weight, value_weight, output_weight
    )
    out_term = contract_rows(middle_rows, mixed_rows)
    mixed_cot = (
        jnp.dot(middle_rows, output_full, preferred_element_type=jnp.float32)
        .astype(jnp.bfloat16)
        .reshape(seq_rows, local_heads, HD)
    )
    scores = (
        jnp.einsum("shd,thd->hst", query_rows, key_rows, preferred_element_type=jnp.float32)
        * inv_root
    )
    soft_weights = jnp.exp(scores - log_total)
    value_cot = jnp.einsum(
        "hst,shd->thd",
        soft_weights.astype(jnp.bfloat16),
        mixed_cot,
        preferred_element_type=jnp.float32,
    )
    value_cot = value_cot.astype(jnp.bfloat16).reshape(seq_rows, head_cols)
    soft_cot = jnp.einsum("shd,thd->hst", mixed_cot, value_rows, preferred_element_type=jnp.float32)
    score_cot = (
        soft_weights
        * (soft_cot - jnp.sum(soft_weights * soft_cot, axis=2, keepdims=True))
        * inv_root
    ).astype(jnp.bfloat16)
    query_cot = (
        jnp.einsum("hst,thd->shd", score_cot, key_rows, preferred_element_type=jnp.float32)
        .astype(jnp.bfloat16)
        .reshape(seq_rows, head_cols)
    )
    key_cot = (
        jnp.einsum("hst,shd->thd", score_cot, query_rows, preferred_element_type=jnp.float32)
        .astype(jnp.bfloat16)
        .reshape(seq_rows, head_cols)
    )
    query_term = contract_rows(normed_rows, query_cot)
    key_term = contract_rows(normed_rows, key_cot)
    value_term = contract_rows(normed_rows, value_cot)
    first_terms = (
        contract_cols(query_cot, query_full)
        + contract_cols(key_cot, key_full)
        + contract_cols(value_cot, value_full)
    )
    first_cot = pair_sums(first_terms)
    weighted_one = first_cot * first_gain
    first_term = jnp.sum(first_cot * block_input * first_scale, axis=0)
    input_grad = middle_grad + first_scale * (
        weighted_one
        - block_input
        * first_scale
        * first_scale
        * jnp.mean(weighted_one * block_input, axis=1, keepdims=True)
    )
    query_grad, key_grad, value_grad, output_grad = (
        lax.psum_scatter(query_term, "fsdp", scatter_dimension=0, tiled=True),
        lax.psum_scatter(key_term, "fsdp", scatter_dimension=0, tiled=True),
        lax.psum_scatter(value_term, "fsdp", scatter_dimension=0, tiled=True),
        lax.psum_scatter(out_term, "fsdp", scatter_dimension=0, tiled=True),
    )
    first_gain_grad, second_gain_grad = lax.psum((first_term, second_term), ("fsdp", "tp"))
    return (
        block_output,
        input_grad,
        first_gain_grad,
        second_gain_grad,
        query_grad,
        key_grad,
        value_grad,
        output_grad,
        gate_grad,
        up_grad,
        down_grad,
        route_grad,
    )


MESH = pl.DeviceIdType.MESH


def place():
    here = lax.axis_index("fsdp")
    return here // 4, (here // 2) % 2, here % 2, lax.axis_index("tp")


def index_of(z, y, c):
    return (z * 2 + y) * 2 + c


LEVELS = 4
LEVEL_ORDER = sum(
    level << (8 * turn + 2 * z)
    for turn, row in enumerate(((3, 3, 0, 0), (2, 2, 1, 1), (1, 0, 3, 2), (0, 1, 2, 3)))
    for z, level in enumerate(row)
) - (1 << 32)


def level_at(turn, z):
    return (jnp.int32(LEVEL_ORDER) >> (8 * turn + 2 * z)) & 3


def line_ends(z):
    return (z + 1) // LEVELS, (LEVELS - z) // LEVELS


def plane_greet(pair=False, far=False):
    z, y, c, x = place()
    top, bottom = line_ends(z)
    barrier = pltpu.get_barrier_semaphore()
    partners = [(index_of(z, 1 - y, c), x), (index_of(z, y, 1 - c), x)]
    if pair:
        partners.append((index_of(z, y, c), 1 - x))
    if far:
        partners.append((index_of((z + 2) % LEVELS, y, c), x))
    for partner in partners:
        pl.semaphore_signal(barrier, inc=1, device_id=partner, device_id_type=MESH)

    @pl.when(top == 0)
    def _():
        above = (index_of(z + 1, y, c), x)
        pl.semaphore_signal(barrier, inc=1, device_id=above, device_id_type=MESH)

    @pl.when(bottom == 0)
    def _():
        below = (index_of(z - 1, y, c), x)
        pl.semaphore_signal(barrier, inc=1, device_id=below, device_id_type=MESH)

    pl.semaphore_wait(barrier, len(partners) + 2 - top - bottom)


def remote(src, dst, send_sem, recv_sem, target):
    return pltpu.make_async_remote_copy(
        src_ref=src,
        dst_ref=dst,
        send_sem=send_sem,
        recv_sem=recv_sem,
        device_id=target,
        device_id_type=MESH,
    )


class PlaneGather:
    def __init__(self, mine, full, send_sems, recv_sems):
        self.mine, self.full = mine, full
        self.send_sems, self.recv_sems = send_sems, recv_sems
        self.z, self.y, self.c, self.x = place()
        self.top, self.bottom = line_ends(self.z)

    def _copy(self, number, src, slot, target):
        return remote(
            src, self.full.at[slot], self.send_sems.at[number], self.recv_sems.at[slot], target
        )

    def arrived(self, slot):
        here = self.full.at[slot]
        remote(here, here, self.send_sems.at[0], self.recv_sems.at[slot], (0, self.x)).wait_recv()

    def start(self):
        z, y, c, x = self.z, self.y, self.c, self.x
        own = index_of(z, y, c)
        up = self._copy(0, self.mine, own, (index_of(z + 1, y, c), x))
        down = self._copy(1, self.mine, own, (index_of(z - 1, y, c), x))
        pl.when(self.top == 0)(up.start)
        pl.when(self.bottom == 0)(down.start)
        self._copy(2, self.mine, own, (index_of(z, 1 - y, c), x)).start()
        self._copy(3, self.mine, own, (index_of(z, y, 1 - c), x)).start()

    def from_line(self, step):
        z, y, c, x = self.z, self.y, self.c, self.x
        level = level_at(3 - step, z)
        slot = index_of(level, y, c)
        self.arrived(slot)
        onward = z + 1 - 2 * ((level + LEVELS - z) // LEVELS)
        src, number = self.full.at[slot], 4 + 3 * (step - 1)
        forward = self._copy(number, src, slot, (index_of(onward, y, c), x))
        pl.when(self.top + self.bottom == 0)(forward.start)
        self._copy(number + 1, src, slot, (index_of(z, 1 - y, c), x)).start()
        self._copy(number + 2, src, slot, (index_of(z, y, 1 - c), x)).start()

    def from_side(self, step):
        z, y, c, x = self.z, self.y, self.c, self.x
        slot = index_of(level_at(3 - step, z), 1 - y, c)
        self.arrived(slot)
        self._copy(13 + step, self.full.at[slot], slot, (index_of(z, y, 1 - c), x)).start()

    def from_core(self, step, side):
        z, y, c = self.z, self.y, self.c
        self.arrived(index_of(level_at(3 - step, z), (y + side) % 2, 1 - c))

    def finish(self):
        for number in range(GATHER_SENDS):
            wait = self._copy(number, self.mine, 0, (0, self.x)).wait_send
            if number == 0:
                pl.when(self.top == 0)(wait)
            elif number == 1:
                pl.when(self.bottom == 0)(wait)
            elif number in (4, 7, 10):
                pl.when(self.top + self.bottom == 0)(wait)
            else:
                wait()


GATHER_SENDS = 17


def attend_kernel(
    query_mine,
    key_mine,
    value_mine,
    output_mine,
    block_input,
    upstream,
    first_gain,
    routes,
    gate_values,
    gate_own,
    up_own,
    down_own,
    query_full,
    key_full,
    value_full,
    output_full,
    upstream_all,
    gates_all,
    normed_pair,
    gate_other,
    up_other,
    down_other,
    query_rows,
    key_rows,
    value_rows,
    mixed_rows,
    out_part,
    first_scale,
    weights,
    normed,
    upstream_mine,
    gates_mine,
    send_sems,
    recv_sems,
    wide_s,
    wide_r,
    own_sems,
    keep_sems,
    pair_s,
    pair_r,
):
    bf16, f32 = jnp.bfloat16, jnp.float32
    z, y, c, x = place()
    own = index_of(z, y, c)
    half_rows, width = block_input.shape
    rows, head_cols = mixed_rows.shape
    inv_root = HD ** (-0.5)
    step = 16

    mine = (query_mine, key_mine, value_mine, output_mine)
    kept = [
        pltpu.make_async_copy(mine[a], weights.at[a, own], own_sems.at[a]) for a in range(4)
    ]
    for copy in kept:
        copy.start()
    plane_greet(pair=True)
    plans = [
        PlaneGather(mine[a], weights.at[a], send_sems.at[a], recv_sems.at[a]) for a in range(4)
    ] + [
        PlaneGather(ref, full, wide_s.at[i], wide_r.at[i])
        for i, (ref, full) in enumerate(((upstream_mine, upstream_all), (gates_mine, gates_all)))
    ]
    first, output, wide = plans[:3], plans[3:4], plans[4:]
    for plan in first:
        plan.start()

    def swap(i, src, dst):
        return remote(src, dst, pair_s.at[i], pair_r.at[i], (own, 1 - x))

    swaps = [
        swap(0, normed.at[x], normed.at[x]),
        swap(1, gate_own, gate_other),
        swap(2, up_own, up_other),
        swap(3, down_own, down_other),
    ]
    gain = first_gain[...]

    @pl.loop(0, half_rows // step)
    def _(i):
        at = pl.ds(pl.multiple_of(i * step, step), step)
        value = block_input[at, :]
        scale = lax.rsqrt(jnp.mean(value * value, axis=1, keepdims=True) + epsilon)
        first_scale[at, :] = scale
        normed[x, at, :] = (value * scale * gain).astype(bf16)

    for copy in swaps:
        copy.start()

    @pl.loop(0, half_rows // step)
    def _(i):
        at = pl.ds(pl.multiple_of(i * step, step), step)
        upstream_mine[at, :] = upstream[at, :].astype(bf16)

    here = pl.ds(pl.multiple_of(x * half_rows, half_rows), half_rows)
    names = jnp.transpose(routes[:, here].astype(f32))
    values = jnp.transpose(gate_values[:, here])
    lane = lax.broadcasted_iota(jnp.int32, (half_rows, ROUTE_COLS), 1).astype(f32)
    table = jnp.zeros((half_rows, ROUTE_COLS), f32)
    for j in range(TOP):
        table = table + jnp.where(lane == names[:, j : j + 1], values[:, j : j + 1], 0.0)
    gates_mine[...] = table
    wide_kept = [
        pltpu.make_async_copy(upstream_mine, upstream_all.at[own], own_sems.at[4]),
        pltpu.make_async_copy(gates_mine, gates_all.at[own], own_sems.at[5]),
    ]
    for copy in wide_kept:
        copy.start()

    def line(group, turn):
        for plan in group:
            plan.from_line(turn)

    def side(group, turn):
        for plan in group:
            plan.from_side(turn)

    def core(group):
        for plan in group:
            for turn in range(LEVELS):
                for which in range(2):
                    plan.from_core(turn, which)

    line(first, 1)
    side(first, 0)
    line(first, 2)
    side(first, 1)
    line(first, 3)
    for plan in output:
        plan.start()
    side(first, 2)
    side(first, 3)
    line(output, 1)
    core(first)
    line(output, 2)
    for plan in wide:
        plan.start()
    swaps[0].wait_recv()
    for copy in kept:
        copy.wait()
    keeps = [
        pltpu.make_async_copy(src, dst, keep_sems.at[i])
        for i, (src, dst) in enumerate(
            (
                (weights.at[0], query_full),
                (weights.at[1], key_full),
                (weights.at[2], value_full),
                (normed, normed_pair),
                (weights.at[3], output_full),
            )
        )
    ]
    for copy in keeps[:4]:
        copy.start()

    def flat(ref):
        value = ref[...]
        return value.reshape(value.shape[0] * value.shape[1], value.shape[2])

    for a, ref in enumerate((query_rows, key_rows, value_rows)):
        ref[...] = nn(flat(normed), flat(weights.at[a])).astype(bf16)
        if a == 0:
            line(output, 3)
            side(output, 0)
    side(output, 1)
    line(wide, 1)

    def head(h):
        cols = pl.ds(pl.multiple_of(h * HD, HD), HD)
        scores = nt(query_rows[:, cols], key_rows[:, cols]) * inv_root
        row_top = jnp.max(scores, axis=1, keepdims=True)
        log_total = row_top + jnp.log(jnp.sum(jnp.exp(scores - row_top), axis=1, keepdims=True))
        soft = jnp.exp(scores - log_total)
        mixed_rows[:, cols] = nn(soft.astype(bf16), value_rows[:, cols]).astype(bf16)

    @pl.loop(0, head_cols // HD // 2)
    def _(h):
        head(2 * h)
        head(2 * h + 1)

    side(output, 2)
    side(output, 3)
    line(wide, 2)
    core(output)
    keeps[4].start()
    panel = 4

    @pl.loop(0, weights.shape[1] // panel)
    def _(n):
        part = weights[3, pl.ds(n * panel, panel)].reshape(panel * half_rows, head_cols)
        cols = pl.ds(pl.multiple_of(n * panel * half_rows, panel * half_rows), panel * half_rows)
        out_part[:, :, cols] = nt(mixed_rows[...], part).reshape(2, half_rows, panel * half_rows)

    side(wide, 0)
    line(wide, 3)
    for turn in range(1, LEVELS):
        side(wide, turn)
    core(wide)
    for plan in plans:
        plan.finish()
    for copy in wide_kept + keeps:
        copy.wait()
    swaps[0].wait_send()
    for copy in swaps[1:]:
        copy.wait()


def run_attend(shards, block_input, upstream, first_gain, routes, gate_values, experts, collective_id):
    bf16, f32 = jnp.bfloat16, jnp.float32
    owner_count = lax.axis_size("fsdp")
    half_rows, width = block_input.shape
    head_cols = shards[0].shape[1]
    rows = 2 * half_rows
    shape = jax.ShapeDtypeStruct
    hbm = pl.BlockSpec(memory_space=pl.ANY)
    vmem = pl.BlockSpec(memory_space=pltpu.VMEM)
    dma = pltpu.SemaphoreType.DMA
    full = (owner_count,) + shards[0].shape
    outs = pl.pallas_call(
        attend_kernel,
        out_shape=[shape(full, bf16)] * 4
        + [
            shape((owner_count, half_rows, width), bf16),
            shape((owner_count, half_rows, ROUTE_COLS), f32),
            shape((2, half_rows, width), bf16),
        ]
        + [shape(w.shape, w.dtype) for w in experts]
        + [shape((rows, head_cols), bf16)] * 4
        + [shape((2, half_rows, width), f32), shape((half_rows, 1), f32)],
        in_specs=[vmem] * 9 + [hbm] * 3,
        out_specs=[hbm] * 10 + [vmem] * 6,
        scratch_shapes=[
            pltpu.VMEM((4,) + full, bf16),
            pltpu.VMEM((2, half_rows, width), bf16),
            pltpu.VMEM((half_rows, width), bf16),
            pltpu.VMEM((half_rows, ROUTE_COLS), f32),
            dma((4, GATHER_SENDS)),
            dma((4, owner_count)),
            dma((2, GATHER_SENDS)),
            dma((2, owner_count)),
            dma((6,)),
            dma((5,)),
            dma((4,)),
            dma((4,)),
        ],
        compiler_params=pltpu.CompilerParams(
            collective_id=collective_id, has_side_effects=True, vmem_limit_bytes=60 * 2**20
        ),
        cost_estimate=pl.CostEstimate(
            flops=2 * 4 * rows * head_cols * width,
            bytes_accessed=16 * shards[0].size * owner_count,
            transcendentals=0,
        ),
        name="attend",
    )(*shards, block_input, upstream, first_gain, routes, gate_values, *experts)
    return outs[:4], outs[4:7], outs[7:10], outs[10:14], outs[14], outs[15]


class PlaneSums:
    def __init__(self, own_parts, from_core, from_side, from_line, sems, kept=0):
        self.own, self.from_core, self.kept = own_parts, from_core, kept
        self.from_side, self.from_line = from_side, from_line
        self.core_s, self.core_r, self.side_s, self.side_r, self.line_s, self.line_r = sems
        self.z, self.y, self.c, self.x = place()
        self.top, self.bottom = line_ends(self.z)

    def side_arrived(self, turn):
        here = self.from_side.at[turn]
        remote(here, here, self.side_s.at[turn], self.side_r.at[turn], (0, self.x)).wait_recv()

    def line_arrived(self, slot):
        here = self.from_line.at[slot]
        remote(here, here, self.line_s.at[0], self.line_r.at[slot], (0, self.x)).wait_recv()

    def to_line(self, turn):
        z, y, c, x = self.z, self.y, self.c, self.x
        mine = self.own.at[self.kept + turn]
        level = level_at(turn, z)

        @pl.when(self.top + self.bottom == 0)
        def _():
            self.line_arrived(level)
            add_block(mine, self.from_line.at[level], mine)

        down = (z + LEVELS - level) // (LEVELS + 1)
        onward = z + 1 - 2 * down
        reached = 1 - jnp.minimum(1, jnp.abs(onward - level))
        slot = level + down * reached * (LEVELS - level)
        copy = remote(
            mine,
            self.from_line.at[slot],
            self.line_s.at[turn],
            self.line_r.at[slot],
            (index_of(onward, y, c), x),
        )
        copy.start()


def add_block(one, two, out):
    step = 32

    @pl.loop(0, out.shape[0] // step)
    def _(i):
        rows = pl.ds(pl.multiple_of(i * step, step), step)
        value = one[rows, :].astype(jnp.float32) + two[rows, :].astype(jnp.float32)
        out[rows, :] = value.astype(out.dtype)


def total_block(plan, total):
    step = 32
    mine = plan.own.at[plan.kept + LEVELS - 1]
    below, above = plan.from_line.at[plan.z], plan.from_line.at[LEVELS]

    @pl.loop(0, total.shape[0] // step)
    def _(i):
        rows = pl.ds(pl.multiple_of(i * step, step), step)
        total[rows, :] = mine[rows, :].astype(jnp.float32)

    for end, block, slot in ((plan.bottom, below, plan.z), (plan.top, above, LEVELS)):

        @pl.when(end == 0)
        def _():
            plan.line_arrived(slot)

            @pl.loop(0, total.shape[0] // step)
            def _(i):
                rows = pl.ds(pl.multiple_of(i * step, step), step)
                total[rows, :] = total[rows, :] + block[rows, :].astype(jnp.float32)


ROUTE_COLS = 128


def nn(left, right):
    return lax.dot_general(
        left, right, (((1,), (0,)), ((), ())), preferred_element_type=jnp.float32
    )


def nt(left, right):
    return lax.dot_general(
        left, right, (((1,), (1,)), ((), ())), preferred_element_type=jnp.float32
    )


def tn(left, right):
    return lax.dot_general(
        left, right, (((0,), (0,)), ((), ())), preferred_element_type=jnp.float32
    )


def pair_block(ref, pair):
    value = ref[pl.ds(2 * pair, 2)]
    return value.reshape(value.shape[0] * value.shape[1], value.shape[2])


def experts_kernel(
    gates,
    second_gain,
    out_part,
    block_input,
    upstream,
    upstream_hbm,
    gate_own,
    up_own,
    down_own,
    gate_other,
    up_other,
    down_other,
    middle,
    middle_grad,
    second_term,
    mixture_hbm,
    gate_mine,
    gate_theirs,
    up_mine,
    up_theirs,
    down_mine,
    down_theirs,
    down_landed,
    rows_all,
    u_all,
    wg,
    wu,
    wd,
    hidden,
    gcot,
    ucot,
    rext,
    tmp,
    from_core,
    from_side,
    from_line,
    gstage,
    wide,
    second_scale,
    route_half,
    gather_s,
    gather_r,
    core_s,
    core_r,
    side_s,
    side_r,
    line_s,
    line_r,
    load_sems,
    out_sems,
    pair_s,
    pair_r,
):
    bf16, f32 = jnp.bfloat16, jnp.float32
    z, y, c, x = place()
    top, bottom = line_ends(z)
    interior = 1 - top - bottom
    me = lax.axis_index("fsdp")
    partner = (me, 1 - x)
    halves, width, units = wg.shape
    half_rows = middle.shape[0]
    pair_rows_ = 2 * half_rows
    pairs = 2 * LEVELS
    panel = 512
    block = 256
    step = 16

    loads = [
        pltpu.make_async_copy(src, dst, load_sems.at[i])
        for i, (src, dst) in enumerate(
            (
                (out_part.at[1 - x], middle_grad),
                (out_part.at[x], middle),
                (block_input, wide),
                (down_own, wd.at[x]),
                (down_other, wd.at[1 - x]),
                (upstream_hbm, u_all),
                (gate_own, wg.at[x]),
                (up_own, wu.at[x]),
                (gate_other, wg.at[1 - x]),
                (up_other, wu.at[1 - x]),
            )
        )
    ]
    for load in loads:
        load.start()

    plane_greet(pair=True)
    gather = PlaneGather(rows_all.at[me], rows_all, gather_s, gather_r)
    sums = PlaneSums(
        from_core,
        from_core,
        from_side,
        from_line,
        (core_s, core_r, side_s, side_r, line_s, line_r),
        LEVELS,
    )

    loads[0].wait()

    @pl.loop(0, half_rows // step)
    def _(i):
        at = pl.ds(pl.multiple_of(i * step, step), step)
        tmp[0, 0, at, :] = middle_grad[at, :].astype(bf16)

    meet = remote(tmp.at[0, 0], tmp.at[0, 1], pair_s.at[0], pair_r.at[0], partner)
    meet.start()
    for load in loads[1:6]:
        load.wait()

    @pl.loop(0, pairs)
    def _(b):
        at_rows = pl.ds(pl.multiple_of(b * pair_rows_, pair_rows_), pair_rows_)
        us = pair_block(u_all, b)
        for h in range(halves):
            ucot[h, at_rows, :] = nt(us, wd[h]).astype(bf16)

    meet.wait()
    gain = second_gain[...]

    @pl.loop(0, half_rows // step)
    def _(i):
        at = pl.ds(pl.multiple_of(i * step, step), step)
        value = wide[at, :] + (middle[at, :] + tmp[0, 1, at, :].astype(f32))
        scale = lax.rsqrt(jnp.mean(value * value, axis=1, keepdims=True) + epsilon)
        middle[at, :] = value
        second_scale[at, :] = scale
        rows_all[me, at, :] = (value * scale * gain).astype(bf16)

    gather.start()
    again = pltpu.make_async_copy(upstream, wide, load_sems.at[2])
    again.start()
    for load in loads[6:]:
        load.wait()

    def forward_pair(b):
        turn = (0b11_10_11_01_10_00_01_00 >> (2 * b)) % 4
        side = (0b11_01_01_00 >> b) % 2
        return level_at(3 - turn, z) * 2 + (y + side) % 2

    def mixture_out(b):
        return pltpu.make_async_copy(
            tmp.at[b % 2],
            mixture_hbm.at[pl.ds(2 * forward_pair(b), 2), :, pl.ds(0, width)],
            out_sems.at[b % 2],
        )

    @pl.loop(0, 2 * pairs)
    def _(turn):
        b, h = turn // 2, turn % 2

        def at(k, work, where=None):
            @pl.when(turn == k)
            def _():
                if where is None:
                    work()
                else:
                    pl.when(where == 1)(work)

        at(0, lambda: gather.from_core(0, 0))
        at(2, lambda: gather.from_line(1))
        at(2, lambda: gather.from_line(2), interior)
        at(2, lambda: gather.from_core(1, 0))
        at(4, lambda: gather.from_side(0))
        at(4, lambda: gather.from_core(0, 1))
        at(6, lambda: gather.from_line(2), 1 - interior)
        at(6, lambda: gather.from_line(3), interior)
        at(6, lambda: gather.from_core(2, 0))
        at(8, lambda: gather.from_side(1))
        at(8, lambda: gather.from_core(1, 1))
        at(10, lambda: gather.from_line(3), 1 - interior)
        at(10, lambda: gather.from_core(3, 0))
        at(12, lambda: gather.from_side(2))
        at(12, lambda: gather.from_core(2, 1))
        at(14, lambda: gather.from_side(3))
        at(14, lambda: gather.from_core(3, 1))

        pair = forward_pair(b)
        xs = pair_block(rows_all, pair)
        lane = lax.broadcasted_iota(jnp.int32, (pair_rows_, ROUTE_COLS), 1)
        table = gates[pl.ds(2 * pair, 2)].reshape(pair_rows_, ROUTE_COLS)
        gate_rows = jnp.sum(jnp.where(lane == me, table, 0.0), axis=1, keepdims=True)
        gate_act = nn(xs, wg[h])
        up_act = nn(xs, wu[h])
        at_rows = pl.ds(pl.multiple_of(pair * pair_rows_, pair_rows_), pair_rows_)
        hidden_cot = ucot[h, at_rows, :].astype(f32)
        sig = lax.logistic(gate_act)
        act = gate_act * sig
        hid = act * up_act
        hidden[h, at_rows, :] = (hid * gate_rows).astype(bf16)
        route = jnp.sum(hid * hidden_cot, axis=1, keepdims=True)
        scaled = hidden_cot * gate_rows
        gcot[h, at_rows, :] = (scaled * up_act * (sig * (1.0 + gate_act * (1.0 - sig)))).astype(bf16)
        ucot[h, at_rows, :] = (scaled * act).astype(bf16)

        @pl.when(h == 0)
        def _():
            route_half[...] = route

        @pl.when(h == 1)
        def _():
            total = route_half[...] + route
            placed = jnp.where(lane == me, total, 0.0).astype(bf16)
            rext[pl.ds(2 * pair, 2)] = placed.reshape(2, half_rows, ROUTE_COLS)

            pl.when(b >= 2)(lambda: mixture_out(b - 2).wait())

            @pl.loop(0, width // panel)
            def _(n):
                cols = pl.ds(pl.multiple_of(n * panel, panel), panel)
                acc = nn(hidden[0, at_rows, :], wd[0, :, cols])
                for h in range(1, halves):
                    acc = acc + nn(hidden[h, at_rows, :], wd[h, :, cols])
                tmp[b % 2, :, :, cols] = acc.astype(bf16).reshape(2, half_rows, panel)

            mixture_out(b).start()

    for b in (pairs - 2, pairs - 1):
        mixture_out(b).wait()

    def core_send(b):
        return remote(
            tmp.at[b % 2, 1 - c],
            from_core.at[b],
            core_s.at[b],
            core_r.at[b],
            (index_of(z, y, 1 - c), x),
        )

    def take_core(b):
        core_send(b).wait_recv()
        add_block(tmp.at[b % 2, c], from_core.at[b], from_core.at[b])

        @pl.when(b < LEVELS)
        def _():
            remote(
                from_core.at[b],
                from_side.at[b],
                side_s.at[b],
                side_r.at[b],
                (index_of(z, 1 - y, c), x),
            ).start()

    def line_step(turn):
        sums.side_arrived(turn)
        mine = from_core.at[LEVELS + turn]
        add_block(mine, from_side.at[turn], mine)
        if turn < LEVELS - 1:
            sums.to_line(turn)

    def last_step():
        line_step(LEVELS - 1)
        total_block(sums, middle_grad)
        again.wait()
        second_term[...] = jnp.zeros_like(second_term)

        @pl.loop(0, half_rows // step)
        def _(i):
            at = pl.ds(pl.multiple_of(i * step, step), step)
            cot, mid, scale = middle_grad[at, :], middle[at, :], second_scale[at, :]
            weighted = cot * gain
            mean = jnp.mean(weighted * mid, axis=1, keepdims=True)
            value = wide[at, :] + scale * (weighted - mid * (scale * scale * mean))
            middle_grad[at, :] = value
            second_term[...] = second_term[...] + jnp.sum(cot * mid * scale, axis=0, keepdims=True)

    @pl.loop(0, pairs)
    def _(b):
        pl.when((b == pairs - 1) & (interior == 0))(lambda: line_step(0))
        pl.when(b >= 2)(lambda: core_send(b - 2).wait_send())
        pair = level_at(b % LEVELS, z) * 2 + (y + 1 - b // LEVELS) % 2
        at_rows = pl.ds(pl.multiple_of(pair * pair_rows_, pair_rows_), pair_rows_)

        @pl.loop(0, width // panel)
        def _(n):
            cols = pl.ds(pl.multiple_of(n * panel, panel), panel)
            acc = nt(gcot[0, at_rows, :], wg[0, cols, :])
            acc = acc + nt(ucot[0, at_rows, :], wu[0, cols, :])
            for h in range(1, halves):
                acc = acc + nt(gcot[h, at_rows, :], wg[h, cols, :])
                acc = acc + nt(ucot[h, at_rows, :], wu[h, cols, :])
            tmp[b % 2, :, :, cols] = acc.astype(bf16).reshape(2, half_rows, panel)

        core_send(b).start()
        pl.when(b >= 1)(lambda: take_core(b - 1))

    take_core(pairs - 1)
    for b in (pairs - 2, pairs - 1):
        core_send(b).wait_send()

    route_out = pltpu.make_async_copy(
        rext, mixture_hbm.at[:, :, pl.ds(width, ROUTE_COLS)], load_sems.at[1]
    )
    route_out.start()
    down_send = remote(
        wd.at[0, pl.ds(0, block)], down_landed, pair_s.at[1], pair_r.at[1], partner
    )
    down_later = pltpu.make_async_copy(wd.at[0, pl.ds(block, block)], down_theirs, load_sems.at[3])
    down_keep = pltpu.make_async_copy(wd.at[1], down_mine, load_sems.at[4])

    @pl.loop(0, 2 * units // block)
    def _(p):
        other, q = p // (units // block), p % (units // block)
        pl.when((p == 1) & (interior == 0))(lambda: line_step(1))
        pl.when((p == 2) & (interior == 1))(lambda: line_step(0))
        units_at = pl.ds(pl.multiple_of(q * block, block), block)
        us = u_all[...]
        us = us.reshape(us.shape[0] * us.shape[1], width)
        h = (1 - x) * (1 - other) + x * other
        wd[other, units_at, :] = tn(hidden[h, :, units_at], us).astype(bf16)
        pl.when(p == 0)(down_send.start)
        pl.when(p == 1)(down_later.start)

    down_keep.start()

    def part_outs(p):
        rows = pl.ds(pl.multiple_of(p * block, block), block)
        return [
            pltpu.make_async_copy(
                gstage.at[p % 2, which, k], ref.at[rows, :], out_sems.at[(p % 2) * 4 + 2 * which + k]
            )
            for which, refs in enumerate(((gate_mine, gate_theirs), (up_mine, up_theirs)))
            for k, ref in enumerate(refs)
        ]

    def wait_outs(p):
        for copy in part_outs(p):
            copy.wait()

    @pl.loop(0, width // block)
    def _(p):
        pl.when((p == 1) & (interior == 0))(lambda: line_step(2))
        pl.when((p == 1) & (interior == 1))(lambda: line_step(1))
        pl.when((p == 2) & (interior == 1))(lambda: line_step(2))
        pl.when(p == 6)(last_step)
        pl.when(p >= 2)(lambda: wait_outs(p - 2))
        cols = pl.ds(pl.multiple_of(p * block, block), block)
        xp = rows_all[:, :, cols]
        xp = xp.reshape(xp.shape[0] * xp.shape[1], block)
        xt = jnp.transpose(xp)
        for which, ref in enumerate((gcot, ucot)):
            for k, h in enumerate((x, 1 - x)):
                gstage[p % 2, which, k] = nn(xt, ref[h]).astype(bf16)
        for copy in part_outs(p):
            copy.start()

    for p in (width // block - 2, width // block - 1):
        wait_outs(p)
    route_out.wait()
    down_send.wait()
    down_later.wait()
    down_keep.wait()
    gather.finish()
    for turn in range(LEVELS):
        remote(
            from_core.at[turn], from_side.at[turn], side_s.at[turn], side_r.at[turn], partner
        ).wait_send()
    for turn in range(LEVELS - 1):
        remote(
            from_core.at[turn], from_line.at[turn], line_s.at[turn], line_r.at[turn], partner
        ).wait_send()


def run_experts(
    gates, second_gain, out_part, block_input, upstream, upstream_all, own, other, collective_id
):
    bf16, f32 = jnp.bfloat16, jnp.float32
    block = block_input.shape
    half_rows, width = block
    owner_count = upstream_all.shape[0]
    units = own[0].shape[1]
    halves = lax.axis_size("tp")
    all_rows = owner_count * half_rows
    hbm = pl.BlockSpec(memory_space=pl.ANY)
    vmem = pl.BlockSpec(memory_space=pltpu.VMEM)
    dma = pltpu.SemaphoreType.DMA
    flops = 2 * 9 * all_rows * width * units * halves
    shape = jax.ShapeDtypeStruct
    return pl.pallas_call(
        experts_kernel,
        out_shape=[
            shape(block, f32),
            shape(block, f32),
            shape((1, width), f32),
            shape((owner_count, half_rows, width + ROUTE_COLS), bf16),
        ]
        + [shape((width, units), bf16)] * 4
        + [shape((units, width), bf16)]
        + [shape((256, width), bf16)] * 2,
        in_specs=[vmem, vmem] + [hbm] * 10,
        out_specs=[vmem] * 3 + [hbm] * 8,
        scratch_shapes=[
            pltpu.VMEM((owner_count,) + block, bf16),
            pltpu.VMEM((owner_count,) + block, bf16),
            pltpu.VMEM((halves, width, units), bf16),
            pltpu.VMEM((halves, width, units), bf16),
            pltpu.VMEM((halves, units, width), bf16),
            pltpu.VMEM((halves, all_rows, units), bf16),
            pltpu.VMEM((halves, all_rows, units), bf16),
            pltpu.VMEM((halves, all_rows, units), bf16),
            pltpu.VMEM((owner_count, half_rows, ROUTE_COLS), bf16),
            pltpu.VMEM((2, 2) + block, bf16),
            pltpu.VMEM((2 * LEVELS,) + block, bf16),
            pltpu.VMEM((LEVELS,) + block, bf16),
            pltpu.VMEM((LEVELS + 1,) + block, bf16),
            pltpu.VMEM((2, 2, halves, 256, units), bf16),
            pltpu.VMEM(block, f32),
            pltpu.VMEM((half_rows, 1), f32),
            pltpu.VMEM((2 * half_rows, 1), f32),
            dma((GATHER_SENDS,)),
            dma((owner_count,)),
            dma((2 * LEVELS,)),
            dma((2 * LEVELS,)),
            dma((LEVELS,)),
            dma((LEVELS,)),
            dma((LEVELS + 1,)),
            dma((LEVELS + 1,)),
            dma((10,)),
            dma((8,)),
            dma((2,)),
            dma((2,)),
        ],
        compiler_params=pltpu.CompilerParams(
            collective_id=collective_id, has_side_effects=True, vmem_limit_bytes=67_043_328
        ),
        cost_estimate=pl.CostEstimate(
            flops=flops, bytes_accessed=64 * 2**20, transcendentals=all_rows * units * halves
        ),
        name="experts",
    )(gates, second_gain, out_part, block_input, upstream, upstream_all, *own, *other)


def last_kernel(
    mixture_part,
    normed_pair,
    mixed_rows,
    query_rows,
    key_rows,
    value_rows,
    output_full,
    query_full,
    key_full,
    value_full,
    gate_theirs,
    up_theirs,
    down_theirs,
    block_input,
    first_scale,
    first_gain,
    middle_grad,
    second_term,
    query_total,
    key_total,
    value_total,
    output_total,
    mixture_total,
    gate_landed,
    up_landed,
    down_landed,
    input_grad,
    gain_grads,
    wide_core,
    wide_side,
    wide_line,
    wide_own,
    from_core,
    from_side,
    from_line,
    tmp,
    middle_pair,
    mixed_cot,
    query_cot,
    key_cot,
    value_cot,
    weight_one,
    weight_two,
    first_terms,
    first_mine,
    first_other,
    gains,
    gains_in,
    core_s,
    core_r,
    side_s,
    side_r,
    line_s,
    line_r,
    own_sems,
    load_sems,
    pair_s,
    pair_r,
    gain_s,
    gain_r,
):
    bf16, f32 = jnp.bfloat16, jnp.float32
    z, y, c, x = place()
    own = index_of(z, y, c)
    rows, head_cols = mixed_rows.shape
    half_rows, width = input_grad.shape
    pairs = 2 * LEVELS
    inv_root = HD ** (-0.5)
    plane_greet(pair=True, far=True)

    def swap(i, src, dst):
        return remote(src, dst, pair_s.at[i], pair_r.at[i], (own, 1 - x))

    expert_swaps = (
        swap(0, gate_theirs, gate_landed),
        swap(1, up_theirs, up_landed),
        swap(2, down_theirs, down_landed),
    )
    first_swap = swap(3, first_mine, first_other)

    def load(i, src, dst):
        return pltpu.make_async_copy(src, dst, load_sems.at[i])

    output_load, query_load = load(0, output_full, weight_one), load(1, query_full, weight_two)
    value_load, key_load = load(2, value_full, weight_one), load(3, key_full, weight_two)
    sums = [
        PlaneSums(
            core,
            core,
            side,
            line,
            tuple(s.at[a] for s in (core_s, core_r, side_s, side_r, line_s, line_r)),
            LEVELS,
        )
        for a, (core, side, line) in enumerate(
            [(wide_core, wide_side, wide_line)]
            + [(from_core.at[i], from_side.at[i], from_line.at[i]) for i in range(4)]
        )
    ]

    def slot_at(b, core):
        level, side = level_at(b % LEVELS, z), (y + 1 - b // LEVELS) % 2
        return index_of(level, side, (c + core) % 2)

    def core_copy(a, b, src):
        plan = sums[a]
        return remote(
            src,
            plan.from_core.at[b],
            plan.core_s.at[b],
            plan.core_r.at[b],
            (index_of(z, y, 1 - c), x),
        )

    def side_copy(a, b):
        plan = sums[a]
        return remote(
            plan.from_core.at[b],
            plan.from_side.at[b],
            plan.side_s.at[b],
            plan.side_r.at[b],
            (index_of(z, 1 - y, c), x),
        )

    def line_step(a, turn):
        plan = sums[a]
        plan.side_arrived(turn)
        mine = plan.from_core.at[LEVELS + turn]
        add_block(mine, plan.from_side.at[turn], mine)
        if turn < LEVELS - 1:
            plan.to_line(turn)

    @pl.loop(0, half_rows // 16)
    def _(i):
        at = pl.ds(pl.multiple_of(i * 16, 16), 16)
        middle_pair[x, at, :] = middle_grad[at, :].astype(bf16)

    middle_swap = swap(4, middle_pair.at[x], middle_pair.at[x])
    middle_swap.start()
    for copy in expert_swaps[:2]:
        copy.start()
    output_load.start()
    query_load.start()

    def wide_load(b):
        return pltpu.make_async_copy(
            mixture_part.at[slot_at(b, 0)], wide_own.at[b], own_sems.at[b]
        )

    @pl.loop(0, pairs)
    def _(b):
        core_copy(0, b, mixture_part.at[slot_at(b, 1)]).start()
        wide_load(b).start()

    @pl.loop(0, pairs)
    def _(b):
        wide_load(b).wait()
        core_copy(0, b, mixture_part.at[slot_at(b, 1)]).wait_recv()
        add_block(wide_own.at[b], wide_core.at[b], wide_core.at[b])
        pl.when(b < LEVELS)(lambda: side_copy(0, b).start())

    def flat(ref):
        value = ref[...]
        return value.reshape(value.shape[0] * value.shape[1], value.shape[2])

    output_load.wait()
    middle_swap.wait()
    mixed_cot[...] = nn(flat(middle_pair), flat(weight_one)).astype(bf16)
    value_load.start()

    def term(a, left, cot):
        def send(b):
            return core_copy(a, b, tmp.at[b % 2, 1 - c])

        def take(b):
            core = sums[a].from_core.at[b]
            send(b).wait_recv()
            add_block(tmp.at[b % 2, c], core, core)
            pl.when(b < LEVELS)(lambda: side_copy(a, b).start())

        @pl.loop(0, pairs)
        def _(b):
            pl.when(b >= 2)(lambda: send(b - 2).wait_send())
            pair = level_at(b % LEVELS, z) * 2 + (y + 1 - b // LEVELS) % 2
            cols = pl.ds(pl.multiple_of(pair * 2 * half_rows, 2 * half_rows), 2 * half_rows)
            lhs = left[:, :, cols].reshape(rows, 2 * half_rows)
            part = tn(lhs, cot[...])
            tmp[b % 2] = part.astype(bf16).reshape(2, half_rows, head_cols)
            send(b).start()
            pl.when(b >= 1)(lambda: take(b - 1))

        take(pairs - 1)
        for b in (pairs - 2, pairs - 1):
            send(b).wait_send()

    top, bottom = line_ends(z)
    interior = 1 - top - bottom

    def head(h):
        cols = pl.ds(pl.multiple_of(h * HD, HD), HD)
        query, key, value = query_rows[:, cols], key_rows[:, cols], value_rows[:, cols]
        mixed = mixed_cot[:, cols]
        scores = nt(query, key) * inv_root
        row_top = jnp.max(scores, axis=1, keepdims=True)
        log_total = row_top + jnp.log(jnp.sum(jnp.exp(scores - row_top), axis=1, keepdims=True))
        soft = jnp.exp(scores - log_total)
        value_cot[:, cols] = tn(soft.astype(bf16), mixed).astype(bf16)
        soft_cot = nt(mixed, value)
        inner = jnp.sum(soft * soft_cot, axis=1, keepdims=True)
        score_cot = (soft * (soft_cot - inner) * inv_root).astype(bf16)
        query_cot[:, cols] = nn(score_cot, key).astype(bf16)
        key_cot[:, cols] = tn(score_cot, query).astype(bf16)

    term(1, middle_pair, mixed_rows)

    @pl.when(interior == 0)
    def _():
        line_step(0, 0)
        line_step(0, 1)

    @pl.loop(0, head_cols // HD // 2)
    def _(h):
        pl.when((h == 1) & (interior == 1))(lambda: line_step(0, 0))
        head(2 * h)
        head(2 * h + 1)

    pl.when(interior == 1)(lambda: line_step(0, 1))
    line_step(0, 2)
    term(2, normed_pair, value_cot)
    line_step(0, 3)
    term(3, normed_pair, query_cot)
    line_step(1, 0)
    line_step(1, 1)
    term(4, normed_pair, key_cot)
    line_step(1, 2)
    line_step(1, 3)

    panel = 4

    def first_add(cot, weight, begin):
        @pl.loop(0, weight.shape[0] // panel)
        def _(n):
            part = weight[pl.ds(n * panel, panel)].reshape(panel * half_rows, head_cols)
            cols = pl.ds(pl.multiple_of(n * panel * half_rows, panel * half_rows), panel * half_rows)
            value = nt(cot[...], part).reshape(2, half_rows, panel * half_rows)
            if begin:
                first_terms[:, :, cols] = value
            else:
                first_terms[:, :, cols] = first_terms[:, :, cols] + value

    query_load.wait()
    first_add(query_cot, weight_two, True)
    key_load.start()
    value_load.wait()
    first_add(value_cot, weight_one, False)
    key_load.wait()
    first_add(key_cot, weight_two, False)
    step = 16

    @pl.loop(0, half_rows // step)
    def _(i):
        at = pl.ds(pl.multiple_of(i * step, step), step)
        first_mine[at, :] = first_terms[1 - x, at, :].astype(bf16)

    first_swap.start()
    total_block(sums[0], mixture_total)
    for turn in range(LEVELS):
        line_step(2, turn)
    total_block(sums[1], output_total)
    line_step(3, 0)
    line_step(3, 1)
    first_swap.wait_recv()
    gain = first_gain[...]
    gains[...] = jnp.concatenate(
        [jnp.zeros((1, width), f32), second_term[...], jnp.zeros((6, width), f32)], axis=0
    )

    @pl.loop(0, half_rows // step)
    def _(i):
        at = pl.ds(pl.multiple_of(i * step, step), step)
        value = first_terms[x, at, :] + first_other[at, :].astype(f32)
        entry, scale = block_input[at, :], first_scale[at, :]
        weighted = value * gain
        mean = jnp.mean(weighted * entry, axis=1, keepdims=True)
        input_grad[at, :] = middle_grad[at, :] + scale * (weighted - entry * (scale * scale * mean))
        gains[0:1, :] = gains[0:1, :] + jnp.sum(value * entry * scale, axis=0, keepdims=True)

    hops = [
        (index_of(z, y, 1 - c), x),
        (own, 1 - x),
        (index_of(z + 1 - 2 * (z % 2), y, c), x),
        (index_of((z + 2) % LEVELS, y, c), x),
        (index_of(z, 1 - y, c), x),
    ]

    def gain_copy(i):
        return remote(gains, gains_in.at[i], gain_s.at[i], gain_r.at[i], hops[i])

    def gain_add(i):
        gain_copy(i).wait()
        gains[...] = gains[...] + gains_in[i]

    for i in range(2):
        gain_copy(i).start()
        gain_add(i)
    expert_swaps[2].start()
    gain_copy(2).start()
    line_step(3, 2)
    line_step(3, 3)
    gain_add(2)
    gain_copy(3).start()
    total_block(sums[2], value_total)
    line_step(4, 0)
    gain_add(3)
    gain_copy(4).start()
    for turn in range(1, LEVELS):
        line_step(4, turn)
    total_block(sums[3], query_total)
    gain_add(4)
    gain_grads[...] = gains[...]
    total_block(sums[4], key_total)

    @pl.loop(0, pairs)
    def _(b):
        core_copy(0, b, mixture_part.at[slot_at(b, 1)]).wait_send()

    for a in range(5):
        for turn in range(LEVELS):
            side_copy(a, turn).wait_send()
        line = sums[a].from_line
        for turn in range(LEVELS - 1):
            remote(
                line.at[0], line.at[turn], sums[a].line_s.at[turn], sums[a].line_r.at[turn], (own, 1 - x)
            ).wait_send()
    first_swap.wait_send()
    for copy in expert_swaps:
        copy.wait()


def run_last(
    mixture_part, normed_pair, attention_rows, weights_full, theirs, norm_args, collective_id
):
    f32, bf16 = jnp.float32, jnp.bfloat16
    shape = jax.ShapeDtypeStruct
    hbm = pl.BlockSpec(memory_space=pl.ANY)
    vmem = pl.BlockSpec(memory_space=pltpu.VMEM)
    dma = pltpu.SemaphoreType.DMA
    rows, head_cols = attention_rows[0].shape
    half_rows, width = norm_args[0].shape
    wide = mixture_part.shape[1:]
    block = (half_rows, head_cols)
    pairs = 2 * LEVELS
    flops = 2 * rows * head_cols * width * 8
    nbytes = 2 * (mixture_part.size + 12 * weights_full[0].size)
    outs = pl.pallas_call(
        last_kernel,
        out_shape=[shape(block, f32)] * 4
        + [shape(wide, f32)]
        + [shape(t.shape, t.dtype) for t in theirs]
        + [shape((half_rows, width), f32), shape((8, width), f32)],
        in_specs=[hbm] + [vmem] * 5 + [hbm] * 7 + [vmem] * 5,
        out_specs=[vmem] * 5 + [hbm] * 3 + [vmem] * 2,
        scratch_shapes=[
            pltpu.VMEM((pairs,) + wide, bf16),
            pltpu.VMEM((LEVELS,) + wide, bf16),
            pltpu.VMEM((LEVELS + 1,) + wide, bf16),
            pltpu.VMEM((pairs,) + wide, bf16),
            pltpu.VMEM((4, pairs) + block, bf16),
            pltpu.VMEM((4, LEVELS) + block, bf16),
            pltpu.VMEM((4, LEVELS + 1) + block, bf16),
            pltpu.VMEM((2, 2) + block, bf16),
            pltpu.VMEM((2, half_rows, width), bf16),
        ]
        + [pltpu.VMEM((rows, head_cols), bf16)] * 4
        + [pltpu.VMEM(weights_full[0].shape, bf16)] * 2
        + [
            pltpu.VMEM((2, half_rows, width), f32),
            pltpu.VMEM((half_rows, width), bf16),
            pltpu.VMEM((half_rows, width), bf16),
            pltpu.VMEM((8, width), f32),
            pltpu.VMEM((5, 8, width), f32),
        ]
        + [dma((5, pairs))] * 2
        + [dma((5, LEVELS))] * 2
        + [dma((5, LEVELS + 1))] * 2
        + [dma((pairs,)), dma((4,)), dma((5,)), dma((5,)), dma((5,)), dma((5,))],
        compiler_params=pltpu.CompilerParams(
            collective_id=collective_id, has_side_effects=True, vmem_limit_bytes=67_043_328
        ),
        cost_estimate=pl.CostEstimate(flops=flops, bytes_accessed=nbytes, transcendentals=0),
        name="last",
    )(mixture_part, normed_pair, *attention_rows, *weights_full, *theirs, *norm_args)
    return outs[:5], outs[5:8], outs[8], outs[9]


def half_of(rows):
    count = rows.shape[0] // lax.axis_size("tp")
    return lax.dynamic_slice_in_dim(rows, lax.axis_index("tp") * count, count, axis=0)


def per_device_dense(
    block_input,
    upstream_grad,
    first_gain,
    second_gain,
    query_weight,
    key_weight,
    value_weight,
    output_weight,
    gate_weight,
    up_weight,
    down_weight,
    routes,
    gate_values,
):
    local_rows, model_width = block_input.shape
    expert_count = EXP_DEV * lax.axis_size("fsdp")
    f32 = jnp.float32
    my_routes = half_of(routes)
    expert_names = jnp.arange(expert_count, dtype=jnp.int32)[None, :]
    own_weights = (gate_weight[0], up_weight[0], down_weight[0])
    weights_full, gathered, other_weights, attention_rows, out_part, first_scale = run_attend(
        (query_weight, key_weight, value_weight, output_weight),
        block_input,
        upstream_grad,
        first_gain[None],
        routes.T,
        gate_values.T,
        own_weights,
        1,
    )
    query_full, key_full, value_full, output_full = weights_full
    query_rows, key_rows, value_rows, mixed_rows = attention_rows
    upstream_all, gates_all, normed_pair = gathered
    (
        middle,
        middle_grad,
        second_term,
        mixture_part,
        gate_mine,
        gate_theirs,
        up_mine,
        up_theirs,
        down_mine,
        down_theirs,
        down_landed,
    ) = run_experts(
        gates_all,
        second_gain[None],
        out_part,
        block_input,
        upstream_grad,
        upstream_all,
        own_weights,
        other_weights,
        2,
    )
    sums, landed, input_grad, gain_grads = run_last(
        mixture_part,
        normed_pair,
        (mixed_rows, query_rows, key_rows, value_rows),
        (output_full, query_full, key_full, value_full),
        (gate_theirs, up_theirs, down_theirs),
        (block_input, first_scale, first_gain[None], middle_grad, second_term),
        4,
    )
    query_grad, key_grad, value_grad, output_grad, mixture = sums
    gate_grad, up_grad, down_grad = (
        mine.astype(f32) + theirs.astype(f32)
        for mine, theirs in (
            (gate_mine, landed[0]),
            (up_mine, landed[1]),
            (down_mine, jnp.concatenate([down_landed, landed[2]], axis=0)),
        )
    )
    block_output = middle + mixture[:, :model_width]
    route_back = mixture[:, model_width : model_width + expert_count]
    route_grad = jnp.sum(
        jnp.where(my_routes[:, :, None] == expert_names[None], route_back[:, None, :], 0.0), axis=2
    )
    return (
        block_output,
        input_grad,
        gain_grads[0],
        gain_grads[1],
        query_grad,
        key_grad,
        value_grad,
        output_grad,
        gate_grad[None],
        up_grad[None],
        down_grad[None],
        route_grad,
    )


def solution(mesh):
    dense = 2 * TOP >= EXP_DEV * mesh.shape["fsdp"] and mesh.shape["fsdp"] == 4 * LEVELS
    per_device = per_device_dense if dense else per_device_slots
    in_specs = (
        P(("fsdp", "tp"), None),
        P(("fsdp", "tp"), None),
        P(),
        P(),
        P("fsdp", "tp"),
        P("fsdp", "tp"),
        P("fsdp", "tp"),
        P("fsdp", "tp"),
        P("fsdp", None, "tp"),
        P("fsdp", None, "tp"),
        P("fsdp", "tp", None),
        P("fsdp", None),
        P("fsdp", None),
    )
    out_specs = (
        P(("fsdp", "tp"), None),
        P(("fsdp", "tp"), None),
        P(),
        P(),
        P("fsdp", "tp"),
        P("fsdp", "tp"),
        P("fsdp", "tp"),
        P("fsdp", "tp"),
        P("fsdp", None, "tp"),
        P("fsdp", None, "tp"),
        P("fsdp", "tp", None),
        P(("fsdp", "tp"), None),
    )
    return jax.shard_map(
        per_device, mesh=mesh, in_specs=in_specs, out_specs=out_specs, check_vma=False
    )
```

```python
import functools

import jax
import jax.numpy as jnp
from jax import lax
from jax.experimental import pallas as pl
from jax.experimental.pallas import tpu as pltpu
from jax.sharding import PartitionSpec as P

HD = 128
TOP = 8
EXP_DEV = 1


epsilon = 1e-05


def route_slots(route_rows, expert_count, capacity):
    flat_routes = route_rows.reshape(-1)
    onehot = (flat_routes[:, None] == jnp.arange(expert_count, dtype=jnp.int32)[None, :]).astype(
        jnp.int32
    )
    earlier = jnp.cumsum(onehot, axis=0, dtype=jnp.int32) - onehot
    ranked = jnp.sum(earlier * onehot, axis=1, dtype=jnp.int32)
    return flat_routes * capacity + ranked


def pair_rows(row_block):
    return lax.all_gather(row_block, "tp", axis=0, tiled=True)


def pair_sums(term_block):
    return lax.psum_scatter(term_block, "tp", scatter_dimension=0, tiled=True)


def to_owners(buffer):
    return lax.all_to_all(buffer, "fsdp", split_axis=0, concat_axis=0, tiled=True)


def to_sources(buffer):
    return lax.all_to_all(buffer, "fsdp", split_axis=0, concat_axis=0, tiled=True)


def projections(query_weight, key_weight, value_weight, output_weight):
    return (
        lax.all_gather(query_weight, "fsdp", axis=0, tiled=True),
        lax.all_gather(key_weight, "fsdp", axis=0, tiled=True),
        lax.all_gather(value_weight, "fsdp", axis=0, tiled=True),
        lax.all_gather(output_weight, "fsdp", axis=0, tiled=True),
    )


def scatter_rows(row_block, slot_index, total_rows):
    return (
        jnp.zeros((total_rows, row_block.shape[1]), row_block.dtype).at[slot_index].set(row_block)
    )


def spread_rows(row_block, copies):
    return jnp.broadcast_to(
        row_block[:, None, :], (row_block.shape[0], copies, row_block.shape[1])
    ).reshape(-1, row_block.shape[1])


def contract_rows(left_block, right_block):
    return lax.dot_general(
        left_block, right_block, (((0,), (0,)), ((), ())), preferred_element_type=jnp.float32
    )


def contract_cols(left_block, right_block):
    return lax.dot_general(
        left_block, right_block, (((1,), (1,)), ((), ())), preferred_element_type=jnp.float32
    )


def send_out(full_buffer):
    return to_owners(full_buffer)


def send_back(group_parts):
    owner_count, local_experts, capacity, model_width = group_parts.shape
    return to_sources(group_parts).reshape(owner_count * local_experts * capacity, model_width)


def per_device_slots(
    block_input,
    upstream_grad,
    first_gain,
    second_gain,
    query_weight,
    key_weight,
    value_weight,
    output_weight,
    gate_weight,
    up_weight,
    down_weight,
    routes,
    gate_values,
):
    pair_count = lax.axis_size("tp")
    owner_count = lax.axis_size("fsdp")
    local_rows = block_input.shape[0]
    seq_rows = local_rows * pair_count
    model_width = block_input.shape[1]
    head_cols = query_weight.shape[1]
    local_heads = head_cols // HD
    expert_count = EXP_DEV * owner_count
    capacity = 3 * seq_rows * TOP // (2 * expert_count)
    inv_root = HD ** (-0.5)
    first_scale = lax.rsqrt(jnp.mean(block_input * block_input, axis=1, keepdims=True) + epsilon)
    first_normed = (block_input * first_scale * first_gain).astype(jnp.bfloat16)
    normed_rows = pair_rows(first_normed)
    query_full, key_full, value_full, output_full = projections(
        query_weight, key_weight, value_weight, output_weight
    )
    query_rows = (
        jnp.dot(normed_rows, query_full, preferred_element_type=jnp.float32)
        .astype(jnp.bfloat16)
        .reshape(seq_rows, local_heads, HD)
    )
    key_rows = (
        jnp.dot(normed_rows, key_full, preferred_element_type=jnp.float32)
        .astype(jnp.bfloat16)
        .reshape(seq_rows, local_heads, HD)
    )
    value_rows = (
        jnp.dot(normed_rows, value_full, preferred_element_type=jnp.float32)
        .astype(jnp.bfloat16)
        .reshape(seq_rows, local_heads, HD)
    )
    scores = (
        jnp.einsum("shd,thd->hst", query_rows, key_rows, preferred_element_type=jnp.float32)
        * inv_root
    )
    row_top = jnp.max(scores, axis=2, keepdims=True)
    log_total = row_top + jnp.log(jnp.sum(jnp.exp(scores - row_top), axis=2, keepdims=True))
    soft_weights = jnp.exp(scores - log_total)
    mixed_rows = jnp.einsum(
        "hst,thd->shd",
        soft_weights.astype(jnp.bfloat16),
        value_rows,
        preferred_element_type=jnp.float32,
    )
    mixed_rows = mixed_rows.astype(jnp.bfloat16).reshape(seq_rows, head_cols)
    middle = block_input + pair_sums(contract_cols(mixed_rows, output_full))
    second_scale = lax.rsqrt(jnp.mean(middle * middle, axis=1, keepdims=True) + epsilon)
    second_normed = (middle * second_scale * second_gain).astype(jnp.bfloat16)
    moe_rows = pair_rows(second_normed)
    slot_index = route_slots(routes, expert_count, capacity)
    send_rows = scatter_rows(spread_rows(moe_rows, TOP), slot_index, expert_count * capacity)
    arrived = send_out(send_rows.reshape(owner_count, EXP_DEV, capacity, model_width))
    gate_act = jnp.einsum(
        "secd,edf->secf", arrived, gate_weight, preferred_element_type=jnp.float32
    )
    up_act = jnp.einsum("secd,edf->secf", arrived, up_weight, preferred_element_type=jnp.float32)
    sigmoid_gate = jax.nn.sigmoid(gate_act)
    hidden = (gate_act * sigmoid_gate * up_act).astype(jnp.bfloat16)
    expert_out = jnp.einsum(
        "secf,efd->secd", hidden, down_weight, preferred_element_type=jnp.float32
    ).astype(jnp.bfloat16)
    returned = send_back(expert_out)
    picked = returned[slot_index].reshape(seq_rows, TOP, model_width).astype(jnp.float32)
    mixture = jnp.sum(gate_values[:, :, None] * picked, axis=1)
    block_output = middle + pair_sums(mixture)
    upstream_rows = lax.all_gather(upstream_grad, "tp", axis=0, tiled=True)
    route_terms = jnp.sum(upstream_rows[:, None, :] * picked, axis=2)
    routed_cot = (
        (gate_values[:, :, None] * upstream_rows[:, None, :])
        .astype(jnp.bfloat16)
        .reshape(seq_rows * TOP, model_width)
    )
    cot_send = scatter_rows(routed_cot, slot_index, expert_count * capacity)
    cot_arrived = send_out(cot_send.reshape(owner_count, EXP_DEV, capacity, model_width))
    hidden_cot = jnp.einsum(
        "secd,efd->secf", cot_arrived, down_weight, preferred_element_type=jnp.float32
    )
    down_grad = jnp.einsum(
        "secf,secd->efd", hidden, cot_arrived, preferred_element_type=jnp.float32
    )
    gate_cot = (
        hidden_cot * up_act * sigmoid_gate * (1.0 + gate_act * (1.0 - sigmoid_gate))
    ).astype(jnp.bfloat16)
    up_cot = (hidden_cot * gate_act * sigmoid_gate).astype(jnp.bfloat16)
    gate_grad = jnp.einsum("secd,secf->edf", arrived, gate_cot, preferred_element_type=jnp.float32)
    up_grad = jnp.einsum("secd,secf->edf", arrived, up_cot, preferred_element_type=jnp.float32)
    input_cot = jnp.einsum(
        "secf,edf->secd", gate_cot, gate_weight, preferred_element_type=jnp.float32
    )
    input_cot = (
        input_cot
        + jnp.einsum("secf,edf->secd", up_cot, up_weight, preferred_element_type=jnp.float32)
    ).astype(jnp.bfloat16)
    came_back = send_back(input_cot)
    normed_cot = jnp.sum(
        came_back[slot_index].reshape(seq_rows, TOP, model_width).astype(jnp.float32), axis=1
    )
    second_cot, route_grad = (
        lax.psum_scatter(
            normed_cot.astype(jnp.bfloat16), "tp", scatter_dimension=0, tiled=True
        ).astype(jnp.float32),
        lax.psum_scatter(
            route_terms.astype(jnp.bfloat16), "tp", scatter_dimension=0, tiled=True
        ).astype(jnp.float32),
    )
    weighted_two = second_cot * second_gain
    second_term = jnp.sum(second_cot * middle * second_scale, axis=0)
    middle_grad = upstream_grad + second_scale * (
        weighted_two
        - middle
        * second_scale
        * second_scale
        * jnp.mean(weighted_two * middle, axis=1, keepdims=True)
    )
    middle_rows = pair_rows(middle_grad.astype(jnp.bfloat16))
    query_full, key_full, value_full, output_full = projections(
        query_weight, key_weight, value_weight, output_weight
    )
    out_term = contract_rows(middle_rows, mixed_rows)
    mixed_cot = (
        jnp.dot(middle_rows, output_full, preferred_element_type=jnp.float32)
        .astype(jnp.bfloat16)
        .reshape(seq_rows, local_heads, HD)
    )
    scores = (
        jnp.einsum("shd,thd->hst", query_rows, key_rows, preferred_element_type=jnp.float32)
        * inv_root
    )
    soft_weights = jnp.exp(scores - log_total)
    value_cot = jnp.einsum(
        "hst,shd->thd",
        soft_weights.astype(jnp.bfloat16),
        mixed_cot,
        preferred_element_type=jnp.float32,
    )
    value_cot = value_cot.astype(jnp.bfloat16).reshape(seq_rows, head_cols)
    soft_cot = jnp.einsum("shd,thd->hst", mixed_cot, value_rows, preferred_element_type=jnp.float32)
    score_cot = (
        soft_weights
        * (soft_cot - jnp.sum(soft_weights * soft_cot, axis=2, keepdims=True))
        * inv_root
    ).astype(jnp.bfloat16)
    query_cot = (
        jnp.einsum("hst,thd->shd", score_cot, key_rows, preferred_element_type=jnp.float32)
        .astype(jnp.bfloat16)
        .reshape(seq_rows, head_cols)
    )
    key_cot = (
        jnp.einsum("hst,shd->thd", score_cot, query_rows, preferred_element_type=jnp.float32)
        .astype(jnp.bfloat16)
        .reshape(seq_rows, head_cols)
    )
    query_term = contract_rows(normed_rows, query_cot)
    key_term = contract_rows(normed_rows, key_cot)
    value_term = contract_rows(normed_rows, value_cot)
    first_terms = (
        contract_cols(query_cot, query_full)
        + contract_cols(key_cot, key_full)
        + contract_cols(value_cot, value_full)
    )
    first_cot = pair_sums(first_terms)
    weighted_one = first_cot * first_gain
    first_term = jnp.sum(first_cot * block_input * first_scale, axis=0)
    input_grad = middle_grad + first_scale * (
        weighted_one
        - block_input
        * first_scale
        * first_scale
        * jnp.mean(weighted_one * block_input, axis=1, keepdims=True)
    )
    query_grad, key_grad, value_grad, output_grad = (
        lax.psum_scatter(query_term, "fsdp", scatter_dimension=0, tiled=True),
        lax.psum_scatter(key_term, "fsdp", scatter_dimension=0, tiled=True),
        lax.psum_scatter(value_term, "fsdp", scatter_dimension=0, tiled=True),
        lax.psum_scatter(out_term, "fsdp", scatter_dimension=0, tiled=True),
    )
    first_gain_grad, second_gain_grad = lax.psum((first_term, second_term), ("fsdp", "tp"))
    return (
        block_output,
        input_grad,
        first_gain_grad,
        second_gain_grad,
        query_grad,
        key_grad,
        value_grad,
        output_grad,
        gate_grad,
        up_grad,
        down_grad,
        route_grad,
    )


MESH = pl.DeviceIdType.MESH


def place():
    here = lax.axis_index("fsdp")
    return here // 4, (here // 2) % 2, here % 2, lax.axis_index("tp")


def index_of(z, y, c):
    return (z * 2 + y) * 2 + c


LEVELS = 4
LEVEL_ORDER = sum(
    level << (8 * turn + 2 * z)
    for turn, row in enumerate(((3, 3, 0, 0), (2, 2, 1, 1), (1, 0, 3, 2), (0, 1, 2, 3)))
    for z, level in enumerate(row)
) - (1 << 32)


def level_at(turn, z):
    return (jnp.int32(LEVEL_ORDER) >> (8 * turn + 2 * z)) & 3


def line_ends(z):
    return (z + 1) // LEVELS, (LEVELS - z) // LEVELS


def plane_greet(pair=False, far=False):
    z, y, c, x = place()
    top, bottom = line_ends(z)
    barrier = pltpu.get_barrier_semaphore()
    partners = [(index_of(z, 1 - y, c), x), (index_of(z, y, 1 - c), x)]
    if pair:
        partners.append((index_of(z, y, c), 1 - x))
    if far:
        partners.append((index_of((z + 2) % LEVELS, y, c), x))
    for partner in partners:
        pl.semaphore_signal(barrier, inc=1, device_id=partner, device_id_type=MESH)

    @pl.when(top == 0)
    def _():
        above = (index_of(z + 1, y, c), x)
        pl.semaphore_signal(barrier, inc=1, device_id=above, device_id_type=MESH)

    @pl.when(bottom == 0)
    def _():
        below = (index_of(z - 1, y, c), x)
        pl.semaphore_signal(barrier, inc=1, device_id=below, device_id_type=MESH)

    pl.semaphore_wait(barrier, len(partners) + 2 - top - bottom)


def remote(src, dst, send_sem, recv_sem, target):
    return pltpu.make_async_remote_copy(
        src_ref=src,
        dst_ref=dst,
        send_sem=send_sem,
        recv_sem=recv_sem,
        device_id=target,
        device_id_type=MESH,
    )


class PlaneGather:
    def __init__(self, mine, full, send_sems, recv_sems):
        self.mine, self.full = mine, full
        self.send_sems, self.recv_sems = send_sems, recv_sems
        self.z, self.y, self.c, self.x = place()
        self.top, self.bottom = line_ends(self.z)

    def _copy(self, number, src, slot, target):
        return remote(
            src, self.full.at[slot], self.send_sems.at[number], self.recv_sems.at[slot], target
        )

    def arrived(self, slot):
        here = self.full.at[slot]
        remote(here, here, self.send_sems.at[0], self.recv_sems.at[slot], (0, self.x)).wait_recv()

    def start(self):
        z, y, c, x = self.z, self.y, self.c, self.x
        own = index_of(z, y, c)
        up = self._copy(0, self.mine, own, (index_of(z + 1, y, c), x))
        down = self._copy(1, self.mine, own, (index_of(z - 1, y, c), x))
        pl.when(self.top == 0)(up.start)
        pl.when(self.bottom == 0)(down.start)
        self._copy(2, self.mine, own, (index_of(z, 1 - y, c), x)).start()
        self._copy(3, self.mine, own, (index_of(z, y, 1 - c), x)).start()

    def from_line(self, step):
        z, y, c, x = self.z, self.y, self.c, self.x
        level = level_at(3 - step, z)
        slot = index_of(level, y, c)
        self.arrived(slot)
        onward = z + 1 - 2 * ((level + LEVELS - z) // LEVELS)
        src, number = self.full.at[slot], 4 + 3 * (step - 1)
        forward = self._copy(number, src, slot, (index_of(onward, y, c), x))
        pl.when(self.top + self.bottom == 0)(forward.start)
        self._copy(number + 1, src, slot, (index_of(z, 1 - y, c), x)).start()
        self._copy(number + 2, src, slot, (index_of(z, y, 1 - c), x)).start()

    def from_side(self, step):
        z, y, c, x = self.z, self.y, self.c, self.x
        slot = index_of(level_at(3 - step, z), 1 - y, c)
        self.arrived(slot)
        self._copy(13 + step, self.full.at[slot], slot, (index_of(z, y, 1 - c), x)).start()

    def from_core(self, step, side):
        z, y, c = self.z, self.y, self.c
        self.arrived(index_of(level_at(3 - step, z), (y + side) % 2, 1 - c))

    def finish(self):
        for number in range(GATHER_SENDS):
            wait = self._copy(number, self.mine, 0, (0, self.x)).wait_send
            if number == 0:
                pl.when(self.top == 0)(wait)
            elif number == 1:
                pl.when(self.bottom == 0)(wait)
            elif number in (4, 7, 10):
                pl.when(self.top + self.bottom == 0)(wait)
            else:
                wait()


GATHER_SENDS = 17


def attend_kernel(
    query_mine,
    key_mine,
    value_mine,
    output_mine,
    block_input,
    upstream,
    first_gain,
    routes,
    gate_values,
    gate_own,
    up_own,
    down_own,
    query_full,
    key_full,
    value_full,
    output_full,
    upstream_all,
    gates_all,
    normed_pair,
    gate_other,
    up_other,
    down_other,
    query_rows,
    key_rows,
    value_rows,
    mixed_rows,
    out_part,
    first_scale,
    weights,
    normed,
    upstream_mine,
    gates_mine,
    send_sems,
    recv_sems,
    wide_s,
    wide_r,
    own_sems,
    keep_sems,
    pair_s,
    pair_r,
):
    bf16, f32 = jnp.bfloat16, jnp.float32
    z, y, c, x = place()
    own = index_of(z, y, c)
    half_rows, width = block_input.shape
    rows, head_cols = mixed_rows.shape
    inv_root = HD ** (-0.5)
    step = 16

    mine = (query_mine, key_mine, value_mine, output_mine)
    kept = [
        pltpu.make_async_copy(mine[a], weights.at[a, own], own_sems.at[a]) for a in range(4)
    ]
    for copy in kept:
        copy.start()
    plane_greet(pair=True)
    plans = [
        PlaneGather(mine[a], weights.at[a], send_sems.at[a], recv_sems.at[a]) for a in range(4)
    ] + [
        PlaneGather(ref, full, wide_s.at[i], wide_r.at[i])
        for i, (ref, full) in enumerate(((upstream_mine, upstream_all), (gates_mine, gates_all)))
    ]
    first, output, wide = plans[:3], plans[3:4], plans[4:]
    for plan in first:
        plan.start()

    def swap(i, src, dst):
        return remote(src, dst, pair_s.at[i], pair_r.at[i], (own, 1 - x))

    swaps = [
        swap(0, normed.at[x], normed.at[x]),
        swap(1, gate_own, gate_other),
        swap(2, up_own, up_other),
        swap(3, down_own, down_other),
    ]
    gain = first_gain[...]

    @pl.loop(0, half_rows // step)
    def _(i):
        at = pl.ds(pl.multiple_of(i * step, step), step)
        value = block_input[at, :]
        scale = lax.rsqrt(jnp.mean(value * value, axis=1, keepdims=True) + epsilon)
        first_scale[at, :] = scale
        normed[x, at, :] = (value * scale * gain).astype(bf16)

    for copy in swaps:
        copy.start()

    @pl.loop(0, half_rows // step)
    def _(i):
        at = pl.ds(pl.multiple_of(i * step, step), step)
        upstream_mine[at, :] = upstream[at, :].astype(bf16)

    here = pl.ds(pl.multiple_of(x * half_rows, half_rows), half_rows)
    names = jnp.transpose(routes[:, here].astype(f32))
    values = jnp.transpose(gate_values[:, here])
    lane = lax.broadcasted_iota(jnp.int32, (half_rows, ROUTE_COLS), 1).astype(f32)
    table = jnp.zeros((half_rows, ROUTE_COLS), f32)
    for j in range(TOP):
        table = table + jnp.where(lane == names[:, j : j + 1], values[:, j : j + 1], 0.0)
    gates_mine[...] = table
    wide_kept = [
        pltpu.make_async_copy(upstream_mine, upstream_all.at[own], own_sems.at[4]),
        pltpu.make_async_copy(gates_mine, gates_all.at[own], own_sems.at[5]),
    ]
    for copy in wide_kept:
        copy.start()

    def line(group, turn):
        for plan in group:
            plan.from_line(turn)

    def side(group, turn):
        for plan in group:
            plan.from_side(turn)

    def core(group):
        for plan in group:
            for turn in range(LEVELS):
                for which in range(2):
                    plan.from_core(turn, which)

    line(first, 1)
    side(first, 0)
    line(first, 2)
    side(first, 1)
    line(first, 3)
    for plan in output:
        plan.start()
    side(first, 2)
    side(first, 3)
    line(output, 1)
    core(first)
    line(output, 2)
    for plan in wide:
        plan.start()
    swaps[0].wait_recv()
    for copy in kept:
        copy.wait()
    keeps = [
        pltpu.make_async_copy(src, dst, keep_sems.at[i])
        for i, (src, dst) in enumerate(
            (
                (weights.at[0], query_full),
                (weights.at[1], key_full),
                (weights.at[2], value_full),
                (normed, normed_pair),
                (weights.at[3], output_full),
            )
        )
    ]
    for copy in keeps[:4]:
        copy.start()

    def flat(ref):
        value = ref[...]
        return value.reshape(value.shape[0] * value.shape[1], value.shape[2])

    for a, ref in enumerate((query_rows, key_rows, value_rows)):
        ref[...] = nn(flat(normed), flat(weights.at[a])).astype(bf16)
        if a == 0:
            line(output, 3)
            side(output, 0)
    side(output, 1)
    line(wide, 1)

    def head(h):
        cols = pl.ds(pl.multiple_of(h * HD, HD), HD)
        scores = nt(query_rows[:, cols], key_rows[:, cols]) * inv_root
        row_top = jnp.max(scores, axis=1, keepdims=True)
        log_total = row_top + jnp.log(jnp.sum(jnp.exp(scores - row_top), axis=1, keepdims=True))
        soft = jnp.exp(scores - log_total)
        mixed_rows[:, cols] = nn(soft.astype(bf16), value_rows[:, cols]).astype(bf16)

    @pl.loop(0, head_cols // HD // 2)
    def _(h):
        head(2 * h)
        head(2 * h + 1)

    side(output, 2)
    side(output, 3)
    line(wide, 2)
    core(output)
    keeps[4].start()
    panel = 4

    @pl.loop(0, weights.shape[1] // panel)
    def _(n):
        part = weights[3, pl.ds(n * panel, panel)].reshape(panel * half_rows, head_cols)
        cols = pl.ds(pl.multiple_of(n * panel * half_rows, panel * half_rows), panel * half_rows)
        out_part[:, :, cols] = nt(mixed_rows[...], part).reshape(2, half_rows, panel * half_rows)

    side(wide, 0)
    line(wide, 3)
    for turn in range(1, LEVELS):
        side(wide, turn)
    core(wide)
    for plan in plans:
        plan.finish()
    for copy in wide_kept + keeps:
        copy.wait()
    swaps[0].wait_send()
    for copy in swaps[1:]:
        copy.wait()


def run_attend(shards, block_input, upstream, first_gain, routes, gate_values, experts, collective_id):
    bf16, f32 = jnp.bfloat16, jnp.float32
    owner_count = lax.axis_size("fsdp")
    half_rows, width = block_input.shape
    head_cols = shards[0].shape[1]
    rows = 2 * half_rows
    shape = jax.ShapeDtypeStruct
    hbm = pl.BlockSpec(memory_space=pl.ANY)
    vmem = pl.BlockSpec(memory_space=pltpu.VMEM)
    dma = pltpu.SemaphoreType.DMA
    full = (owner_count,) + shards[0].shape
    outs = pl.pallas_call(
        attend_kernel,
        out_shape=[shape(full, bf16)] * 4
        + [
            shape((owner_count, half_rows, width), bf16),
            shape((owner_count, half_rows, ROUTE_COLS), f32),
            shape((2, half_rows, width), bf16),
        ]
        + [shape(w.shape, w.dtype) for w in experts]
        + [shape((rows, head_cols), bf16)] * 4
        + [shape((2, half_rows, width), f32), shape((half_rows, 1), f32)],
        in_specs=[vmem] * 9 + [hbm] * 3,
        out_specs=[hbm] * 10 + [vmem] * 6,
        scratch_shapes=[
            pltpu.VMEM((4,) + full, bf16),
            pltpu.VMEM((2, half_rows, width), bf16),
            pltpu.VMEM((half_rows, width), bf16),
            pltpu.VMEM((half_rows, ROUTE_COLS), f32),
            dma((4, GATHER_SENDS)),
            dma((4, owner_count)),
            dma((2, GATHER_SENDS)),
            dma((2, owner_count)),
            dma((6,)),
            dma((5,)),
            dma((4,)),
            dma((4,)),
        ],
        compiler_params=pltpu.CompilerParams(
            collective_id=collective_id, has_side_effects=True, vmem_limit_bytes=60 * 2**20
        ),
        cost_estimate=pl.CostEstimate(
            flops=2 * 4 * rows * head_cols * width,
            bytes_accessed=16 * shards[0].size * owner_count,
            transcendentals=0,
        ),
        name="attend",
    )(*shards, block_input, upstream, first_gain, routes, gate_values, *experts)
    return outs[:4], outs[4:7], outs[7:10], outs[10:14], outs[14], outs[15]


class PlaneSums:
    def __init__(self, own_parts, from_core, from_side, from_line, sems, kept=0):
        self.own, self.from_core, self.kept = own_parts, from_core, kept
        self.from_side, self.from_line = from_side, from_line
        self.core_s, self.core_r, self.side_s, self.side_r, self.line_s, self.line_r = sems
        self.z, self.y, self.c, self.x = place()
        self.top, self.bottom = line_ends(self.z)

    def side_arrived(self, turn):
        here = self.from_side.at[turn]
        remote(here, here, self.side_s.at[turn], self.side_r.at[turn], (0, self.x)).wait_recv()

    def line_arrived(self, slot):
        here = self.from_line.at[slot]
        remote(here, here, self.line_s.at[0], self.line_r.at[slot], (0, self.x)).wait_recv()

    def to_line(self, turn):
        z, y, c, x = self.z, self.y, self.c, self.x
        mine = self.own.at[self.kept + turn]
        level = level_at(turn, z)

        @pl.when(self.top + self.bottom == 0)
        def _():
            self.line_arrived(level)
            add_block(mine, self.from_line.at[level], mine)

        down = (z + LEVELS - level) // (LEVELS + 1)
        onward = z + 1 - 2 * down
        reached = 1 - jnp.minimum(1, jnp.abs(onward - level))
        slot = level + down * reached * (LEVELS - level)
        copy = remote(
            mine,
            self.from_line.at[slot],
            self.line_s.at[turn],
            self.line_r.at[slot],
            (index_of(onward, y, c), x),
        )
        copy.start()


def add_block(one, two, out):
    step = 32

    @pl.loop(0, out.shape[0] // step)
    def _(i):
        rows = pl.ds(pl.multiple_of(i * step, step), step)
        value = one[rows, :].astype(jnp.float32) + two[rows, :].astype(jnp.float32)
        out[rows, :] = value.astype(out.dtype)


def total_block(plan, total):
    step = 32
    mine = plan.own.at[plan.kept + LEVELS - 1]
    below, above = plan.from_line.at[plan.z], plan.from_line.at[LEVELS]

    @pl.loop(0, total.shape[0] // step)
    def _(i):
        rows = pl.ds(pl.multiple_of(i * step, step), step)
        total[rows, :] = mine[rows, :].astype(jnp.float32)

    for end, block, slot in ((plan.bottom, below, plan.z), (plan.top, above, LEVELS)):

        @pl.when(end == 0)
        def _():
            plan.line_arrived(slot)

            @pl.loop(0, total.shape[0] // step)
            def _(i):
                rows = pl.ds(pl.multiple_of(i * step, step), step)
                total[rows, :] = total[rows, :] + block[rows, :].astype(jnp.float32)


ROUTE_COLS = 128


def nn(left, right):
    return lax.dot_general(
        left, right, (((1,), (0,)), ((), ())), preferred_element_type=jnp.float32
    )


def nt(left, right):
    return lax.dot_general(
        left, right, (((1,), (1,)), ((), ())), preferred_element_type=jnp.float32
    )


def tn(left, right):
    return lax.dot_general(
        left, right, (((0,), (0,)), ((), ())), preferred_element_type=jnp.float32
    )


def pair_block(ref, pair):
    value = ref[pl.ds(2 * pair, 2)]
    return value.reshape(value.shape[0] * value.shape[1], value.shape[2])


def experts_kernel(
    gates,
    second_gain,
    out_part,
    block_input,
    upstream,
    upstream_hbm,
    gate_own,
    up_own,
    down_own,
    gate_other,
    up_other,
    down_other,
    middle,
    middle_grad,
    second_term,
    mixture_hbm,
    gate_mine,
    gate_theirs,
    up_mine,
    up_theirs,
    down_mine,
    down_theirs,
    down_landed,
    rows_all,
    u_all,
    wg,
    wu,
    wd,
    hidden,
    gcot,
    ucot,
    rext,
    tmp,
    from_core,
    from_side,
    from_line,
    gstage,
    wide,
    second_scale,
    route_half,
    gather_s,
    gather_r,
    core_s,
    core_r,
    side_s,
    side_r,
    line_s,
    line_r,
    load_sems,
    out_sems,
    pair_s,
    pair_r,
):
    bf16, f32 = jnp.bfloat16, jnp.float32
    z, y, c, x = place()
    top, bottom = line_ends(z)
    interior = 1 - top - bottom
    me = lax.axis_index("fsdp")
    partner = (me, 1 - x)
    halves, width, units = wg.shape
    half_rows = middle.shape[0]
    pair_rows_ = 2 * half_rows
    pairs = 2 * LEVELS
    panel = 512
    block = 256
    step = 16

    loads = [
        pltpu.make_async_copy(src, dst, load_sems.at[i])
        for i, (src, dst) in enumerate(
            (
                (out_part.at[1 - x], middle_grad),
                (out_part.at[x], middle),
                (block_input, wide),
                (down_own, wd.at[x]),
                (down_other, wd.at[1 - x]),
                (upstream_hbm, u_all),
                (gate_own, wg.at[x]),
                (up_own, wu.at[x]),
                (gate_other, wg.at[1 - x]),
                (up_other, wu.at[1 - x]),
            )
        )
    ]
    for load in loads:
        load.start()

    plane_greet(pair=True)
    gather = PlaneGather(rows_all.at[me], rows_all, gather_s, gather_r)
    sums = PlaneSums(
        from_core,
        from_core,
        from_side,
        from_line,
        (core_s, core_r, side_s, side_r, line_s, line_r),
        LEVELS,
    )

    loads[0].wait()

    @pl.loop(0, half_rows // step)
    def _(i):
        at = pl.ds(pl.multiple_of(i * step, step), step)
        tmp[0, 0, at, :] = middle_grad[at, :].astype(bf16)

    meet = remote(tmp.at[0, 0], tmp.at[0, 1], pair_s.at[0], pair_r.at[0], partner)
    meet.start()
    for load in loads[1:6]:
        load.wait()

    @pl.loop(0, pairs)
    def _(b):
        at_rows = pl.ds(pl.multiple_of(b * pair_rows_, pair_rows_), pair_rows_)
        us = pair_block(u_all, b)
        for h in range(halves):
            ucot[h, at_rows, :] = nt(us, wd[h]).astype(bf16)

    meet.wait()
    gain = second_gain[...]

    @pl.loop(0, half_rows // step)
    def _(i):
        at = pl.ds(pl.multiple_of(i * step, step), step)
        value = wide[at, :] + (middle[at, :] + tmp[0, 1, at, :].astype(f32))
        scale = lax.rsqrt(jnp.mean(value * value, axis=1, keepdims=True) + epsilon)
        middle[at, :] = value
        second_scale[at, :] = scale
        rows_all[me, at, :] = (value * scale * gain).astype(bf16)

    gather.start()
    again = pltpu.make_async_copy(upstream, wide, load_sems.at[2])
    again.start()
    for load in loads[6:]:
        load.wait()

    def forward_pair(b):
        turn = (0b11_10_11_01_10_00_01_00 >> (2 * b)) % 4
        side = (0b11_01_01_00 >> b) % 2
        return level_at(3 - turn, z) * 2 + (y + side) % 2

    def mixture_out(b):
        return pltpu.make_async_copy(
            tmp.at[b % 2],
            mixture_hbm.at[pl.ds(2 * forward_pair(b), 2), :, pl.ds(0, width)],
            out_sems.at[b % 2],
        )

    @pl.loop(0, 2 * pairs)
    def _(turn):
        b, h = turn // 2, turn % 2

        def at(k, work, where=None):
            @pl.when(turn == k)
            def _():
                if where is None:
                    work()
                else:
                    pl.when(where == 1)(work)

        at(0, lambda: gather.from_core(0, 0))
        at(2, lambda: gather.from_line(1))
        at(2, lambda: gather.from_line(2), interior)
        at(2, lambda: gather.from_core(1, 0))
        at(4, lambda: gather.from_side(0))
        at(4, lambda: gather.from_core(0, 1))
        at(6, lambda: gather.from_line(2), 1 - interior)
        at(6, lambda: gather.from_line(3), interior)
        at(6, lambda: gather.from_core(2, 0))
        at(8, lambda: gather.from_side(1))
        at(8, lambda: gather.from_core(1, 1))
        at(10, lambda: gather.from_line(3), 1 - interior)
        at(10, lambda: gather.from_core(3, 0))
        at(12, lambda: gather.from_side(2))
        at(12, lambda: gather.from_core(2, 1))
        at(14, lambda: gather.from_side(3))
        at(14, lambda: gather.from_core(3, 1))

        pair = forward_pair(b)
        xs = pair_block(rows_all, pair)
        lane = lax.broadcasted_iota(jnp.int32, (pair_rows_, ROUTE_COLS), 1)
        table = gates[pl.ds(2 * pair, 2)].reshape(pair_rows_, ROUTE_COLS)
        gate_rows = jnp.sum(jnp.where(lane == me, table, 0.0), axis=1, keepdims=True)
        gate_act = nn(xs, wg[h])
        up_act = nn(xs, wu[h])
        at_rows = pl.ds(pl.multiple_of(pair * pair_rows_, pair_rows_), pair_rows_)
        hidden_cot = ucot[h, at_rows, :].astype(f32)
        sig = lax.logistic(gate_act)
        act = gate_act * sig
        hid = act * up_act
        hidden[h, at_rows, :] = (hid * gate_rows).astype(bf16)
        route = jnp.sum(hid * hidden_cot, axis=1, keepdims=True)
        scaled = hidden_cot * gate_rows
        gcot[h, at_rows, :] = (scaled * up_act * (sig * (1.0 + gate_act * (1.0 - sig)))).astype(bf16)
        ucot[h, at_rows, :] = (scaled * act).astype(bf16)

        @pl.when(h == 0)
        def _():
            route_half[...] = route

        @pl.when(h == 1)
        def _():
            total = route_half[...] + route
            placed = jnp.where(lane == me, total, 0.0).astype(bf16)
            rext[pl.ds(2 * pair, 2)] = placed.reshape(2, half_rows, ROUTE_COLS)

            pl.when(b >= 2)(lambda: mixture_out(b - 2).wait())

            @pl.loop(0, width // panel)
            def _(n):
                cols = pl.ds(pl.multiple_of(n * panel, panel), panel)
                acc = nn(hidden[0, at_rows, :], wd[0, :, cols])
                for h in range(1, halves):
                    acc = acc + nn(hidden[h, at_rows, :], wd[h, :, cols])
                tmp[b % 2, :, :, cols] = acc.astype(bf16).reshape(2, half_rows, panel)

            mixture_out(b).start()

    for b in (pairs - 2, pairs - 1):
        mixture_out(b).wait()

    def core_send(b):
        return remote(
            tmp.at[b % 2, 1 - c],
            from_core.at[b],
            core_s.at[b],
            core_r.at[b],
            (index_of(z, y, 1 - c), x),
        )

    def take_core(b):
        core_send(b).wait_recv()
        add_block(tmp.at[b % 2, c], from_core.at[b], from_core.at[b])

        @pl.when(b < LEVELS)
        def _():
            remote(
                from_core.at[b],
                from_side.at[b],
                side_s.at[b],
                side_r.at[b],
                (index_of(z, 1 - y, c), x),
            ).start()

    def line_step(turn):
        sums.side_arrived(turn)
        mine = from_core.at[LEVELS + turn]
        add_block(mine, from_side.at[turn], mine)
        if turn < LEVELS - 1:
            sums.to_line(turn)

    def last_step():
        line_step(LEVELS - 1)
        total_block(sums, middle_grad)
        again.wait()
        second_term[...] = jnp.zeros_like(second_term)

        @pl.loop(0, half_rows // step)
        def _(i):
            at = pl.ds(pl.multiple_of(i * step, step), step)
            cot, mid, scale = middle_grad[at, :], middle[at, :], second_scale[at, :]
            weighted = cot * gain
            mean = jnp.mean(weighted * mid, axis=1, keepdims=True)
            value = wide[at, :] + scale * (weighted - mid * (scale * scale * mean))
            middle_grad[at, :] = value
            second_term[...] = second_term[...] + jnp.sum(cot * mid * scale, axis=0, keepdims=True)

    @pl.loop(0, pairs)
    def _(b):
        pl.when((b == pairs - 1) & (interior == 0))(lambda: line_step(0))
        pl.when(b >= 2)(lambda: core_send(b - 2).wait_send())
        pair = level_at(b % LEVELS, z) * 2 + (y + 1 - b // LEVELS) % 2
        at_rows = pl.ds(pl.multiple_of(pair * pair_rows_, pair_rows_), pair_rows_)

        @pl.loop(0, width // panel)
        def _(n):
            cols = pl.ds(pl.multiple_of(n * panel, panel), panel)
            acc = nt(gcot[0, at_rows, :], wg[0, cols, :])
            acc = acc + nt(ucot[0, at_rows, :], wu[0, cols, :])
            for h in range(1, halves):
                acc = acc + nt(gcot[h, at_rows, :], wg[h, cols, :])
                acc = acc + nt(ucot[h, at_rows, :], wu[h, cols, :])
            tmp[b % 2, :, :, cols] = acc.astype(bf16).reshape(2, half_rows, panel)

        core_send(b).start()
        pl.when(b >= 1)(lambda: take_core(b - 1))

    take_core(pairs - 1)
    for b in (pairs - 2, pairs - 1):
        core_send(b).wait_send()

    route_out = pltpu.make_async_copy(
        rext, mixture_hbm.at[:, :, pl.ds(width, ROUTE_COLS)], load_sems.at[1]
    )
    route_out.start()
    down_send = remote(
        wd.at[0, pl.ds(0, block)], down_landed, pair_s.at[1], pair_r.at[1], partner
    )
    down_later = pltpu.make_async_copy(wd.at[0, pl.ds(block, block)], down_theirs, load_sems.at[3])
    down_keep = pltpu.make_async_copy(wd.at[1], down_mine, load_sems.at[4])

    @pl.loop(0, 2 * units // block)
    def _(p):
        other, q = p // (units // block), p % (units // block)
        pl.when((p == 1) & (interior == 0))(lambda: line_step(1))
        pl.when((p == 2) & (interior == 1))(lambda: line_step(0))
        units_at = pl.ds(pl.multiple_of(q * block, block), block)
        us = u_all[...]
        us = us.reshape(us.shape[0] * us.shape[1], width)
        h = (1 - x) * (1 - other) + x * other
        wd[other, units_at, :] = tn(hidden[h, :, units_at], us).astype(bf16)
        pl.when(p == 0)(down_send.start)
        pl.when(p == 1)(down_later.start)

    down_keep.start()

    def part_outs(p):
        rows = pl.ds(pl.multiple_of(p * block, block), block)
        return [
            pltpu.make_async_copy(
                gstage.at[p % 2, which, k], ref.at[rows, :], out_sems.at[(p % 2) * 4 + 2 * which + k]
            )
            for which, refs in enumerate(((gate_mine, gate_theirs), (up_mine, up_theirs)))
            for k, ref in enumerate(refs)
        ]

    def wait_outs(p):
        for copy in part_outs(p):
            copy.wait()

    @pl.loop(0, width // block)
    def _(p):
        pl.when((p == 1) & (interior == 0))(lambda: line_step(2))
        pl.when((p == 1) & (interior == 1))(lambda: line_step(1))
        pl.when((p == 2) & (interior == 1))(lambda: line_step(2))
        pl.when(p == 6)(last_step)
        pl.when(p >= 2)(lambda: wait_outs(p - 2))
        cols = pl.ds(pl.multiple_of(p * block, block), block)
        xp = rows_all[:, :, cols]
        xp = xp.reshape(xp.shape[0] * xp.shape[1], block)
        xt = jnp.transpose(xp)
        for which, ref in enumerate((gcot, ucot)):
            for k, h in enumerate((x, 1 - x)):
                gstage[p % 2, which, k] = nn(xt, ref[h]).astype(bf16)
        for copy in part_outs(p):
            copy.start()

    for p in (width // block - 2, width // block - 1):
        wait_outs(p)
    route_out.wait()
    down_send.wait()
    down_later.wait()
    down_keep.wait()
    gather.finish()
    for turn in range(LEVELS):
        remote(
            from_core.at[turn], from_side.at[turn], side_s.at[turn], side_r.at[turn], partner
        ).wait_send()
    for turn in range(LEVELS - 1):
        remote(
            from_core.at[turn], from_line.at[turn], line_s.at[turn], line_r.at[turn], partner
        ).wait_send()


def run_experts(
    gates, second_gain, out_part, block_input, upstream, upstream_all, own, other, collective_id
):
    bf16, f32 = jnp.bfloat16, jnp.float32
    block = block_input.shape
    half_rows, width = block
    owner_count = upstream_all.shape[0]
    units = own[0].shape[1]
    halves = lax.axis_size("tp")
    all_rows = owner_count * half_rows
    hbm = pl.BlockSpec(memory_space=pl.ANY)
    vmem = pl.BlockSpec(memory_space=pltpu.VMEM)
    dma = pltpu.SemaphoreType.DMA
    flops = 2 * 9 * all_rows * width * units * halves
    shape = jax.ShapeDtypeStruct
    return pl.pallas_call(
        experts_kernel,
        out_shape=[
            shape(block, f32),
            shape(block, f32),
            shape((1, width), f32),
            shape((owner_count, half_rows, width + ROUTE_COLS), bf16),
        ]
        + [shape((width, units), bf16)] * 4
        + [shape((units, width), bf16)]
        + [shape((256, width), bf16)] * 2,
        in_specs=[vmem, vmem] + [hbm] * 10,
        out_specs=[vmem] * 3 + [hbm] * 8,
        scratch_shapes=[
            pltpu.VMEM((owner_count,) + block, bf16),
            pltpu.VMEM((owner_count,) + block, bf16),
            pltpu.VMEM((halves, width, units), bf16),
            pltpu.VMEM((halves, width, units), bf16),
            pltpu.VMEM((halves, units, width), bf16),
            pltpu.VMEM((halves, all_rows, units), bf16),
            pltpu.VMEM((halves, all_rows, units), bf16),
            pltpu.VMEM((halves, all_rows, units), bf16),
            pltpu.VMEM((owner_count, half_rows, ROUTE_COLS), bf16),
            pltpu.VMEM((2, 2) + block, bf16),
            pltpu.VMEM((2 * LEVELS,) + block, bf16),
            pltpu.VMEM((LEVELS,) + block, bf16),
            pltpu.VMEM((LEVELS + 1,) + block, bf16),
            pltpu.VMEM((2, 2, halves, 256, units), bf16),
            pltpu.VMEM(block, f32),
            pltpu.VMEM((half_rows, 1), f32),
            pltpu.VMEM((2 * half_rows, 1), f32),
            dma((GATHER_SENDS,)),
            dma((owner_count,)),
            dma((2 * LEVELS,)),
            dma((2 * LEVELS,)),
            dma((LEVELS,)),
            dma((LEVELS,)),
            dma((LEVELS + 1,)),
            dma((LEVELS + 1,)),
            dma((10,)),
            dma((8,)),
            dma((2,)),
            dma((2,)),
        ],
        compiler_params=pltpu.CompilerParams(
            collective_id=collective_id, has_side_effects=True, vmem_limit_bytes=67_043_328
        ),
        cost_estimate=pl.CostEstimate(
            flops=flops, bytes_accessed=64 * 2**20, transcendentals=all_rows * units * halves
        ),
        name="experts",
    )(gates, second_gain, out_part, block_input, upstream, upstream_all, *own, *other)


def last_kernel(
    mixture_part,
    normed_pair,
    mixed_rows,
    query_rows,
    key_rows,
    value_rows,
    output_full,
    query_full,
    key_full,
    value_full,
    gate_theirs,
    up_theirs,
    down_theirs,
    block_input,
    first_scale,
    first_gain,
    middle_grad,
    second_term,
    query_total,
    key_total,
    value_total,
    output_total,
    mixture_total,
    gate_landed,
    up_landed,
    down_landed,
    input_grad,
    gain_grads,
    wide_core,
    wide_side,
    wide_line,
    wide_own,
    from_core,
    from_side,
    from_line,
    tmp,
    middle_pair,
    mixed_cot,
    query_cot,
    key_cot,
    value_cot,
    weight_one,
    weight_two,
    first_terms,
    first_mine,
    first_other,
    gains,
    gains_in,
    core_s,
    core_r,
    side_s,
    side_r,
    line_s,
    line_r,
    own_sems,
    load_sems,
    pair_s,
    pair_r,
    gain_s,
    gain_r,
):
    bf16, f32 = jnp.bfloat16, jnp.float32
    z, y, c, x = place()
    own = index_of(z, y, c)
    rows, head_cols = mixed_rows.shape
    half_rows, width = input_grad.shape
    pairs = 2 * LEVELS
    inv_root = HD ** (-0.5)
    plane_greet(pair=True, far=True)

    def swap(i, src, dst):
        return remote(src, dst, pair_s.at[i], pair_r.at[i], (own, 1 - x))

    expert_swaps = (
        swap(0, gate_theirs, gate_landed),
        swap(1, up_theirs, up_landed),
        swap(2, down_theirs, down_landed),
    )
    first_swap = swap(3, first_mine, first_other)

    def load(i, src, dst):
        return pltpu.make_async_copy(src, dst, load_sems.at[i])

    output_load, query_load = load(0, output_full, weight_one), load(1, query_full, weight_two)
    value_load, key_load = load(2, value_full, weight_one), load(3, key_full, weight_two)
    sums = [
        PlaneSums(
            core,
            core,
            side,
            line,
            tuple(s.at[a] for s in (core_s, core_r, side_s, side_r, line_s, line_r)),
            LEVELS,
        )
        for a, (core, side, line) in enumerate(
            [(wide_core, wide_side, wide_line)]
            + [(from_core.at[i], from_side.at[i], from_line.at[i]) for i in range(4)]
        )
    ]

    def slot_at(b, core):
        level, side = level_at(b % LEVELS, z), (y + 1 - b // LEVELS) % 2
        return index_of(level, side, (c + core) % 2)

    def core_copy(a, b, src):
        plan = sums[a]
        return remote(
            src,
            plan.from_core.at[b],
            plan.core_s.at[b],
            plan.core_r.at[b],
            (index_of(z, y, 1 - c), x),
        )

    def side_copy(a, b):
        plan = sums[a]
        return remote(
            plan.from_core.at[b],
            plan.from_side.at[b],
            plan.side_s.at[b],
            plan.side_r.at[b],
            (index_of(z, 1 - y, c), x),
        )

    def line_step(a, turn):
        plan = sums[a]
        plan.side_arrived(turn)
        mine = plan.from_core.at[LEVELS + turn]
        add_block(mine, plan.from_side.at[turn], mine)
        if turn < LEVELS - 1:
            plan.to_line(turn)

    def wide_load(b):
        return pltpu.make_async_copy(
            mixture_part.at[slot_at(b, 0)], wide_own.at[b], own_sems.at[b]
        )

    @pl.loop(0, pairs)
    def _(b):
        core_copy(0, b, mixture_part.at[slot_at(b, 1)]).start()
        wide_load(b).start()

    @pl.loop(0, half_rows // 16)
    def _(i):
        at = pl.ds(pl.multiple_of(i * 16, 16), 16)
        middle_pair[x, at, :] = middle_grad[at, :].astype(bf16)

    middle_swap = swap(4, middle_pair.at[x], middle_pair.at[x])
    middle_swap.start()
    for copy in expert_swaps[:2]:
        copy.start()

    @pl.loop(0, pairs)
    def _(b):
        wide_load(b).wait()
        core_copy(0, b, mixture_part.at[slot_at(b, 1)]).wait_recv()
        add_block(wide_own.at[b], wide_core.at[b], wide_core.at[b])
        pl.when(b < LEVELS)(lambda: side_copy(0, b).start())

        @pl.when(b == 0)
        def _():
            output_load.start()
            query_load.start()

    def flat(ref):
        value = ref[...]
        return value.reshape(value.shape[0] * value.shape[1], value.shape[2])

    output_load.wait()
    middle_swap.wait()
    mixed_cot[...] = nn(flat(middle_pair), flat(weight_one)).astype(bf16)
    value_load.start()

    def term(a, left, cot):
        def send(b):
            return core_copy(a, b, tmp.at[b % 2, 1 - c])

        def take(b):
            core = sums[a].from_core.at[b]
            send(b).wait_recv()
            add_block(tmp.at[b % 2, c], core, core)
            pl.when(b < LEVELS)(lambda: side_copy(a, b).start())

        @pl.loop(0, pairs)
        def _(b):
            pl.when(b >= 2)(lambda: send(b - 2).wait_send())
            pair = level_at(b % LEVELS, z) * 2 + (y + 1 - b // LEVELS) % 2
            cols = pl.ds(pl.multiple_of(pair * 2 * half_rows, 2 * half_rows), 2 * half_rows)
            lhs = left[:, :, cols].reshape(rows, 2 * half_rows)
            part = tn(lhs, cot[...])
            tmp[b % 2] = part.astype(bf16).reshape(2, half_rows, head_cols)
            send(b).start()
            pl.when(b >= 1)(lambda: take(b - 1))

        take(pairs - 1)
        for b in (pairs - 2, pairs - 1):
            send(b).wait_send()

    top, bottom = line_ends(z)
    interior = 1 - top - bottom

    def head(h):
        cols = pl.ds(pl.multiple_of(h * HD, HD), HD)
        query, key, value = query_rows[:, cols], key_rows[:, cols], value_rows[:, cols]
        mixed = mixed_cot[:, cols]
        scores = nt(query, key) * inv_root
        row_top = jnp.max(scores, axis=1, keepdims=True)
        log_total = row_top + jnp.log(jnp.sum(jnp.exp(scores - row_top), axis=1, keepdims=True))
        soft = jnp.exp(scores - log_total)
        value_cot[:, cols] = tn(soft.astype(bf16), mixed).astype(bf16)
        soft_cot = nt(mixed, value)
        inner = jnp.sum(soft * soft_cot, axis=1, keepdims=True)
        score_cot = (soft * (soft_cot - inner) * inv_root).astype(bf16)
        query_cot[:, cols] = nn(score_cot, key).astype(bf16)
        key_cot[:, cols] = tn(score_cot, query).astype(bf16)

    term(1, middle_pair, mixed_rows)

    @pl.when(interior == 0)
    def _():
        line_step(0, 0)
        line_step(0, 1)

    @pl.loop(0, head_cols // HD // 2)
    def _(h):
        pl.when((h == 1) & (interior == 1))(lambda: line_step(0, 0))
        head(2 * h)
        head(2 * h + 1)

    pl.when(interior == 1)(lambda: line_step(0, 1))
    line_step(0, 2)
    term(2, normed_pair, value_cot)
    line_step(0, 3)
    term(3, normed_pair, query_cot)
    line_step(1, 0)
    line_step(1, 1)
    term(4, normed_pair, key_cot)
    line_step(1, 2)
    line_step(1, 3)

    panel = 4

    def first_add(cot, weight, begin):
        @pl.loop(0, weight.shape[0] // panel)
        def _(n):
            part = weight[pl.ds(n * panel, panel)].reshape(panel * half_rows, head_cols)
            cols = pl.ds(pl.multiple_of(n * panel * half_rows, panel * half_rows), panel * half_rows)
            value = nt(cot[...], part).reshape(2, half_rows, panel * half_rows)
            if begin:
                first_terms[:, :, cols] = value
            else:
                first_terms[:, :, cols] = first_terms[:, :, cols] + value

    query_load.wait()
    first_add(query_cot, weight_two, True)
    key_load.start()
    value_load.wait()
    first_add(value_cot, weight_one, False)
    key_load.wait()
    first_add(key_cot, weight_two, False)
    step = 16

    @pl.loop(0, half_rows // step)
    def _(i):
        at = pl.ds(pl.multiple_of(i * step, step), step)
        first_mine[at, :] = first_terms[1 - x, at, :].astype(bf16)

    first_swap.start()
    total_block(sums[0], mixture_total)
    for turn in range(LEVELS):
        line_step(2, turn)
    total_block(sums[1], output_total)
    line_step(3, 0)
    line_step(3, 1)
    first_swap.wait_recv()
    gain = first_gain[...]
    gains[...] = jnp.concatenate(
        [jnp.zeros((1, width), f32), second_term[...], jnp.zeros((6, width), f32)], axis=0
    )

    @pl.loop(0, half_rows // step)
    def _(i):
        at = pl.ds(pl.multiple_of(i * step, step), step)
        value = first_terms[x, at, :] + first_other[at, :].astype(f32)
        entry, scale = block_input[at, :], first_scale[at, :]
        weighted = value * gain
        mean = jnp.mean(weighted * entry, axis=1, keepdims=True)
        input_grad[at, :] = middle_grad[at, :] + scale * (weighted - entry * (scale * scale * mean))
        gains[0:1, :] = gains[0:1, :] + jnp.sum(value * entry * scale, axis=0, keepdims=True)

    hops = [
        (index_of(z, y, 1 - c), x),
        (own, 1 - x),
        (index_of(z + 1 - 2 * (z % 2), y, c), x),
        (index_of((z + 2) % LEVELS, y, c), x),
        (index_of(z, 1 - y, c), x),
    ]

    def gain_copy(i):
        return remote(gains, gains_in.at[i], gain_s.at[i], gain_r.at[i], hops[i])

    def gain_add(i):
        gain_copy(i).wait()
        gains[...] = gains[...] + gains_in[i]

    for i in range(2):
        gain_copy(i).start()
        gain_add(i)
    expert_swaps[2].start()
    gain_copy(2).start()
    line_step(3, 2)
    line_step(3, 3)
    gain_add(2)
    gain_copy(3).start()
    total_block(sums[2], value_total)
    line_step(4, 0)
    gain_add(3)
    gain_copy(4).start()
    for turn in range(1, LEVELS):
        line_step(4, turn)
    total_block(sums[3], query_total)
    gain_add(4)
    gain_grads[...] = gains[...]
    total_block(sums[4], key_total)

    @pl.loop(0, pairs)
    def _(b):
        core_copy(0, b, mixture_part.at[slot_at(b, 1)]).wait_send()

    for a in range(5):
        for turn in range(LEVELS):
            side_copy(a, turn).wait_send()
        line = sums[a].from_line
        for turn in range(LEVELS - 1):
            remote(
                line.at[0], line.at[turn], sums[a].line_s.at[turn], sums[a].line_r.at[turn], (own, 1 - x)
            ).wait_send()
    first_swap.wait_send()
    for copy in expert_swaps:
        copy.wait()


def run_last(
    mixture_part, normed_pair, attention_rows, weights_full, theirs, norm_args, collective_id
):
    f32, bf16 = jnp.float32, jnp.bfloat16
    shape = jax.ShapeDtypeStruct
    hbm = pl.BlockSpec(memory_space=pl.ANY)
    vmem = pl.BlockSpec(memory_space=pltpu.VMEM)
    dma = pltpu.SemaphoreType.DMA
    rows, head_cols = attention_rows[0].shape
    half_rows, width = norm_args[0].shape
    wide = mixture_part.shape[1:]
    block = (half_rows, head_cols)
    pairs = 2 * LEVELS
    flops = 2 * rows * head_cols * width * 8
    nbytes = 2 * (mixture_part.size + 12 * weights_full[0].size)
    outs = pl.pallas_call(
        last_kernel,
        out_shape=[shape(block, f32)] * 4
        + [shape(wide, f32)]
        + [shape(t.shape, t.dtype) for t in theirs]
        + [shape((half_rows, width), f32), shape((8, width), f32)],
        in_specs=[hbm] + [vmem] * 5 + [hbm] * 7 + [vmem] * 5,
        out_specs=[vmem] * 5 + [hbm] * 3 + [vmem] * 2,
        scratch_shapes=[
            pltpu.VMEM((pairs,) + wide, bf16),
            pltpu.VMEM((LEVELS,) + wide, bf16),
            pltpu.VMEM((LEVELS + 1,) + wide, bf16),
            pltpu.VMEM((pairs,) + wide, bf16),
            pltpu.VMEM((4, pairs) + block, bf16),
            pltpu.VMEM((4, LEVELS) + block, bf16),
            pltpu.VMEM((4, LEVELS + 1) + block, bf16),
            pltpu.VMEM((2, 2) + block, bf16),
            pltpu.VMEM((2, half_rows, width), bf16),
        ]
        + [pltpu.VMEM((rows, head_cols), bf16)] * 4
        + [pltpu.VMEM(weights_full[0].shape, bf16)] * 2
        + [
            pltpu.VMEM((2, half_rows, width), f32),
            pltpu.VMEM((half_rows, width), bf16),
            pltpu.VMEM((half_rows, width), bf16),
            pltpu.VMEM((8, width), f32),
            pltpu.VMEM((5, 8, width), f32),
        ]
        + [dma((5, pairs))] * 2
        + [dma((5, LEVELS))] * 2
        + [dma((5, LEVELS + 1))] * 2
        + [dma((pairs,)), dma((4,)), dma((5,)), dma((5,)), dma((5,)), dma((5,))],
        compiler_params=pltpu.CompilerParams(
            collective_id=collective_id, has_side_effects=True, vmem_limit_bytes=67_043_328
        ),
        cost_estimate=pl.CostEstimate(flops=flops, bytes_accessed=nbytes, transcendentals=0),
        name="last",
    )(mixture_part, normed_pair, *attention_rows, *weights_full, *theirs, *norm_args)
    return outs[:5], outs[5:8], outs[8], outs[9]


def half_of(rows):
    count = rows.shape[0] // lax.axis_size("tp")
    return lax.dynamic_slice_in_dim(rows, lax.axis_index("tp") * count, count, axis=0)


def per_device_dense(
    block_input,
    upstream_grad,
    first_gain,
    second_gain,
    query_weight,
    key_weight,
    value_weight,
    output_weight,
    gate_weight,
    up_weight,
    down_weight,
    routes,
    gate_values,
):
    local_rows, model_width = block_input.shape
    expert_count = EXP_DEV * lax.axis_size("fsdp")
    f32 = jnp.float32
    my_routes = half_of(routes)
    expert_names = jnp.arange(expert_count, dtype=jnp.int32)[None, :]
    own_weights = (gate_weight[0], up_weight[0], down_weight[0])
    weights_full, gathered, other_weights, attention_rows, out_part, first_scale = run_attend(
        (query_weight, key_weight, value_weight, output_weight),
        block_input,
        upstream_grad,
        first_gain[None],
        routes.T,
        gate_values.T,
        own_weights,
        1,
    )
    query_full, key_full, value_full, output_full = weights_full
    query_rows, key_rows, value_rows, mixed_rows = attention_rows
    upstream_all, gates_all, normed_pair = gathered
    (
        middle,
        middle_grad,
        second_term,
        mixture_part,
        gate_mine,
        gate_theirs,
        up_mine,
        up_theirs,
        down_mine,
        down_theirs,
        down_landed,
    ) = run_experts(
        gates_all,
        second_gain[None],
        out_part,
        block_input,
        upstream_grad,
        upstream_all,
        own_weights,
        other_weights,
        2,
    )
    sums, landed, input_grad, gain_grads = run_last(
        mixture_part,
        normed_pair,
        (mixed_rows, query_rows, key_rows, value_rows),
        (output_full, query_full, key_full, value_full),
        (gate_theirs, up_theirs, down_theirs),
        (block_input, first_scale, first_gain[None], middle_grad, second_term),
        4,
    )
    query_grad, key_grad, value_grad, output_grad, mixture = sums
    gate_grad, up_grad, down_grad = (
        mine.astype(f32) + theirs.astype(f32)
        for mine, theirs in (
            (gate_mine, landed[0]),
            (up_mine, landed[1]),
            (down_mine, jnp.concatenate([down_landed, landed[2]], axis=0)),
        )
    )
    block_output = middle + mixture[:, :model_width]
    route_back = mixture[:, model_width : model_width + expert_count]
    route_grad = jnp.sum(
        jnp.where(my_routes[:, :, None] == expert_names[None], route_back[:, None, :], 0.0), axis=2
    )
    return (
        block_output,
        input_grad,
        gain_grads[0],
        gain_grads[1],
        query_grad,
        key_grad,
        value_grad,
        output_grad,
        gate_grad[None],
        up_grad[None],
        down_grad[None],
        route_grad,
    )


def solution(mesh):
    dense = 2 * TOP >= EXP_DEV * mesh.shape["fsdp"] and mesh.shape["fsdp"] == 4 * LEVELS
    per_device = per_device_dense if dense else per_device_slots
    in_specs = (
        P(("fsdp", "tp"), None),
        P(("fsdp", "tp"), None),
        P(),
        P(),
        P("fsdp", "tp"),
        P("fsdp", "tp"),
        P("fsdp", "tp"),
        P("fsdp", "tp"),
        P("fsdp", None, "tp"),
        P("fsdp", None, "tp"),
        P("fsdp", "tp", None),
        P("fsdp", None),
        P("fsdp", None),
    )
    out_specs = (
        P(("fsdp", "tp"), None),
        P(("fsdp", "tp"), None),
        P(),
        P(),
        P("fsdp", "tp"),
        P("fsdp", "tp"),
        P("fsdp", "tp"),
        P("fsdp", "tp"),
        P("fsdp", None, "tp"),
        P("fsdp", None, "tp"),
        P("fsdp", "tp", None),
        P(("fsdp", "tp"), None),
    )
    return jax.shard_map(
        per_device, mesh=mesh, in_specs=in_specs, out_specs=out_specs, check_vma=False
    )
```
